32 devices in a mesh: dp: 2 (over x), tp: 4 (over z), cp: 4 (over y, core).
Axes of the slice: x: 2, y: 2, z: 4, core: 2. Of those that a mesh axis runs over, the one named last changes fastest.
Arguments:
- x_in: bfloat16 [12, 1536, 2048], P('dp', 'cp'), parts along dimension 0
- segment_ids: int32 [12, 1536], P('dp', 'cp'), parts along dimension 0
- positions: int32 [12, 1536], P('dp', 'cp'), parts along dimension 0
- w_query: bfloat16 [2048, 2048], P(None, 'tp')
- w_key: bfloat16 [2048, 2048], P(None, 'tp')
- w_value: bfloat16 [2048, 2048], P(None, 'tp')
- w_out: bfloat16 [2048, 2048], P('tp')
- norm_gain: float32 [2048], replicated
- grad_out: bfloat16 [12, 1536, 2048], P('dp', 'cp'), parts along dimension 0
Outputs:
- output 1: bfloat16 [12, 1536, 2048], P('dp', 'cp'), parts along dimension 0
- output 2: bfloat16 [12, 1536, 2048], P('dp', 'cp'), parts along dimension 0
- output 3: float32 [4096], P('dp'), parts along dimension 0
- output 4: float32 [4096, 2048], P('dp', 'tp'), parts along dimension 0
- output 5: float32 [4096, 2048], P('dp', 'tp'), parts along dimension 0
- output 6: float32 [4096, 2048], P('dp', 'tp'), parts along dimension 0
- output 7: float32 [4096, 2048], P(('dp', 'tp')), parts along dimension 0
There are 2 independent parts. The reference program is written for one: setup_inputs(seed, part) draws one part's arguments, and reference() takes and returns one part's arrays. A program takes and returns all parts, laid end to end along the dimension named above; an argument that names none is the same for every part.
All inputs are finite; a program needn't handle non-finite values.
Results may differ from the reference program's by a relative error of at most 0.00969891.
Values are sent between devices in bfloat16 or wider.
A program may use at most 1 GiB of HBM per device.

```python
import jax
import jax.numpy as jnp
from jax import lax

BATCH = 6
SEQ_DEV = 384
SEQ = 1536
D_MODEL = 2048
HEADS = 16
HEAD_DIM = 128

ROPE_THETA = 8000000.0
LN_EPS = 1e-5
NEG_BIG = -1e30
SCALE = HEAD_DIM ** -0.5
HIDDEN = HEADS * HEAD_DIM
NUM_PIECES = SEQ // SEQ_DEV


def draw_documents(doc_key, batch_rows, seq_len, piece_len):
    key_len, key_flag, key_win, key_off = jax.random.split(doc_key, 4)
    len_table = jnp.array([piece_len // 4, piece_len, 4 * piece_len], dtype=jnp.int32)
    mean_len = len_table[jax.random.randint(key_len, (batch_rows,), 0, 3)]
    start_flag = jax.random.randint(key_flag, (batch_rows, seq_len), 0, mean_len[:, None]) == 0
    long_len = min(seq_len, 2 * piece_len)
    win_start = jax.random.randint(key_win, (batch_rows, 1), 0, seq_len - long_len + 1)
    tok_index = jnp.arange(seq_len, dtype=jnp.int32)[None, :]
    inside = (tok_index > win_start) & (tok_index < win_start + long_len)
    start_flag = (start_flag & jnp.logical_not(inside)) | (tok_index == 0)
    seg_ids = jnp.cumsum(start_flag.astype(jnp.int32), axis=1) + jax.random.randint(key_off, (batch_rows, 1), 0, 1000)
    start_pos = lax.cummax(jnp.where(start_flag, tok_index, 0), axis=1)
    return seg_ids.astype(jnp.int32), (tok_index - start_pos).astype(jnp.int32)


def setup_inputs(seed: int = 0, part: int = 0) -> dict:
    part_keys = jax.random.split(jax.random.fold_in(jax.random.key(seed), part), 3)
    shared_keys = jax.random.split(jax.random.key(seed + 1), 5)
    x_in = jax.random.normal(part_keys[0], (BATCH, SEQ, D_MODEL), jnp.float32).astype(jnp.bfloat16)
    segment_ids, positions = draw_documents(part_keys[1], BATCH, SEQ, SEQ_DEV)
    grad_out = jax.random.normal(part_keys[2], (BATCH, SEQ, D_MODEL), jnp.float32).astype(jnp.bfloat16)
    in_scale = D_MODEL ** -0.5
    w_query = (jax.random.normal(shared_keys[0], (D_MODEL, HIDDEN), jnp.float32) * in_scale).astype(jnp.bfloat16)
    w_key = (jax.random.normal(shared_keys[1], (D_MODEL, HIDDEN), jnp.float32) * in_scale).astype(jnp.bfloat16)
    w_value = (jax.random.normal(shared_keys[2], (D_MODEL, HIDDEN), jnp.float32) * in_scale).astype(jnp.bfloat16)
    w_out = (jax.random.normal(shared_keys[3], (HIDDEN, D_MODEL), jnp.float32) * HIDDEN ** -0.5).astype(jnp.bfloat16)
    norm_gain = 1.0 + 0.25 * jax.random.normal(shared_keys[4], (D_MODEL,), jnp.float32)
    return {"x_in": x_in, "segment_ids": segment_ids, "positions": positions, "w_query": w_query, "w_key": w_key, "w_value": w_value, "w_out": w_out, "norm_gain": norm_gain, "grad_out": grad_out}


def rope_tables(pos_ids):
    inv_freq = ROPE_THETA ** (-jnp.arange(0, HEAD_DIM, 2).astype(jnp.float32) / HEAD_DIM)
    angles = pos_ids.astype(jnp.float32)[:, :, None] * inv_freq
    return jnp.cos(angles)[:, :, None, :], jnp.sin(angles)[:, :, None, :]


def rotate(vec_in, cos_t, sin_t, sign_val):
    pair_view = vec_in.reshape(vec_in.shape[:-1] + (HEAD_DIM // 2, 2))
    even_part = pair_view[..., 0]
    odd_part = pair_view[..., 1]
    sin_s = sign_val * sin_t
    return jnp.stack([even_part * cos_t - odd_part * sin_s, even_part * sin_s + odd_part * cos_t], axis=-1).reshape(vec_in.shape)


def reference(x_in, segment_ids, positions, w_query, w_key, w_value, w_out, norm_gain, grad_out):
    x_f32 = x_in.astype(jnp.float32)
    centred = x_f32 - jnp.mean(x_f32, axis=-1, keepdims=True)
    inv_std = lax.rsqrt(jnp.mean(centred * centred, axis=-1, keepdims=True) + LN_EPS)
    x_hat = centred * inv_std
    normed = (x_hat * norm_gain).astype(jnp.bfloat16).reshape(BATCH * SEQ, D_MODEL)
    cos_t, sin_t = rope_tables(positions)
    head_shape = (BATCH, SEQ, HEADS, HEAD_DIM)
    flat_shape = (BATCH * SEQ, HIDDEN)
    q_rot = rotate(jnp.dot(normed, w_query, preferred_element_type=jnp.float32).reshape(head_shape), cos_t, sin_t, 1.0).astype(jnp.bfloat16)
    k_rot = rotate(jnp.dot(normed, w_key, preferred_element_type=jnp.float32).reshape(head_shape), cos_t, sin_t, 1.0).astype(jnp.bfloat16)
    v_val = jnp.dot(normed, w_value, preferred_element_type=jnp.float32).astype(jnp.bfloat16).reshape(head_shape)
    grad_flat = grad_out.reshape(BATCH * SEQ, D_MODEL)
    grad_heads = jnp.dot(grad_flat, w_out.T, preferred_element_type=jnp.float32).astype(jnp.bfloat16).reshape(head_shape)
    k_f32 = k_rot.astype(jnp.float32)
    v_f32 = v_val.astype(jnp.float32)
    key_index = jnp.arange(SEQ)

    def to_pieces(array_in):
        return jnp.moveaxis(array_in.reshape((BATCH, NUM_PIECES, SEQ_DEV) + array_in.shape[2:]), 1, 0)

    def from_pieces(array_in):
        return jnp.moveaxis(array_in, 0, 1).reshape((BATCH, SEQ) + array_in.shape[3:])

    def query_step(acc_pair, piece):
        dk_acc, dv_acc = acc_pair
        q_piece, dout_piece, seg_piece, piece_id = piece
        q_f32 = q_piece.astype(jnp.float32)
        dout_f32 = dout_piece.astype(jnp.float32)
        query_index = piece_id * SEQ_DEV + jnp.arange(SEQ_DEV)
        allowed = ((key_index[None, :] <= query_index[:, None])[None] & (seg_piece[:, :, None] == segment_ids[:, None, :]))[:, None]
        scores = jnp.where(allowed, jnp.einsum("bqhe,bkhe->bhqk", q_f32, k_f32) * SCALE, NEG_BIG)
        exp_scores = jnp.exp(scores - jnp.max(scores, axis=-1, keepdims=True))
        attn_prob = exp_scores / jnp.sum(exp_scores, axis=-1, keepdims=True)
        prob_low = attn_prob.astype(jnp.bfloat16).astype(jnp.float32)
        attn_piece = jnp.einsum("bhqk,bkhe->bqhe", prob_low, v_f32).astype(jnp.bfloat16)
        grad_prob = jnp.einsum("bqhe,bkhe->bhqk", dout_f32, v_f32)
        grad_score = (attn_prob * (grad_prob - jnp.sum(attn_prob * grad_prob, axis=-1, keepdims=True))).astype(jnp.bfloat16).astype(jnp.float32)
        dq_piece = jnp.einsum("bhqk,bkhe->bqhe", grad_score, k_f32) * SCALE
        dk_acc = dk_acc + jnp.einsum("bhqk,bqhe->bkhe", grad_score, q_f32) * SCALE
        dv_acc = dv_acc + jnp.einsum("bhqk,bqhe->bkhe", prob_low, dout_f32)
        return (dk_acc, dv_acc), (attn_piece, dq_piece)

    zero_acc = jnp.zeros(head_shape, jnp.float32)
    acc_pair, outs_pair = lax.scan(query_step, (zero_acc, zero_acc), (to_pieces(q_rot), to_pieces(grad_heads), to_pieces(segment_ids), jnp.arange(NUM_PIECES)))
    dk_acc, dv_acc = acc_pair
    attn_flat = from_pieces(outs_pair[0]).reshape(flat_shape)
    dq_full = from_pieces(outs_pair[1])
    y_out = (x_f32 + jnp.dot(attn_flat, w_out, preferred_element_type=jnp.float32).reshape(BATCH, SEQ, D_MODEL)).astype(jnp.bfloat16)
    grad_wo = jnp.dot(attn_flat.T, grad_flat, preferred_element_type=jnp.float32)
    dq_pre = rotate(dq_full, cos_t, sin_t, -1.0).astype(jnp.bfloat16).reshape(flat_shape)
    dk_pre = rotate(dk_acc.astype(jnp.bfloat16).astype(jnp.float32), cos_t, sin_t, -1.0).astype(jnp.bfloat16).reshape(flat_shape)
    dv_pre = dv_acc.astype(jnp.bfloat16).reshape(flat_shape)
    grad_wq = jnp.dot(normed.T, dq_pre, preferred_element_type=jnp.float32)
    grad_wk = jnp.dot(normed.T, dk_pre, preferred_element_type=jnp.float32)
    grad_wv = jnp.dot(normed.T, dv_pre, preferred_element_type=jnp.float32)
    grad_norm = (jnp.dot(dq_pre, w_query.T, preferred_element_type=jnp.float32) + jnp.dot(dk_pre, w_key.T, preferred_element_type=jnp.float32) + jnp.dot(dv_pre, w_value.T, preferred_element_type=jnp.float32)).reshape(BATCH, SEQ, D_MODEL)
    d_hat = grad_norm * norm_gain
    dx_norm = inv_std * (d_hat - jnp.mean(d_hat, axis=-1, keepdims=True) - x_hat * jnp.mean(d_hat * x_hat, axis=-1, keepdims=True))
    grad_x = (grad_out.astype(jnp.float32) + dx_norm).astype(jnp.bfloat16)
    grad_gain = jnp.sum(grad_norm * x_hat, axis=(0, 1))
    return (y_out, grad_x, grad_gain, grad_wq, grad_wk, grad_wv, grad_wo)
```

```python
import functools
import math

import jax
import jax.numpy as jnp
from jax import lax
from jax.experimental import pallas as pl
from jax.experimental.pallas import tpu as pltpu
from jax.sharding import PartitionSpec as P

HEAD_DIM = 128
ROPE_THETA = 8000000.0
LN_EPS = 1e-5
NEG_BIG = -1e30
SCALE = HEAD_DIM ** -0.5
EXP2_SCALE = SCALE * math.log2(math.e)
F32 = jnp.float32
BF16 = jnp.bfloat16
NT = (((1,), (1,)), ((), ()))


def dot_nn(a, b):
    return jnp.dot(a, b, preferred_element_type=F32)


def dot_nt(a, b):
    return lax.dot_general(a, b, NT, preferred_element_type=F32)


def dot_tn(a, b):
    return lax.dot_general(a, b, (((0,), (0,)), ((), ())), preferred_element_type=F32)


def swap_pairs(t, sign):
    lane = lax.broadcasted_iota(jnp.int32, t.shape, 1)
    even = (lane % 2) == 0
    up = pltpu.roll(t, HEAD_DIM - 1, 1)
    down = pltpu.roll(t, 1, 1)
    return jnp.where(even, -up, down) if sign > 0 else jnp.where(even, up, -down)


def rope(t, cos_t, sin_t, sign):
    return t * cos_t + swap_pairs(t, sign) * sin_t


def proj_kernel(x_ref, dy_ref, cos_ref, sin_ref, gain_ref, wq_ref, wk_ref, wv_ref, wo_ref, n_ref, q_ref, kv_ref, do_ref):
    x = x_ref[...].astype(F32)
    centred = x - jnp.mean(x, axis=-1, keepdims=True)
    inv_std = lax.rsqrt(jnp.mean(centred * centred, axis=-1, keepdims=True) + LN_EPS)
    normed = ((centred * inv_std) * gain_ref[...]).astype(BF16)
    n_ref[...] = normed
    cos_t = cos_ref[...]
    sin_t = sin_ref[...]

    def put_rope(dst, raw):
        for h in range(raw.shape[1] // HEAD_DIM):
            cols = slice(h * HEAD_DIM, (h + 1) * HEAD_DIM)
            dst[:, cols] = rope(raw[:, cols], cos_t, sin_t, 1.0).astype(BF16)

    put_rope(kv_ref.at[0], dot_nn(normed, wk_ref[...]))
    kv_ref[1] = dot_nn(normed, wv_ref[...]).astype(BF16)
    put_rope(q_ref, dot_nn(normed, wq_ref[...]))
    do_ref[...] = dot_nt(dy_ref[...], wo_ref[...]).astype(BF16)


def project(x, dy, cos_t, sin_t, gain, wq, wk, wv, wo, rows):
    tokens, d_model = x.shape
    hidden = wq.shape[1]
    whole = pl.BlockSpec(memory_space=pltpu.VMEM)
    tile = lambda width: pl.BlockSpec((rows, width), lambda i: (i, 0))
    return pl.pallas_call(
        proj_kernel,
        grid=(tokens // rows,),
        in_specs=[tile(d_model), tile(d_model), tile(HEAD_DIM), tile(HEAD_DIM), whole, whole, whole, whole, whole],
        out_specs=[tile(d_model), tile(hidden), pl.BlockSpec((2, rows, hidden), lambda i: (0, i, 0)), tile(hidden)],
        out_shape=[
            jax.ShapeDtypeStruct((tokens, d_model), BF16),
            jax.ShapeDtypeStruct((tokens, hidden), BF16),
            jax.ShapeDtypeStruct((2, tokens, hidden), BF16),
            jax.ShapeDtypeStruct((tokens, hidden), BF16),
        ],
        compiler_params=pltpu.CompilerParams(dimension_semantics=("arbitrary",), vmem_limit_bytes=60 << 20),
        cost_estimate=pl.CostEstimate(flops=8 * tokens * d_model * hidden, bytes_accessed=8 * tokens * d_model + 8 * d_model * hidden, transcendentals=0),
        name="project",
    )(x, dy, cos_t, sin_t, gain, wq, wk, wv, wo)


SUB = 128


def attn_kernel(info_ref, start_ref, cos_ref, sin_ref, q_ref, do_ref, kv0_ref, kv1_ref, kv2_ref, kv3_ref,
                o_ref, dq_ref, g0_ref, g1_ref, g2_ref, g3_ref, s_scr, dp_scr, m_scr, l_scr, d_scr, ot_scr, dqt_scr):
    b = pl.program_id(0)
    rank = info_ref[0]
    first = info_ref[1 + b]
    seq = q_ref.shape[0]
    kvs = (kv0_ref, kv1_ref, kv2_ref, kv3_ref)
    grads = (g0_ref, g1_ref, g2_ref, g3_ref)
    q = q_ref[...]
    do = do_ref[...]
    start = start_ref[0]
    subs = range(0, seq, SUB)

    def piece_of(slot):
        return rank ^ slot if slot else rank

    def live(slot):
        piece = piece_of(slot)
        return jnp.logical_and(piece < rank, first < (piece + 1) * seq)

    def each(body):
        body(0)
        for slot in (1, 2, 3):
            pl.when(live(slot))(functools.partial(body, slot))

    m_scr[...] = jnp.full(m_scr.shape, NEG_BIG, F32)
    l_scr[...] = jnp.zeros_like(l_scr)
    d_scr[...] = jnp.zeros_like(d_scr)
    ot_scr[...] = jnp.zeros_like(ot_scr)
    dqt_scr[...] = jnp.zeros_like(dqt_scr)

    def scores(slot):
        base = piece_of(slot) * seq
        for s in subs:
            raw = dot_nt(kvs[slot][0, s:s + SUB, :], q)
            local = lax.broadcasted_iota(jnp.int32, raw.shape, 0) + s
            allowed = (local + base) >= start
            if slot == 0:
                allowed = jnp.logical_and(allowed, local <= lax.broadcasted_iota(jnp.int32, raw.shape, 1))
            raw = jnp.where(allowed, raw, NEG_BIG)
            s_scr[slot, s:s + SUB, :] = raw
            m_scr[...] = jnp.maximum(m_scr[...], jnp.max(raw, axis=0, keepdims=True))

    each(scores)

    def exps(slot):
        for s in subs:
            e = jnp.exp2((s_scr[slot, s:s + SUB, :] - m_scr[...]) * EXP2_SCALE)
            s_scr[slot, s:s + SUB, :] = e
            l_scr[...] += jnp.sum(e, axis=0, keepdims=True)

    each(exps)
    l_scr[...] = 1.0 / l_scr[...]

    def values(slot):
        for s in subs:
            v = kvs[slot][1, s:s + SUB, :]
            prob = s_scr[slot, s:s + SUB, :] * l_scr[...]
            low = prob.astype(BF16)
            dp = dot_nt(v, do)
            s_scr[slot, s:s + SUB, :] = prob
            dp_scr[slot, s:s + SUB, :] = dp
            d_scr[...] += jnp.sum(prob * dp, axis=0, keepdims=True)
            grads[slot][1, s:s + SUB, :] = dot_nn(low, do).astype(BF16)
            ot_scr[...] += dot_nn(v.T, low)

    each(values)

    def keys(slot):
        for s in subs:
            k = kvs[slot][0, s:s + SUB, :]
            ds = (s_scr[slot, s:s + SUB, :] * (dp_scr[slot, s:s + SUB, :] - d_scr[...])).astype(BF16)
            grads[slot][0, s:s + SUB, :] = (dot_nn(ds, q) * SCALE).astype(BF16)
            dqt_scr[...] += dot_nn(k.T, ds)

    each(keys)
    for slot in (1, 2, 3):
        @pl.when(jnp.logical_not(live(slot)))
        def _(slot=slot):
            grads[slot][...] = jnp.zeros_like(grads[slot])

    o_ref[...] = ot_scr[...].T.astype(BF16)
    dq = dqt_scr[...].T * SCALE
    dq_ref[...] = rope(dq, cos_ref[...], sin_ref[...], -1.0).astype(BF16)


def attend(info, start, cos_t, sin_t, q, do, kvs, seq):
    tokens, hidden = q.shape
    batch, heads = tokens // seq, hidden // HEAD_DIM
    tile = pl.BlockSpec((seq, HEAD_DIM), lambda b, h, _: (b, h))
    table = pl.BlockSpec((seq, HEAD_DIM), lambda b, h, _: (b, 0))
    pair = pl.BlockSpec((2, seq, HEAD_DIM), lambda b, h, _: (0, b, h))
    return pl.pallas_call(
        attn_kernel,
        grid_spec=pltpu.PrefetchScalarGridSpec(
            num_scalar_prefetch=1,
            grid=(batch, heads),
            in_specs=[pl.BlockSpec((1, 1, seq), lambda b, h, _: (b, 0, 0)), table, table, tile, tile, pair, pair, pair, pair],
            out_specs=[tile, tile, pair, pair, pair, pair],
            scratch_shapes=[
                pltpu.VMEM((4, seq, seq), F32),
                pltpu.VMEM((4, seq, seq), F32),
                pltpu.VMEM((1, seq), F32),
                pltpu.VMEM((1, seq), F32),
                pltpu.VMEM((1, seq), F32),
                pltpu.VMEM((HEAD_DIM, seq), F32),
                pltpu.VMEM((HEAD_DIM, seq), F32),
            ],
        ),
        out_shape=[jax.ShapeDtypeStruct((tokens, hidden), BF16)] * 2 + [jax.ShapeDtypeStruct((2, tokens, hidden), BF16)] * 4,
        compiler_params=pltpu.CompilerParams(dimension_semantics=("arbitrary", "arbitrary"), vmem_limit_bytes=48 << 20),
        cost_estimate=pl.CostEstimate(flops=48 * tokens * seq * hidden, bytes_accessed=36 * tokens * hidden, transcendentals=4 * tokens * seq * heads),
        name="attend",
    )(info, start, cos_t, sin_t, q, do, *kvs)


def out_kernel(x_ref, o_ref, w_ref, y_ref):
    total = x_ref[...].astype(F32)
    parts = dot_nn(o_ref[0], w_ref[0])
    for t in range(1, o_ref.shape[0]):
        parts += dot_nn(o_ref[t], w_ref[t])
    y_ref[...] = (total + parts).astype(BF16)


def out_project(x, o_all, w_all, rows):
    tokens, d_model = x.shape
    tp, _, hidden = o_all.shape
    return pl.pallas_call(
        out_kernel,
        grid=(tokens // rows,),
        in_specs=[pl.BlockSpec((rows, d_model), lambda i: (i, 0)), pl.BlockSpec((tp, rows, hidden), lambda i: (0, i, 0)), pl.BlockSpec(memory_space=pltpu.VMEM)],
        out_specs=pl.BlockSpec((rows, d_model), lambda i: (i, 0)),
        out_shape=jax.ShapeDtypeStruct((tokens, d_model), BF16),
        compiler_params=pltpu.CompilerParams(dimension_semantics=("arbitrary",), vmem_limit_bytes=48 << 20),
        cost_estimate=pl.CostEstimate(flops=2 * tokens * tp * hidden * d_model, bytes_accessed=8 * tokens * d_model, transcendentals=0),
        name="out_project",
    )(x, o_all, w_all)


def dn_kernel(dq_ref, dkv_ref, wq_ref, wk_ref, wv_ref, dn_ref):
    dn = dot_nt(dq_ref[...], wq_ref[...]) + dot_nt(dkv_ref[0], wk_ref[...]) + dot_nt(dkv_ref[1], wv_ref[...])
    dn_ref[...] = dn.astype(BF16)


def norm_partial(dq, dkv, wq, wk, wv, rows):
    tokens, hidden = dq.shape
    d_model = wq.shape[0]
    whole = pl.BlockSpec(memory_space=pltpu.VMEM)
    return pl.pallas_call(
        dn_kernel,
        grid=(tokens // rows,),
        in_specs=[pl.BlockSpec((rows, hidden), lambda i: (i, 0)), pl.BlockSpec((2, rows, hidden), lambda i: (0, i, 0)), whole, whole, whole],
        out_specs=pl.BlockSpec((rows, d_model), lambda i: (i, 0)),
        out_shape=jax.ShapeDtypeStruct((tokens, d_model), BF16),
        compiler_params=pltpu.CompilerParams(dimension_semantics=("arbitrary",), vmem_limit_bytes=48 << 20),
        cost_estimate=pl.CostEstimate(flops=6 * tokens * hidden * d_model, bytes_accessed=2 * tokens * (d_model + 3 * hidden), transcendentals=0),
        name="norm_partial",
    )(dq, dkv, wq, wk, wv)


def solution(mesh):
    cp_size = mesh.shape["cp"]
    tp_size = mesh.shape["tp"]

    def device_step(x_in, segment_ids, positions, w_query, w_key, w_value, w_out, norm_gain, grad_out):
        batch, seq, d_model = x_in.shape
        hidden = w_query.shape[1]
        tokens = batch * seq
        rank = lax.axis_index("cp")
        core = rank % 2
        x = x_in.reshape(tokens, d_model)
        dy = grad_out.reshape(tokens, d_model)

        inv_freq = ROPE_THETA ** (-jnp.arange(0, HEAD_DIM, 2).astype(F32) / HEAD_DIM)
        angles = positions.reshape(tokens, 1).astype(F32) * jnp.repeat(inv_freq, 2)[None, :]
        cos_t, sin_t = jnp.cos(angles), jnp.sin(angles)
        start = (rank * seq + jnp.arange(seq, dtype=jnp.int32))[None, :] - positions
        info = jnp.concatenate([jnp.full((1,), rank, jnp.int32), start[:, 0]])

        w_all = lax.all_gather(w_out, "tp", axis=0)
        rows = min(384, tokens)
        normed, q, kv, do = project(x, dy, cos_t, sin_t, norm_gain.reshape(1, d_model), w_query, w_key, w_value, w_out, rows)

        def perm(value, pairs):
            return lax.ppermute(value, "cp", pairs)

        from_chip = perm(kv, [(0, 2), (1, 3)])
        from_partner = perm(kv, [(0, 1), (2, 3)])
        from_far = perm(from_chip, [(2, 3), (3, 2)])
        o, dq, g_own, g_partner, g_chip, g_far = attend(info, start.reshape(batch, 1, seq), cos_t, sin_t, q, do, (kv, from_partner, from_chip, from_far), seq)
        o_all = lax.all_gather(o, "tp", axis=0)

        far_sum = perm(g_far, [(2, 3), (3, 2)])
        chip_sum = (g_chip.astype(F32) + far_sum.astype(F32)).astype(BF16)
        partner_in = perm(g_partner, [(1, 0), (3, 2)])
        chip_in = perm(chip_sum, [(2, 0), (3, 1)])
        dkv_sum = (g_own.astype(F32) + partner_in.astype(F32) + chip_in.astype(F32)).astype(BF16)
        dk_f32 = dkv_sum[0].astype(F32)
        lane = lax.broadcasted_iota(jnp.int32, (tokens, hidden), 1)
        swapped = jnp.where(lane % 2 == 0, jnp.roll(dk_f32, -1, 1), -jnp.roll(dk_f32, 1, 1))
        wide = lambda t: jnp.tile(t, (1, hidden // HEAD_DIM))
        dk = (dk_f32 * wide(cos_t) + swapped * wide(sin_t)).astype(BF16)
        dkv = jnp.stack([dk, dkv_sum[1]])

        dn_part = norm_partial(dq, dkv, w_query, w_key, w_value, rows)
        dn = lax.psum_scatter(dn_part, "tp", scatter_dimension=0, tiled=True).astype(F32)
        quarter = tokens // tp_size
        here = lax.axis_index("tp") * quarter
        x_q = lax.dynamic_slice(x, (here, 0), (quarter, d_model)).astype(F32)
        dy_q = lax.dynamic_slice(dy, (here, 0), (quarter, d_model)).astype(F32)
        centred = x_q - jnp.mean(x_q, axis=-1, keepdims=True)
        inv_std = lax.rsqrt(jnp.mean(centred * centred, axis=-1, keepdims=True) + LN_EPS)
        x_hat = centred * inv_std
        d_hat = dn * norm_gain
        dx = inv_std * (d_hat - jnp.mean(d_hat, axis=-1, keepdims=True) - x_hat * jnp.mean(d_hat * x_hat, axis=-1, keepdims=True))
        grad_x_q = (dy_q + dx).astype(BF16)
        grad_x = lax.all_gather(grad_x_q, "tp", axis=0, tiled=True)
        grad_gain = lax.psum(jnp.sum(dn * x_hat, axis=0), ("tp", "cp"))

        def tn(a, b):
            return lax.dot_general(a, b, (((0,), (0,)), ((), ())), preferred_element_type=F32)

        def reduce_cp(part):
            half = part.shape[0] // 2
            away = lax.dynamic_slice(part, ((1 - core) * half, 0), (half, part.shape[1]))
            mine = lax.dynamic_slice(part, (core * half, 0), (half, part.shape[1]))
            mine = (mine + perm(away, [(0, 1), (1, 0), (2, 3), (3, 2)])).astype(BF16)
            other = perm(mine, [(0, 2), (2, 0), (1, 3), (3, 1)])
            total = mine.astype(F32) + other.astype(F32)
            rest = perm(total, [(0, 1), (1, 0), (2, 3), (3, 2)])
            return jnp.where(core == 0, jnp.concatenate([total, rest]), jnp.concatenate([rest, total]))

        grad_wo = reduce_cp(tn(o, dy))
        grad_wq = reduce_cp(tn(normed, dq))
        grad_wk = reduce_cp(tn(normed, dkv[0]))
        grad_wv = reduce_cp(tn(normed, dkv[1]))
        y_out = out_project(x, o_all, w_all, rows)
        return y_out.reshape(x_in.shape), grad_x.reshape(x_in.shape), grad_gain, grad_wq, grad_wk, grad_wv, grad_wo

    in_specs = (P("dp", "cp", None), P("dp", "cp"), P("dp", "cp"), P(None, "tp"), P(None, "tp"), P(None, "tp"), P("tp", None), P(None), P("dp", "cp", None))
    out_specs = (P("dp", "cp", None), P("dp", "cp", None), P("dp"), P("dp", "tp"), P("dp", "tp"), P("dp", "tp"), P(("dp", "tp"), None))
    return jax.shard_map(device_step, mesh=mesh, in_specs=in_specs, out_specs=out_specs, check_vma=False)
```

```python
import functools
import math

import jax
import jax.numpy as jnp
from jax import lax
from jax.experimental import pallas as pl
from jax.experimental.pallas import tpu as pltpu
from jax.sharding import PartitionSpec as P

HEAD_DIM = 128
ROPE_THETA = 8000000.0
LN_EPS = 1e-5
NEG_BIG = -1e30
SCALE = HEAD_DIM ** -0.5
EXP2_SCALE = SCALE * math.log2(math.e)
F32 = jnp.float32
BF16 = jnp.bfloat16
NT = (((1,), (1,)), ((), ()))


def dot_nn(a, b):
    return jnp.dot(a, b, preferred_element_type=F32)


def dot_nt(a, b):
    return lax.dot_general(a, b, NT, preferred_element_type=F32)


def dot_tn(a, b):
    return lax.dot_general(a, b, (((0,), (0,)), ((), ())), preferred_element_type=F32)


def swap_pairs(t, sign):
    lane = lax.broadcasted_iota(jnp.int32, t.shape, 1)
    even = (lane % 2) == 0
    up = pltpu.roll(t, HEAD_DIM - 1, 1)
    down = pltpu.roll(t, 1, 1)
    return jnp.where(even, -up, down) if sign > 0 else jnp.where(even, up, -down)


def rope(t, cos_t, sin_t, sign):
    return t * cos_t + swap_pairs(t, sign) * sin_t


def proj_kernel(x_ref, dy_ref, cos_ref, sin_ref, gain_ref, wq_ref, wk_ref, wv_ref, wo_ref, n_ref, q_ref, kv_ref, do_ref):
    x = x_ref[...].astype(F32)
    centred = x - jnp.mean(x, axis=-1, keepdims=True)
    inv_std = lax.rsqrt(jnp.mean(centred * centred, axis=-1, keepdims=True) + LN_EPS)
    normed = ((centred * inv_std) * gain_ref[...]).astype(BF16)
    n_ref[...] = normed
    cos_t = cos_ref[...]
    sin_t = sin_ref[...]

    def put_rope(dst, raw):
        for h in range(raw.shape[1] // HEAD_DIM):
            cols = slice(h * HEAD_DIM, (h + 1) * HEAD_DIM)
            dst[:, cols] = rope(raw[:, cols], cos_t, sin_t, 1.0).astype(BF16)

    put_rope(kv_ref.at[0], dot_nn(normed, wk_ref[...]))
    kv_ref[1] = dot_nn(normed, wv_ref[...]).astype(BF16)
    put_rope(q_ref, dot_nn(normed, wq_ref[...]))
    do_ref[...] = dot_nt(dy_ref[...], wo_ref[...]).astype(BF16)


def project(x, dy, cos_t, sin_t, gain, wq, wk, wv, wo, rows):
    tokens, d_model = x.shape
    hidden = wq.shape[1]
    whole = pl.BlockSpec(memory_space=pltpu.VMEM)
    tile = lambda width: pl.BlockSpec((rows, width), lambda i: (i, 0))
    return pl.pallas_call(
        proj_kernel,
        grid=(tokens // rows,),
        in_specs=[tile(d_model), tile(d_model), tile(HEAD_DIM), tile(HEAD_DIM), whole, whole, whole, whole, whole],
        out_specs=[tile(d_model), tile(hidden), pl.BlockSpec((2, rows, hidden), lambda i: (0, i, 0)), tile(hidden)],
        out_shape=[
            jax.ShapeDtypeStruct((tokens, d_model), BF16),
            jax.ShapeDtypeStruct((tokens, hidden), BF16),
            jax.ShapeDtypeStruct((2, tokens, hidden), BF16),
            jax.ShapeDtypeStruct((tokens, hidden), BF16),
        ],
        compiler_params=pltpu.CompilerParams(dimension_semantics=("arbitrary",), vmem_limit_bytes=60 << 20),
        cost_estimate=pl.CostEstimate(flops=8 * tokens * d_model * hidden, bytes_accessed=8 * tokens * d_model + 8 * d_model * hidden, transcendentals=0),
        name="project",
    )(x, dy, cos_t, sin_t, gain, wq, wk, wv, wo)


SUB = 128
ROWS = 48


def attn_kernel(info_ref, start_ref, cos_ref, sin_ref, q_ref, do_ref, kv0_ref, kv1_ref, kv2_ref, kv3_ref,
                o_ref, dq_ref, g0_ref, g1_ref, g2_ref, g3_ref, s_scr, dp_scr, m_scr, l_scr, d_scr, ot_scr, dqt_scr):
    b = pl.program_id(0)
    rank = info_ref[0]
    first = info_ref[1 + b]
    seq = q_ref.shape[0]
    kvs = (kv0_ref, kv1_ref, kv2_ref, kv3_ref)
    grads = (g0_ref, g1_ref, g2_ref, g3_ref)
    q = q_ref[...]
    do = do_ref[...]
    start = start_ref[0]
    subs = range(0, seq, SUB)

    def piece_of(slot):
        return rank ^ slot if slot else rank

    def live(slot):
        piece = piece_of(slot)
        return jnp.logical_and(piece < rank, first < (piece + 1) * seq)

    def each(body):
        body(0)
        for slot in (1, 2, 3):
            pl.when(live(slot))(functools.partial(body, slot))

    m_scr[...] = jnp.full(m_scr.shape, NEG_BIG, F32)
    l_scr[...] = jnp.zeros_like(l_scr)
    d_scr[...] = jnp.zeros_like(d_scr)
    ot_scr[...] = jnp.zeros_like(ot_scr)
    dqt_scr[...] = jnp.zeros_like(dqt_scr)

    def scores(slot):
        base = piece_of(slot) * seq
        for s in subs:
            raw = dot_nt(kvs[slot][0, s:s + SUB, :], q)
            local = lax.broadcasted_iota(jnp.int32, raw.shape, 0) + s
            allowed = (local + base) >= start
            if slot == 0:
                allowed = jnp.logical_and(allowed, local <= lax.broadcasted_iota(jnp.int32, raw.shape, 1))
            raw = jnp.where(allowed, raw, NEG_BIG)
            s_scr[slot, s:s + SUB, :] = raw
            m_scr[...] = jnp.maximum(m_scr[...], jnp.max(raw, axis=0, keepdims=True))

    each(scores)

    def exps(slot):
        for s in subs:
            e = jnp.exp2((s_scr[slot, s:s + SUB, :] - m_scr[...]) * EXP2_SCALE)
            s_scr[slot, s:s + SUB, :] = e
            l_scr[...] += jnp.sum(e, axis=0, keepdims=True)

    each(exps)
    l_scr[...] = 1.0 / l_scr[...]

    def values(slot):
        for s in subs:
            v = kvs[slot][1, s:s + SUB, :]
            prob = s_scr[slot, s:s + SUB, :] * l_scr[...]
            low = prob.astype(BF16)
            dp = dot_nt(v, do)
            s_scr[slot, s:s + SUB, :] = prob
            dp_scr[slot, s:s + SUB, :] = dp
            d_scr[...] += jnp.sum(prob * dp, axis=0, keepdims=True)
            grads[slot][1, s:s + SUB, :] = dot_nn(low, do).astype(BF16)
            ot_scr[...] += dot_nn(v.T, low)

    each(values)

    def keys(slot):
        for s in subs:
            k = kvs[slot][0, s:s + SUB, :]
            ds = (s_scr[slot, s:s + SUB, :] * (dp_scr[slot, s:s + SUB, :] - d_scr[...])).astype(BF16)
            grads[slot][0, s:s + SUB, :] = (dot_nn(ds, q) * SCALE).astype(BF16)
            dqt_scr[...] += dot_nn(k.T, ds)

    each(keys)
    for slot in (1, 2, 3):
        @pl.when(jnp.logical_not(live(slot)))
        def _(slot=slot):
            grads[slot][...] = jnp.zeros_like(grads[slot])

    o_ref[...] = ot_scr[...].T.astype(BF16)
    dq = dqt_scr[...].T * SCALE
    dq_ref[...] = rope(dq, cos_ref[...], sin_ref[...], -1.0).astype(BF16)


def attend(info, start, cos_t, sin_t, q, do, kvs, seq):
    tokens, hidden = q.shape
    batch, heads = tokens // seq, hidden // HEAD_DIM
    tile = pl.BlockSpec((seq, HEAD_DIM), lambda b, h, _: (b, h))
    table = pl.BlockSpec((seq, HEAD_DIM), lambda b, h, _: (b, 0))
    pair = pl.BlockSpec((2, seq, HEAD_DIM), lambda b, h, _: (0, b, h))
    return pl.pallas_call(
        attn_kernel,
        grid_spec=pltpu.PrefetchScalarGridSpec(
            num_scalar_prefetch=1,
            grid=(batch, heads),
            in_specs=[pl.BlockSpec((1, 1, seq), lambda b, h, _: (b, 0, 0)), table, table, tile, tile, pair, pair, pair, pair],
            out_specs=[tile, tile, pair, pair, pair, pair],
            scratch_shapes=[
                pltpu.VMEM((4, seq, seq), F32),
                pltpu.VMEM((4, seq, seq), F32),
                pltpu.VMEM((1, seq), F32),
                pltpu.VMEM((1, seq), F32),
                pltpu.VMEM((1, seq), F32),
                pltpu.VMEM((HEAD_DIM, seq), F32),
                pltpu.VMEM((HEAD_DIM, seq), F32),
            ],
        ),
        out_shape=[jax.ShapeDtypeStruct((tokens, hidden), BF16)] * 2 + [jax.ShapeDtypeStruct((2, tokens, hidden), BF16)] * 4,
        compiler_params=pltpu.CompilerParams(dimension_semantics=("arbitrary", "arbitrary"), vmem_limit_bytes=48 << 20),
        cost_estimate=pl.CostEstimate(flops=48 * tokens * seq * hidden, bytes_accessed=36 * tokens * hidden, transcendentals=4 * tokens * seq * heads),
        name="attend",
    )(info, start, cos_t, sin_t, q, do, *kvs)


MESH = pl.DeviceIdType.MESH


def back_kernel(groups, rows, tp, cp, dq_hbm, dkv_hbm, x_hbm, dy_hbm, o_hbm, wq_ref, wk_ref, wv_ref, wo_ref, gain_ref,
                gx_hbm, y_hbm, gg_ref, part, rs_r, rs_l, send_r, send_l, tot, gx_buf, dq_in, dkv_in, o_in, x_in, dy_in, y_buf, gain_all,
                in_sem, y_sem, own_sem, rss_r, rss_l, rsr_r, rsr_l, ag0_r, ag0_l, agf_r, agf_l, agr_r, agr_l, gs_sem, gr_sem):
    z = lax.axis_index("tp")
    r = lax.axis_index("cp")
    last = tp - 1
    slots = tp - 1
    span = tp * rows
    d_model = x_hbm.shape[1]
    chunk = min(512, d_model)

    barrier = pltpu.get_barrier_semaphore()
    peers = [(dt, dc) for dt in range(tp) for dc in range(cp) if dt or dc]
    for dt, dc in peers:
        pl.semaphore_signal(barrier, inc=1, device_id={"tp": lax.rem(z + dt, tp), "cp": lax.rem(r + dc, cp)}, device_id_type=MESH)
    pl.semaphore_wait(barrier, len(peers))

    def remote(src, dst, ssem, rsem, dev):
        return pltpu.make_async_remote_copy(src_ref=src, dst_ref=dst, send_sem=ssem, recv_sem=rsem, device_id=dev, device_id_type=MESH)

    def move(dir_right):
        return {"tp": jnp.where(z < last, z + 1, z)} if dir_right else {"tp": jnp.where(z > 0, z - 1, z)}

    right, left = move(True), move(False)

    def group_rows(i):
        return pl.ds(pl.multiple_of(i * span, span), span)

    def tile_rows(i, owner):
        return pl.ds(pl.multiple_of(i * span + owner * rows, rows), rows)

    def inputs(i, slot):
        g = group_rows(i)
        return [
            pltpu.make_async_copy(dq_hbm.at[g, :], dq_in.at[slot], in_sem.at[slot, 0]),
            pltpu.make_async_copy(dkv_hbm.at[:, g, :], dkv_in.at[slot], in_sem.at[slot, 1]),
            pltpu.make_async_copy(o_hbm.at[:, g, :], o_in.at[slot], in_sem.at[slot, 2]),
            pltpu.make_async_copy(x_hbm.at[g, :], x_in.at[slot], in_sem.at[slot, 3]),
            pltpu.make_async_copy(dy_hbm.at[tile_rows(i, z), :], dy_in.at[slot], in_sem.at[slot, 4]),
        ]

    def y_copy(i, slot):
        return pltpu.make_async_copy(y_buf.at[slot], y_hbm.at[group_rows(i), :], y_sem.at[slot])

    def rs_copy(i, s, to_right):
        if to_right:
            return remote(send_r.at[s], rs_r.at[i, s], rss_r.at[s], rsr_r.at[i, s], right)
        return remote(send_l.at[s], rs_l.at[i, s], rss_l.at[s], rsr_l.at[i, s], left)

    def rs_send(i, cur, s):
        for to_right in (True, False):
            far = z if to_right else last - z
            owner = (z + slots - s) if to_right else (z - slots + s)
            buf, held = (send_r, rs_r) if to_right else (send_l, rs_l)

            @pl.when(jnp.logical_and(i < groups, jnp.logical_and(far <= s, far < last)))
            def _(to_right=to_right, far=far, owner=owner, buf=buf, held=held):
                @pl.when(i > 0)
                def _():
                    rs_copy(i - 1, s, to_right).wait_send()

                mine = pl.ds(pl.multiple_of(owner * rows, rows), rows)
                if s == 0:
                    buf[s] = part[cur, mine, :].astype(BF16)
                else:
                    @pl.when(far == 0)
                    def _():
                        buf[s] = part[cur, mine, :].astype(BF16)

                    @pl.when(far > 0)
                    def _():
                        rs_copy(i, s - 1, to_right).wait_recv()
                        buf[s] = (part[cur, mine, :] + held[i, s - 1].astype(F32)).astype(BF16)

                rs_copy(i, s, to_right).start()

    def ag_own(i, slot, to_right):
        src = gx_buf.at[slot]
        dst = gx_hbm.at[tile_rows(i, z), :]
        if to_right:
            return remote(src, dst, ag0_r.at[slot], agr_r.at[i, 0], right)
        return remote(src, dst, ag0_l.at[slot], agr_l.at[i, 0], left)

    def own_copy(i, slot):
        return pltpu.make_async_copy(gx_buf.at[slot], gx_hbm.at[tile_rows(i, z), :], own_sem.at[slot])

    def ag_forward(i, a, to_right):
        owner = z - a if to_right else z + a
        tile = gx_hbm.at[tile_rows(i, owner), :]
        if to_right:
            return remote(tile, tile, agf_r.at[a], agr_r.at[i, a], right)
        return remote(tile, tile, agf_l.at[a], agr_l.at[i, a], left)

    def ag_wait(i, a, to_right):
        tile = gx_hbm.at[tile_rows(i, 0), :]
        sem = agr_r.at[i, a] if to_right else agr_l.at[i, a]
        remote(tile, tile, agf_r.at[a], sem, right).wait_recv()

    def ag_step(i, a):
        for to_right in (True, False):
            far = z if to_right else last - z

            @pl.when(jnp.logical_and(jnp.logical_and(i >= 0, i < groups), far >= a))
            def _(to_right=to_right, far=far):
                ag_wait(i, a - 1, to_right)
                if a < slots:
                    @pl.when(far < last)
                    def _():
                        @pl.when(i > 0)
                        def _():
                            ag_forward(i - 1, a, to_right).wait_send()

                        ag_forward(i, a, to_right).start()

    def ag_first(i, slot):
        own_copy(i, slot).start()
        for to_right in (True, False):
            far = z if to_right else last - z

            @pl.when(far < last)
            def _(to_right=to_right):
                ag_own(i, slot, to_right).start()

    def ag_first_done(i, slot):
        own_copy(i, slot).wait()
        for to_right in (True, False):
            far = z if to_right else last - z

            @pl.when(far < last)
            def _(to_right=to_right):
                ag_own(i, slot, to_right).wait_send()

    def partial_norm(cur):
        for c in range(0, d_model, chunk):
            cols = slice(c, c + chunk)
            part[cur, :, cols] = (
                dot_nt(dq_in[cur], wq_ref[cols, :]) + dot_nt(dkv_in[cur, 0], wk_ref[cols, :]) + dot_nt(dkv_in[cur, 1], wv_ref[cols, :])
            )

    def project_out(cur, lo, hi):
        for c in range(lo, hi, chunk):
            cols = slice(c, c + chunk)
            acc = dot_nn(o_in[cur, 0], wo_ref[0, :, cols])
            for t in range(1, tp):
                acc += dot_nn(o_in[cur, t], wo_ref[t, :, cols])
            y_buf[cur, :, cols] = (x_in[cur, :, cols].astype(F32) + acc).astype(BF16)

    def finalize(i, slot):
        mine = pl.ds(pl.multiple_of(z * rows, rows), rows)
        tot[...] = part[slot, mine, :]

        @pl.when(z > 0)
        def _():
            rs_copy(i, slots - 1, True).wait_recv()
            tot[...] += rs_r[i, slots - 1].astype(F32)

        @pl.when(z < last)
        def _():
            rs_copy(i, slots - 1, False).wait_recv()
            tot[...] += rs_l[i, slots - 1].astype(F32)

        @pl.when(i > 1)
        def _():
            ag_first_done(i - 2, slot)

        x = x_in[slot, mine, :].astype(F32)
        centred = x - jnp.mean(x, axis=-1, keepdims=True)
        inv_std = lax.rsqrt(jnp.mean(centred * centred, axis=-1, keepdims=True) + LN_EPS)
        x_hat = centred * inv_std
        dn = tot[...]
        gg_ref[...] += jnp.sum(dn * x_hat, axis=0, keepdims=True)
        d_hat = dn * gain_ref[...]
        dx = inv_std * (d_hat - jnp.mean(d_hat, axis=-1, keepdims=True) - x_hat * jnp.mean(d_hat * x_hat, axis=-1, keepdims=True))
        gx_buf[slot] = (dy_in[slot].astype(F32) + dx).astype(BF16)

    gg_ref[...] = jnp.zeros_like(gg_ref)
    for copy in inputs(0, 0):
        copy.start()

    me = z * cp + r

    def gain_copy(dt, dc):
        to = {"tp": lax.rem(z + dt, tp), "cp": lax.rem(r + dc, cp)}
        return remote(gain_all.at[me], gain_all.at[me], gs_sem.at[dt * cp + dc], gr_sem.at[me], to)

    def gain_wait(dt, dc):
        sender = lax.rem(z + dt, tp) * cp + lax.rem(r + dc, cp)
        remote(gain_all.at[sender], gain_all.at[sender], gs_sem.at[0], gr_sem.at[sender], right).wait_recv()

    def step(i, carry):
        cur = lax.rem(i, 2)
        prv = 1 - cur

        @pl.when(i < groups)
        def _():
            for copy in inputs(i, cur):
                copy.wait()
            partial_norm(cur)

        rs_send(i, cur, 0)
        ag_step(i - 2, 1)

        @pl.when(jnp.logical_and(i >= 1, i <= groups))
        def _():
            finalize(i - 1, prv)

        @pl.when(i + 1 < groups)
        def _():
            for copy in inputs(i + 1, prv):
                copy.start()

        @pl.when(jnp.logical_and(i >= 2, i < groups))
        def _():
            y_copy(i - 2, cur).wait()

        @pl.when(i < groups)
        def _():
            project_out(cur, 0, d_model // 2)

        rs_send(i, cur, 1)
        ag_step(i - 2, 2)

        @pl.when(i < groups)
        def _():
            project_out(cur, d_model // 2, d_model)
            y_copy(i, cur).start()

        rs_send(i, cur, 2)

        @pl.when(jnp.logical_and(i >= 1, i <= groups))
        def _():
            ag_first(i - 1, prv)

        @pl.when(i == groups)
        def _():
            gain_all[me] = gg_ref[...]
            for dt, dc in peers:
                gain_copy(dt, dc).start()

        ag_step(i - 2, 3)
        return carry

    lax.fori_loop(0, groups + 2, step, 0)

    for i in (groups - 2, groups - 1):
        y_copy(i, i % 2).wait()
        ag_first_done(i, i % 2)
    for to_right in (True, False):
        far = z if to_right else last - z
        for s in range(slots):
            @pl.when(jnp.logical_and(far <= s, far < last))
            def _(s=s, to_right=to_right):
                rs_copy(groups - 1, s, to_right).wait_send()
        for a in range(1, slots):
            @pl.when(jnp.logical_and(far >= a, far < last))
            def _(a=a, to_right=to_right):
                ag_forward(groups - 1, a, to_right).wait_send()
    for dt, dc in peers:
        gain_wait(dt, dc)
        gain_copy(dt, dc).wait_send()
    total = gain_all[0]
    for j in range(1, tp * cp):
        total += gain_all[j]
    gg_ref[...] = total


def backward_norm(dq, dkv, x, dy, o_all, wq, wk, wv, wo_all, gain, rows, tp, cp):
    tokens, hidden = dq.shape
    d_model = x.shape[1]
    span = tp * rows
    groups = tokens // span
    slots = tp - 1
    hbm = pl.BlockSpec(memory_space=pl.ANY)
    vmem = pl.BlockSpec(memory_space=pltpu.VMEM)
    dma = pltpu.SemaphoreType.DMA
    return pl.pallas_call(
        functools.partial(back_kernel, groups, rows, tp, cp),
        in_specs=[hbm] * 5 + [vmem] * 5,
        out_specs=[hbm, hbm, vmem],
        out_shape=[
            jax.ShapeDtypeStruct((tokens, d_model), BF16),
            jax.ShapeDtypeStruct((tokens, d_model), BF16),
            jax.ShapeDtypeStruct((1, d_model), F32),
        ],
        scratch_shapes=[
            pltpu.VMEM((2, span, d_model), F32),
            pltpu.VMEM((groups, slots, rows, d_model), BF16),
            pltpu.VMEM((groups, slots, rows, d_model), BF16),
            pltpu.VMEM((slots, rows, d_model), BF16),
            pltpu.VMEM((slots, rows, d_model), BF16),
            pltpu.VMEM((rows, d_model), F32),
            pltpu.VMEM((2, rows, d_model), BF16),
            pltpu.VMEM((2, span, hidden), BF16),
            pltpu.VMEM((2, 2, span, hidden), BF16),
            pltpu.VMEM((2, tp, span, hidden), BF16),
            pltpu.VMEM((2, span, d_model), BF16),
            pltpu.VMEM((2, rows, d_model), BF16),
            pltpu.VMEM((2, span, d_model), BF16),
            pltpu.VMEM((tp * cp, 1, d_model), F32),
            dma((2, 5)),
            dma((2,)),
            dma((2,)),
            dma((slots,)),
            dma((slots,)),
            dma((groups, slots)),
            dma((groups, slots)),
            dma((2,)),
            dma((2,)),
            dma((slots,)),
            dma((slots,)),
            dma((groups, slots)),
            dma((groups, slots)),
            dma((tp * cp,)),
            dma((tp * cp,)),
        ],
        compiler_params=pltpu.CompilerParams(collective_id=0, has_side_effects=True, vmem_limit_bytes=60 << 20),
        cost_estimate=pl.CostEstimate(flops=14 * tokens * hidden * d_model, bytes_accessed=16 * tokens * d_model, transcendentals=0),
        name="backward_norm",
    )(dq, dkv, x, dy, o_all, wq, wk, wv, wo_all, gain)


def solution(mesh):
    cp_size = mesh.shape["cp"]
    tp_size = mesh.shape["tp"]

    def device_step(x_in, segment_ids, positions, w_query, w_key, w_value, w_out, norm_gain, grad_out):
        batch, seq, d_model = x_in.shape
        hidden = w_query.shape[1]
        tokens = batch * seq
        rank = lax.axis_index("cp")
        core = rank % 2
        x = x_in.reshape(tokens, d_model)
        dy = grad_out.reshape(tokens, d_model)

        inv_freq = ROPE_THETA ** (-jnp.arange(0, HEAD_DIM, 2).astype(F32) / HEAD_DIM)
        angles = positions.reshape(tokens, 1).astype(F32) * jnp.repeat(inv_freq, 2)[None, :]
        cos_t, sin_t = jnp.cos(angles), jnp.sin(angles)
        start = (rank * seq + jnp.arange(seq, dtype=jnp.int32))[None, :] - positions
        info = jnp.concatenate([jnp.full((1,), rank, jnp.int32), start[:, 0]])

        w_all = lax.all_gather(w_out, "tp", axis=0)
        rows = min(384, tokens)
        normed, q, kv, do = project(x, dy, cos_t, sin_t, norm_gain.reshape(1, d_model), w_query, w_key, w_value, w_out, rows)

        def perm(value, pairs):
            return lax.ppermute(value, "cp", pairs)

        from_chip = perm(kv, [(0, 2), (1, 3)])
        from_partner = perm(kv, [(0, 1), (2, 3)])
        from_far = perm(from_chip, [(2, 3), (3, 2)])
        o, dq, g_own, g_partner, g_chip, g_far = attend(info, start.reshape(batch, 1, seq), cos_t, sin_t, q, do, (kv, from_partner, from_chip, from_far), seq)
        o_all = lax.all_gather(o, "tp", axis=0)

        far_sum = perm(g_far, [(2, 3), (3, 2)])
        chip_sum = (g_chip.astype(F32) + far_sum.astype(F32)).astype(BF16)
        partner_in = perm(g_partner, [(1, 0), (3, 2)])
        chip_in = perm(chip_sum, [(2, 0), (3, 1)])
        dkv_sum = (g_own.astype(F32) + partner_in.astype(F32) + chip_in.astype(F32)).astype(BF16)
        dk_f32 = dkv_sum[0].astype(F32)
        lane = lax.broadcasted_iota(jnp.int32, (tokens, hidden), 1)
        swapped = jnp.where(lane % 2 == 0, jnp.roll(dk_f32, -1, 1), -jnp.roll(dk_f32, 1, 1))
        wide = lambda t: jnp.tile(t, (1, hidden // HEAD_DIM))
        dk = (dk_f32 * wide(cos_t) + swapped * wide(sin_t)).astype(BF16)
        dkv = jnp.stack([dk, dkv_sum[1]])

        grad_x, y_out, grad_gain = backward_norm(dq, dkv, x, dy, o_all, w_query, w_key, w_value, w_all, norm_gain.reshape(1, d_model), ROWS, tp_size, cp_size)
        grad_gain = grad_gain.reshape(d_model)

        def tn(a, b):
            return lax.dot_general(a, b, (((0,), (0,)), ((), ())), preferred_element_type=F32)

        def reduce_cp(part):
            half = part.shape[0] // 2
            away = lax.dynamic_slice(part, ((1 - core) * half, 0), (half, part.shape[1]))
            mine = lax.dynamic_slice(part, (core * half, 0), (half, part.shape[1]))
            mine = (mine + perm(away, [(0, 1), (1, 0), (2, 3), (3, 2)])).astype(BF16)
            other = perm(mine, [(0, 2), (2, 0), (1, 3), (3, 1)])
            total = mine.astype(F32) + other.astype(F32)
            rest = perm(total, [(0, 1), (1, 0), (2, 3), (3, 2)])
            return jnp.where(core == 0, jnp.concatenate([total, rest]), jnp.concatenate([rest, total]))

        grad_wo = reduce_cp(tn(o, dy))
        grad_wq = reduce_cp(tn(normed, dq))
        grad_wk = reduce_cp(tn(normed, dkv[0]))
        grad_wv = reduce_cp(tn(normed, dkv[1]))
        return y_out.reshape(x_in.shape), grad_x.reshape(x_in.shape), grad_gain, grad_wq, grad_wk, grad_wv, grad_wo

    in_specs = (P("dp", "cp", None), P("dp", "cp"), P("dp", "cp"), P(None, "tp"), P(None, "tp"), P(None, "tp"), P("tp", None), P(None), P("dp", "cp", None))
    out_specs = (P("dp", "cp", None), P("dp", "cp", None), P("dp"), P("dp", "tp"), P("dp", "tp"), P("dp", "tp"), P(("dp", "tp"), None))
    return jax.shard_map(device_step, mesh=mesh, in_specs=in_specs, out_specs=out_specs, check_vma=False)
```

```python
import functools
import math

import jax
import jax.numpy as jnp
from jax import lax
from jax.experimental import pallas as pl
from jax.experimental.pallas import tpu as pltpu
from jax.sharding import PartitionSpec as P

HEAD_DIM = 128
ROPE_THETA = 8000000.0
LN_EPS = 1e-5
NEG_BIG = -1e30
SCALE = HEAD_DIM ** -0.5
EXP2_SCALE = SCALE * math.log2(math.e)
F32 = jnp.float32
BF16 = jnp.bfloat16
NT = (((1,), (1,)), ((), ()))


def dot_nn(a, b):
    return jnp.dot(a, b, preferred_element_type=F32)


def dot_nt(a, b):
    return lax.dot_general(a, b, NT, preferred_element_type=F32)


def dot_tn(a, b):
    return lax.dot_general(a, b, (((0,), (0,)), ((), ())), preferred_element_type=F32)


def swap_pairs(t, sign):
    lane = lax.broadcasted_iota(jnp.int32, t.shape, 1)
    even = (lane % 2) == 0
    up = pltpu.roll(t, HEAD_DIM - 1, 1)
    down = pltpu.roll(t, 1, 1)
    return jnp.where(even, -up, down) if sign > 0 else jnp.where(even, up, -down)


def rope(t, cos_t, sin_t, sign):
    return t * cos_t + swap_pairs(t, sign) * sin_t


def put_rope(dst, raw, cos_t, sin_t):
    for h in range(raw.shape[1] // HEAD_DIM):
        cols = slice(h * HEAD_DIM, (h + 1) * HEAD_DIM)
        dst[:, cols] = rope(raw[:, cols], cos_t, sin_t, 1.0).astype(BF16)


def keys_kernel(x_ref, cos_ref, sin_ref, gain_ref, wk_ref, wv_ref, n_ref, kv_ref):
    x = x_ref[...].astype(F32)
    centred = x - jnp.mean(x, axis=-1, keepdims=True)
    inv_std = lax.rsqrt(jnp.mean(centred * centred, axis=-1, keepdims=True) + LN_EPS)
    normed = ((centred * inv_std) * gain_ref[...]).astype(BF16)
    n_ref[...] = normed
    put_rope(kv_ref.at[0], dot_nn(normed, wk_ref[...]), cos_ref[...], sin_ref[...])
    kv_ref[1] = dot_nn(normed, wv_ref[...]).astype(BF16)


def project_keys(x, cos_t, sin_t, gain, wk, wv, rows):
    tokens, d_model = x.shape
    hidden = wk.shape[1]
    whole = pl.BlockSpec(memory_space=pltpu.VMEM)
    tile = lambda width: pl.BlockSpec((rows, width), lambda i: (i, 0))
    return pl.pallas_call(
        keys_kernel,
        grid=(tokens // rows,),
        in_specs=[tile(d_model), tile(HEAD_DIM), tile(HEAD_DIM), whole, whole, whole],
        out_specs=[tile(d_model), pl.BlockSpec((2, rows, hidden), lambda i: (0, i, 0))],
        out_shape=[jax.ShapeDtypeStruct((tokens, d_model), BF16), jax.ShapeDtypeStruct((2, tokens, hidden), BF16)],
        compiler_params=pltpu.CompilerParams(dimension_semantics=("arbitrary",), vmem_limit_bytes=48 << 20),
        cost_estimate=pl.CostEstimate(flops=4 * tokens * d_model * hidden, bytes_accessed=4 * tokens * (d_model + hidden), transcendentals=0),
        name="project_keys",
    )(x, cos_t, sin_t, gain, wk, wv)


MESH = pl.DeviceIdType.MESH
SUB = 128
ROWS = 48
RELAY_LAG = 2
CHIP_BUFS = 3


def front_kernel(batch, seq, tp, cp, kv_hbm, n_hbm, dy_hbm, cos_ref, sin_ref, start_ref, wq_ref, wo_ref,
                 o_all, dq_hbm, dkv_hbm,
                 q_all, do_all, n_in, dy_in, kv_own, kvr, s_scr, dp_scr, m_scr, l_scr, d_scr, ot_scr, dqt_scr,
                 o_buf, dq_buf, g_own, g_part, g_chip, g_far, xin, part_in, dkv_out,
                 tile_sem, own_sem, kvs_part, kvs_chip, kvs_far, kv_recv, o_local, o_send, o_recv, relay_send, dq_sem,
                 far_send, part_send, chip_send, x_recv, part_recv, dkv_sem):
    z = lax.axis_index("tp")
    r = lax.axis_index("cp")
    core = lax.rem(r, 2)
    chip = lax.div(r, 2)
    hidden = q_all.shape[1]
    heads = hidden // HEAD_DIM
    first_chip, second_chip = chip == 0, chip == 1
    first_core, second_core = core == 0, core == 1
    partner = {"cp": r + 1 - 2 * core}
    peer = {"cp": r + 2 - 4 * chip}

    barrier = pltpu.get_barrier_semaphore()
    for dev in [partner, peer] + [{"tp": lax.rem(z + dt, tp)} for dt in range(1, tp)]:
        pl.semaphore_signal(barrier, inc=1, device_id=dev, device_id_type=MESH)
    pl.semaphore_wait(barrier, tp + 1)

    def remote(src, dst, ssem, rsem, dev):
        return pltpu.make_async_remote_copy(src_ref=src, dst_ref=dst, send_sem=ssem, recv_sem=rsem, device_id=dev, device_id_type=MESH)

    def row(b):
        return pl.ds(pl.multiple_of(b * seq, seq), seq)

    def kv_to_partner(b):
        return remote(kv_hbm.at[:, row(b), :], kvr.at[0, b], kvs_part.at[b], kv_recv.at[0, b], partner)

    def kv_to_chip(b):
        return remote(kv_hbm.at[:, row(b), :], kvr.at[1, b], kvs_chip.at[b], kv_recv.at[1, b], peer)

    def kv_forward(b):
        return remote(kvr.at[1, b], kvr.at[2, b], kvs_far.at[b], kv_recv.at[2, b], partner)

    for b in range(batch):
        @pl.when(first_chip)
        def _(b=b):
            kv_to_chip(b).start()

        @pl.when(first_core)
        def _(b=b):
            kv_to_partner(b).start()

    def own_load(b, par):
        return pltpu.make_async_copy(kv_hbm.at[:, row(b), :], kv_own.at[par], own_sem.at[par])

    own_load(0, 0).start()

    tile = n_in.shape[1]
    tiles = batch * seq // tile

    def tile_rows(t):
        return pl.ds(pl.multiple_of(t * tile, tile), tile)

    def tile_loads(t, par):
        return [
            pltpu.make_async_copy(n_hbm.at[tile_rows(t), :], n_in.at[par], tile_sem.at[par, 0]),
            pltpu.make_async_copy(dy_hbm.at[tile_rows(t), :], dy_in.at[par], tile_sem.at[par, 1]),
        ]

    for copy in tile_loads(0, 0):
        copy.start()

    def project(t, carry):
        par = lax.rem(t, 2)
        for copy in tile_loads(t, par):
            copy.wait()

        @pl.when(t + 1 < tiles)
        def _():
            for copy in tile_loads(t + 1, 1 - par):
                copy.start()

        rows = tile_rows(t)
        put_rope(q_all.at[rows, :], dot_nn(n_in[par], wq_ref[...]), cos_ref[rows, :], sin_ref[rows, :])
        do_all[rows, :] = dot_nt(dy_in[par], wo_ref[...]).astype(BF16)
        return carry

    lax.fori_loop(0, tiles, project, 0)

    def o_local_copy(b):
        return pltpu.make_async_copy(o_buf.at[b], o_all.at[z, row(b), :], o_local.at[b])

    def o_copy(b, k, step):
        return remote(o_buf.at[b], o_all.at[z, row(b), :], o_send.at[k, b], o_recv.at[z, b], {"tp": jnp.clip(z + step, 0, tp - 1)})

    hops = [(k, step, jnp.logical_and(z + step >= 0, z + step < tp)) for k, step in enumerate((1, -1, 2, -2))]

    def o_start(b):
        o_local_copy(b).start()
        for k, step, ok in hops:
            @pl.when(ok)
            def _(k=k, step=step):
                o_copy(b, k, step).start()

    def o_arrived(src, b):
        remote(o_all.at[src, row(b), :], o_all.at[src, row(b), :], relay_send.at[b], o_recv.at[src, b], partner).wait_recv()

    def relay_copy(b, src, dst):
        return remote(o_all.at[src, row(b), :], o_all.at[src, row(b), :], relay_send.at[b], o_recv.at[src, b], {"tp": dst})

    def relay(b):
        @pl.when(z == tp - 2)
        def _():
            o_arrived(0, b)
            relay_copy(b, 0, tp - 1).start()

        @pl.when(z == 1)
        def _():
            o_arrived(tp - 1, b)
            relay_copy(b, tp - 1, 0).start()

    def far_copy(b, par):
        return remote(g_far.at[par], xin.at[b], far_send.at[par], x_recv.at[b], partner)

    def part_copy(b, par):
        return remote(g_part.at[par], part_in.at[b], part_send.at[par], part_recv.at[b], partner)

    def chip_copy(b):
        par = lax.rem(b, CHIP_BUFS)
        return remote(g_chip.at[par], xin.at[b], chip_send.at[par], x_recv.at[b], peer)

    def chip_sum(b):
        @pl.when(second_chip)
        def _():
            par = lax.rem(b, CHIP_BUFS)
            far_copy(b, 0).wait_recv()
            g_chip[par] = (g_chip[par].astype(F32) + xin[b].astype(F32)).astype(BF16)
            chip_copy(b).start()

    def dkv_store(b, par):
        return pltpu.make_async_copy(dkv_out.at[par], dkv_hbm.at[:, row(b), :], dkv_sem.at[par])

    def key_grads(b):
        par = lax.rem(b, 2)

        @pl.when(first_core)
        def _():
            part_copy(b, 0).wait_recv()

        @pl.when(first_chip)
        def _():
            chip_copy(b).wait_recv()

        @pl.when(b >= 2)
        def _():
            dkv_store(b - 2, par).wait()

        rows = row(b)
        for which in range(2):
            for h in range(heads):
                cols = slice(h * HEAD_DIM, (h + 1) * HEAD_DIM)
                acc = g_own[b, which, :, cols].astype(F32)
                acc = acc + jnp.where(first_core, part_in[b, which, :, cols].astype(F32), 0.0)
                acc = (acc + jnp.where(first_chip, xin[b, which, :, cols].astype(F32), 0.0)).astype(BF16)
                if which == 0:
                    acc = rope(acc.astype(F32), cos_ref[rows, :], sin_ref[rows, :], -1.0).astype(BF16)
                dkv_out[par, which, :, cols] = acc
        dkv_store(b, par).start()

    def dq_store(b, par):
        return pltpu.make_async_copy(dq_buf.at[par], dq_hbm.at[row(b), :], dq_sem.at[par])

    subs = range(0, seq, SUB)

    def attend_row(i, par):
        rows = row(i)
        start = start_ref[i]
        chip_par = lax.rem(i, CHIP_BUFS)
        keys_of = [kv_own.at[par]] + [kvr.at[s, i] for s in range(3)]
        grads = [g_own.at[i], g_part.at[par], g_chip.at[chip_par], g_far.at[par]]
        live = [None, second_core, second_chip, second_chip]
        piece = [r, r + 1 - 2 * core, r + 2 - 4 * chip, r + 3 - 2 * core - 4 * chip]

        def each(body):
            body(0)
            for slot in (1, 2, 3):
                pl.when(live[slot])(functools.partial(body, slot))

        def one_head(h, carry):
            cols = pl.ds(pl.multiple_of(h * HEAD_DIM, HEAD_DIM), HEAD_DIM)
            q = q_all[rows, cols]
            do = do_all[rows, cols]
            m_scr[...] = jnp.full(m_scr.shape, NEG_BIG, F32)
            l_scr[...] = jnp.zeros_like(l_scr)
            d_scr[...] = jnp.zeros_like(d_scr)
            ot_scr[...] = jnp.zeros_like(ot_scr)
            dqt_scr[...] = jnp.zeros_like(dqt_scr)

            def scores(slot):
                base = piece[slot] * seq
                for s in subs:
                    raw = dot_nt(keys_of[slot][0, s:s + SUB, cols], q)
                    local = lax.broadcasted_iota(jnp.int32, raw.shape, 0) + s
                    allowed = (local + base) >= start
                    if slot == 0:
                        allowed = jnp.logical_and(allowed, local <= lax.broadcasted_iota(jnp.int32, raw.shape, 1))
                    raw = jnp.where(allowed, raw, NEG_BIG)
                    s_scr[slot, s:s + SUB, :] = raw
                    m_scr[...] = jnp.maximum(m_scr[...], jnp.max(raw, axis=0, keepdims=True))

            def exps(slot):
                for s in subs:
                    e = jnp.exp2((s_scr[slot, s:s + SUB, :] - m_scr[...]) * EXP2_SCALE)
                    s_scr[slot, s:s + SUB, :] = e
                    l_scr[...] += jnp.sum(e, axis=0, keepdims=True)

            def values(slot):
                for s in subs:
                    v = keys_of[slot][1, s:s + SUB, cols]
                    prob = s_scr[slot, s:s + SUB, :] * l_scr[...]
                    low = prob.astype(BF16)
                    dp = dot_nt(v, do)
                    s_scr[slot, s:s + SUB, :] = prob
                    dp_scr[slot, s:s + SUB, :] = dp
                    d_scr[...] += jnp.sum(prob * dp, axis=0, keepdims=True)
                    grads[slot][1, s:s + SUB, cols] = dot_nn(low, do).astype(BF16)
                    ot_scr[...] += dot_nn(v.T, low)

            def keys(slot):
                for s in subs:
                    k = keys_of[slot][0, s:s + SUB, cols]
                    ds = (s_scr[slot, s:s + SUB, :] * (dp_scr[slot, s:s + SUB, :] - d_scr[...])).astype(BF16)
                    grads[slot][0, s:s + SUB, cols] = (dot_nn(ds, q) * SCALE).astype(BF16)
                    dqt_scr[...] += dot_nn(k.T, ds)

            each(scores)
            each(exps)
            l_scr[...] = 1.0 / l_scr[...]
            each(values)
            each(keys)
            o_buf[i, :, cols] = ot_scr[...].T.astype(BF16)
            dq_buf[par, :, cols] = rope(dqt_scr[...].T * SCALE, cos_ref[rows, :], sin_ref[rows, :], -1.0).astype(BF16)
            return carry

        lax.fori_loop(0, heads, one_head, 0)

    def step(i, carry):
        par = lax.rem(i, 2)
        own_load(i, par).wait()

        @pl.when(i + 1 < batch)
        def _():
            own_load(i + 1, 1 - par).start()

        @pl.when(second_chip)
        def _():
            kv_to_chip(i).wait_recv()
            kv_forward(i).start()

        @pl.when(second_core)
        def _():
            kv_to_partner(i).wait_recv()

        @pl.when(second_chip)
        def _():
            kv_forward(i).wait_recv()

        @pl.when(i >= 2)
        def _():
            dq_store(i - 2, par).wait()

            @pl.when(second_core)
            def _():
                part_copy(i - 2, par).wait_send()

            @pl.when(second_chip)
            def _():
                far_copy(i - 2, par).wait_send()

        @pl.when(jnp.logical_and(second_chip, i >= CHIP_BUFS))
        def _():
            chip_copy(i - CHIP_BUFS).wait_send()

        attend_row(i, par)
        o_start(i)
        dq_store(i, par).start()

        @pl.when(second_chip)
        def _():
            far_copy(i, par).start()

        @pl.when(second_core)
        def _():
            part_copy(i, par).start()

        @pl.when(i >= 1)
        def _():
            chip_sum(i - 1)

        @pl.when(i >= RELAY_LAG)
        def _():
            relay(i - RELAY_LAG)

        return carry

    lax.fori_loop(0, batch, step, 0)
    chip_sum(batch - 1)
    lag = min(RELAY_LAG, batch)
    for k in range(lag):
        relay(batch - lag + k)

    def finish(b, carry):
        key_grads(b)
        return carry

    lax.fori_loop(0, batch, finish, 0)

    for b in range(batch):
        @pl.when(first_chip)
        def _(b=b):
            kv_to_chip(b).wait_send()

        @pl.when(first_core)
        def _(b=b):
            kv_to_partner(b).wait_send()

        @pl.when(second_chip)
        def _(b=b):
            kv_forward(b).wait_send()

        o_local_copy(b).wait()
        for k, step_, ok in hops:
            @pl.when(ok)
            def _(b=b, k=k, step_=step_):
                o_copy(b, k, step_).wait_send()

        @pl.when(jnp.logical_or(z == 1, z == tp - 2))
        def _(b=b):
            relay_copy(b, 0, tp - 1).wait_send()

        for src in range(tp):
            taken = jnp.logical_or(jnp.logical_and(z == tp - 2, src == 0), jnp.logical_and(z == 1, src == tp - 1))

            @pl.when(jnp.logical_and(z != src, jnp.logical_not(taken)))
            def _(b=b, src=src):
                o_arrived(src, b)

    for b in range(max(0, batch - 2), batch):
        dq_store(b, b % 2).wait()
        dkv_store(b, b % 2).wait()

        @pl.when(second_core)
        def _(b=b):
            part_copy(b, b % 2).wait_send()

        @pl.when(second_chip)
        def _(b=b):
            far_copy(b, b % 2).wait_send()

    for b in range(max(0, batch - CHIP_BUFS), batch):
        @pl.when(second_chip)
        def _(b=b):
            chip_copy(b).wait_send()


def front(kv, normed, dy, cos_t, sin_t, start, wq, wo, seq, tp, cp):
    _, tokens, hidden = kv.shape
    d_model = normed.shape[1]
    batch = tokens // seq
    tile = seq // 2
    hbm = pl.BlockSpec(memory_space=pl.ANY)
    vmem = pl.BlockSpec(memory_space=pltpu.VMEM)
    dma = pltpu.SemaphoreType.DMA
    bf = lambda *shape: pltpu.VMEM(shape, BF16)
    f32 = lambda *shape: pltpu.VMEM(shape, F32)
    return pl.pallas_call(
        functools.partial(front_kernel, batch, seq, tp, cp),
        in_specs=[hbm] * 3 + [vmem] * 5,
        out_specs=[hbm] * 3,
        out_shape=[
            jax.ShapeDtypeStruct((tp, tokens, hidden), BF16),
            jax.ShapeDtypeStruct((tokens, hidden), BF16),
            jax.ShapeDtypeStruct((2, tokens, hidden), BF16),
        ],
        scratch_shapes=[
            bf(tokens, hidden), bf(tokens, hidden), bf(2, tile, d_model), bf(2, tile, d_model),
            bf(2, 2, seq, hidden), bf(3, batch, 2, seq, hidden),
            f32(4, seq, seq), f32(4, seq, seq), f32(1, seq), f32(1, seq), f32(1, seq), f32(HEAD_DIM, seq), f32(HEAD_DIM, seq),
            bf(batch, seq, hidden), bf(2, seq, hidden),
            bf(batch, 2, seq, hidden), bf(2, 2, seq, hidden), bf(CHIP_BUFS, 2, seq, hidden), bf(2, 2, seq, hidden),
            bf(batch, 2, seq, hidden), bf(batch, 2, seq, hidden), bf(2, 2, seq, hidden),
            dma((2, 2)), dma((2,)), dma((batch,)), dma((batch,)), dma((batch,)), dma((3, batch)),
            dma((batch,)), dma((4, batch)), dma((tp, batch)), dma((batch,)), dma((2,)),
            dma((2,)), dma((2,)), dma((CHIP_BUFS,)), dma((batch,)), dma((batch,)), dma((2,)),
        ],
        compiler_params=pltpu.CompilerParams(collective_id=1, has_side_effects=True, vmem_limit_bytes=63 << 20),
        cost_estimate=pl.CostEstimate(flops=48 * tokens * seq * hidden, bytes_accessed=16 * tokens * d_model, transcendentals=4 * tokens * seq * (hidden // HEAD_DIM)),
        name="front",
    )(kv, normed, dy, cos_t, sin_t, start, wq, wo)


def back_kernel(groups, rows, tp, cp, dq_hbm, dkv_hbm, x_hbm, dy_hbm, o_hbm, wq_ref, wk_ref, wv_ref, wo_ref, gain_ref,
                gx_hbm, y_hbm, gg_ref, part, rs_r, rs_l, send_r, send_l, tot, gx_buf, dq_in, dkv_in, o_in, x_in, dy_in, y_buf, gain_all,
                in_sem, y_sem, own_sem, rss_r, rss_l, rsr_r, rsr_l, ag0_r, ag0_l, agf_r, agf_l, agr_r, agr_l, gs_sem, gr_sem):
    z = lax.axis_index("tp")
    r = lax.axis_index("cp")
    last = tp - 1
    slots = tp - 1
    span = tp * rows
    d_model = x_hbm.shape[1]
    chunk = min(512, d_model)

    barrier = pltpu.get_barrier_semaphore()
    peers = [(dt, dc) for dt in range(tp) for dc in range(cp) if dt or dc]
    for dt, dc in peers:
        pl.semaphore_signal(barrier, inc=1, device_id={"tp": lax.rem(z + dt, tp), "cp": lax.rem(r + dc, cp)}, device_id_type=MESH)
    pl.semaphore_wait(barrier, len(peers))

    def remote(src, dst, ssem, rsem, dev):
        return pltpu.make_async_remote_copy(src_ref=src, dst_ref=dst, send_sem=ssem, recv_sem=rsem, device_id=dev, device_id_type=MESH)

    def move(dir_right):
        return {"tp": jnp.where(z < last, z + 1, z)} if dir_right else {"tp": jnp.where(z > 0, z - 1, z)}

    right, left = move(True), move(False)

    def group_rows(i):
        return pl.ds(pl.multiple_of(i * span, span), span)

    def tile_rows(i, owner):
        return pl.ds(pl.multiple_of(i * span + owner * rows, rows), rows)

    def inputs(i, slot):
        g = group_rows(i)
        return [
            pltpu.make_async_copy(dq_hbm.at[g, :], dq_in.at[slot], in_sem.at[slot, 0]),
            pltpu.make_async_copy(dkv_hbm.at[:, g, :], dkv_in.at[slot], in_sem.at[slot, 1]),
            pltpu.make_async_copy(o_hbm.at[:, g, :], o_in.at[slot], in_sem.at[slot, 2]),
            pltpu.make_async_copy(x_hbm.at[g, :], x_in.at[slot], in_sem.at[slot, 3]),
            pltpu.make_async_copy(dy_hbm.at[tile_rows(i, z), :], dy_in.at[slot], in_sem.at[slot, 4]),
        ]

    def y_copy(i, slot):
        return pltpu.make_async_copy(y_buf.at[slot], y_hbm.at[group_rows(i), :], y_sem.at[slot])

    def rs_copy(i, s, to_right):
        if to_right:
            return remote(send_r.at[s], rs_r.at[i, s], rss_r.at[s], rsr_r.at[i, s], right)
        return remote(send_l.at[s], rs_l.at[i, s], rss_l.at[s], rsr_l.at[i, s], left)

    def rs_send(i, cur, s):
        for to_right in (True, False):
            far = z if to_right else last - z
            owner = (z + slots - s) if to_right else (z - slots + s)
            buf, held = (send_r, rs_r) if to_right else (send_l, rs_l)

            @pl.when(jnp.logical_and(i < groups, jnp.logical_and(far <= s, far < last)))
            def _(to_right=to_right, far=far, owner=owner, buf=buf, held=held):
                @pl.when(i > 0)
                def _():
                    rs_copy(i - 1, s, to_right).wait_send()

                mine = pl.ds(pl.multiple_of(owner * rows, rows), rows)
                if s == 0:
                    buf[s] = part[cur, mine, :].astype(BF16)
                else:
                    @pl.when(far == 0)
                    def _():
                        buf[s] = part[cur, mine, :].astype(BF16)

                    @pl.when(far > 0)
                    def _():
                        rs_copy(i, s - 1, to_right).wait_recv()
                        buf[s] = (part[cur, mine, :] + held[i, s - 1].astype(F32)).astype(BF16)

                rs_copy(i, s, to_right).start()

    def ag_own(i, slot, to_right):
        src = gx_buf.at[slot]
        dst = gx_hbm.at[tile_rows(i, z), :]
        if to_right:
            return remote(src, dst, ag0_r.at[slot], agr_r.at[i, 0], right)
        return remote(src, dst, ag0_l.at[slot], agr_l.at[i, 0], left)

    def own_copy(i, slot):
        return pltpu.make_async_copy(gx_buf.at[slot], gx_hbm.at[tile_rows(i, z), :], own_sem.at[slot])

    def ag_forward(i, a, to_right):
        owner = z - a if to_right else z + a
        tile = gx_hbm.at[tile_rows(i, owner), :]
        if to_right:
            return remote(tile, tile, agf_r.at[a], agr_r.at[i, a], right)
        return remote(tile, tile, agf_l.at[a], agr_l.at[i, a], left)

    def ag_wait(i, a, to_right):
        tile = gx_hbm.at[tile_rows(i, 0), :]
        sem = agr_r.at[i, a] if to_right else agr_l.at[i, a]
        remote(tile, tile, agf_r.at[a], sem, right).wait_recv()

    def ag_step(i, a):
        for to_right in (True, False):
            far = z if to_right else last - z

            @pl.when(jnp.logical_and(jnp.logical_and(i >= 0, i < groups), far >= a))
            def _(to_right=to_right, far=far):
                ag_wait(i, a - 1, to_right)
                if a < slots:
                    @pl.when(far < last)
                    def _():
                        @pl.when(i > 0)
                        def _():
                            ag_forward(i - 1, a, to_right).wait_send()

                        ag_forward(i, a, to_right).start()

    def ag_first(i, slot):
        own_copy(i, slot).start()
        for to_right in (True, False):
            far = z if to_right else last - z

            @pl.when(far < last)
            def _(to_right=to_right):
                ag_own(i, slot, to_right).start()

    def ag_first_done(i, slot):
        own_copy(i, slot).wait()
        for to_right in (True, False):
            far = z if to_right else last - z

            @pl.when(far < last)
            def _(to_right=to_right):
                ag_own(i, slot, to_right).wait_send()

    def partial_norm(cur):
        for c in range(0, d_model, chunk):
            cols = slice(c, c + chunk)
            part[cur, :, cols] = (
                dot_nt(dq_in[cur], wq_ref[cols, :]) + dot_nt(dkv_in[cur, 0], wk_ref[cols, :]) + dot_nt(dkv_in[cur, 1], wv_ref[cols, :])
            )

    def project_out(cur, lo, hi):
        for c in range(lo, hi, chunk):
            cols = slice(c, c + chunk)
            shares, share = wo_ref.shape[0], wo_ref.shape[2]
            acc = x_in[cur, :, cols].astype(F32)
            for t in range(tp):
                for g in range(shares):
                    acc += dot_nn(o_in[cur, t, :, g * share:(g + 1) * share], wo_ref[g, t, :, cols])
            y_buf[cur, :, cols] = acc.astype(BF16)

    def finalize(i, slot):
        mine = pl.ds(pl.multiple_of(z * rows, rows), rows)
        tot[...] = part[slot, mine, :]

        @pl.when(z > 0)
        def _():
            rs_copy(i, slots - 1, True).wait_recv()
            tot[...] += rs_r[i, slots - 1].astype(F32)

        @pl.when(z < last)
        def _():
            rs_copy(i, slots - 1, False).wait_recv()
            tot[...] += rs_l[i, slots - 1].astype(F32)

        @pl.when(i > 1)
        def _():
            ag_first_done(i - 2, slot)

        x = x_in[slot, mine, :].astype(F32)
        centred = x - jnp.mean(x, axis=-1, keepdims=True)
        inv_std = lax.rsqrt(jnp.mean(centred * centred, axis=-1, keepdims=True) + LN_EPS)
        x_hat = centred * inv_std
        dn = tot[...]
        gg_ref[...] += jnp.sum(dn * x_hat, axis=0, keepdims=True)
        d_hat = dn * gain_ref[...]
        dx = inv_std * (d_hat - jnp.mean(d_hat, axis=-1, keepdims=True) - x_hat * jnp.mean(d_hat * x_hat, axis=-1, keepdims=True))
        gx_buf[slot] = (dy_in[slot].astype(F32) + dx).astype(BF16)

    gg_ref[...] = jnp.zeros_like(gg_ref)
    for copy in inputs(0, 0):
        copy.start()

    me = z * cp + r

    def gain_copy(dt, dc):
        to = {"tp": lax.rem(z + dt, tp), "cp": lax.rem(r + dc, cp)}
        return remote(gain_all.at[me], gain_all.at[me], gs_sem.at[dt * cp + dc], gr_sem.at[me], to)

    def gain_wait(dt, dc):
        sender = lax.rem(z + dt, tp) * cp + lax.rem(r + dc, cp)
        remote(gain_all.at[sender], gain_all.at[sender], gs_sem.at[0], gr_sem.at[sender], right).wait_recv()

    def step(i, carry):
        cur = lax.rem(i, 2)
        prv = 1 - cur

        @pl.when(i < groups)
        def _():
            for copy in inputs(i, cur):
                copy.wait()
            partial_norm(cur)

        rs_send(i, cur, 0)
        ag_step(i - 2, 1)

        @pl.when(jnp.logical_and(i >= 1, i <= groups))
        def _():
            finalize(i - 1, prv)

        @pl.when(i + 1 < groups)
        def _():
            for copy in inputs(i + 1, prv):
                copy.start()

        @pl.when(jnp.logical_and(i >= 2, i < groups))
        def _():
            y_copy(i - 2, cur).wait()

        @pl.when(i < groups)
        def _():
            project_out(cur, 0, d_model // 2)

        rs_send(i, cur, 1)
        ag_step(i - 2, 2)

        @pl.when(i < groups)
        def _():
            project_out(cur, d_model // 2, d_model)
            y_copy(i, cur).start()

        rs_send(i, cur, 2)

        @pl.when(jnp.logical_and(i >= 1, i <= groups))
        def _():
            ag_first(i - 1, prv)

        @pl.when(i == groups)
        def _():
            gain_all[me] = gg_ref[...]
            for dt, dc in peers:
                gain_copy(dt, dc).start()

        ag_step(i - 2, 3)
        return carry

    lax.fori_loop(0, groups + 2, step, 0)

    for i in (groups - 2, groups - 1):
        y_copy(i, i % 2).wait()
        ag_first_done(i, i % 2)
    for to_right in (True, False):
        far = z if to_right else last - z
        for s in range(slots):
            @pl.when(jnp.logical_and(far <= s, far < last))
            def _(s=s, to_right=to_right):
                rs_copy(groups - 1, s, to_right).wait_send()
        for a in range(1, slots):
            @pl.when(jnp.logical_and(far >= a, far < last))
            def _(a=a, to_right=to_right):
                ag_forward(groups - 1, a, to_right).wait_send()
    for dt, dc in peers:
        gain_wait(dt, dc)
        gain_copy(dt, dc).wait_send()
    total = gain_all[0]
    for j in range(1, tp * cp):
        total += gain_all[j]
    gg_ref[...] = total


def backward_norm(dq, dkv, x, dy, o_all, wq, wk, wv, wo_all, gain, rows, tp, cp):
    tokens, hidden = dq.shape
    d_model = x.shape[1]
    span = tp * rows
    groups = tokens // span
    slots = tp - 1
    hbm = pl.BlockSpec(memory_space=pl.ANY)
    vmem = pl.BlockSpec(memory_space=pltpu.VMEM)
    dma = pltpu.SemaphoreType.DMA
    return pl.pallas_call(
        functools.partial(back_kernel, groups, rows, tp, cp),
        in_specs=[hbm] * 5 + [vmem] * 5,
        out_specs=[hbm, hbm, vmem],
        out_shape=[
            jax.ShapeDtypeStruct((tokens, d_model), BF16),
            jax.ShapeDtypeStruct((tokens, d_model), BF16),
            jax.ShapeDtypeStruct((1, d_model), F32),
        ],
        scratch_shapes=[
            pltpu.VMEM((2, span, d_model), F32),
            pltpu.VMEM((groups, slots, rows, d_model), BF16),
            pltpu.VMEM((groups, slots, rows, d_model), BF16),
            pltpu.VMEM((slots, rows, d_model), BF16),
            pltpu.VMEM((slots, rows, d_model), BF16),
            pltpu.VMEM((rows, d_model), F32),
            pltpu.VMEM((2, rows, d_model), BF16),
            pltpu.VMEM((2, span, hidden), BF16),
            pltpu.VMEM((2, 2, span, hidden), BF16),
            pltpu.VMEM((2, tp, span, hidden), BF16),
            pltpu.VMEM((2, span, d_model), BF16),
            pltpu.VMEM((2, rows, d_model), BF16),
            pltpu.VMEM((2, span, d_model), BF16),
            pltpu.VMEM((tp * cp, 1, d_model), F32),
            dma((2, 5)),
            dma((2,)),
            dma((2,)),
            dma((slots,)),
            dma((slots,)),
            dma((groups, slots)),
            dma((groups, slots)),
            dma((2,)),
            dma((2,)),
            dma((slots,)),
            dma((slots,)),
            dma((groups, slots)),
            dma((groups, slots)),
            dma((tp * cp,)),
            dma((tp * cp,)),
        ],
        compiler_params=pltpu.CompilerParams(collective_id=0, has_side_effects=True, vmem_limit_bytes=60 << 20),
        cost_estimate=pl.CostEstimate(flops=14 * tokens * hidden * d_model, bytes_accessed=16 * tokens * d_model, transcendentals=0),
        name="backward_norm",
    )(dq, dkv, x, dy, o_all, wq, wk, wv, wo_all, gain)

def solution(mesh):
    cp_size = mesh.shape["cp"]
    tp_size = mesh.shape["tp"]
    dp_size = mesh.shape["dp"]

    def device_step(x_in, segment_ids, positions, w_query, w_key, w_value, w_out, norm_gain, grad_out):
        batch, seq, d_model = x_in.shape
        hidden = w_query.shape[1]
        tokens = batch * seq
        rank = lax.axis_index("cp")
        core = rank % 2
        x = x_in.reshape(tokens, d_model)
        dy = grad_out.reshape(tokens, d_model)

        inv_freq = ROPE_THETA ** (-jnp.arange(0, HEAD_DIM, 2).astype(F32) / HEAD_DIM)
        angles = positions.reshape(tokens, 1).astype(F32) * jnp.repeat(inv_freq, 2)[None, :]
        cos_t, sin_t = jnp.cos(angles), jnp.sin(angles)
        start = (rank * seq + jnp.arange(seq, dtype=jnp.int32))[None, :] - positions

        share = w_out.shape[0] // (cp_size * dp_size)
        mine = (lax.axis_index("dp") * cp_size + rank) * share
        w_all = lax.all_gather(lax.dynamic_slice(w_out, (mine, 0), (share, d_model)), ("dp", "tp", "cp"), axis=0)
        w_all = w_all.reshape(dp_size, tp_size, cp_size * share, d_model)

        rows = min(384, tokens)
        normed, kv = project_keys(x, cos_t, sin_t, norm_gain.reshape(1, d_model), w_key, w_value, rows)
        o_all, dq, dkv = front(kv, normed, dy, cos_t, sin_t, start.reshape(batch, 1, seq), w_query, w_out, seq, tp_size, cp_size)
        grad_x, y_out, grad_gain = backward_norm(dq, dkv, x, dy, o_all, w_query, w_key, w_value, w_all, norm_gain.reshape(1, d_model), ROWS, tp_size, cp_size)
        grad_gain = grad_gain.reshape(d_model)

        def perm(value, pairs):
            return lax.ppermute(value, "cp", pairs)

        def tn(a, b):
            return lax.dot_general(a, b, (((0,), (0,)), ((), ())), preferred_element_type=F32)

        def reduce_cp(part):
            half = part.shape[0] // 2
            away = lax.dynamic_slice(part, ((1 - core) * half, 0), (half, part.shape[1]))
            mine = lax.dynamic_slice(part, (core * half, 0), (half, part.shape[1]))
            mine = (mine + perm(away, [(0, 1), (1, 0), (2, 3), (3, 2)])).astype(BF16)
            other = perm(mine, [(0, 2), (2, 0), (1, 3), (3, 1)])
            total = mine.astype(F32) + other.astype(F32)
            rest = perm(total, [(0, 1), (1, 0), (2, 3), (3, 2)])
            return jnp.where(core == 0, jnp.concatenate([total, rest]), jnp.concatenate([rest, total]))

        o = lax.dynamic_index_in_dim(o_all, lax.axis_index("tp"), 0, keepdims=False)
        grad_wo = reduce_cp(tn(o, dy))
        grad_wq = reduce_cp(tn(normed, dq))
        grad_wk = reduce_cp(tn(normed, dkv[0]))
        grad_wv = reduce_cp(tn(normed, dkv[1]))
        return y_out.reshape(x_in.shape), grad_x.reshape(x_in.shape), grad_gain, grad_wq, grad_wk, grad_wv, grad_wo

    in_specs = (P("dp", "cp", None), P("dp", "cp"), P("dp", "cp"), P(None, "tp"), P(None, "tp"), P(None, "tp"), P("tp", None), P(None), P("dp", "cp", None))
    out_specs = (P("dp", "cp", None), P("dp", "cp", None), P("dp"), P("dp", "tp"), P("dp", "tp"), P("dp", "tp"), P(("dp", "tp"), None))
    return jax.shard_map(device_step, mesh=mesh, in_specs=in_specs, out_specs=out_specs, check_vma=False)
```

```python
import functools
import math

import jax
import jax.numpy as jnp
from jax import lax
from jax.experimental import pallas as pl
from jax.experimental.pallas import tpu as pltpu
from jax.sharding import PartitionSpec as P

HEAD_DIM = 128
ROPE_THETA = 8000000.0
LN_EPS = 1e-5
NEG_BIG = -1e30
SCALE = HEAD_DIM ** -0.5
EXP2_SCALE = SCALE * math.log2(math.e)
F32 = jnp.float32
BF16 = jnp.bfloat16
NT = (((1,), (1,)), ((), ()))


def dot_nn(a, b):
    return jnp.dot(a, b, preferred_element_type=F32)


def dot_nt(a, b):
    return lax.dot_general(a, b, NT, preferred_element_type=F32)


def dot_tn(a, b):
    return lax.dot_general(a, b, (((0,), (0,)), ((), ())), preferred_element_type=F32)


def swap_pairs(t, sign):
    lane = lax.broadcasted_iota(jnp.int32, t.shape, 1)
    even = (lane % 2) == 0
    up = pltpu.roll(t, HEAD_DIM - 1, 1)
    down = pltpu.roll(t, 1, 1)
    return jnp.where(even, -up, down) if sign > 0 else jnp.where(even, up, -down)


def rope(t, cos_t, sin_t, sign):
    return t * cos_t + swap_pairs(t, sign) * sin_t


def put_rope(dst, raw, cos_t, sin_t):
    for h in range(raw.shape[1] // HEAD_DIM):
        cols = slice(h * HEAD_DIM, (h + 1) * HEAD_DIM)
        dst[:, cols] = rope(raw[:, cols], cos_t, sin_t, 1.0).astype(BF16)


def keys_kernel(x_ref, cos_ref, sin_ref, gain_ref, wk_ref, wv_ref, n_ref, kv_ref):
    x = x_ref[...].astype(F32)
    centred = x - jnp.mean(x, axis=-1, keepdims=True)
    inv_std = lax.rsqrt(jnp.mean(centred * centred, axis=-1, keepdims=True) + LN_EPS)
    normed = ((centred * inv_std) * gain_ref[...]).astype(BF16)
    n_ref[...] = normed
    put_rope(kv_ref.at[0], dot_nn(normed, wk_ref[...]), cos_ref[...], sin_ref[...])
    kv_ref[1] = dot_nn(normed, wv_ref[...]).astype(BF16)


def project_keys(x, cos_t, sin_t, gain, wk, wv, rows):
    tokens, d_model = x.shape
    hidden = wk.shape[1]
    whole = pl.BlockSpec(memory_space=pltpu.VMEM)
    tile = lambda width: pl.BlockSpec((rows, width), lambda i: (i, 0))
    return pl.pallas_call(
        keys_kernel,
        grid=(tokens // rows,),
        in_specs=[tile(d_model), tile(HEAD_DIM), tile(HEAD_DIM), whole, whole, whole],
        out_specs=[tile(d_model), pl.BlockSpec((2, rows, hidden), lambda i: (0, i, 0))],
        out_shape=[jax.ShapeDtypeStruct((tokens, d_model), BF16), jax.ShapeDtypeStruct((2, tokens, hidden), BF16)],
        compiler_params=pltpu.CompilerParams(dimension_semantics=("arbitrary",), vmem_limit_bytes=48 << 20),
        cost_estimate=pl.CostEstimate(flops=4 * tokens * d_model * hidden, bytes_accessed=4 * tokens * (d_model + hidden), transcendentals=0),
        name="project_keys",
    )(x, cos_t, sin_t, gain, wk, wv)


MESH = pl.DeviceIdType.MESH
SUB = 128
ROWS = 48
WIDTH = 256
RELAY_LAG = 2
CHIP_BUFS = 3


def front_kernel(batch, seq, tp, cp, kv_hbm, n_hbm, dy_hbm, cos_ref, sin_ref, start_ref, wq_ref, wo_ref,
                 o_all, dq_hbm, dkv_hbm,
                 q_all, do_all, n_in, dy_in, kv_own, kvr, s_scr, dp_scr, m_scr, l_scr, d_scr, ot_scr, dqt_scr,
                 o_buf, dq_buf, g_own, g_part, g_chip, g_far, xin, part_in, dkv_out,
                 tile_sem, own_sem, kvs_part, kvs_chip, kvs_far, kv_recv, o_local, o_send, o_recv, relay_send, dq_sem,
                 far_send, part_send, chip_send, x_recv, part_recv, dkv_sem):
    z = lax.axis_index("tp")
    r = lax.axis_index("cp")
    core = lax.rem(r, 2)
    chip = lax.div(r, 2)
    hidden = q_all.shape[1]
    heads = hidden // HEAD_DIM
    first_chip, second_chip = chip == 0, chip == 1
    first_core, second_core = core == 0, core == 1
    partner = {"cp": r + 1 - 2 * core}
    peer = {"cp": r + 2 - 4 * chip}

    barrier = pltpu.get_barrier_semaphore()
    for dev in [partner, peer] + [{"tp": lax.rem(z + dt, tp)} for dt in range(1, tp)]:
        pl.semaphore_signal(barrier, inc=1, device_id=dev, device_id_type=MESH)
    pl.semaphore_wait(barrier, tp + 1)

    def remote(src, dst, ssem, rsem, dev):
        return pltpu.make_async_remote_copy(src_ref=src, dst_ref=dst, send_sem=ssem, recv_sem=rsem, device_id=dev, device_id_type=MESH)

    def row(b):
        return pl.ds(pl.multiple_of(b * seq, seq), seq)

    def kv_to_partner(b):
        return remote(kv_hbm.at[:, row(b), :], kvr.at[0, b], kvs_part.at[b], kv_recv.at[0, b], partner)

    def kv_to_chip(b):
        return remote(kv_hbm.at[:, row(b), :], kvr.at[1, b], kvs_chip.at[b], kv_recv.at[1, b], peer)

    def kv_forward(b):
        return remote(kvr.at[1, b], kvr.at[2, b], kvs_far.at[b], kv_recv.at[2, b], partner)

    for b in range(batch):
        @pl.when(first_chip)
        def _(b=b):
            kv_to_chip(b).start()

        @pl.when(first_core)
        def _(b=b):
            kv_to_partner(b).start()

    def own_load(b, par):
        return pltpu.make_async_copy(kv_hbm.at[:, row(b), :], kv_own.at[par], own_sem.at[par])

    own_load(0, 0).start()

    tile = n_in.shape[1]
    tiles = batch * seq // tile

    def tile_rows(t):
        return pl.ds(pl.multiple_of(t * tile, tile), tile)

    def tile_loads(t, par):
        return [
            pltpu.make_async_copy(n_hbm.at[tile_rows(t), :], n_in.at[par], tile_sem.at[par, 0]),
            pltpu.make_async_copy(dy_hbm.at[tile_rows(t), :], dy_in.at[par], tile_sem.at[par, 1]),
        ]

    for copy in tile_loads(0, 0):
        copy.start()

    def project(t, carry):
        par = lax.rem(t, 2)
        for copy in tile_loads(t, par):
            copy.wait()

        @pl.when(t + 1 < tiles)
        def _():
            for copy in tile_loads(t + 1, 1 - par):
                copy.start()

        rows = tile_rows(t)
        put_rope(q_all.at[rows, :], dot_nn(n_in[par], wq_ref[...]), cos_ref[rows, :], sin_ref[rows, :])
        do_all[rows, :] = dot_nt(dy_in[par], wo_ref[...]).astype(BF16)
        return carry

    lax.fori_loop(0, tiles, project, 0)

    def o_local_copy(b):
        return pltpu.make_async_copy(o_buf.at[b], o_all.at[z, row(b), :], o_local.at[b])

    def o_copy(b, k, step):
        return remote(o_buf.at[b], o_all.at[z, row(b), :], o_send.at[k, b], o_recv.at[z, b], {"tp": jnp.clip(z + step, 0, tp - 1)})

    hops = [(k, step, jnp.logical_and(z + step >= 0, z + step < tp)) for k, step in enumerate((1, -1, 2, -2))]

    def o_start(b):
        o_local_copy(b).start()
        for k, step, ok in hops:
            @pl.when(ok)
            def _(k=k, step=step):
                o_copy(b, k, step).start()

    def o_arrived(src, b):
        remote(o_all.at[src, row(b), :], o_all.at[src, row(b), :], relay_send.at[b], o_recv.at[src, b], partner).wait_recv()

    def relay_copy(b, src, dst):
        return remote(o_all.at[src, row(b), :], o_all.at[src, row(b), :], relay_send.at[b], o_recv.at[src, b], {"tp": dst})

    def relay(b):
        @pl.when(z == tp - 2)
        def _():
            o_arrived(0, b)
            relay_copy(b, 0, tp - 1).start()

        @pl.when(z == 1)
        def _():
            o_arrived(tp - 1, b)
            relay_copy(b, tp - 1, 0).start()

    def far_copy(b, par):
        return remote(g_far.at[par], xin.at[b], far_send.at[par], x_recv.at[b], partner)

    def part_copy(b, par):
        return remote(g_part.at[par], part_in.at[b], part_send.at[par], part_recv.at[b], partner)

    def chip_copy(b):
        par = lax.rem(b, CHIP_BUFS)
        return remote(g_chip.at[par], xin.at[b], chip_send.at[par], x_recv.at[b], peer)

    def chip_sum(b):
        @pl.when(second_chip)
        def _():
            par = lax.rem(b, CHIP_BUFS)
            far_copy(b, 0).wait_recv()
            g_chip[par] = (g_chip[par].astype(F32) + xin[b].astype(F32)).astype(BF16)
            chip_copy(b).start()

    def dkv_store(b, par):
        return pltpu.make_async_copy(dkv_out.at[par], dkv_hbm.at[:, row(b), :], dkv_sem.at[par])

    def key_grads(b):
        par = lax.rem(b, 2)

        @pl.when(first_core)
        def _():
            part_copy(b, 0).wait_recv()

        @pl.when(first_chip)
        def _():
            chip_copy(b).wait_recv()

        @pl.when(b >= 2)
        def _():
            dkv_store(b - 2, par).wait()

        rows = row(b)
        for which in range(2):
            for h in range(heads):
                cols = slice(h * HEAD_DIM, (h + 1) * HEAD_DIM)
                acc = g_own[b, which, :, cols].astype(F32)
                acc = acc + jnp.where(first_core, part_in[b, which, :, cols].astype(F32), 0.0)
                acc = (acc + jnp.where(first_chip, xin[b, which, :, cols].astype(F32), 0.0)).astype(BF16)
                if which == 0:
                    acc = rope(acc.astype(F32), cos_ref[rows, :], sin_ref[rows, :], -1.0).astype(BF16)
                dkv_out[par, which, :, cols] = acc
        dkv_store(b, par).start()

    def dq_store(b, par):
        return pltpu.make_async_copy(dq_buf.at[par], dq_hbm.at[row(b), :], dq_sem.at[par])

    subs = range(0, seq, SUB)

    def attend_row(i, par):
        rows = row(i)
        start = start_ref[i]
        chip_par = lax.rem(i, CHIP_BUFS)
        keys_of = [kv_own.at[par]] + [kvr.at[s, i] for s in range(3)]
        grads = [g_own.at[i], g_part.at[par], g_chip.at[chip_par], g_far.at[par]]
        live = [None, second_core, second_chip, second_chip]
        piece = [r, r + 1 - 2 * core, r + 2 - 4 * chip, r + 3 - 2 * core - 4 * chip]

        def each(body):
            body(0)
            for slot in (1, 2, 3):
                pl.when(live[slot])(functools.partial(body, slot))

        def one_head(h, carry):
            cols = pl.ds(pl.multiple_of(h * HEAD_DIM, HEAD_DIM), HEAD_DIM)
            q = q_all[rows, cols]
            do = do_all[rows, cols]
            m_scr[...] = jnp.full(m_scr.shape, NEG_BIG, F32)
            l_scr[...] = jnp.zeros_like(l_scr)
            d_scr[...] = jnp.zeros_like(d_scr)
            ot_scr[...] = jnp.zeros_like(ot_scr)
            dqt_scr[...] = jnp.zeros_like(dqt_scr)

            def scores(slot):
                base = piece[slot] * seq
                for s in subs:
                    raw = dot_nt(keys_of[slot][0, s:s + SUB, cols], q)
                    local = lax.broadcasted_iota(jnp.int32, raw.shape, 0) + s
                    allowed = (local + base) >= start
                    if slot == 0:
                        allowed = jnp.logical_and(allowed, local <= lax.broadcasted_iota(jnp.int32, raw.shape, 1))
                    raw = jnp.where(allowed, raw, NEG_BIG)
                    s_scr[slot, s:s + SUB, :] = raw
                    m_scr[...] = jnp.maximum(m_scr[...], jnp.max(raw, axis=0, keepdims=True))

            def exps(slot):
                for s in subs:
                    e = jnp.exp2((s_scr[slot, s:s + SUB, :] - m_scr[...]) * EXP2_SCALE)
                    s_scr[slot, s:s + SUB, :] = e
                    l_scr[...] += jnp.sum(e, axis=0, keepdims=True)

            def values(slot):
                for s in subs:
                    v = keys_of[slot][1, s:s + SUB, cols]
                    prob = s_scr[slot, s:s + SUB, :] * l_scr[...]
                    low = prob.astype(BF16)
                    dp = dot_nt(v, do)
                    s_scr[slot, s:s + SUB, :] = prob
                    dp_scr[slot, s:s + SUB, :] = dp
                    d_scr[...] += jnp.sum(prob * dp, axis=0, keepdims=True)
                    grads[slot][1, s:s + SUB, cols] = dot_nn(low, do).astype(BF16)
                    ot_scr[...] += dot_nn(v.T, low)

            def keys(slot):
                for s in subs:
                    k = keys_of[slot][0, s:s + SUB, cols]
                    ds = (s_scr[slot, s:s + SUB, :] * (dp_scr[slot, s:s + SUB, :] - d_scr[...])).astype(BF16)
                    grads[slot][0, s:s + SUB, cols] = (dot_nn(ds, q) * SCALE).astype(BF16)
                    dqt_scr[...] += dot_nn(k.T, ds)

            each(scores)
            each(exps)
            l_scr[...] = 1.0 / l_scr[...]
            each(values)
            each(keys)
            o_buf[i, :, cols] = ot_scr[...].T.astype(BF16)
            dq_buf[par, :, cols] = rope(dqt_scr[...].T * SCALE, cos_ref[rows, :], sin_ref[rows, :], -1.0).astype(BF16)
            return carry

        lax.fori_loop(0, heads, one_head, 0)

    def step(i, carry):
        par = lax.rem(i, 2)
        own_load(i, par).wait()

        @pl.when(i + 1 < batch)
        def _():
            own_load(i + 1, 1 - par).start()

        @pl.when(second_chip)
        def _():
            kv_to_chip(i).wait_recv()
            kv_forward(i).start()

        @pl.when(second_core)
        def _():
            kv_to_partner(i).wait_recv()

        @pl.when(second_chip)
        def _():
            kv_forward(i).wait_recv()

        @pl.when(i >= 2)
        def _():
            dq_store(i - 2, par).wait()

            @pl.when(second_core)
            def _():
                part_copy(i - 2, par).wait_send()

            @pl.when(second_chip)
            def _():
                far_copy(i - 2, par).wait_send()

        @pl.when(jnp.logical_and(second_chip, i >= CHIP_BUFS))
        def _():
            chip_copy(i - CHIP_BUFS).wait_send()

        attend_row(i, par)
        o_start(i)
        dq_store(i, par).start()

        @pl.when(second_chip)
        def _():
            far_copy(i, par).start()

        @pl.when(second_core)
        def _():
            part_copy(i, par).start()

        @pl.when(i >= 1)
        def _():
            chip_sum(i - 1)

        @pl.when(i >= RELAY_LAG)
        def _():
            relay(i - RELAY_LAG)

        return carry

    lax.fori_loop(0, batch, step, 0)
    chip_sum(batch - 1)
    lag = min(RELAY_LAG, batch)
    for k in range(lag):
        relay(batch - lag + k)

    def finish(b, carry):
        key_grads(b)
        return carry

    lax.fori_loop(0, batch, finish, 0)

    for b in range(batch):
        @pl.when(first_chip)
        def _(b=b):
            kv_to_chip(b).wait_send()

        @pl.when(first_core)
        def _(b=b):
            kv_to_partner(b).wait_send()

        @pl.when(second_chip)
        def _(b=b):
            kv_forward(b).wait_send()

        o_local_copy(b).wait()
        for k, step_, ok in hops:
            @pl.when(ok)
            def _(b=b, k=k, step_=step_):
                o_copy(b, k, step_).wait_send()

        @pl.when(jnp.logical_or(z == 1, z == tp - 2))
        def _(b=b):
            relay_copy(b, 0, tp - 1).wait_send()

        for src in range(tp):
            taken = jnp.logical_or(jnp.logical_and(z == tp - 2, src == 0), jnp.logical_and(z == 1, src == tp - 1))

            @pl.when(jnp.logical_and(z != src, jnp.logical_not(taken)))
            def _(b=b, src=src):
                o_arrived(src, b)

    for b in range(max(0, batch - 2), batch):
        dq_store(b, b % 2).wait()
        dkv_store(b, b % 2).wait()

        @pl.when(second_core)
        def _(b=b):
            part_copy(b, b % 2).wait_send()

        @pl.when(second_chip)
        def _(b=b):
            far_copy(b, b % 2).wait_send()

    for b in range(max(0, batch - CHIP_BUFS), batch):
        @pl.when(second_chip)
        def _(b=b):
            chip_copy(b).wait_send()


def front(kv, normed, dy, cos_t, sin_t, start, wq, wo, seq, tp, cp):
    _, tokens, hidden = kv.shape
    d_model = normed.shape[1]
    batch = tokens // seq
    tile = seq // 2
    hbm = pl.BlockSpec(memory_space=pl.ANY)
    vmem = pl.BlockSpec(memory_space=pltpu.VMEM)
    dma = pltpu.SemaphoreType.DMA
    bf = lambda *shape: pltpu.VMEM(shape, BF16)
    f32 = lambda *shape: pltpu.VMEM(shape, F32)
    return pl.pallas_call(
        functools.partial(front_kernel, batch, seq, tp, cp),
        in_specs=[hbm] * 3 + [vmem] * 5,
        out_specs=[hbm] * 3,
        out_shape=[
            jax.ShapeDtypeStruct((tp, tokens, hidden), BF16),
            jax.ShapeDtypeStruct((tokens, hidden), BF16),
            jax.ShapeDtypeStruct((2, tokens, hidden), BF16),
        ],
        scratch_shapes=[
            bf(tokens, hidden), bf(tokens, hidden), bf(2, tile, d_model), bf(2, tile, d_model),
            bf(2, 2, seq, hidden), bf(3, batch, 2, seq, hidden),
            f32(4, seq, seq), f32(4, seq, seq), f32(1, seq), f32(1, seq), f32(1, seq), f32(HEAD_DIM, seq), f32(HEAD_DIM, seq),
            bf(batch, seq, hidden), bf(2, seq, hidden),
            bf(batch, 2, seq, hidden), bf(2, 2, seq, hidden), bf(CHIP_BUFS, 2, seq, hidden), bf(2, 2, seq, hidden),
            bf(batch, 2, seq, hidden), bf(batch, 2, seq, hidden), bf(2, 2, seq, hidden),
            dma((2, 2)), dma((2,)), dma((batch,)), dma((batch,)), dma((batch,)), dma((3, batch)),
            dma((batch,)), dma((4, batch)), dma((tp, batch)), dma((batch,)), dma((2,)),
            dma((2,)), dma((2,)), dma((CHIP_BUFS,)), dma((batch,)), dma((batch,)), dma((2,)),
        ],
        compiler_params=pltpu.CompilerParams(collective_id=1, has_side_effects=True, vmem_limit_bytes=63 << 20),
        cost_estimate=pl.CostEstimate(flops=48 * tokens * seq * hidden, bytes_accessed=16 * tokens * d_model, transcendentals=4 * tokens * seq * (hidden // HEAD_DIM)),
        name="front",
    )(kv, normed, dy, cos_t, sin_t, start, wq, wo)


PART_RING = 4
RS_RING = 5


def back_kernel(groups, rows, tp, cp, dq_hbm, dkv_hbm, x_hbm, dy_hbm, o_hbm, n_hbm, wq_hbm, wk_hbm, wv_hbm, wo_hbm, gain_ref,
                gx_hbm, y_hbm, ga_hbm, gb_hbm, gg_ref,
                wq_ref, wk_ref, wv_ref, wo_ref, dq_all, dkv_all, o_t, part, rs_r, rs_l, send_r, send_l, tot, gx_buf,
                o_in, x_in, xo_in, dyo_in, y_buf, n_in, dy_in, away, part_in, mine, gain_all,
                w_sem, in_sem, fin_sem, job_sem, y_sem, own_sem, rss_r, rss_l, rsr_r, rsr_l, ag0_r, ag0_l, agf_r, agf_l, agr_r, agr_l,
                away_send, away_recv, mine_own, mine_part, mine_chip, ga_recv, chip_recv, gb_send, gb_recv, gs_sem, gr_sem):
    z = lax.axis_index("tp")
    r = lax.axis_index("cp")
    core = lax.rem(r, 2)
    chip = lax.div(r, 2)
    last = tp - 1
    slots = tp - 1
    span = tp * rows
    tokens, d_model = x_hbm.shape
    hidden = dq_hbm.shape[1]
    chunk = min(512, d_model)
    blocks = ga_hbm.shape[0]
    width = ga_hbm.shape[1]
    pairs = blocks // 2
    partner = {"cp": r + 1 - 2 * core}
    peer = {"cp": r + 2 - 4 * chip}

    shares, share = wo_hbm.shape[0], wo_hbm.shape[2]
    weight_loads = [pltpu.make_async_copy(src, dst, w_sem.at[k]) for k, (src, dst) in enumerate(((wq_hbm, wq_ref), (wk_hbm, wk_ref), (wv_hbm, wv_ref), (dq_hbm, dq_all), (dkv_hbm, dkv_all)))]
    out_loads = [
        pltpu.make_async_copy(wo_hbm.at[g, t], wo_ref.at[t, g * share:(g + 1) * share, :], w_sem.at[5 + g * tp + t])
        for g in range(shares) for t in range(tp)
    ]
    for copy in weight_loads:
        copy.start()

    barrier = pltpu.get_barrier_semaphore()
    peers = [(dt, dc) for dt in range(tp) for dc in range(cp) if dt or dc]
    for dt, dc in peers:
        pl.semaphore_signal(barrier, inc=1, device_id={"tp": lax.rem(z + dt, tp), "cp": lax.rem(r + dc, cp)}, device_id_type=MESH)
    pl.semaphore_wait(barrier, len(peers))

    def remote(src, dst, ssem, rsem, dev):
        return pltpu.make_async_remote_copy(src_ref=src, dst_ref=dst, send_sem=ssem, recv_sem=rsem, device_id=dev, device_id_type=MESH)

    right = {"tp": jnp.where(z < last, z + 1, z)}
    left = {"tp": jnp.where(z > 0, z - 1, z)}

    def group_rows(i):
        return pl.ds(pl.multiple_of(i * span, span), span)

    def tile_rows(i, owner):
        return pl.ds(pl.multiple_of(i * span + owner * rows, rows), rows)

    def inputs(i, slot):
        g = group_rows(i)
        return [
            pltpu.make_async_copy(o_hbm.at[:, g, :], o_in.at[slot], in_sem.at[slot, 0]),
            pltpu.make_async_copy(x_hbm.at[g, :], x_in.at[slot], in_sem.at[slot, 1]),
        ]

    def final_inputs(i, slot):
        g = tile_rows(i, z)
        return [
            pltpu.make_async_copy(x_hbm.at[g, :], xo_in.at[slot], fin_sem.at[slot, 0]),
            pltpu.make_async_copy(dy_hbm.at[g, :], dyo_in.at[slot], fin_sem.at[slot, 1]),
        ]

    def y_copy(i, slot):
        return pltpu.make_async_copy(y_buf.at[slot], y_hbm.at[group_rows(i), :], y_sem.at[slot])

    def rs_copy(i, s, to_right):
        ring = lax.rem(i, RS_RING)
        if to_right:
            return remote(send_r.at[s], rs_r.at[ring, s], rss_r.at[s], rsr_r.at[ring, s], right)
        return remote(send_l.at[s], rs_l.at[ring, s], rss_l.at[s], rsr_l.at[ring, s], left)

    def rs_send(i, s):
        for to_right in (True, False):
            far = z if to_right else last - z
            owner = (z + slots - s) if to_right else (z - slots + s)
            buf, held = (send_r, rs_r) if to_right else (send_l, rs_l)

            @pl.when(jnp.logical_and(jnp.logical_and(i >= 0, i < groups), jnp.logical_and(far <= s, far < last)))
            def _(to_right=to_right, far=far, owner=owner, buf=buf, held=held):
                @pl.when(i > 0)
                def _():
                    rs_copy(i - 1, s, to_right).wait_send()

                cur = lax.rem(i, PART_RING)
                own = pl.ds(pl.multiple_of(owner * rows, rows), rows)
                if s == 0:
                    buf[s] = part[cur, own, :].astype(BF16)
                else:
                    @pl.when(far == 0)
                    def _():
                        buf[s] = part[cur, own, :].astype(BF16)

                    @pl.when(far > 0)
                    def _():
                        rs_copy(i, s - 1, to_right).wait_recv()
                        buf[s] = (part[cur, own, :] + held[lax.rem(i, RS_RING), s - 1].astype(F32)).astype(BF16)

                rs_copy(i, s, to_right).start()

    def ag_own(i, slot, to_right):
        src = gx_buf.at[slot]
        dst = gx_hbm.at[tile_rows(i, z), :]
        if to_right:
            return remote(src, dst, ag0_r.at[slot], agr_r.at[i, 0], right)
        return remote(src, dst, ag0_l.at[slot], agr_l.at[i, 0], left)

    def own_copy(i, slot):
        return pltpu.make_async_copy(gx_buf.at[slot], gx_hbm.at[tile_rows(i, z), :], own_sem.at[slot])

    def ag_forward(i, a, to_right):
        owner = z - a if to_right else z + a
        tile = gx_hbm.at[tile_rows(i, owner), :]
        if to_right:
            return remote(tile, tile, agf_r.at[a], agr_r.at[i, a], right)
        return remote(tile, tile, agf_l.at[a], agr_l.at[i, a], left)

    def ag_wait(i, a, to_right):
        tile = gx_hbm.at[tile_rows(i, 0), :]
        sem = agr_r.at[i, a] if to_right else agr_l.at[i, a]
        remote(tile, tile, agf_r.at[a], sem, right).wait_recv()

    def ag_step(i, a):
        for to_right in (True, False):
            far = z if to_right else last - z

            @pl.when(jnp.logical_and(jnp.logical_and(i >= 0, i < groups), far >= a))
            def _(to_right=to_right, far=far):
                ag_wait(i, a - 1, to_right)
                if a < slots:
                    @pl.when(far < last)
                    def _():
                        @pl.when(i > 0)
                        def _():
                            ag_forward(i - 1, a, to_right).wait_send()

                        ag_forward(i, a, to_right).start()

    def ag_first(i, slot):
        own_copy(i, slot).start()
        for to_right in (True, False):
            far = z if to_right else last - z

            @pl.when(far < last)
            def _(to_right=to_right):
                ag_own(i, slot, to_right).start()

    def ag_first_done(i, slot):
        own_copy(i, slot).wait()
        for to_right in (True, False):
            far = z if to_right else last - z

            @pl.when(far < last)
            def _(to_right=to_right):
                ag_own(i, slot, to_right).wait_send()

    def partial_norm(i):
        cur = lax.rem(i, PART_RING)
        g = group_rows(i)
        for c in range(0, d_model, chunk):
            cols = slice(c, c + chunk)
            part[cur, :, cols] = (
                dot_nt(dq_all[g, :], wq_ref[cols, :]) + dot_nt(dkv_all[0, g, :], wk_ref[cols, :]) + dot_nt(dkv_all[1, g, :], wv_ref[cols, :])
            )

    def project_out(cur):
        for c in range(0, d_model, chunk):
            cols = slice(c, c + chunk)
            acc = x_in[cur, :, cols].astype(F32)
            for t in range(tp):
                acc += dot_nn(o_in[cur, t], wo_ref[t, :, cols])
            y_buf[cur, :, cols] = acc.astype(BF16)

    def finalize(i):
        slot = lax.rem(i, 2)
        own = pl.ds(pl.multiple_of(z * rows, rows), rows)
        tot[...] = part[lax.rem(i, PART_RING), own, :]

        @pl.when(z > 0)
        def _():
            rs_copy(i, slots - 1, True).wait_recv()
            tot[...] += rs_r[lax.rem(i, RS_RING), slots - 1].astype(F32)

        @pl.when(z < last)
        def _():
            rs_copy(i, slots - 1, False).wait_recv()
            tot[...] += rs_l[lax.rem(i, RS_RING), slots - 1].astype(F32)

        @pl.when(i > 1)
        def _():
            ag_first_done(i - 2, slot)

        for copy in final_inputs(i, slot):
            copy.wait()
        x = xo_in[slot].astype(F32)
        centred = x - jnp.mean(x, axis=-1, keepdims=True)
        inv_std = lax.rsqrt(jnp.mean(centred * centred, axis=-1, keepdims=True) + LN_EPS)
        x_hat = centred * inv_std
        dn = tot[...]
        gg_ref[...] += jnp.sum(dn * x_hat, axis=0, keepdims=True)
        d_hat = dn * gain_ref[...]
        dx = inv_std * (d_hat - jnp.mean(d_hat, axis=-1, keepdims=True) - x_hat * jnp.mean(d_hat * x_hat, axis=-1, keepdims=True))
        gx_buf[slot] = (dyo_in[slot].astype(F32) + dx).astype(BF16)
        ag_first(i, slot)

    def block_of(t):
        return 2 * lax.div(t, 2) + jnp.where(lax.rem(t, 2) == 0, 1 - core, core)

    def job_loads(t, slot):
        cols = pl.ds(pl.multiple_of(block_of(t) * width, width), width)
        return [
            pltpu.make_async_copy(n_hbm.at[:, cols], n_in.at[slot], job_sem.at[slot, 0]),
            pltpu.make_async_copy(dy_hbm.at[:, cols], dy_in.at[slot], job_sem.at[slot, 1]),
        ]

    def away_copy(p):
        ring = lax.rem(p, 2)
        return remote(away, part_in.at[ring], away_send.at[0], away_recv.at[ring], partner)

    def job_block(t, put):
        slot = lax.rem(t, 2)
        n_t = n_in[slot].T
        put(0, hidden, dot_nn(n_t, dq_all[...]))
        put(hidden, hidden, dot_nn(n_t, dkv_all[0]))
        put(2 * hidden, hidden, dot_nn(n_t, dkv_all[1]))
        for k in range(hidden // width):
            put(3 * hidden + k * width, width, dot_nn(o_t[k * width:(k + 1) * width, :], dy_in[slot]))

    def mine_to_own(p, slot):
        return pltpu.make_async_copy(mine.at[slot], ga_hbm.at[2 * p + core], mine_own.at[slot])

    def mine_to_part(p, slot):
        return remote(mine.at[slot], ga_hbm.at[2 * p + core], mine_part.at[slot], ga_recv.at[p], partner)

    def mine_to_chip(p, slot):
        return remote(mine.at[slot], gb_hbm.at[2 * p + core], mine_chip.at[slot], chip_recv.at[p], peer)

    def mine_done(p, slot):
        mine_to_own(p, slot).wait()
        mine_to_part(p, slot).wait_send()
        mine_to_chip(p, slot).wait_send()

    def chip_forward(p):
        b = 2 * p + core
        return remote(gb_hbm.at[b], gb_hbm.at[b], gb_send.at[p], gb_recv.at[p], partner)

    def job(t):
        p = lax.div(t, 2)
        for copy in job_loads(t, lax.rem(t, 2)):
            copy.wait()

        @pl.when(t + 1 < blocks)
        def _():
            for copy in job_loads(t + 1, 1 - lax.rem(t, 2)):
                copy.start()

        @pl.when(lax.rem(t, 2) == 0)
        def _():
            @pl.when(p > 0)
            def _():
                away_copy(p - 1).wait_send()

            def put(at, size, value):
                away[:, at:at + size] = value

            job_block(t, put)
            away_copy(p).start()

        @pl.when(lax.rem(t, 2) == 1)
        def _():
            slot = lax.rem(p, 2)
            away_copy(p).wait_recv()

            @pl.when(p > 1)
            def _():
                mine_done(p - 2, slot)

            def put(at, size, value):
                mine[slot, :, at:at + size] = (value + part_in[slot, :, at:at + size]).astype(BF16)

            job_block(t, put)
            mine_to_chip(p, slot).start()
            mine_to_part(p, slot).start()
            mine_to_own(p, slot).start()

    gg_ref[...] = jnp.zeros_like(gg_ref)
    o_loads = [pltpu.make_async_copy(o_hbm.at[z, :, k * width:(k + 1) * width], n_in.at[k], job_sem.at[k, 0]) for k in range(hidden // width)]
    for copy in o_loads:
        copy.start()
    for copy in inputs(0, 0):
        copy.start()
    for copy in out_loads:
        copy.start()
    me = z * cp + r

    def gain_copy(dt, dc):
        to = {"tp": lax.rem(z + dt, tp), "cp": lax.rem(r + dc, cp)}
        return remote(gain_all.at[me], gain_all.at[me], gs_sem.at[dt * cp + dc], gr_sem.at[me], to)

    def gain_wait(dt, dc):
        sender = lax.rem(z + dt, tp) * cp + lax.rem(r + dc, cp)
        remote(gain_all.at[sender], gain_all.at[sender], gs_sem.at[0], gr_sem.at[sender], right).wait_recv()

    for copy in weight_loads:
        copy.wait()

    def step(i, carry):
        cur = lax.rem(i, 2)

        @pl.when(i < groups)
        def _():
            partial_norm(i)

        for a in range(1, slots + 1):
            ag_step(i - slots - a, a)
        for s in reversed(range(slots)):
            rs_send(i - s, s)

        @pl.when(jnp.logical_and(i >= slots, i < groups + slots))
        def _():
            finalize(i - slots)

        @pl.when(i == groups + slots - 1)
        def _():
            gain_all[me] = gg_ref[...]
            for dt, dc in peers:
                gain_copy(dt, dc).start()

        @pl.when(jnp.logical_and(i >= slots - 1, i < groups + slots - 1))
        def _():
            for copy in final_inputs(i - slots + 1, lax.rem(i - slots + 1, 2)):
                copy.start()

        @pl.when(i == 0)
        def _():
            for copy in out_loads:
                copy.wait()
            for k, copy in enumerate(o_loads):
                copy.wait()
                o_t[k * width:(k + 1) * width, :] = n_in[k].T
            for copy in job_loads(0, 0):
                copy.start()

        @pl.when(i < groups)
        def _():
            for copy in inputs(i, cur):
                copy.wait()

            @pl.when(i + 1 < groups)
            def _():
                for copy in inputs(i + 1, 1 - cur):
                    copy.start()

            @pl.when(i >= 2)
            def _():
                y_copy(i - 2, cur).wait()

            project_out(cur)
            y_copy(i, cur).start()

        @pl.when(jnp.logical_and(i >= 1, i <= blocks))
        def _():
            job(i - 1)

        @pl.when(jnp.logical_and(lax.rem(i, 2) == 1, jnp.logical_and(i >= 5, i < 5 + 2 * pairs)))
        def _():
            p = lax.div(i - 5, 2)
            mine_to_chip(p, 0).wait_recv()
            chip_forward(p).start()

        return carry

    lax.fori_loop(0, max(groups + 2 * slots, 2 * pairs + 4), step, 0)

    for i in (groups - 2, groups - 1):
        y_copy(i, i % 2).wait()
        ag_first_done(i, i % 2)
    for to_right in (True, False):
        far = z if to_right else last - z
        for s in range(slots):
            @pl.when(jnp.logical_and(far <= s, far < last))
            def _(s=s, to_right=to_right):
                rs_copy(groups - 1, s, to_right).wait_send()
        for a in range(1, slots):
            @pl.when(jnp.logical_and(far >= a, far < last))
            def _(a=a, to_right=to_right):
                ag_forward(groups - 1, a, to_right).wait_send()
    away_copy(pairs - 1).wait_send()
    for p in range(max(0, pairs - 2), pairs):
        mine_done(p, p % 2)
    for p in range(pairs):
        chip_forward(p).wait_send()
        chip_forward(p).wait_recv()
        mine_to_part(p, 0).wait_recv()
    for dt, dc in peers:
        gain_wait(dt, dc)
        gain_copy(dt, dc).wait_send()
    total = gain_all[0]
    for j in range(1, tp * cp):
        total += gain_all[j]
    gg_ref[...] = total


def backward_norm(dq, dkv, x, dy, o_all, normed, wq, wk, wv, wo_all, gain, rows, tp, cp):
    tokens, hidden = dq.shape
    d_model = x.shape[1]
    span = tp * rows
    groups = tokens // span
    slots = tp - 1
    width = WIDTH
    blocks = d_model // width
    pairs = blocks // 2
    hbm = pl.BlockSpec(memory_space=pl.ANY)
    vmem = pl.BlockSpec(memory_space=pltpu.VMEM)
    dma = pltpu.SemaphoreType.DMA
    bf = lambda *shape: pltpu.VMEM(shape, BF16)
    f32 = lambda *shape: pltpu.VMEM(shape, F32)
    return pl.pallas_call(
        functools.partial(back_kernel, groups, rows, tp, cp),
        in_specs=[hbm] * 10 + [vmem],
        out_specs=[hbm, hbm, hbm, hbm, vmem],
        out_shape=[
            jax.ShapeDtypeStruct((tokens, d_model), BF16),
            jax.ShapeDtypeStruct((tokens, d_model), BF16),
            jax.ShapeDtypeStruct((blocks, width, 4 * hidden), BF16),
            jax.ShapeDtypeStruct((blocks, width, 4 * hidden), BF16),
            jax.ShapeDtypeStruct((1, d_model), F32),
        ],
        scratch_shapes=[
            bf(d_model, hidden), bf(d_model, hidden), bf(d_model, hidden), bf(tp, hidden, d_model),
            bf(tokens, hidden), bf(2, tokens, hidden), bf(hidden, tokens),
            f32(PART_RING, span, d_model), bf(RS_RING, slots, rows, d_model), bf(RS_RING, slots, rows, d_model),
            bf(slots, rows, d_model), bf(slots, rows, d_model), f32(rows, d_model), bf(2, rows, d_model),
            bf(2, tp, span, hidden), bf(2, span, d_model), bf(2, rows, d_model), bf(2, rows, d_model), bf(2, span, d_model),
            bf(2, tokens, width), bf(2, tokens, width),
            f32(width, 4 * hidden), f32(2, width, 4 * hidden), bf(2, width, 4 * hidden), f32(tp * cp, 1, d_model),
            dma((5 + tp * wo_all.shape[0],)), dma((2, 2)), dma((2, 2)), dma((2, 2)), dma((2,)), dma((2,)),
            dma((slots,)), dma((slots,)), dma((RS_RING, slots)), dma((RS_RING, slots)),
            dma((2,)), dma((2,)), dma((slots,)), dma((slots,)), dma((groups, slots)), dma((groups, slots)),
            dma((1,)), dma((2,)), dma((2,)), dma((2,)), dma((2,)), dma((pairs,)), dma((pairs,)), dma((pairs,)), dma((pairs,)),
            dma((tp * cp,)), dma((tp * cp,)),
        ],
        compiler_params=pltpu.CompilerParams(collective_id=0, has_side_effects=True, vmem_limit_bytes=63 << 20),
        cost_estimate=pl.CostEstimate(flops=22 * tokens * hidden * d_model, bytes_accessed=16 * tokens * d_model, transcendentals=0),
        name="backward_norm",
    )(dq, dkv, x, dy, o_all, normed, wq, wk, wv, wo_all, gain)


def finish_kernel(y_ref, gx_ref, ga_ref, gb_ref, yo_ref, gxo_ref, wq_ref, wk_ref, wv_ref, wo_ref):
    yo_ref[...] = y_ref[...]
    gxo_ref[...] = gx_ref[...]
    width = ga_ref.shape[1]
    hidden = wq_ref.shape[1]
    for k, ref in enumerate((wq_ref, wk_ref, wv_ref)):
        cols = slice(k * hidden, (k + 1) * hidden)
        ref[...] = ga_ref[0, :, cols].astype(F32) + gb_ref[0, :, cols].astype(F32)
    for k in range(hidden // width):
        cols = slice(3 * hidden + k * width, 3 * hidden + (k + 1) * width)
        wo_ref[k * width:(k + 1) * width, :] = ga_ref[0, :, cols].astype(F32) + gb_ref[0, :, cols].astype(F32)


def finish(y, gx, ga, gb):
    tokens, d_model = y.shape
    blocks, width, packed = ga.shape
    hidden = packed // 4
    rows = tokens // blocks
    tile = pl.BlockSpec((rows, d_model), lambda j: (j, 0))
    block = pl.BlockSpec((1, width, packed), lambda j: (j, 0, 0))
    wide = pl.BlockSpec((width, hidden), lambda j: (j, 0))
    return pl.pallas_call(
        finish_kernel,
        grid=(blocks,),
        in_specs=[tile, tile, block, block],
        out_specs=[tile, tile, wide, wide, wide, pl.BlockSpec((hidden, width), lambda j: (0, j))],
        out_shape=[jax.ShapeDtypeStruct((tokens, d_model), BF16)] * 2 + [jax.ShapeDtypeStruct((d_model, hidden), F32)] * 3 + [jax.ShapeDtypeStruct((hidden, d_model), F32)],
        compiler_params=pltpu.CompilerParams(dimension_semantics=("arbitrary",), vmem_limit_bytes=48 << 20),
        cost_estimate=pl.CostEstimate(flops=8 * d_model * hidden, bytes_accessed=8 * tokens * d_model + 32 * d_model * hidden, transcendentals=0),
        name="finish",
    )(y, gx, ga, gb)


def solution(mesh):
    cp_size = mesh.shape["cp"]
    tp_size = mesh.shape["tp"]
    dp_size = mesh.shape["dp"]

    def device_step(x_in, segment_ids, positions, w_query, w_key, w_value, w_out, norm_gain, grad_out):
        batch, seq, d_model = x_in.shape
        tokens = batch * seq
        rank = lax.axis_index("cp")
        x = x_in.reshape(tokens, d_model)
        dy = grad_out.reshape(tokens, d_model)

        inv_freq = ROPE_THETA ** (-jnp.arange(0, HEAD_DIM, 2).astype(F32) / HEAD_DIM)
        angles = positions.reshape(tokens, 1).astype(F32) * jnp.repeat(inv_freq, 2)[None, :]
        cos_t, sin_t = jnp.cos(angles), jnp.sin(angles)
        start = (rank * seq + jnp.arange(seq, dtype=jnp.int32))[None, :] - positions

        share = w_out.shape[0] // (cp_size * dp_size)
        mine = (lax.axis_index("dp") * cp_size + rank) * share
        w_all = lax.all_gather(lax.dynamic_slice(w_out, (mine, 0), (share, d_model)), ("dp", "tp", "cp"), axis=0)
        w_all = w_all.reshape(dp_size, tp_size, cp_size * share, d_model)

        rows = min(384, tokens)
        normed, kv = project_keys(x, cos_t, sin_t, norm_gain.reshape(1, d_model), w_key, w_value, rows)
        o_all, dq, dkv = front(kv, normed, dy, cos_t, sin_t, start.reshape(batch, 1, seq), w_query, w_out, seq, tp_size, cp_size)
        grad_x, y_out, sum_a, sum_b, grad_gain = backward_norm(dq, dkv, x, dy, o_all, normed, w_query, w_key, w_value, w_all, norm_gain.reshape(1, d_model), ROWS, tp_size, cp_size)
        grad_gain = grad_gain.reshape(d_model)
        y_out, grad_x, grad_wq, grad_wk, grad_wv, grad_wo = finish(y_out, grad_x, sum_a, sum_b)
        return y_out.reshape(x_in.shape), grad_x.reshape(x_in.shape), grad_gain, grad_wq, grad_wk, grad_wv, grad_wo

    in_specs = (P("dp", "cp", None), P("dp", "cp"), P("dp", "cp"), P(None, "tp"), P(None, "tp"), P(None, "tp"), P("tp", None), P(None), P("dp", "cp", None))
    out_specs = (P("dp", "cp", None), P("dp", "cp", None), P("dp"), P("dp", "tp"), P("dp", "tp"), P("dp", "tp"), P(("dp", "tp"), None))
    return jax.shard_map(device_step, mesh=mesh, in_specs=in_specs, out_specs=out_specs, check_vma=False)
```

```python
import functools
import math

import jax
import jax.numpy as jnp
from jax import lax
from jax.experimental import pallas as pl
from jax.experimental.pallas import tpu as pltpu
from jax.sharding import PartitionSpec as P

HEAD_DIM = 128
ROPE_THETA = 8000000.0
LN_EPS = 1e-5
NEG_BIG = -1e30
SCALE = HEAD_DIM ** -0.5
EXP2_SCALE = SCALE * math.log2(math.e)
F32 = jnp.float32
BF16 = jnp.bfloat16
NT = (((1,), (1,)), ((), ()))


def dot_nn(a, b):
    return jnp.dot(a, b, preferred_element_type=F32)


def dot_nt(a, b):
    return lax.dot_general(a, b, NT, preferred_element_type=F32)


def dot_tn(a, b):
    return lax.dot_general(a, b, (((0,), (0,)), ((), ())), preferred_element_type=F32)


def swap_pairs(t, sign):
    lane = lax.broadcasted_iota(jnp.int32, t.shape, 1)
    even = (lane % 2) == 0
    up = pltpu.roll(t, HEAD_DIM - 1, 1)
    down = pltpu.roll(t, 1, 1)
    return jnp.where(even, -up, down) if sign > 0 else jnp.where(even, up, -down)


def rope(t, cos_t, sin_t, sign):
    return t * cos_t + swap_pairs(t, sign) * sin_t


def put_rope(dst, raw, cos_t, sin_t):
    for h in range(raw.shape[1] // HEAD_DIM):
        cols = slice(h * HEAD_DIM, (h + 1) * HEAD_DIM)
        dst[:, cols] = rope(raw[:, cols], cos_t, sin_t, 1.0).astype(BF16)


MESH = pl.DeviceIdType.MESH
SUB = 128
ROWS = 32
WIDTH = 256
RELAY_LAG = 2
CHIP_BUFS = 3
W_TWIN = 1
W_PARTNER = 4


def front_kernel(batch, seq, tp, cp, x_hbm, dy_hbm, wq_hbm, wk_hbm, wv_hbm, wo_hbm, cos_ref, sin_ref, start_ref, gain_ref,
                 n_hbm, o_all, dq_hbm, dkv_hbm, w_all,
                 big, wo_ref, q_row, do_row, a_in, b_in, kv_own, kvr, s_scr, dp_scr, m_scr, l_scr, d_scr, ot_scr, dqt_scr,
                 o_buf, dq_buf, g_part, g_chip, g_far, xin, part_in,
                 w_sem, wl_sem, wz_send, wz_recv, wx_send, wx_recv, wp_send, wp_recv, wf_send, wf_recv,
                 tile_sem, n_sem, kvs_part, kvs_chip, kvs_far, kv_recv, o_local, o_send, o_recv, relay_send, dq_sem,
                 far_send, part_send, chip_send, x_recv, part_recv, dkv_sem):
    z = lax.axis_index("tp")
    r = lax.axis_index("cp")
    dp = lax.axis_index("dp")
    core = lax.rem(r, 2)
    chip = lax.div(r, 2)
    d_model = x_hbm.shape[1]
    hidden = wq_hbm.shape[1]
    heads = hidden // HEAD_DIM
    first_chip, second_chip = chip == 0, chip == 1
    first_core, second_core = core == 0, core == 1
    partner = {"cp": r + 1 - 2 * core}
    peer = {"cp": r + 2 - 4 * chip}
    twin = {"dp": 1 - dp}

    weight_loads = [pltpu.make_async_copy(src, dst, w_sem.at[k]) for k, (src, dst) in enumerate(((wk_hbm, big.at[0]), (wv_hbm, big.at[1]), (wq_hbm, big.at[2]), (wo_hbm, wo_ref)))]
    for copy in weight_loads:
        copy.start()

    tile = a_in.shape[1]
    per_row = seq // tile
    tiles = batch * per_row

    def tile_rows(t):
        return pl.ds(pl.multiple_of(t * tile, tile), tile)

    def row(b):
        return pl.ds(pl.multiple_of(b * seq, seq), seq)

    def x_load(t, par):
        return pltpu.make_async_copy(x_hbm.at[tile_rows(t), :], a_in.at[par], tile_sem.at[par, 0])

    def n_load(t, par):
        return pltpu.make_async_copy(n_hbm.at[tile_rows(t), :], a_in.at[par], tile_sem.at[par, 0])

    def dy_load(t, par):
        return pltpu.make_async_copy(dy_hbm.at[tile_rows(t), :], b_in.at[par], tile_sem.at[par, 1])

    def n_store(t, par):
        return pltpu.make_async_copy(b_in.at[par], n_hbm.at[tile_rows(t), :], n_sem.at[par])

    x_load(0, 0).start()

    barrier = pltpu.get_barrier_semaphore()
    for dev in [partner, peer, twin] + [{"tp": lax.rem(z + dt, tp)} for dt in range(1, tp)]:
        pl.semaphore_signal(barrier, inc=1, device_id=dev, device_id_type=MESH)
    pl.semaphore_wait(barrier, tp + 2)

    def remote(src, dst, ssem, rsem, dev):
        return pltpu.make_async_remote_copy(src_ref=src, dst_ref=dst, send_sem=ssem, recv_sem=rsem, device_id=dev, device_id_type=MESH)

    share = hidden // 4

    def share_rows(c, g):
        return pl.ds(pl.multiple_of((2 * c + g) * share, share), share)

    mine, twins = share_rows(core, dp), share_rows(core, 1 - dp)

    def wz_copy(d):
        return remote(wo_hbm.at[mine, :], w_all.at[z, mine, :], wz_send.at[d], wz_recv.at[z], {"tp": lax.rem(z + d, tp)})

    def wz_wait(d):
        src = lax.rem(z + d, tp)
        remote(wo_hbm.at[mine, :], w_all.at[src, mine, :], wz_send.at[d], wz_recv.at[src], partner).wait_recv()

    def w_slice(d, rows):
        return w_all.at[lax.rem(z + d, tp), rows, :]

    def wx_copy(d):
        return remote(w_slice(d, mine), w_slice(d, mine), wx_send.at[d], wx_recv.at[d], twin)

    def wp_copy(d):
        return remote(w_slice(d, mine), w_slice(d, mine), wp_send.at[d], wp_recv.at[d], partner)

    def wf_copy(d):
        return remote(w_slice(d, twins), w_slice(d, twins), wf_send.at[d], wf_recv.at[d], partner)

    for d in range(1, tp):
        wz_copy(d).start()

    def kv_to_partner(b):
        return remote(kv_own.at[b], kvr.at[0, b], kvs_part.at[b], kv_recv.at[0, b], partner)

    def kv_to_chip(b):
        return remote(kv_own.at[b], kvr.at[1, b], kvs_chip.at[b], kv_recv.at[1, b], peer)

    def kv_forward(b):
        return remote(kvr.at[1, b], kvr.at[2, b], kvs_far.at[b], kv_recv.at[2, b], partner)

    for copy in weight_loads:
        copy.wait()
    w_local = pltpu.make_async_copy(wo_ref, w_all.at[z], wl_sem.at[0])
    w_local.start()

    def key_tile(t, carry):
        par = lax.rem(t, 2)
        x_load(t, par).wait()

        @pl.when(t + 1 < tiles)
        def _():
            x_load(t + 1, 1 - par).start()

        @pl.when(t >= 2)
        def _():
            n_store(t - 2, par).wait()

        x = a_in[par].astype(F32)
        centred = x - jnp.mean(x, axis=-1, keepdims=True)
        inv_std = lax.rsqrt(jnp.mean(centred * centred, axis=-1, keepdims=True) + LN_EPS)
        normed = ((centred * inv_std) * gain_ref[...]).astype(BF16)
        b_in[par] = normed
        n_store(t, par).start()
        b = lax.div(t, per_row)
        part = lax.rem(t, per_row)
        inside = pl.ds(pl.multiple_of(part * tile, tile), tile)
        rows = tile_rows(t)
        put_rope(kv_own.at[b, 0, inside, :], dot_nn(normed, big[0]), cos_ref[rows, :], sin_ref[rows, :])
        kv_own[b, 1, inside, :] = dot_nn(normed, big[1]).astype(BF16)

        @pl.when(part == per_row - 1)
        def _():
            @pl.when(first_chip)
            def _():
                kv_to_chip(b).start()

            @pl.when(first_core)
            def _():
                kv_to_partner(b).start()

        return carry

    lax.fori_loop(0, tiles, key_tile, 0)
    for t in range(tiles - 2, tiles):
        n_store(t, t % 2).wait()

    def query_loads(t, par):
        return [n_load(t, par), dy_load(t, par)]

    for copy in query_loads(0, 0):
        copy.start()

    def query_row(i):
        for k in range(per_row):
            t = i * per_row + k
            par = lax.rem(t, 2)
            for copy in query_loads(t, par):
                copy.wait()

            @pl.when(t + 1 < tiles)
            def _(t=t, par=par):
                for copy in query_loads(t + 1, 1 - par):
                    copy.start()

            rows = tile_rows(t)
            inside = slice(k * tile, (k + 1) * tile)
            put_rope(q_row.at[inside, :], dot_nn(a_in[par], big[2]), cos_ref[rows, :], sin_ref[rows, :])
            do_row[inside, :] = dot_nt(b_in[par], wo_ref[...]).astype(BF16)

    fit = d_model // seq

    def g_own(b, which):
        k = 2 * b + which
        return big.at[lax.div(k, fit), pl.ds(pl.multiple_of(lax.rem(k, fit) * seq, seq), seq), :]

    def o_local_copy(b):
        return pltpu.make_async_copy(o_buf.at[b], o_all.at[z, row(b), :], o_local.at[b])

    def o_copy(b, k, step):
        return remote(o_buf.at[b], o_all.at[z, row(b), :], o_send.at[k, b], o_recv.at[z, b], {"tp": jnp.clip(z + step, 0, tp - 1)})

    hops = [(k, step, jnp.logical_and(z + step >= 0, z + step < tp)) for k, step in enumerate((1, -1, 2, -2))]

    def o_start(b):
        o_local_copy(b).start()
        for k, step, ok in hops:
            @pl.when(ok)
            def _(k=k, step=step):
                o_copy(b, k, step).start()

    def o_arrived(src, b):
        remote(o_all.at[src, row(b), :], o_all.at[src, row(b), :], relay_send.at[b], o_recv.at[src, b], partner).wait_recv()

    def relay_copy(b, src, dst):
        return remote(o_all.at[src, row(b), :], o_all.at[src, row(b), :], relay_send.at[b], o_recv.at[src, b], {"tp": dst})

    def relay(b):
        @pl.when(z == tp - 2)
        def _():
            o_arrived(0, b)
            relay_copy(b, 0, tp - 1).start()

        @pl.when(z == 1)
        def _():
            o_arrived(tp - 1, b)
            relay_copy(b, tp - 1, 0).start()

    def far_copy(b, par):
        return remote(g_far.at[par], xin.at[b], far_send.at[par], x_recv.at[b], partner)

    def part_copy(b, par):
        return remote(g_part.at[par], part_in.at[b], part_send.at[par], part_recv.at[b], partner)

    def chip_copy(b):
        par = lax.rem(b, CHIP_BUFS)
        return remote(g_chip.at[par], xin.at[b], chip_send.at[par], x_recv.at[b], peer)

    def chip_sum(b):
        @pl.when(second_chip)
        def _():
            par = lax.rem(b, CHIP_BUFS)
            far_copy(b, 0).wait_recv()
            g_chip[par] = (g_chip[par].astype(F32) + xin[b].astype(F32)).astype(BF16)
            chip_copy(b).start()

    def dkv_store(b, which):
        return pltpu.make_async_copy(g_own(b, which), dkv_hbm.at[which, row(b), :], dkv_sem.at[b, which])

    def key_grads(b):
        @pl.when(first_core)
        def _():
            part_copy(b, 0).wait_recv()

        @pl.when(first_chip)
        def _():
            chip_copy(b).wait_recv()

        rows = row(b)
        for which in range(2):
            own = g_own(b, which)
            for h in range(heads):
                cols = slice(h * HEAD_DIM, (h + 1) * HEAD_DIM)
                acc = own[:, cols].astype(F32)
                acc = acc + jnp.where(first_core, part_in[b, which, :, cols].astype(F32), 0.0)
                acc = (acc + jnp.where(first_chip, xin[b, which, :, cols].astype(F32), 0.0)).astype(BF16)
                if which == 0:
                    acc = rope(acc.astype(F32), cos_ref[rows, :], sin_ref[rows, :], -1.0).astype(BF16)
                own[:, cols] = acc
            dkv_store(b, which).start()

    def dq_store(b, par):
        return pltpu.make_async_copy(dq_buf.at[par], dq_hbm.at[row(b), :], dq_sem.at[par])

    subs = range(0, seq, SUB)

    def attend_row(i, par):
        rows = row(i)
        start = start_ref[i]
        chip_par = lax.rem(i, CHIP_BUFS)
        keys_of = [kv_own.at[i]] + [kvr.at[s, i] for s in range(3)]
        places = [g_part.at[par], g_chip.at[chip_par], g_far.at[par]]

        def grad(slot, which):
            return places[slot - 1].at[which] if slot else g_own(i, which)

        live = [None, second_core, second_chip, second_chip]
        piece = [r, r + 1 - 2 * core, r + 2 - 4 * chip, r + 3 - 2 * core - 4 * chip]

        def each(body):
            body(0)
            for slot in (1, 2, 3):
                pl.when(live[slot])(functools.partial(body, slot))

        def one_head(h, carry):
            cols = pl.ds(pl.multiple_of(h * HEAD_DIM, HEAD_DIM), HEAD_DIM)
            q = q_row[:, cols]
            do = do_row[:, cols]
            m_scr[...] = jnp.full(m_scr.shape, NEG_BIG, F32)
            l_scr[...] = jnp.zeros_like(l_scr)
            d_scr[...] = jnp.zeros_like(d_scr)
            ot_scr[...] = jnp.zeros_like(ot_scr)
            dqt_scr[...] = jnp.zeros_like(dqt_scr)

            def scores(slot):
                base = piece[slot] * seq
                for s in subs:
                    raw = dot_nt(keys_of[slot][0, s:s + SUB, cols], q)
                    local = lax.broadcasted_iota(jnp.int32, raw.shape, 0) + s
                    allowed = (local + base) >= start
                    if slot == 0:
                        allowed = jnp.logical_and(allowed, local <= lax.broadcasted_iota(jnp.int32, raw.shape, 1))
                    raw = jnp.where(allowed, raw, NEG_BIG)
                    s_scr[slot, s:s + SUB, :] = raw
                    m_scr[...] = jnp.maximum(m_scr[...], jnp.max(raw, axis=0, keepdims=True))

            def exps(slot):
                for s in subs:
                    e = jnp.exp2((s_scr[slot, s:s + SUB, :] - m_scr[...]) * EXP2_SCALE)
                    s_scr[slot, s:s + SUB, :] = e
                    l_scr[...] += jnp.sum(e, axis=0, keepdims=True)

            def values(slot):
                for s in subs:
                    v = keys_of[slot][1, s:s + SUB, cols]
                    prob = s_scr[slot, s:s + SUB, :] * l_scr[...]
                    low = prob.astype(BF16)
                    dp = dot_nt(v, do)
                    s_scr[slot, s:s + SUB, :] = prob
                    dp_scr[slot, s:s + SUB, :] = dp
                    d_scr[...] += jnp.sum(prob * dp, axis=0, keepdims=True)
                    grad(slot, 1)[s:s + SUB, cols] = dot_nn(low, do).astype(BF16)
                    ot_scr[...] += dot_nn(v.T, low)

            def keys(slot):
                for s in subs:
                    k = keys_of[slot][0, s:s + SUB, cols]
                    ds = (s_scr[slot, s:s + SUB, :] * (dp_scr[slot, s:s + SUB, :] - d_scr[...])).astype(BF16)
                    grad(slot, 0)[s:s + SUB, cols] = (dot_nn(ds, q) * SCALE).astype(BF16)
                    dqt_scr[...] += dot_nn(k.T, ds)

            each(scores)
            each(exps)
            l_scr[...] = 1.0 / l_scr[...]
            each(values)
            each(keys)
            o_buf[i, :, cols] = ot_scr[...].T.astype(BF16)
            dq_buf[par, :, cols] = rope(dqt_scr[...].T * SCALE, cos_ref[rows, :], sin_ref[rows, :], -1.0).astype(BF16)
            return carry

        lax.fori_loop(0, heads, one_head, 0)

    def step(i, carry):
        par = lax.rem(i, 2)
        query_row(i)

        @pl.when(second_chip)
        def _():
            kv_to_chip(i).wait_recv()
            kv_forward(i).start()

        @pl.when(second_core)
        def _():
            kv_to_partner(i).wait_recv()

        @pl.when(second_chip)
        def _():
            kv_forward(i).wait_recv()

        @pl.when(i >= 2)
        def _():
            dq_store(i - 2, par).wait()

            @pl.when(second_core)
            def _():
                part_copy(i - 2, par).wait_send()

            @pl.when(second_chip)
            def _():
                far_copy(i - 2, par).wait_send()

        @pl.when(jnp.logical_and(second_chip, i >= CHIP_BUFS))
        def _():
            chip_copy(i - CHIP_BUFS).wait_send()

        attend_row(i, par)
        o_start(i)
        dq_store(i, par).start()

        @pl.when(second_chip)
        def _():
            far_copy(i, par).start()

        @pl.when(second_core)
        def _():
            part_copy(i, par).start()

        @pl.when(i >= 1)
        def _():
            chip_sum(i - 1)

        @pl.when(i >= RELAY_LAG)
        def _():
            relay(i - RELAY_LAG)

        @pl.when(i == min(W_TWIN, batch - 1))
        def _():
            for d in range(1, tp):
                wz_wait(d)
                wx_copy(d).start()
                wp_copy(d).start()

        @pl.when(i == min(W_PARTNER, batch - 1))
        def _():
            for d in range(1, tp):
                wx_copy(d).wait_recv()
                wf_copy(d).start()

        return carry

    lax.fori_loop(0, batch, step, 0)
    chip_sum(batch - 1)
    lag = min(RELAY_LAG, batch)
    for k in range(lag):
        relay(batch - lag + k)

    def finish(b, carry):
        key_grads(b)
        return carry

    lax.fori_loop(0, batch, finish, 0)

    w_local.wait()
    for d in range(1, tp):
        wz_copy(d).wait_send()
        wx_copy(d).wait_send()
        for copy in (wp_copy(d), wf_copy(d)):
            copy.wait_send()
            copy.wait_recv()
    for b in range(batch):
        for which in range(2):
            dkv_store(b, which).wait()

        @pl.when(first_chip)
        def _(b=b):
            kv_to_chip(b).wait_send()

        @pl.when(first_core)
        def _(b=b):
            kv_to_partner(b).wait_send()

        @pl.when(second_chip)
        def _(b=b):
            kv_forward(b).wait_send()

        o_local_copy(b).wait()
        for k, step_, ok in hops:
            @pl.when(ok)
            def _(b=b, k=k, step_=step_):
                o_copy(b, k, step_).wait_send()

        @pl.when(jnp.logical_or(z == 1, z == tp - 2))
        def _(b=b):
            relay_copy(b, 0, tp - 1).wait_send()

        for src in range(tp):
            taken = jnp.logical_or(jnp.logical_and(z == tp - 2, src == 0), jnp.logical_and(z == 1, src == tp - 1))

            @pl.when(jnp.logical_and(z != src, jnp.logical_not(taken)))
            def _(b=b, src=src):
                o_arrived(src, b)

    for b in range(max(0, batch - 2), batch):
        dq_store(b, b % 2).wait()

        @pl.when(second_core)
        def _(b=b):
            part_copy(b, b % 2).wait_send()

        @pl.when(second_chip)
        def _(b=b):
            far_copy(b, b % 2).wait_send()

    for b in range(max(0, batch - CHIP_BUFS), batch):
        @pl.when(second_chip)
        def _(b=b):
            chip_copy(b).wait_send()


def front(x, dy, wq, wk, wv, wo, cos_t, sin_t, start, gain, seq, tp, cp):
    tokens, d_model = x.shape
    hidden = wq.shape[1]
    batch = tokens // seq
    tile = seq // 2
    hbm = pl.BlockSpec(memory_space=pl.ANY)
    vmem = pl.BlockSpec(memory_space=pltpu.VMEM)
    dma = pltpu.SemaphoreType.DMA
    bf = lambda *shape: pltpu.VMEM(shape, BF16)
    f32 = lambda *shape: pltpu.VMEM(shape, F32)
    return pl.pallas_call(
        functools.partial(front_kernel, batch, seq, tp, cp),
        in_specs=[hbm] * 6 + [vmem] * 4,
        out_specs=[hbm] * 5,
        out_shape=[
            jax.ShapeDtypeStruct((tokens, d_model), BF16),
            jax.ShapeDtypeStruct((tp, tokens, hidden), BF16),
            jax.ShapeDtypeStruct((tokens, hidden), BF16),
            jax.ShapeDtypeStruct((2, tokens, hidden), BF16),
            jax.ShapeDtypeStruct((tp, hidden, d_model), BF16),
        ],
        scratch_shapes=[
            bf(3, d_model, hidden), bf(hidden, d_model), bf(seq, hidden), bf(seq, hidden), bf(2, tile, d_model), bf(2, tile, d_model),
            bf(batch, 2, seq, hidden), bf(3, batch, 2, seq, hidden),
            f32(4, seq, seq), f32(4, seq, seq), f32(1, seq), f32(1, seq), f32(1, seq), f32(HEAD_DIM, seq), f32(HEAD_DIM, seq),
            bf(batch, seq, hidden), bf(2, seq, hidden),
            bf(2, 2, seq, hidden), bf(CHIP_BUFS, 2, seq, hidden), bf(2, 2, seq, hidden),
            bf(batch, 2, seq, hidden), bf(batch, 2, seq, hidden),
            dma((4,)), dma((1,)), dma((tp,)), dma((tp,)), dma((tp,)), dma((tp,)), dma((tp,)), dma((tp,)), dma((tp,)), dma((tp,)),
            dma((2, 2)), dma((2,)), dma((batch,)), dma((batch,)), dma((batch,)), dma((3, batch)),
            dma((batch,)), dma((4, batch)), dma((tp, batch)), dma((batch,)), dma((2,)),
            dma((2,)), dma((2,)), dma((CHIP_BUFS,)), dma((batch,)), dma((batch,)), dma((batch, 2)),
        ],
        compiler_params=pltpu.CompilerParams(collective_id=1, has_side_effects=True, vmem_limit_bytes=63 << 20),
        cost_estimate=pl.CostEstimate(flops=60 * tokens * seq * hidden, bytes_accessed=16 * tokens * d_model, transcendentals=4 * tokens * seq * (hidden // HEAD_DIM)),
        name="front",
    )(x, dy, wq, wk, wv, wo, cos_t, sin_t, start, gain)


PART_RING = 4
RS_RING = 5
FORWARD_LAG = 7


def back_kernel(groups, rows, tp, cp, dq_hbm, dkv_hbm, x_hbm, dy_hbm, o_hbm, n_hbm, wq_hbm, wk_hbm, wv_hbm, wo_hbm, gain_ref,
                gx_hbm, y_hbm, ga_hbm, gb_hbm, gg_ref,
                wq_ref, wk_ref, wv_ref, wo_ref, dq_all, dkv_all, o_t, part, rs_r, rs_l, send_r, send_l, tot, gx_buf,
                o_in, x_in, xo_in, dyo_in, y_buf, n_in, dy_in, away, part_in, mine, gain_all,
                w_sem, in_sem, fin_sem, job_sem, y_sem, own_sem, rss_r, rss_l, rsr_r, rsr_l, ag0_r, ag0_l, agf_r, agf_l, agr_r, agr_l,
                away_send, away_recv, mine_own, mine_part, mine_chip, ga_recv, chip_recv, gb_send, gb_recv, gs_sem, gr_sem):
    z = lax.axis_index("tp")
    r = lax.axis_index("cp")
    core = lax.rem(r, 2)
    chip = lax.div(r, 2)
    last = tp - 1
    slots = tp - 1
    span = tp * rows
    tokens, d_model = x_hbm.shape
    hidden = dq_hbm.shape[1]
    chunk = min(512, d_model)
    blocks = ga_hbm.shape[0]
    width = ga_hbm.shape[1]
    pairs = blocks // 2
    partner = {"cp": r + 1 - 2 * core}
    peer = {"cp": r + 2 - 4 * chip}

    weight_loads = [pltpu.make_async_copy(src, dst, w_sem.at[k]) for k, (src, dst) in enumerate(((wq_hbm, wq_ref), (wk_hbm, wk_ref), (wv_hbm, wv_ref), (dq_hbm, dq_all), (dkv_hbm, dkv_all)))]
    out_loads = [pltpu.make_async_copy(wo_hbm, wo_ref, w_sem.at[5])]
    for copy in weight_loads:
        copy.start()

    barrier = pltpu.get_barrier_semaphore()
    peers = [(dt, dc) for dt in range(tp) for dc in range(cp) if dt or dc]
    for dt, dc in peers:
        pl.semaphore_signal(barrier, inc=1, device_id={"tp": lax.rem(z + dt, tp), "cp": lax.rem(r + dc, cp)}, device_id_type=MESH)
    pl.semaphore_wait(barrier, len(peers))

    def remote(src, dst, ssem, rsem, dev):
        return pltpu.make_async_remote_copy(src_ref=src, dst_ref=dst, send_sem=ssem, recv_sem=rsem, device_id=dev, device_id_type=MESH)

    right = {"tp": jnp.where(z < last, z + 1, z)}
    left = {"tp": jnp.where(z > 0, z - 1, z)}

    def group_rows(i):
        return pl.ds(pl.multiple_of(i * span, span), span)

    def tile_rows(i, owner):
        return pl.ds(pl.multiple_of(i * span + owner * rows, rows), rows)

    def inputs(i, slot):
        g = group_rows(i)
        return [
            pltpu.make_async_copy(o_hbm.at[:, g, :], o_in.at[slot], in_sem.at[slot, 0]),
            pltpu.make_async_copy(x_hbm.at[g, :], x_in.at[slot], in_sem.at[slot, 1]),
        ]

    def final_inputs(i, slot):
        g = tile_rows(i, z)
        return [
            pltpu.make_async_copy(x_hbm.at[g, :], xo_in.at[slot], fin_sem.at[slot, 0]),
            pltpu.make_async_copy(dy_hbm.at[g, :], dyo_in.at[slot], fin_sem.at[slot, 1]),
        ]

    def y_copy(i, slot):
        return pltpu.make_async_copy(y_buf.at[slot], y_hbm.at[group_rows(i), :], y_sem.at[slot])

    def rs_copy(i, s, to_right):
        ring = lax.rem(i, RS_RING)
        if to_right:
            return remote(send_r.at[s], rs_r.at[ring, s], rss_r.at[s], rsr_r.at[ring, s], right)
        return remote(send_l.at[s], rs_l.at[ring, s], rss_l.at[s], rsr_l.at[ring, s], left)

    def rs_send(i, s):
        for to_right in (True, False):
            far = z if to_right else last - z
            owner = (z + slots - s) if to_right else (z - slots + s)
            buf, held = (send_r, rs_r) if to_right else (send_l, rs_l)

            @pl.when(jnp.logical_and(jnp.logical_and(i >= 0, i < groups), jnp.logical_and(far <= s, far < last)))
            def _(to_right=to_right, far=far, owner=owner, buf=buf, held=held):
                @pl.when(i > 0)
                def _():
                    rs_copy(i - 1, s, to_right).wait_send()

                cur = lax.rem(i, PART_RING)
                own = pl.ds(pl.multiple_of(owner * rows, rows), rows)
                if s == 0:
                    buf[s] = part[cur, own, :].astype(BF16)
                else:
                    @pl.when(far == 0)
                    def _():
                        buf[s] = part[cur, own, :].astype(BF16)

                    @pl.when(far > 0)
                    def _():
                        rs_copy(i, s - 1, to_right).wait_recv()
                        buf[s] = (part[cur, own, :] + held[lax.rem(i, RS_RING), s - 1].astype(F32)).astype(BF16)

                rs_copy(i, s, to_right).start()

    def ag_own(i, slot, to_right):
        src = gx_buf.at[slot]
        dst = gx_hbm.at[tile_rows(i, z), :]
        if to_right:
            return remote(src, dst, ag0_r.at[slot], agr_r.at[i, 0], right)
        return remote(src, dst, ag0_l.at[slot], agr_l.at[i, 0], left)

    def own_copy(i, slot):
        return pltpu.make_async_copy(gx_buf.at[slot], gx_hbm.at[tile_rows(i, z), :], own_sem.at[slot])

    def ag_forward(i, a, to_right):
        owner = z - a if to_right else z + a
        tile = gx_hbm.at[tile_rows(i, owner), :]
        if to_right:
            return remote(tile, tile, agf_r.at[a], agr_r.at[i, a], right)
        return remote(tile, tile, agf_l.at[a], agr_l.at[i, a], left)

    def ag_wait(i, a, to_right):
        tile = gx_hbm.at[tile_rows(i, 0), :]
        sem = agr_r.at[i, a] if to_right else agr_l.at[i, a]
        remote(tile, tile, agf_r.at[a], sem, right).wait_recv()

    def ag_step(i, a):
        for to_right in (True, False):
            far = z if to_right else last - z

            @pl.when(jnp.logical_and(jnp.logical_and(i >= 0, i < groups), far >= a))
            def _(to_right=to_right, far=far):
                ag_wait(i, a - 1, to_right)
                if a < slots:
                    @pl.when(far < last)
                    def _():
                        @pl.when(i > 0)
                        def _():
                            ag_forward(i - 1, a, to_right).wait_send()

                        ag_forward(i, a, to_right).start()

    def ag_first(i, slot):
        own_copy(i, slot).start()
        for to_right in (True, False):
            far = z if to_right else last - z

            @pl.when(far < last)
            def _(to_right=to_right):
                ag_own(i, slot, to_right).start()

    def ag_first_done(i, slot):
        own_copy(i, slot).wait()
        for to_right in (True, False):
            far = z if to_right else last - z

            @pl.when(far < last)
            def _(to_right=to_right):
                ag_own(i, slot, to_right).wait_send()

    def partial_norm(i):
        cur = lax.rem(i, PART_RING)
        g = group_rows(i)
        for c in range(0, d_model, chunk):
            cols = slice(c, c + chunk)
            part[cur, :, cols] = (
                dot_nt(dq_all[g, :], wq_ref[cols, :]) + dot_nt(dkv_all[0, g, :], wk_ref[cols, :]) + dot_nt(dkv_all[1, g, :], wv_ref[cols, :])
            )

    def project_out(cur):
        for c in range(0, d_model, chunk):
            cols = slice(c, c + chunk)
            acc = x_in[cur, :, cols].astype(F32)
            for t in range(tp):
                acc += dot_nn(o_in[cur, t], wo_ref[t, :, cols])
            y_buf[cur, :, cols] = acc.astype(BF16)

    def finalize(i):
        slot = lax.rem(i, 2)
        own = pl.ds(pl.multiple_of(z * rows, rows), rows)
        tot[...] = part[lax.rem(i, PART_RING), own, :]

        @pl.when(z > 0)
        def _():
            rs_copy(i, slots - 1, True).wait_recv()
            tot[...] += rs_r[lax.rem(i, RS_RING), slots - 1].astype(F32)

        @pl.when(z < last)
        def _():
            rs_copy(i, slots - 1, False).wait_recv()
            tot[...] += rs_l[lax.rem(i, RS_RING), slots - 1].astype(F32)

        @pl.when(i > 1)
        def _():
            ag_first_done(i - 2, slot)

        for copy in final_inputs(i, slot):
            copy.wait()
        x = xo_in[slot].astype(F32)
        centred = x - jnp.mean(x, axis=-1, keepdims=True)
        inv_std = lax.rsqrt(jnp.mean(centred * centred, axis=-1, keepdims=True) + LN_EPS)
        x_hat = centred * inv_std
        dn = tot[...]
        gg_ref[...] += jnp.sum(dn * x_hat, axis=0, keepdims=True)
        d_hat = dn * gain_ref[...]
        dx = inv_std * (d_hat - jnp.mean(d_hat, axis=-1, keepdims=True) - x_hat * jnp.mean(d_hat * x_hat, axis=-1, keepdims=True))
        gx_buf[slot] = (dyo_in[slot].astype(F32) + dx).astype(BF16)
        ag_first(i, slot)

    def block_of(t):
        return 2 * lax.div(t, 2) + jnp.where(lax.rem(t, 2) == 0, 1 - core, core)

    def job_loads(t, slot):
        cols = pl.ds(pl.multiple_of(block_of(t) * width, width), width)
        return [
            pltpu.make_async_copy(n_hbm.at[:, cols], n_in.at[slot], job_sem.at[slot, 0]),
            pltpu.make_async_copy(dy_hbm.at[:, cols], dy_in.at[slot], job_sem.at[slot, 1]),
        ]

    def away_copy(p):
        ring = lax.rem(p, 2)
        return remote(away, part_in.at[ring], away_send.at[0], away_recv.at[ring], partner)

    def job_block(t, put):
        slot = lax.rem(t, 2)
        n_t = n_in[slot].T
        put(0, hidden, dot_nn(n_t, dq_all[...]))
        put(hidden, hidden, dot_nn(n_t, dkv_all[0]))
        put(2 * hidden, hidden, dot_nn(n_t, dkv_all[1]))
        for k in range(hidden // width):
            put(3 * hidden + k * width, width, dot_nn(o_t[k * width:(k + 1) * width, :], dy_in[slot]))

    def mine_to_own(p, slot):
        return pltpu.make_async_copy(mine.at[slot], ga_hbm.at[2 * p + core], mine_own.at[slot])

    def mine_to_part(p, slot):
        return remote(mine.at[slot], ga_hbm.at[2 * p + core], mine_part.at[slot], ga_recv.at[p], partner)

    def mine_to_chip(p, slot):
        return remote(mine.at[slot], gb_hbm.at[2 * p + core], mine_chip.at[slot], chip_recv.at[p], peer)

    def mine_done(p, slot):
        mine_to_own(p, slot).wait()
        mine_to_part(p, slot).wait_send()
        mine_to_chip(p, slot).wait_send()

    def chip_forward(p):
        b = 2 * p + core
        return remote(gb_hbm.at[b], gb_hbm.at[b], gb_send.at[p], gb_recv.at[p], partner)

    def job(t):
        p = lax.div(t, 2)
        for copy in job_loads(t, lax.rem(t, 2)):
            copy.wait()

        @pl.when(t + 1 < blocks)
        def _():
            for copy in job_loads(t + 1, 1 - lax.rem(t, 2)):
                copy.start()

        @pl.when(lax.rem(t, 2) == 0)
        def _():
            @pl.when(p > 0)
            def _():
                away_copy(p - 1).wait_send()

            def put(at, size, value):
                away[:, at:at + size] = value

            job_block(t, put)
            away_copy(p).start()

        @pl.when(lax.rem(t, 2) == 1)
        def _():
            slot = lax.rem(p, 2)
            away_copy(p).wait_recv()

            @pl.when(p > 1)
            def _():
                mine_done(p - 2, slot)

            def put(at, size, value):
                mine[slot, :, at:at + size] = (value + part_in[slot, :, at:at + size]).astype(BF16)

            job_block(t, put)
            mine_to_chip(p, slot).start()
            mine_to_part(p, slot).start()
            mine_to_own(p, slot).start()

    gg_ref[...] = jnp.zeros_like(gg_ref)
    o_loads = [pltpu.make_async_copy(o_hbm.at[z, :, k * width:(k + 1) * width], n_in.at[k], job_sem.at[k, 0]) for k in range(hidden // width)]
    for copy in o_loads:
        copy.start()
    for copy in inputs(0, 0):
        copy.start()
    for copy in out_loads:
        copy.start()
    me = z * cp + r

    def gain_copy(dt, dc):
        to = {"tp": lax.rem(z + dt, tp), "cp": lax.rem(r + dc, cp)}
        return remote(gain_all.at[me], gain_all.at[me], gs_sem.at[dt * cp + dc], gr_sem.at[me], to)

    def gain_wait(dt, dc):
        sender = lax.rem(z + dt, tp) * cp + lax.rem(r + dc, cp)
        remote(gain_all.at[sender], gain_all.at[sender], gs_sem.at[0], gr_sem.at[sender], right).wait_recv()

    for copy in weight_loads:
        copy.wait()

    def step(i, carry):
        cur = lax.rem(i, 2)

        @pl.when(i < groups)
        def _():
            partial_norm(i)

        for a in range(1, slots + 1):
            ag_step(i - slots - a, a)
        for s in reversed(range(slots)):
            rs_send(i - s, s)

        @pl.when(jnp.logical_and(i >= slots, i < groups + slots))
        def _():
            finalize(i - slots)

        @pl.when(i == groups + slots - 1)
        def _():
            gain_all[me] = gg_ref[...]
            for dt, dc in peers:
                gain_copy(dt, dc).start()

        @pl.when(jnp.logical_and(i >= slots - 1, i < groups + slots - 1))
        def _():
            for copy in final_inputs(i - slots + 1, lax.rem(i - slots + 1, 2)):
                copy.start()

        @pl.when(i == 0)
        def _():
            for copy in out_loads:
                copy.wait()
            for k, copy in enumerate(o_loads):
                copy.wait()
                o_t[k * width:(k + 1) * width, :] = n_in[k].T
            for copy in job_loads(0, 0):
                copy.start()

        @pl.when(i < groups)
        def _():
            for copy in inputs(i, cur):
                copy.wait()

            @pl.when(i + 1 < groups)
            def _():
                for copy in inputs(i + 1, 1 - cur):
                    copy.start()

            @pl.when(i >= 2)
            def _():
                y_copy(i - 2, cur).wait()

            project_out(cur)
            y_copy(i, cur).start()

        @pl.when(jnp.logical_and(i >= 1, i <= blocks))
        def _():
            job(i - 1)

        @pl.when(jnp.logical_and(lax.rem(i, 2) == 1, jnp.logical_and(i >= FORWARD_LAG, i < FORWARD_LAG + 2 * pairs)))
        def _():
            p = lax.div(i - FORWARD_LAG, 2)
            mine_to_chip(p, 0).wait_recv()
            chip_forward(p).start()

        return carry

    lax.fori_loop(0, max(groups + 2 * slots, 2 * pairs + FORWARD_LAG - 1), step, 0)

    for i in (groups - 2, groups - 1):
        y_copy(i, i % 2).wait()
        ag_first_done(i, i % 2)
    for to_right in (True, False):
        far = z if to_right else last - z
        for s in range(slots):
            @pl.when(jnp.logical_and(far <= s, far < last))
            def _(s=s, to_right=to_right):
                rs_copy(groups - 1, s, to_right).wait_send()
        for a in range(1, slots):
            @pl.when(jnp.logical_and(far >= a, far < last))
            def _(a=a, to_right=to_right):
                ag_forward(groups - 1, a, to_right).wait_send()
    away_copy(pairs - 1).wait_send()
    for p in range(max(0, pairs - 2), pairs):
        mine_done(p, p % 2)
    for p in range(pairs):
        chip_forward(p).wait_send()
        chip_forward(p).wait_recv()
        mine_to_part(p, 0).wait_recv()
    for dt, dc in peers:
        gain_wait(dt, dc)
        gain_copy(dt, dc).wait_send()
    total = gain_all[0]
    for j in range(1, tp * cp):
        total += gain_all[j]
    gg_ref[...] = total


def backward_norm(dq, dkv, x, dy, o_all, normed, wq, wk, wv, wo_all, gain, rows, tp, cp):
    tokens, hidden = dq.shape
    d_model = x.shape[1]
    span = tp * rows
    groups = tokens // span
    slots = tp - 1
    width = WIDTH
    blocks = d_model // width
    pairs = blocks // 2
    hbm = pl.BlockSpec(memory_space=pl.ANY)
    vmem = pl.BlockSpec(memory_space=pltpu.VMEM)
    dma = pltpu.SemaphoreType.DMA
    bf = lambda *shape: pltpu.VMEM(shape, BF16)
    f32 = lambda *shape: pltpu.VMEM(shape, F32)
    return pl.pallas_call(
        functools.partial(back_kernel, groups, rows, tp, cp),
        in_specs=[hbm] * 10 + [vmem],
        out_specs=[hbm, hbm, hbm, hbm, vmem],
        out_shape=[
            jax.ShapeDtypeStruct((tokens, d_model), BF16),
            jax.ShapeDtypeStruct((tokens, d_model), BF16),
            jax.ShapeDtypeStruct((blocks, width, 4 * hidden), BF16),
            jax.ShapeDtypeStruct((blocks, width, 4 * hidden), BF16),
            jax.ShapeDtypeStruct((1, d_model), F32),
        ],
        scratch_shapes=[
            bf(d_model, hidden), bf(d_model, hidden), bf(d_model, hidden), bf(tp, hidden, d_model),
            bf(tokens, hidden), bf(2, tokens, hidden), bf(hidden, tokens),
            f32(PART_RING, span, d_model), bf(RS_RING, slots, rows, d_model), bf(RS_RING, slots, rows, d_model),
            bf(slots, rows, d_model), bf(slots, rows, d_model), f32(rows, d_model), bf(2, rows, d_model),
            bf(2, tp, span, hidden), bf(2, span, d_model), bf(2, rows, d_model), bf(2, rows, d_model), bf(2, span, d_model),
            bf(2, tokens, width), bf(2, tokens, width),
            f32(width, 4 * hidden), f32(2, width, 4 * hidden), bf(2, width, 4 * hidden), f32(tp * cp, 1, d_model),
            dma((6,)), dma((2, 2)), dma((2, 2)), dma((2, 2)), dma((2,)), dma((2,)),
            dma((slots,)), dma((slots,)), dma((RS_RING, slots)), dma((RS_RING, slots)),
            dma((2,)), dma((2,)), dma((slots,)), dma((slots,)), dma((groups, slots)), dma((groups, slots)),
            dma((1,)), dma((2,)), dma((2,)), dma((2,)), dma((2,)), dma((pairs,)), dma((pairs,)), dma((pairs,)), dma((pairs,)),
            dma((tp * cp,)), dma((tp * cp,)),
        ],
        compiler_params=pltpu.CompilerParams(collective_id=0, has_side_effects=True, vmem_limit_bytes=63 << 20),
        cost_estimate=pl.CostEstimate(flops=22 * tokens * hidden * d_model, bytes_accessed=16 * tokens * d_model, transcendentals=0),
        name="backward_norm",
    )(dq, dkv, x, dy, o_all, normed, wq, wk, wv, wo_all, gain)


def finish_kernel(y_ref, gx_ref, ga_ref, gb_ref, yo_ref, gxo_ref, wq_ref, wk_ref, wv_ref, wo_ref):
    yo_ref[...] = y_ref[...]
    gxo_ref[...] = gx_ref[...]
    width = ga_ref.shape[1]
    hidden = wq_ref.shape[1]
    for k, ref in enumerate((wq_ref, wk_ref, wv_ref)):
        cols = slice(k * hidden, (k + 1) * hidden)
        ref[...] = ga_ref[0, :, cols].astype(F32) + gb_ref[0, :, cols].astype(F32)
    for k in range(hidden // width):
        cols = slice(3 * hidden + k * width, 3 * hidden + (k + 1) * width)
        wo_ref[k * width:(k + 1) * width, :] = ga_ref[0, :, cols].astype(F32) + gb_ref[0, :, cols].astype(F32)


def finish(y, gx, ga, gb):
    tokens, d_model = y.shape
    blocks, width, packed = ga.shape
    hidden = packed // 4
    rows = tokens // blocks
    tile = pl.BlockSpec((rows, d_model), lambda j: (j, 0))
    block = pl.BlockSpec((1, width, packed), lambda j: (j, 0, 0))
    wide = pl.BlockSpec((width, hidden), lambda j: (j, 0))
    return pl.pallas_call(
        finish_kernel,
        grid=(blocks,),
        in_specs=[tile, tile, block, block],
        out_specs=[tile, tile, wide, wide, wide, pl.BlockSpec((hidden, width), lambda j: (0, j))],
        out_shape=[jax.ShapeDtypeStruct((tokens, d_model), BF16)] * 2 + [jax.ShapeDtypeStruct((d_model, hidden), F32)] * 3 + [jax.ShapeDtypeStruct((hidden, d_model), F32)],
        compiler_params=pltpu.CompilerParams(dimension_semantics=("arbitrary",), vmem_limit_bytes=48 << 20),
        cost_estimate=pl.CostEstimate(flops=8 * d_model * hidden, bytes_accessed=8 * tokens * d_model + 32 * d_model * hidden, transcendentals=0),
        name="finish",
    )(y, gx, ga, gb)


def solution(mesh):
    cp_size = mesh.shape["cp"]
    tp_size = mesh.shape["tp"]

    def device_step(x_in, segment_ids, positions, w_query, w_key, w_value, w_out, norm_gain, grad_out):
        batch, seq, d_model = x_in.shape
        tokens = batch * seq
        rank = lax.axis_index("cp")
        x = x_in.reshape(tokens, d_model)
        dy = grad_out.reshape(tokens, d_model)

        inv_freq = ROPE_THETA ** (-jnp.arange(0, HEAD_DIM, 2).astype(F32) / HEAD_DIM)
        angles = positions.reshape(tokens, 1).astype(F32) * jnp.repeat(inv_freq, 2)[None, :]
        cos_t, sin_t = jnp.cos(angles), jnp.sin(angles)
        start = (rank * seq + jnp.arange(seq, dtype=jnp.int32))[None, :] - positions

        gain = norm_gain.reshape(1, d_model)
        normed, o_all, dq, dkv, w_all = front(x, dy, w_query, w_key, w_value, w_out, cos_t, sin_t, start.reshape(batch, 1, seq), gain, seq, tp_size, cp_size)
        grad_x, y_out, sum_a, sum_b, grad_gain = backward_norm(dq, dkv, x, dy, o_all, normed, w_query, w_key, w_value, w_all, gain, ROWS, tp_size, cp_size)
        grad_gain = grad_gain.reshape(d_model)
        y_out, grad_x, grad_wq, grad_wk, grad_wv, grad_wo = finish(y_out, grad_x, sum_a, sum_b)
        return y_out.reshape(x_in.shape), grad_x.reshape(x_in.shape), grad_gain, grad_wq, grad_wk, grad_wv, grad_wo

    in_specs = (P("dp", "cp", None), P("dp", "cp"), P("dp", "cp"), P(None, "tp"), P(None, "tp"), P(None, "tp"), P("tp", None), P(None), P("dp", "cp", None))
    out_specs = (P("dp", "cp", None), P("dp", "cp", None), P("dp"), P("dp", "tp"), P("dp", "tp"), P("dp", "tp"), P(("dp", "tp"), None))
    return jax.shard_map(device_step, mesh=mesh, in_specs=in_specs, out_specs=out_specs, check_vma=False)
```

```python
import functools
import math

import jax
import jax.numpy as jnp
from jax import lax
from jax.experimental import pallas as pl
from jax.experimental.pallas import tpu as pltpu
from jax.sharding import PartitionSpec as P

HEAD_DIM = 128
ROPE_THETA = 8000000.0
LN_EPS = 1e-5
NEG_BIG = -1e30
SCALE = HEAD_DIM ** -0.5
EXP2_SCALE = SCALE * math.log2(math.e)
F32 = jnp.float32
BF16 = jnp.bfloat16
NT = (((1,), (1,)), ((), ()))


def dot_nn(a, b):
    return jnp.dot(a, b, preferred_element_type=F32)


def dot_nt(a, b):
    return lax.dot_general(a, b, NT, preferred_element_type=F32)


def dot_tn(a, b):
    return lax.dot_general(a, b, (((0,), (0,)), ((), ())), preferred_element_type=F32)


def swap_pairs(t, sign):
    lane = lax.broadcasted_iota(jnp.int32, t.shape, 1)
    even = (lane % 2) == 0
    up = pltpu.roll(t, HEAD_DIM - 1, 1)
    down = pltpu.roll(t, 1, 1)
    return jnp.where(even, -up, down) if sign > 0 else jnp.where(even, up, -down)


def rope(t, cos_t, sin_t, sign):
    return t * cos_t + swap_pairs(t, sign) * sin_t


def put_rope(dst, raw, cos_t, sin_t):
    for h in range(raw.shape[1] // HEAD_DIM):
        cols = slice(h * HEAD_DIM, (h + 1) * HEAD_DIM)
        dst[:, cols] = rope(raw[:, cols], cos_t, sin_t, 1.0).astype(BF16)


MESH = pl.DeviceIdType.MESH
SUB = 128
ROWS = 32
WIDTH = 256
RELAY_LAG = 2
CHIP_BUFS = 3
W_TWIN = 1
W_PARTNER = 4


def front_kernel(batch, seq, tp, cp, x_hbm, dy_hbm, wq_hbm, wk_hbm, wv_hbm, wo_hbm, cos_ref, sin_ref, start_ref, gain_ref,
                 n_hbm, o_all, dq_hbm, dkv_hbm, w_all,
                 big, wo_ref, q_row, do_row, a_in, b_in, kv_own, kvr, s_scr, dp_scr, m_scr, l_scr, d_scr, ot_scr, dqt_scr,
                 o_buf, dq_buf, g_part, g_chip, g_far, xin, part_in,
                 w_sem, wl_sem, wz_send, wz_recv, wx_send, wx_recv, wp_send, wp_recv, wf_send, wf_recv,
                 tile_sem, n_sem, kvs_part, kvs_chip, kvs_far, kv_recv, o_local, o_send, o_recv, relay_send, dq_sem,
                 far_send, part_send, chip_send, x_recv, part_recv, dkv_sem):
    z = lax.axis_index("tp")
    r = lax.axis_index("cp")
    dp = lax.axis_index("dp")
    core = lax.rem(r, 2)
    chip = lax.div(r, 2)
    d_model = x_hbm.shape[1]
    hidden = wq_hbm.shape[1]
    heads = hidden // HEAD_DIM
    first_chip, second_chip = chip == 0, chip == 1
    first_core, second_core = core == 0, core == 1
    partner = {"cp": r + 1 - 2 * core}
    peer = {"cp": r + 2 - 4 * chip}
    twin = {"dp": 1 - dp}

    weight_loads = [pltpu.make_async_copy(src, dst, w_sem.at[k]) for k, (src, dst) in enumerate(((wk_hbm, big.at[0]), (wv_hbm, big.at[1]), (wq_hbm, big.at[2]), (wo_hbm, wo_ref)))]
    for copy in weight_loads:
        copy.start()

    tile = a_in.shape[1]
    per_row = seq // tile
    tiles = batch * per_row

    def tile_rows(t):
        return pl.ds(pl.multiple_of(t * tile, tile), tile)

    def row(b):
        return pl.ds(pl.multiple_of(b * seq, seq), seq)

    def x_load(t, par):
        return pltpu.make_async_copy(x_hbm.at[tile_rows(t), :], a_in.at[par], tile_sem.at[par, 0])

    def n_load(t, par):
        return pltpu.make_async_copy(n_hbm.at[tile_rows(t), :], a_in.at[par], tile_sem.at[par, 0])

    def dy_load(t, par):
        return pltpu.make_async_copy(dy_hbm.at[tile_rows(t), :], b_in.at[par], tile_sem.at[par, 1])

    def n_store(t, par):
        return pltpu.make_async_copy(b_in.at[par], n_hbm.at[tile_rows(t), :], n_sem.at[par])

    x_load(0, 0).start()

    barrier = pltpu.get_barrier_semaphore()
    for dev in [partner, peer, twin] + [{"tp": lax.rem(z + dt, tp)} for dt in range(1, tp)]:
        pl.semaphore_signal(barrier, inc=1, device_id=dev, device_id_type=MESH)
    pl.semaphore_wait(barrier, tp + 2)

    def remote(src, dst, ssem, rsem, dev):
        return pltpu.make_async_remote_copy(src_ref=src, dst_ref=dst, send_sem=ssem, recv_sem=rsem, device_id=dev, device_id_type=MESH)

    share = hidden // 4

    def share_rows(c, g):
        return pl.ds(pl.multiple_of((2 * c + g) * share, share), share)

    mine, twins = share_rows(core, dp), share_rows(core, 1 - dp)

    def wz_copy(d):
        return remote(wo_hbm.at[mine, :], w_all.at[z, mine, :], wz_send.at[d], wz_recv.at[z], {"tp": lax.rem(z + d, tp)})

    def wz_wait(d):
        src = lax.rem(z + d, tp)
        remote(wo_hbm.at[mine, :], w_all.at[src, mine, :], wz_send.at[d], wz_recv.at[src], partner).wait_recv()

    def w_slice(d, rows):
        return w_all.at[lax.rem(z + d, tp), rows, :]

    def wx_copy(d):
        return remote(w_slice(d, mine), w_slice(d, mine), wx_send.at[d], wx_recv.at[d], twin)

    def wp_copy(d):
        return remote(w_slice(d, mine), w_slice(d, mine), wp_send.at[d], wp_recv.at[d], partner)

    def wf_copy(d):
        return remote(w_slice(d, twins), w_slice(d, twins), wf_send.at[d], wf_recv.at[d], partner)

    for d in range(1, tp):
        wz_copy(d).start()

    def kv_to_partner(b):
        return remote(kv_own.at[b], kvr.at[0, b], kvs_part.at[b], kv_recv.at[0, b], partner)

    def kv_to_chip(b):
        return remote(kv_own.at[b], kvr.at[1, b], kvs_chip.at[b], kv_recv.at[1, b], peer)

    def kv_forward(b):
        return remote(kvr.at[1, b], kvr.at[2, b], kvs_far.at[b], kv_recv.at[2, b], partner)

    for copy in weight_loads:
        copy.wait()
    w_local = pltpu.make_async_copy(wo_ref, w_all.at[z], wl_sem.at[0])
    w_local.start()

    def key_tile(t, carry):
        par = lax.rem(t, 2)
        x_load(t, par).wait()

        @pl.when(t + 1 < tiles)
        def _():
            x_load(t + 1, 1 - par).start()

        @pl.when(t >= 2)
        def _():
            n_store(t - 2, par).wait()

        x = a_in[par].astype(F32)
        centred = x - jnp.mean(x, axis=-1, keepdims=True)
        inv_std = lax.rsqrt(jnp.mean(centred * centred, axis=-1, keepdims=True) + LN_EPS)
        normed = ((centred * inv_std) * gain_ref[...]).astype(BF16)
        b_in[par] = normed
        n_store(t, par).start()
        b = lax.div(t, per_row)
        part = lax.rem(t, per_row)
        inside = pl.ds(pl.multiple_of(part * tile, tile), tile)
        rows = tile_rows(t)
        put_rope(kv_own.at[b, 0, inside, :], dot_nn(normed, big[0]), cos_ref[rows, :], sin_ref[rows, :])
        kv_own[b, 1, inside, :] = dot_nn(normed, big[1]).astype(BF16)

        @pl.when(part == per_row - 1)
        def _():
            @pl.when(first_chip)
            def _():
                kv_to_chip(b).start()

            @pl.when(first_core)
            def _():
                kv_to_partner(b).start()

        return carry

    lax.fori_loop(0, tiles, key_tile, 0)
    for t in range(tiles - 2, tiles):
        n_store(t, t % 2).wait()

    def query_loads(t, par):
        return [n_load(t, par), dy_load(t, par)]

    for copy in query_loads(0, 0):
        copy.start()

    def query_row(i):
        for k in range(per_row):
            t = i * per_row + k
            par = lax.rem(t, 2)
            for copy in query_loads(t, par):
                copy.wait()

            @pl.when(t + 1 < tiles)
            def _(t=t, par=par):
                for copy in query_loads(t + 1, 1 - par):
                    copy.start()

            rows = tile_rows(t)
            inside = slice(k * tile, (k + 1) * tile)
            put_rope(q_row.at[inside, :], dot_nn(a_in[par], big[2]), cos_ref[rows, :], sin_ref[rows, :])
            do_row[inside, :] = dot_nt(b_in[par], wo_ref[...]).astype(BF16)

    fit = d_model // seq

    def g_own(b, which):
        k = 2 * b + which
        return big.at[lax.div(k, fit), pl.ds(pl.multiple_of(lax.rem(k, fit) * seq, seq), seq), :]

    def o_local_copy(b):
        return pltpu.make_async_copy(o_buf.at[b], o_all.at[z, row(b), :], o_local.at[b])

    def o_copy(b, k, step):
        return remote(o_buf.at[b], o_all.at[z, row(b), :], o_send.at[k, b], o_recv.at[z, b], {"tp": jnp.clip(z + step, 0, tp - 1)})

    hops = [(k, step, jnp.logical_and(z + step >= 0, z + step < tp)) for k, step in enumerate((1, -1, 2, -2))]

    def o_start(b):
        o_local_copy(b).start()
        for k, step, ok in hops:
            @pl.when(ok)
            def _(k=k, step=step):
                o_copy(b, k, step).start()

    def o_arrived(src, b):
        remote(o_all.at[src, row(b), :], o_all.at[src, row(b), :], relay_send.at[b], o_recv.at[src, b], partner).wait_recv()

    def relay_copy(b, src, dst):
        return remote(o_all.at[src, row(b), :], o_all.at[src, row(b), :], relay_send.at[b], o_recv.at[src, b], {"tp": dst})

    def relay(b):
        @pl.when(z == tp - 2)
        def _():
            o_arrived(0, b)
            relay_copy(b, 0, tp - 1).start()

        @pl.when(z == 1)
        def _():
            o_arrived(tp - 1, b)
            relay_copy(b, tp - 1, 0).start()

    def far_copy(b, par):
        return remote(g_far.at[par], xin.at[b], far_send.at[par], x_recv.at[b], partner)

    def part_copy(b, par):
        return remote(g_part.at[par], part_in.at[b], part_send.at[par], part_recv.at[b], partner)

    def chip_copy(b):
        par = lax.rem(b, CHIP_BUFS)
        return remote(g_chip.at[par], xin.at[b], chip_send.at[par], x_recv.at[b], peer)

    def chip_sum(b):
        @pl.when(second_chip)
        def _():
            par = lax.rem(b, CHIP_BUFS)
            far_copy(b, 0).wait_recv()
            g_chip[par] = (g_chip[par].astype(F32) + xin[b].astype(F32)).astype(BF16)
            chip_copy(b).start()

    def dkv_store(b, which):
        return pltpu.make_async_copy(g_own(b, which), dkv_hbm.at[which, row(b), :], dkv_sem.at[b, which])

    def key_grads(b):
        @pl.when(first_core)
        def _():
            part_copy(b, 0).wait_recv()

        @pl.when(first_chip)
        def _():
            chip_copy(b).wait_recv()

        rows = row(b)
        for which in range(2):
            own = g_own(b, which)
            for h in range(heads):
                cols = slice(h * HEAD_DIM, (h + 1) * HEAD_DIM)
                acc = own[:, cols].astype(F32)
                acc = acc + jnp.where(first_core, part_in[b, which, :, cols].astype(F32), 0.0)
                acc = (acc + jnp.where(first_chip, xin[b, which, :, cols].astype(F32), 0.0)).astype(BF16)
                if which == 0:
                    acc = rope(acc.astype(F32), cos_ref[rows, :], sin_ref[rows, :], -1.0).astype(BF16)
                own[:, cols] = acc
            dkv_store(b, which).start()

    def dq_store(b, par):
        return pltpu.make_async_copy(dq_buf.at[par], dq_hbm.at[row(b), :], dq_sem.at[par])

    subs = range(0, seq, SUB)

    def attend_row(i, par):
        rows = row(i)
        start = start_ref[i]
        chip_par = lax.rem(i, CHIP_BUFS)
        keys_of = [kv_own.at[i]] + [kvr.at[s, i] for s in range(3)]
        places = [g_part.at[par], g_chip.at[chip_par], g_far.at[par]]

        def grad(slot, which):
            return places[slot - 1].at[which] if slot else g_own(i, which)

        live = [None, second_core, second_chip, second_chip]
        piece = [r, r + 1 - 2 * core, r + 2 - 4 * chip, r + 3 - 2 * core - 4 * chip]

        def each(body):
            body(0)
            for slot in (1, 2, 3):
                pl.when(live[slot])(functools.partial(body, slot))

        def one_head(h, carry):
            cols = pl.ds(pl.multiple_of(h * HEAD_DIM, HEAD_DIM), HEAD_DIM)
            q = q_row[:, cols]
            do = do_row[:, cols]
            m_scr[...] = jnp.full(m_scr.shape, NEG_BIG, F32)
            l_scr[...] = jnp.zeros_like(l_scr)
            d_scr[...] = jnp.zeros_like(d_scr)
            ot_scr[...] = jnp.zeros_like(ot_scr)
            dqt_scr[...] = jnp.zeros_like(dqt_scr)

            def scores(slot):
                base = piece[slot] * seq
                for s in subs:
                    raw = dot_nt(keys_of[slot][0, s:s + SUB, cols], q)
                    local = lax.broadcasted_iota(jnp.int32, raw.shape, 0) + s
                    allowed = (local + base) >= start
                    if slot == 0:
                        allowed = jnp.logical_and(allowed, local <= lax.broadcasted_iota(jnp.int32, raw.shape, 1))
                    raw = jnp.where(allowed, raw, NEG_BIG)
                    s_scr[slot, s:s + SUB, :] = raw
                    m_scr[...] = jnp.maximum(m_scr[...], jnp.max(raw, axis=0, keepdims=True))

            def exps(slot):
                for s in subs:
                    e = jnp.exp2((s_scr[slot, s:s + SUB, :] - m_scr[...]) * EXP2_SCALE)
                    s_scr[slot, s:s + SUB, :] = e
                    l_scr[...] += jnp.sum(e, axis=0, keepdims=True)

            def values(slot):
                for s in subs:
                    v = keys_of[slot][1, s:s + SUB, cols]
                    prob = s_scr[slot, s:s + SUB, :] * l_scr[...]
                    low = prob.astype(BF16)
                    dp = dot_nt(v, do)
                    s_scr[slot, s:s + SUB, :] = prob
                    dp_scr[slot, s:s + SUB, :] = dp
                    d_scr[...] += jnp.sum(prob * dp, axis=0, keepdims=True)
                    grad(slot, 1)[s:s + SUB, cols] = dot_nn(low, do).astype(BF16)
                    ot_scr[...] += dot_nn(v.T, low)

            def keys(slot):
                for s in subs:
                    k = keys_of[slot][0, s:s + SUB, cols]
                    ds = (s_scr[slot, s:s + SUB, :] * (dp_scr[slot, s:s + SUB, :] - d_scr[...])).astype(BF16)
                    grad(slot, 0)[s:s + SUB, cols] = (dot_nn(ds, q) * SCALE).astype(BF16)
                    dqt_scr[...] += dot_nn(k.T, ds)

            each(scores)
            each(exps)
            l_scr[...] = 1.0 / l_scr[...]
            each(values)
            each(keys)
            o_buf[i, :, cols] = ot_scr[...].T.astype(BF16)
            dq_buf[par, :, cols] = rope(dqt_scr[...].T * SCALE, cos_ref[rows, :], sin_ref[rows, :], -1.0).astype(BF16)
            return carry

        lax.fori_loop(0, heads, one_head, 0)

    def step(i, carry):
        par = lax.rem(i, 2)
        query_row(i)

        @pl.when(second_chip)
        def _():
            kv_to_chip(i).wait_recv()
            kv_forward(i).start()

        @pl.when(second_core)
        def _():
            kv_to_partner(i).wait_recv()

        @pl.when(second_chip)
        def _():
            kv_forward(i).wait_recv()

        @pl.when(i >= 2)
        def _():
            dq_store(i - 2, par).wait()

            @pl.when(second_core)
            def _():
                part_copy(i - 2, par).wait_send()

            @pl.when(second_chip)
            def _():
                far_copy(i - 2, par).wait_send()

        @pl.when(jnp.logical_and(second_chip, i >= CHIP_BUFS))
        def _():
            chip_copy(i - CHIP_BUFS).wait_send()

        attend_row(i, par)
        o_start(i)
        dq_store(i, par).start()

        @pl.when(second_chip)
        def _():
            far_copy(i, par).start()

        @pl.when(second_core)
        def _():
            part_copy(i, par).start()

        @pl.when(i >= 1)
        def _():
            chip_sum(i - 1)

        @pl.when(i >= RELAY_LAG)
        def _():
            relay(i - RELAY_LAG)

        @pl.when(i == min(W_TWIN, batch - 1))
        def _():
            for d in range(1, tp):
                wz_wait(d)
                wx_copy(d).start()
                wp_copy(d).start()

        @pl.when(i == min(W_PARTNER, batch - 1))
        def _():
            for d in range(1, tp):
                wx_copy(d).wait_recv()
                wf_copy(d).start()

        return carry

    lax.fori_loop(0, batch, step, 0)
    chip_sum(batch - 1)
    lag = min(RELAY_LAG, batch)
    for k in range(lag):
        relay(batch - lag + k)

    def finish(b, carry):
        key_grads(b)
        return carry

    lax.fori_loop(0, batch, finish, 0)

    w_local.wait()
    for d in range(1, tp):
        wz_copy(d).wait_send()
        wx_copy(d).wait_send()
        for copy in (wp_copy(d), wf_copy(d)):
            copy.wait_send()
            copy.wait_recv()
    for b in range(batch):
        for which in range(2):
            dkv_store(b, which).wait()

        @pl.when(first_chip)
        def _(b=b):
            kv_to_chip(b).wait_send()

        @pl.when(first_core)
        def _(b=b):
            kv_to_partner(b).wait_send()

        @pl.when(second_chip)
        def _(b=b):
            kv_forward(b).wait_send()

        o_local_copy(b).wait()
        for k, step_, ok in hops:
            @pl.when(ok)
            def _(b=b, k=k, step_=step_):
                o_copy(b, k, step_).wait_send()

        @pl.when(jnp.logical_or(z == 1, z == tp - 2))
        def _(b=b):
            relay_copy(b, 0, tp - 1).wait_send()

        for src in range(tp):
            taken = jnp.logical_or(jnp.logical_and(z == tp - 2, src == 0), jnp.logical_and(z == 1, src == tp - 1))

            @pl.when(jnp.logical_and(z != src, jnp.logical_not(taken)))
            def _(b=b, src=src):
                o_arrived(src, b)

    for b in range(max(0, batch - 2), batch):
        dq_store(b, b % 2).wait()

        @pl.when(second_core)
        def _(b=b):
            part_copy(b, b % 2).wait_send()

        @pl.when(second_chip)
        def _(b=b):
            far_copy(b, b % 2).wait_send()

    for b in range(max(0, batch - CHIP_BUFS), batch):
        @pl.when(second_chip)
        def _(b=b):
            chip_copy(b).wait_send()


def front(x, dy, wq, wk, wv, wo, cos_t, sin_t, start, gain, seq, tp, cp):
    tokens, d_model = x.shape
    hidden = wq.shape[1]
    batch = tokens // seq
    tile = seq // 2
    hbm = pl.BlockSpec(memory_space=pl.ANY)
    vmem = pl.BlockSpec(memory_space=pltpu.VMEM)
    dma = pltpu.SemaphoreType.DMA
    bf = lambda *shape: pltpu.VMEM(shape, BF16)
    f32 = lambda *shape: pltpu.VMEM(shape, F32)
    return pl.pallas_call(
        functools.partial(front_kernel, batch, seq, tp, cp),
        in_specs=[hbm] * 6 + [vmem] * 4,
        out_specs=[hbm] * 5,
        out_shape=[
            jax.ShapeDtypeStruct((tokens, d_model), BF16),
            jax.ShapeDtypeStruct((tp, tokens, hidden), BF16),
            jax.ShapeDtypeStruct((tokens, hidden), BF16),
            jax.ShapeDtypeStruct((2, tokens, hidden), BF16),
            jax.ShapeDtypeStruct((tp, hidden, d_model), BF16),
        ],
        scratch_shapes=[
            bf(3, d_model, hidden), bf(hidden, d_model), bf(seq, hidden), bf(seq, hidden), bf(2, tile, d_model), bf(2, tile, d_model),
            bf(batch, 2, seq, hidden), bf(3, batch, 2, seq, hidden),
            f32(4, seq, seq), f32(4, seq, seq), f32(1, seq), f32(1, seq), f32(1, seq), f32(HEAD_DIM, seq), f32(HEAD_DIM, seq),
            bf(batch, seq, hidden), bf(2, seq, hidden),
            bf(2, 2, seq, hidden), bf(CHIP_BUFS, 2, seq, hidden), bf(2, 2, seq, hidden),
            bf(batch, 2, seq, hidden), bf(batch, 2, seq, hidden),
            dma((4,)), dma((1,)), dma((tp,)), dma((tp,)), dma((tp,)), dma((tp,)), dma((tp,)), dma((tp,)), dma((tp,)), dma((tp,)),
            dma((2, 2)), dma((2,)), dma((batch,)), dma((batch,)), dma((batch,)), dma((3, batch)),
            dma((batch,)), dma((4, batch)), dma((tp, batch)), dma((batch,)), dma((2,)),
            dma((2,)), dma((2,)), dma((CHIP_BUFS,)), dma((batch,)), dma((batch,)), dma((batch, 2)),
        ],
        compiler_params=pltpu.CompilerParams(collective_id=1, has_side_effects=True, vmem_limit_bytes=63 << 20),
        cost_estimate=pl.CostEstimate(flops=60 * tokens * seq * hidden, bytes_accessed=16 * tokens * d_model, transcendentals=4 * tokens * seq * (hidden // HEAD_DIM)),
        name="front",
    )(x, dy, wq, wk, wv, wo, cos_t, sin_t, start, gain)


PART_RING = 4
RS_RING = 5
FORWARD_LAG = 11
JOB_LAG = 5
OUT_LAG = 4
EARLY = 4


def back_kernel(groups, rows, tp, cp, dq_hbm, dkv_hbm, x_hbm, dy_hbm, o_hbm, n_hbm, wq_hbm, wk_hbm, wv_hbm, wo_hbm, gain_ref,
                gx_hbm, y_hbm, ga_hbm, gb_hbm, gg_ref,
                wq_ref, wk_ref, wv_ref, wo_ref, dq_all, dkv_all, o_t, part, rs_r, rs_l, send_r, send_l, tot, gx_buf,
                o_in, x_in, xo_in, dyo_in, y_buf, n_in, dy_in, away, part_in, mine, gain_all,
                w_sem, in_sem, fin_sem, job_sem, y_sem, own_sem, rss_r, rss_l, rsr_r, rsr_l, ag0_r, ag0_l, agf_r, agf_l, agr_r, agr_l,
                away_send, away_recv, mine_own, mine_part, mine_chip, ga_recv, chip_recv, gb_send, gb_recv, gs_sem, gr_sem):
    z = lax.axis_index("tp")
    r = lax.axis_index("cp")
    core = lax.rem(r, 2)
    chip = lax.div(r, 2)
    last = tp - 1
    slots = tp - 1
    span = tp * rows
    tokens, d_model = x_hbm.shape
    hidden = dq_hbm.shape[1]
    chunk = min(512, d_model)
    blocks = ga_hbm.shape[0]
    width = ga_hbm.shape[1]
    pairs = blocks // 2
    partner = {"cp": r + 1 - 2 * core}
    peer = {"cp": r + 2 - 4 * chip}

    head = min(EARLY, groups) * span
    weight_loads = [pltpu.make_async_copy(src, dst, w_sem.at[k]) for k, (src, dst) in enumerate((
        (dq_hbm.at[:head, :], dq_all.at[:head, :]), (dkv_hbm.at[:, :head, :], dkv_all.at[:, :head, :]), (wq_hbm, wq_ref), (wk_hbm, wk_ref), (wv_hbm, wv_ref)))]
    rest_loads = [] if head == tokens else [
        pltpu.make_async_copy(dq_hbm.at[head:, :], dq_all.at[head:, :], w_sem.at[6]),
        pltpu.make_async_copy(dkv_hbm.at[:, head:, :], dkv_all.at[:, head:, :], w_sem.at[7]),
    ]
    out_loads = [pltpu.make_async_copy(wo_hbm, wo_ref, w_sem.at[5])]
    for copy in weight_loads:
        copy.start()

    barrier = pltpu.get_barrier_semaphore()
    peers = [(dt, dc) for dt in range(tp) for dc in range(cp) if dt or dc]
    for dt, dc in peers:
        pl.semaphore_signal(barrier, inc=1, device_id={"tp": lax.rem(z + dt, tp), "cp": lax.rem(r + dc, cp)}, device_id_type=MESH)
    pl.semaphore_wait(barrier, len(peers))

    def remote(src, dst, ssem, rsem, dev):
        return pltpu.make_async_remote_copy(src_ref=src, dst_ref=dst, send_sem=ssem, recv_sem=rsem, device_id=dev, device_id_type=MESH)

    right = {"tp": jnp.where(z < last, z + 1, z)}
    left = {"tp": jnp.where(z > 0, z - 1, z)}

    def group_rows(i):
        return pl.ds(pl.multiple_of(i * span, span), span)

    def tile_rows(i, owner):
        return pl.ds(pl.multiple_of(i * span + owner * rows, rows), rows)

    def inputs(i, slot):
        g = group_rows(i)
        return [
            pltpu.make_async_copy(o_hbm.at[:, g, :], o_in.at[slot], in_sem.at[slot, 0]),
            pltpu.make_async_copy(x_hbm.at[g, :], x_in.at[slot], in_sem.at[slot, 1]),
        ]

    def final_inputs(i, slot):
        g = tile_rows(i, z)
        return [
            pltpu.make_async_copy(x_hbm.at[g, :], xo_in.at[slot], fin_sem.at[slot, 0]),
            pltpu.make_async_copy(dy_hbm.at[g, :], dyo_in.at[slot], fin_sem.at[slot, 1]),
        ]

    def y_copy(i, slot):
        return pltpu.make_async_copy(y_buf.at[slot], y_hbm.at[group_rows(i), :], y_sem.at[slot])

    def rs_copy(i, s, to_right):
        ring = lax.rem(i, RS_RING)
        if to_right:
            return remote(send_r.at[s], rs_r.at[ring, s], rss_r.at[s], rsr_r.at[ring, s], right)
        return remote(send_l.at[s], rs_l.at[ring, s], rss_l.at[s], rsr_l.at[ring, s], left)

    def rs_send(i, s):
        for to_right in (True, False):
            far = z if to_right else last - z
            owner = (z + slots - s) if to_right else (z - slots + s)
            buf, held = (send_r, rs_r) if to_right else (send_l, rs_l)

            @pl.when(jnp.logical_and(jnp.logical_and(i >= 0, i < groups), jnp.logical_and(far <= s, far < last)))
            def _(to_right=to_right, far=far, owner=owner, buf=buf, held=held):
                @pl.when(i > 0)
                def _():
                    rs_copy(i - 1, s, to_right).wait_send()

                cur = lax.rem(i, PART_RING)
                own = pl.ds(pl.multiple_of(owner * rows, rows), rows)
                if s == 0:
                    buf[s] = part[cur, own, :].astype(BF16)
                else:
                    @pl.when(far == 0)
                    def _():
                        buf[s] = part[cur, own, :].astype(BF16)

                    @pl.when(far > 0)
                    def _():
                        rs_copy(i, s - 1, to_right).wait_recv()
                        buf[s] = (part[cur, own, :] + held[lax.rem(i, RS_RING), s - 1].astype(F32)).astype(BF16)

                rs_copy(i, s, to_right).start()

    def ag_own(i, slot, to_right):
        src = gx_buf.at[slot]
        dst = gx_hbm.at[tile_rows(i, z), :]
        if to_right:
            return remote(src, dst, ag0_r.at[slot], agr_r.at[i, 0], right)
        return remote(src, dst, ag0_l.at[slot], agr_l.at[i, 0], left)

    def own_copy(i, slot):
        return pltpu.make_async_copy(gx_buf.at[slot], gx_hbm.at[tile_rows(i, z), :], own_sem.at[slot])

    def ag_forward(i, a, to_right):
        owner = z - a if to_right else z + a
        tile = gx_hbm.at[tile_rows(i, owner), :]
        if to_right:
            return remote(tile, tile, agf_r.at[a], agr_r.at[i, a], right)
        return remote(tile, tile, agf_l.at[a], agr_l.at[i, a], left)

    def ag_wait(i, a, to_right):
        tile = gx_hbm.at[tile_rows(i, 0), :]
        sem = agr_r.at[i, a] if to_right else agr_l.at[i, a]
        remote(tile, tile, agf_r.at[a], sem, right).wait_recv()

    def ag_step(i, a):
        for to_right in (True, False):
            far = z if to_right else last - z

            @pl.when(jnp.logical_and(jnp.logical_and(i >= 0, i < groups), far >= a))
            def _(to_right=to_right, far=far):
                ag_wait(i, a - 1, to_right)
                if a < slots:
                    @pl.when(far < last)
                    def _():
                        @pl.when(i > 0)
                        def _():
                            ag_forward(i - 1, a, to_right).wait_send()

                        ag_forward(i, a, to_right).start()

    def ag_first(i, slot):
        own_copy(i, slot).start()
        for to_right in (True, False):
            far = z if to_right else last - z

            @pl.when(far < last)
            def _(to_right=to_right):
                ag_own(i, slot, to_right).start()

    def ag_first_done(i, slot):
        own_copy(i, slot).wait()
        for to_right in (True, False):
            far = z if to_right else last - z

            @pl.when(far < last)
            def _(to_right=to_right):
                ag_own(i, slot, to_right).wait_send()

    def partial_norm(i):
        cur = lax.rem(i, PART_RING)
        g = group_rows(i)
        for c in range(0, d_model, chunk):
            cols = slice(c, c + chunk)
            part[cur, :, cols] = (
                dot_nt(dq_all[g, :], wq_ref[cols, :]) + dot_nt(dkv_all[0, g, :], wk_ref[cols, :]) + dot_nt(dkv_all[1, g, :], wv_ref[cols, :])
            )

    def project_out(cur):
        for c in range(0, d_model, chunk):
            cols = slice(c, c + chunk)
            acc = x_in[cur, :, cols].astype(F32)
            for t in range(tp):
                acc += dot_nn(o_in[cur, t], wo_ref[t, :, cols])
            y_buf[cur, :, cols] = acc.astype(BF16)

    def finalize(i):
        slot = lax.rem(i, 2)
        own = pl.ds(pl.multiple_of(z * rows, rows), rows)
        tot[...] = part[lax.rem(i, PART_RING), own, :]

        @pl.when(z > 0)
        def _():
            rs_copy(i, slots - 1, True).wait_recv()
            tot[...] += rs_r[lax.rem(i, RS_RING), slots - 1].astype(F32)

        @pl.when(z < last)
        def _():
            rs_copy(i, slots - 1, False).wait_recv()
            tot[...] += rs_l[lax.rem(i, RS_RING), slots - 1].astype(F32)

        @pl.when(i > 1)
        def _():
            ag_first_done(i - 2, slot)

        for copy in final_inputs(i, slot):
            copy.wait()
        x = xo_in[slot].astype(F32)
        centred = x - jnp.mean(x, axis=-1, keepdims=True)
        inv_std = lax.rsqrt(jnp.mean(centred * centred, axis=-1, keepdims=True) + LN_EPS)
        x_hat = centred * inv_std
        dn = tot[...]
        gg_ref[...] += jnp.sum(dn * x_hat, axis=0, keepdims=True)
        d_hat = dn * gain_ref[...]
        dx = inv_std * (d_hat - jnp.mean(d_hat, axis=-1, keepdims=True) - x_hat * jnp.mean(d_hat * x_hat, axis=-1, keepdims=True))
        gx_buf[slot] = (dyo_in[slot].astype(F32) + dx).astype(BF16)
        ag_first(i, slot)

    def block_of(t):
        return 2 * lax.div(t, 2) + jnp.where(lax.rem(t, 2) == 0, 1 - core, core)

    def job_loads(t, slot):
        cols = pl.ds(pl.multiple_of(block_of(t) * width, width), width)
        return [
            pltpu.make_async_copy(n_hbm.at[:, cols], n_in.at[slot], job_sem.at[slot, 0]),
            pltpu.make_async_copy(dy_hbm.at[:, cols], dy_in.at[slot], job_sem.at[slot, 1]),
        ]

    def away_copy(p):
        ring = lax.rem(p, 2)
        return remote(away, part_in.at[ring], away_send.at[0], away_recv.at[ring], partner)

    def job_block(t, put):
        slot = lax.rem(t, 2)
        n_t = n_in[slot].T
        put(0, hidden, dot_nn(n_t, dq_all[...]))
        put(hidden, hidden, dot_nn(n_t, dkv_all[0]))
        put(2 * hidden, hidden, dot_nn(n_t, dkv_all[1]))
        for k in range(hidden // width):
            put(3 * hidden + k * width, width, dot_nn(o_t[k * width:(k + 1) * width, :], dy_in[slot]))

    def mine_to_own(p, slot):
        return pltpu.make_async_copy(mine.at[slot], ga_hbm.at[2 * p + core], mine_own.at[slot])

    def mine_to_part(p, slot):
        return remote(mine.at[slot], ga_hbm.at[2 * p + core], mine_part.at[slot], ga_recv.at[p], partner)

    def mine_to_chip(p, slot):
        return remote(mine.at[slot], gb_hbm.at[2 * p + core], mine_chip.at[slot], chip_recv.at[p], peer)

    def mine_done(p, slot):
        mine_to_own(p, slot).wait()
        mine_to_part(p, slot).wait_send()
        mine_to_chip(p, slot).wait_send()

    def chip_forward(p):
        b = 2 * p + core
        return remote(gb_hbm.at[b], gb_hbm.at[b], gb_send.at[p], gb_recv.at[p], partner)

    def job(t):
        p = lax.div(t, 2)
        for copy in job_loads(t, lax.rem(t, 2)):
            copy.wait()

        @pl.when(t + 1 < blocks)
        def _():
            for copy in job_loads(t + 1, 1 - lax.rem(t, 2)):
                copy.start()

        @pl.when(lax.rem(t, 2) == 0)
        def _():
            @pl.when(p > 0)
            def _():
                away_copy(p - 1).wait_send()

            def put(at, size, value):
                away[:, at:at + size] = value

            job_block(t, put)
            away_copy(p).start()

        @pl.when(lax.rem(t, 2) == 1)
        def _():
            slot = lax.rem(p, 2)
            away_copy(p).wait_recv()

            @pl.when(p > 1)
            def _():
                mine_done(p - 2, slot)

            def put(at, size, value):
                mine[slot, :, at:at + size] = (value + part_in[slot, :, at:at + size]).astype(BF16)

            job_block(t, put)
            mine_to_chip(p, slot).start()
            mine_to_part(p, slot).start()
            mine_to_own(p, slot).start()

    gg_ref[...] = jnp.zeros_like(gg_ref)
    o_loads = [pltpu.make_async_copy(o_hbm.at[z, :, k * width:(k + 1) * width], n_in.at[k], job_sem.at[k, 0]) for k in range(hidden // width)]
    for copy in o_loads:
        copy.start()
    for copy in inputs(0, 0):
        copy.start()
    for copy in rest_loads + out_loads:
        copy.start()
    me = z * cp + r

    def gain_copy(dt, dc):
        to = {"tp": lax.rem(z + dt, tp), "cp": lax.rem(r + dc, cp)}
        return remote(gain_all.at[me], gain_all.at[me], gs_sem.at[dt * cp + dc], gr_sem.at[me], to)

    def gain_wait(dt, dc):
        sender = lax.rem(z + dt, tp) * cp + lax.rem(r + dc, cp)
        remote(gain_all.at[sender], gain_all.at[sender], gs_sem.at[0], gr_sem.at[sender], right).wait_recv()

    for copy in weight_loads:
        copy.wait()

    def step(i, carry):
        @pl.when(i == EARLY)
        def _():
            for copy in rest_loads:
                copy.wait()

        @pl.when(i < groups)
        def _():
            partial_norm(i)

        for a in range(1, slots + 1):
            ag_step(i - slots - a, a)
        for s in reversed(range(slots)):
            rs_send(i - s, s)

        @pl.when(jnp.logical_and(i >= slots, i < groups + slots))
        def _():
            finalize(i - slots)

        @pl.when(i == groups + slots - 1)
        def _():
            gain_all[me] = gg_ref[...]
            for dt, dc in peers:
                gain_copy(dt, dc).start()

        @pl.when(jnp.logical_and(i >= slots - 1, i < groups + slots - 1))
        def _():
            for copy in final_inputs(i - slots + 1, lax.rem(i - slots + 1, 2)):
                copy.start()

        @pl.when(i == JOB_LAG - 1)
        def _():
            for k, copy in enumerate(o_loads):
                copy.wait()
                o_t[k * width:(k + 1) * width, :] = n_in[k].T
            for copy in job_loads(0, 0):
                copy.start()

        @pl.when(i == OUT_LAG)
        def _():
            for copy in out_loads:
                copy.wait()

        @pl.when(jnp.logical_and(i >= OUT_LAG, i < groups + OUT_LAG))
        def _():
            j = i - OUT_LAG
            at = lax.rem(j, 2)
            for copy in inputs(j, at):
                copy.wait()

            @pl.when(j + 1 < groups)
            def _():
                for copy in inputs(j + 1, 1 - at):
                    copy.start()

            @pl.when(j >= 2)
            def _():
                y_copy(j - 2, at).wait()

            project_out(at)
            y_copy(j, at).start()

        @pl.when(jnp.logical_and(i >= JOB_LAG, i < JOB_LAG + blocks))
        def _():
            job(i - JOB_LAG)

        @pl.when(jnp.logical_and(lax.rem(i, 2) == 1, jnp.logical_and(i >= FORWARD_LAG, i < FORWARD_LAG + 2 * pairs)))
        def _():
            p = lax.div(i - FORWARD_LAG, 2)
            mine_to_chip(p, 0).wait_recv()
            chip_forward(p).start()

        return carry

    lax.fori_loop(0, max(groups + 2 * slots, groups + OUT_LAG, blocks + JOB_LAG, 2 * pairs + FORWARD_LAG - 1), step, 0)

    for i in (groups - 2, groups - 1):
        y_copy(i, i % 2).wait()
        ag_first_done(i, i % 2)
    for to_right in (True, False):
        far = z if to_right else last - z
        for s in range(slots):
            @pl.when(jnp.logical_and(far <= s, far < last))
            def _(s=s, to_right=to_right):
                rs_copy(groups - 1, s, to_right).wait_send()
        for a in range(1, slots):
            @pl.when(jnp.logical_and(far >= a, far < last))
            def _(a=a, to_right=to_right):
                ag_forward(groups - 1, a, to_right).wait_send()
    away_copy(pairs - 1).wait_send()
    for p in range(max(0, pairs - 2), pairs):
        mine_done(p, p % 2)
    for p in range(pairs):
        chip_forward(p).wait_send()
        chip_forward(p).wait_recv()
        mine_to_part(p, 0).wait_recv()
    for dt, dc in peers:
        gain_wait(dt, dc)
        gain_copy(dt, dc).wait_send()
    total = gain_all[0]
    for j in range(1, tp * cp):
        total += gain_all[j]
    gg_ref[...] = total


def backward_norm(dq, dkv, x, dy, o_all, normed, wq, wk, wv, wo_all, gain, rows, tp, cp):
    tokens, hidden = dq.shape
    d_model = x.shape[1]
    span = tp * rows
    groups = tokens // span
    slots = tp - 1
    width = WIDTH
    blocks = d_model // width
    pairs = blocks // 2
    hbm = pl.BlockSpec(memory_space=pl.ANY)
    vmem = pl.BlockSpec(memory_space=pltpu.VMEM)
    dma = pltpu.SemaphoreType.DMA
    bf = lambda *shape: pltpu.VMEM(shape, BF16)
    f32 = lambda *shape: pltpu.VMEM(shape, F32)
    return pl.pallas_call(
        functools.partial(back_kernel, groups, rows, tp, cp),
        in_specs=[hbm] * 10 + [vmem],
        out_specs=[hbm, hbm, hbm, hbm, vmem],
        out_shape=[
            jax.ShapeDtypeStruct((tokens, d_model), BF16),
            jax.ShapeDtypeStruct((tokens, d_model), BF16),
            jax.ShapeDtypeStruct((blocks, width, 4 * hidden), BF16),
            jax.ShapeDtypeStruct((blocks, width, 4 * hidden), BF16),
            jax.ShapeDtypeStruct((1, d_model), F32),
        ],
        scratch_shapes=[
            bf(d_model, hidden), bf(d_model, hidden), bf(d_model, hidden), bf(tp, hidden, d_model),
            bf(tokens, hidden), bf(2, tokens, hidden), bf(hidden, tokens),
            f32(PART_RING, span, d_model), bf(RS_RING, slots, rows, d_model), bf(RS_RING, slots, rows, d_model),
            bf(slots, rows, d_model), bf(slots, rows, d_model), f32(rows, d_model), bf(2, rows, d_model),
            bf(2, tp, span, hidden), bf(2, span, d_model), bf(2, rows, d_model), bf(2, rows, d_model), bf(2, span, d_model),
            bf(2, tokens, width), bf(2, tokens, width),
            f32(width, 4 * hidden), f32(2, width, 4 * hidden), bf(2, width, 4 * hidden), f32(tp * cp, 1, d_model),
            dma((8,)), dma((2, 2)), dma((2, 2)), dma((2, 2)), dma((2,)), dma((2,)),
            dma((slots,)), dma((slots,)), dma((RS_RING, slots)), dma((RS_RING, slots)),
            dma((2,)), dma((2,)), dma((slots,)), dma((slots,)), dma((groups, slots)), dma((groups, slots)),
            dma((1,)), dma((2,)), dma((2,)), dma((2,)), dma((2,)), dma((pairs,)), dma((pairs,)), dma((pairs,)), dma((pairs,)),
            dma((tp * cp,)), dma((tp * cp,)),
        ],
        compiler_params=pltpu.CompilerParams(collective_id=0, has_side_effects=True, vmem_limit_bytes=63 << 20),
        cost_estimate=pl.CostEstimate(flops=22 * tokens * hidden * d_model, bytes_accessed=16 * tokens * d_model, transcendentals=0),
        name="backward_norm",
    )(dq, dkv, x, dy, o_all, normed, wq, wk, wv, wo_all, gain)


def finish_kernel(y_ref, gx_ref, ga_ref, gb_ref, yo_ref, gxo_ref, wq_ref, wk_ref, wv_ref, wo_ref):
    yo_ref[...] = y_ref[...]
    gxo_ref[...] = gx_ref[...]
    width = ga_ref.shape[1]
    hidden = wq_ref.shape[1]
    for k, ref in enumerate((wq_ref, wk_ref, wv_ref)):
        cols = slice(k * hidden, (k + 1) * hidden)
        ref[...] = ga_ref[0, :, cols].astype(F32) + gb_ref[0, :, cols].astype(F32)
    for k in range(hidden // width):
        cols = slice(3 * hidden + k * width, 3 * hidden + (k + 1) * width)
        wo_ref[k * width:(k + 1) * width, :] = ga_ref[0, :, cols].astype(F32) + gb_ref[0, :, cols].astype(F32)


def finish(y, gx, ga, gb):
    tokens, d_model = y.shape
    blocks, width, packed = ga.shape
    hidden = packed // 4
    rows = tokens // blocks
    tile = pl.BlockSpec((rows, d_model), lambda j: (j, 0))
    block = pl.BlockSpec((1, width, packed), lambda j: (j, 0, 0))
    wide = pl.BlockSpec((width, hidden), lambda j: (j, 0))
    return pl.pallas_call(
        finish_kernel,
        grid=(blocks,),
        in_specs=[tile, tile, block, block],
        out_specs=[tile, tile, wide, wide, wide, pl.BlockSpec((hidden, width), lambda j: (0, j))],
        out_shape=[jax.ShapeDtypeStruct((tokens, d_model), BF16)] * 2 + [jax.ShapeDtypeStruct((d_model, hidden), F32)] * 3 + [jax.ShapeDtypeStruct((hidden, d_model), F32)],
        compiler_params=pltpu.CompilerParams(dimension_semantics=("arbitrary",), vmem_limit_bytes=48 << 20),
        cost_estimate=pl.CostEstimate(flops=8 * d_model * hidden, bytes_accessed=8 * tokens * d_model + 32 * d_model * hidden, transcendentals=0),
        name="finish",
    )(y, gx, ga, gb)


def solution(mesh):
    cp_size = mesh.shape["cp"]
    tp_size = mesh.shape["tp"]

    def device_step(x_in, segment_ids, positions, w_query, w_key, w_value, w_out, norm_gain, grad_out):
        batch, seq, d_model = x_in.shape
        tokens = batch * seq
        rank = lax.axis_index("cp")
        x = x_in.reshape(tokens, d_model)
        dy = grad_out.reshape(tokens, d_model)

        inv_freq = ROPE_THETA ** (-jnp.arange(0, HEAD_DIM, 2).astype(F32) / HEAD_DIM)
        angles = positions.reshape(tokens, 1).astype(F32) * jnp.repeat(inv_freq, 2)[None, :]
        cos_t, sin_t = jnp.cos(angles), jnp.sin(angles)
        start = (rank * seq + jnp.arange(seq, dtype=jnp.int32))[None, :] - positions

        gain = norm_gain.reshape(1, d_model)
        normed, o_all, dq, dkv, w_all = front(x, dy, w_query, w_key, w_value, w_out, cos_t, sin_t, start.reshape(batch, 1, seq), gain, seq, tp_size, cp_size)
        grad_x, y_out, sum_a, sum_b, grad_gain = backward_norm(dq, dkv, x, dy, o_all, normed, w_query, w_key, w_value, w_all, gain, ROWS, tp_size, cp_size)
        grad_gain = grad_gain.reshape(d_model)
        y_out, grad_x, grad_wq, grad_wk, grad_wv, grad_wo = finish(y_out, grad_x, sum_a, sum_b)
        return y_out.reshape(x_in.shape), grad_x.reshape(x_in.shape), grad_gain, grad_wq, grad_wk, grad_wv, grad_wo

    in_specs = (P("dp", "cp", None), P("dp", "cp"), P("dp", "cp"), P(None, "tp"), P(None, "tp"), P(None, "tp"), P("tp", None), P(None), P("dp", "cp", None))
    out_specs = (P("dp", "cp", None), P("dp", "cp", None), P("dp"), P("dp", "tp"), P("dp", "tp"), P("dp", "tp"), P(("dp", "tp"), None))
    return jax.shard_map(device_step, mesh=mesh, in_specs=in_specs, out_specs=out_specs, check_vma=False)
```

```python
import functools
import math

import jax
import jax.numpy as jnp
from jax import lax
from jax.experimental import pallas as pl
from jax.experimental.pallas import tpu as pltpu
from jax.sharding import PartitionSpec as P

HEAD_DIM = 128
ROPE_THETA = 8000000.0
LN_EPS = 1e-5
NEG_BIG = -1e30
SCALE = HEAD_DIM ** -0.5
EXP2_SCALE = SCALE * math.log2(math.e)
F32 = jnp.float32
BF16 = jnp.bfloat16
NT = (((1,), (1,)), ((), ()))


def dot_nn(a, b):
    return jnp.dot(a, b, preferred_element_type=F32)


def dot_nt(a, b):
    return lax.dot_general(a, b, NT, preferred_element_type=F32)


def dot_tn(a, b):
    return lax.dot_general(a, b, (((0,), (0,)), ((), ())), preferred_element_type=F32)


def swap_pairs(t, sign):
    lane = lax.broadcasted_iota(jnp.int32, t.shape, 1)
    even = (lane % 2) == 0
    up = pltpu.roll(t, HEAD_DIM - 1, 1)
    down = pltpu.roll(t, 1, 1)
    return jnp.where(even, -up, down) if sign > 0 else jnp.where(even, up, -down)


def rope(t, cos_t, sin_t, sign):
    return t * cos_t + swap_pairs(t, sign) * sin_t


def put_rope(dst, raw, cos_t, sin_t):
    for h in range(raw.shape[1] // HEAD_DIM):
        cols = slice(h * HEAD_DIM, (h + 1) * HEAD_DIM)
        dst[:, cols] = rope(raw[:, cols], cos_t, sin_t, 1.0).astype(BF16)


MESH = pl.DeviceIdType.MESH
SUB = 128
ROWS = 16
WIDTH = 256
RELAY_LAG = 2
CHIP_BUFS = 3
W_TWIN = 1
W_PARTNER = 4


def front_kernel(batch, seq, tp, cp, x_hbm, dy_hbm, wq_hbm, wk_hbm, wv_hbm, wo_hbm, cos_ref, sin_ref, start_ref, gain_ref,
                 n_hbm, o_all, dq_hbm, dkv_hbm, w_all,
                 big, wo_ref, q_row, do_row, a_in, b_in, kv_own, kvr, s_scr, dp_scr, m_scr, l_scr, d_scr, ot_scr, dqt_scr,
                 o_buf, dq_buf, g_part, g_chip, g_far, xin, part_in,
                 w_sem, wl_sem, wz_send, wz_recv, wx_send, wx_recv, wp_send, wp_recv, wf_send, wf_recv,
                 tile_sem, n_sem, kvs_part, kvs_chip, kvs_far, kv_recv, o_local, o_send, o_recv, relay_send, dq_sem,
                 far_send, part_send, chip_send, x_recv, part_recv, dkv_sem):
    z = lax.axis_index("tp")
    r = lax.axis_index("cp")
    dp = lax.axis_index("dp")
    core = lax.rem(r, 2)
    chip = lax.div(r, 2)
    d_model = x_hbm.shape[1]
    hidden = wq_hbm.shape[1]
    heads = hidden // HEAD_DIM
    first_chip, second_chip = chip == 0, chip == 1
    first_core, second_core = core == 0, core == 1
    partner = {"cp": r + 1 - 2 * core}
    peer = {"cp": r + 2 - 4 * chip}
    twin = {"dp": 1 - dp}

    weight_loads = [pltpu.make_async_copy(src, dst, w_sem.at[k]) for k, (src, dst) in enumerate(((wk_hbm, big.at[0]), (wv_hbm, big.at[1]), (wq_hbm, big.at[2]), (wo_hbm, wo_ref)))]
    for copy in weight_loads:
        copy.start()

    tile = a_in.shape[1]
    per_row = seq // tile
    tiles = batch * per_row

    def tile_rows(t):
        return pl.ds(pl.multiple_of(t * tile, tile), tile)

    def row(b):
        return pl.ds(pl.multiple_of(b * seq, seq), seq)

    def x_load(t, par):
        return pltpu.make_async_copy(x_hbm.at[tile_rows(t), :], a_in.at[par], tile_sem.at[par, 0])

    def n_load(t, par):
        return pltpu.make_async_copy(n_hbm.at[tile_rows(t), :], a_in.at[par], tile_sem.at[par, 0])

    def dy_load(t, par):
        return pltpu.make_async_copy(dy_hbm.at[tile_rows(t), :], b_in.at[par], tile_sem.at[par, 1])

    def n_store(t, par):
        return pltpu.make_async_copy(b_in.at[par], n_hbm.at[tile_rows(t), :], n_sem.at[par])

    x_load(0, 0).start()

    barrier = pltpu.get_barrier_semaphore()
    for dev in [partner, peer, twin] + [{"tp": lax.rem(z + dt, tp)} for dt in range(1, tp)]:
        pl.semaphore_signal(barrier, inc=1, device_id=dev, device_id_type=MESH)
    pl.semaphore_wait(barrier, tp + 2)

    def remote(src, dst, ssem, rsem, dev):
        return pltpu.make_async_remote_copy(src_ref=src, dst_ref=dst, send_sem=ssem, recv_sem=rsem, device_id=dev, device_id_type=MESH)

    share = hidden // 4

    def share_rows(c, g):
        return pl.ds(pl.multiple_of((2 * c + g) * share, share), share)

    mine, twins = share_rows(core, dp), share_rows(core, 1 - dp)

    def wz_copy(d):
        return remote(wo_hbm.at[mine, :], w_all.at[z, mine, :], wz_send.at[d], wz_recv.at[z], {"tp": lax.rem(z + d, tp)})

    def wz_wait(d):
        src = lax.rem(z + d, tp)
        remote(wo_hbm.at[mine, :], w_all.at[src, mine, :], wz_send.at[d], wz_recv.at[src], partner).wait_recv()

    def w_slice(d, rows):
        return w_all.at[lax.rem(z + d, tp), rows, :]

    def wx_copy(d):
        return remote(w_slice(d, mine), w_slice(d, mine), wx_send.at[d], wx_recv.at[d], twin)

    def wp_copy(d):
        return remote(w_slice(d, mine), w_slice(d, mine), wp_send.at[d], wp_recv.at[d], partner)

    def wf_copy(d):
        return remote(w_slice(d, twins), w_slice(d, twins), wf_send.at[d], wf_recv.at[d], partner)

    for d in range(1, tp):
        wz_copy(d).start()

    def kv_to_partner(b):
        return remote(kv_own.at[b], kvr.at[0, b], kvs_part.at[b], kv_recv.at[0, b], partner)

    def kv_to_chip(b):
        return remote(kv_own.at[b], kvr.at[1, b], kvs_chip.at[b], kv_recv.at[1, b], peer)

    def kv_forward(b):
        return remote(kvr.at[1, b], kvr.at[2, b], kvs_far.at[b], kv_recv.at[2, b], partner)

    for copy in weight_loads:
        copy.wait()
    w_local = pltpu.make_async_copy(wo_ref, w_all.at[z], wl_sem.at[0])
    w_local.start()

    def key_tile(t, carry):
        par = lax.rem(t, 2)
        x_load(t, par).wait()

        @pl.when(t + 1 < tiles)
        def _():
            x_load(t + 1, 1 - par).start()

        @pl.when(t >= 2)
        def _():
            n_store(t - 2, par).wait()

        x = a_in[par].astype(F32)
        centred = x - jnp.mean(x, axis=-1, keepdims=True)
        inv_std = lax.rsqrt(jnp.mean(centred * centred, axis=-1, keepdims=True) + LN_EPS)
        normed = ((centred * inv_std) * gain_ref[...]).astype(BF16)
        b_in[par] = normed
        n_store(t, par).start()
        b = lax.div(t, per_row)
        part = lax.rem(t, per_row)
        inside = pl.ds(pl.multiple_of(part * tile, tile), tile)
        rows = tile_rows(t)
        put_rope(kv_own.at[b, 0, inside, :], dot_nn(normed, big[0]), cos_ref[rows, :], sin_ref[rows, :])
        kv_own[b, 1, inside, :] = dot_nn(normed, big[1]).astype(BF16)

        @pl.when(part == per_row - 1)
        def _():
            @pl.when(first_chip)
            def _():
                kv_to_chip(b).start()

            @pl.when(first_core)
            def _():
                kv_to_partner(b).start()

        return carry

    lax.fori_loop(0, tiles, key_tile, 0)
    for t in range(tiles - 2, tiles):
        n_store(t, t % 2).wait()

    def query_loads(t, par):
        return [n_load(t, par), dy_load(t, par)]

    for copy in query_loads(0, 0):
        copy.start()

    def query_row(i):
        for k in range(per_row):
            t = i * per_row + k
            par = lax.rem(t, 2)
            for copy in query_loads(t, par):
                copy.wait()

            @pl.when(t + 1 < tiles)
            def _(t=t, par=par):
                for copy in query_loads(t + 1, 1 - par):
                    copy.start()

            rows = tile_rows(t)
            inside = slice(k * tile, (k + 1) * tile)
            put_rope(q_row.at[inside, :], dot_nn(a_in[par], big[2]), cos_ref[rows, :], sin_ref[rows, :])
            do_row[inside, :] = dot_nt(b_in[par], wo_ref[...]).astype(BF16)

    fit = d_model // seq

    def g_own(b, which):
        k = 2 * b + which
        return big.at[lax.div(k, fit), pl.ds(pl.multiple_of(lax.rem(k, fit) * seq, seq), seq), :]

    def o_local_copy(b):
        return pltpu.make_async_copy(o_buf.at[b], o_all.at[z, row(b), :], o_local.at[b])

    def o_copy(b, k, step):
        return remote(o_buf.at[b], o_all.at[z, row(b), :], o_send.at[k, b], o_recv.at[z, b], {"tp": jnp.clip(z + step, 0, tp - 1)})

    hops = [(k, step, jnp.logical_and(z + step >= 0, z + step < tp)) for k, step in enumerate((1, -1, 2, -2))]

    def o_start(b):
        o_local_copy(b).start()
        for k, step, ok in hops:
            @pl.when(ok)
            def _(k=k, step=step):
                o_copy(b, k, step).start()

    def o_arrived(src, b):
        remote(o_all.at[src, row(b), :], o_all.at[src, row(b), :], relay_send.at[b], o_recv.at[src, b], partner).wait_recv()

    def relay_copy(b, src, dst):
        return remote(o_all.at[src, row(b), :], o_all.at[src, row(b), :], relay_send.at[b], o_recv.at[src, b], {"tp": dst})

    def relay(b):
        @pl.when(z == tp - 2)
        def _():
            o_arrived(0, b)
            relay_copy(b, 0, tp - 1).start()

        @pl.when(z == 1)
        def _():
            o_arrived(tp - 1, b)
            relay_copy(b, tp - 1, 0).start()

    def far_copy(b, par):
        return remote(g_far.at[par], xin.at[b], far_send.at[par], x_recv.at[b], partner)

    def part_copy(b, par):
        return remote(g_part.at[par], part_in.at[b], part_send.at[par], part_recv.at[b], partner)

    def chip_copy(b):
        par = lax.rem(b, CHIP_BUFS)
        return remote(g_chip.at[par], xin.at[b], chip_send.at[par], x_recv.at[b], peer)

    def chip_sum(b):
        @pl.when(second_chip)
        def _():
            par = lax.rem(b, CHIP_BUFS)
            far_copy(b, 0).wait_recv()
            g_chip[par] = (g_chip[par].astype(F32) + xin[b].astype(F32)).astype(BF16)
            chip_copy(b).start()

    def dkv_store(b, which):
        return pltpu.make_async_copy(g_own(b, which), dkv_hbm.at[which, row(b), :], dkv_sem.at[b, which])

    def key_grads(b):
        @pl.when(first_core)
        def _():
            part_copy(b, 0).wait_recv()

        @pl.when(first_chip)
        def _():
            chip_copy(b).wait_recv()

        rows = row(b)
        for which in range(2):
            own = g_own(b, which)
            for h in range(heads):
                cols = slice(h * HEAD_DIM, (h + 1) * HEAD_DIM)
                acc = own[:, cols].astype(F32)
                acc = acc + jnp.where(first_core, part_in[b, which, :, cols].astype(F32), 0.0)
                acc = (acc + jnp.where(first_chip, xin[b, which, :, cols].astype(F32), 0.0)).astype(BF16)
                if which == 0:
                    acc = rope(acc.astype(F32), cos_ref[rows, :], sin_ref[rows, :], -1.0).astype(BF16)
                own[:, cols] = acc
            dkv_store(b, which).start()

    def dq_store(b, par):
        return pltpu.make_async_copy(dq_buf.at[par], dq_hbm.at[row(b), :], dq_sem.at[par])

    subs = range(0, seq, SUB)

    def attend_row(i, par):
        rows = row(i)
        start = start_ref[i]
        chip_par = lax.rem(i, CHIP_BUFS)
        keys_of = [kv_own.at[i]] + [kvr.at[s, i] for s in range(3)]
        places = [g_part.at[par], g_chip.at[chip_par], g_far.at[par]]

        def grad(slot, which):
            return places[slot - 1].at[which] if slot else g_own(i, which)

        live = [None, second_core, second_chip, second_chip]
        piece = [r, r + 1 - 2 * core, r + 2 - 4 * chip, r + 3 - 2 * core - 4 * chip]

        def each(body):
            body(0)
            for slot in (1, 2, 3):
                pl.when(live[slot])(functools.partial(body, slot))

        def one_head(h, carry):
            cols = pl.ds(pl.multiple_of(h * HEAD_DIM, HEAD_DIM), HEAD_DIM)
            q = q_row[:, cols]
            do = do_row[:, cols]
            m_scr[...] = jnp.full(m_scr.shape, NEG_BIG, F32)
            l_scr[...] = jnp.zeros_like(l_scr)
            d_scr[...] = jnp.zeros_like(d_scr)
            ot_scr[...] = jnp.zeros_like(ot_scr)
            dqt_scr[...] = jnp.zeros_like(dqt_scr)

            def scores(slot):
                base = piece[slot] * seq
                for s in subs:
                    raw = dot_nt(keys_of[slot][0, s:s + SUB, cols], q)
                    local = lax.broadcasted_iota(jnp.int32, raw.shape, 0) + s
                    allowed = (local + base) >= start
                    if slot == 0:
                        allowed = jnp.logical_and(allowed, local <= lax.broadcasted_iota(jnp.int32, raw.shape, 1))
                    raw = jnp.where(allowed, raw, NEG_BIG)
                    s_scr[slot, s:s + SUB, :] = raw
                    m_scr[...] = jnp.maximum(m_scr[...], jnp.max(raw, axis=0, keepdims=True))

            def exps(slot):
                for s in subs:
                    e = jnp.exp2((s_scr[slot, s:s + SUB, :] - m_scr[...]) * EXP2_SCALE)
                    s_scr[slot, s:s + SUB, :] = e
                    l_scr[...] += jnp.sum(e, axis=0, keepdims=True)

            def values(slot):
                for s in subs:
                    v = keys_of[slot][1, s:s + SUB, cols]
                    prob = s_scr[slot, s:s + SUB, :] * l_scr[...]
                    low = prob.astype(BF16)
                    dp = dot_nt(v, do)
                    s_scr[slot, s:s + SUB, :] = prob
                    dp_scr[slot, s:s + SUB, :] = dp
                    d_scr[...] += jnp.sum(prob * dp, axis=0, keepdims=True)
                    grad(slot, 1)[s:s + SUB, cols] = dot_nn(low, do).astype(BF16)
                    ot_scr[...] += dot_nn(v.T, low)

            def keys(slot):
                for s in subs:
                    k = keys_of[slot][0, s:s + SUB, cols]
                    ds = (s_scr[slot, s:s + SUB, :] * (dp_scr[slot, s:s + SUB, :] - d_scr[...])).astype(BF16)
                    grad(slot, 0)[s:s + SUB, cols] = (dot_nn(ds, q) * SCALE).astype(BF16)
                    dqt_scr[...] += dot_nn(k.T, ds)

            each(scores)
            each(exps)
            l_scr[...] = 1.0 / l_scr[...]
            each(values)
            each(keys)
            o_buf[i, :, cols] = ot_scr[...].T.astype(BF16)
            dq_buf[par, :, cols] = rope(dqt_scr[...].T * SCALE, cos_ref[rows, :], sin_ref[rows, :], -1.0).astype(BF16)
            return carry

        lax.fori_loop(0, heads, one_head, 0)

    def step(i, carry):
        par = lax.rem(i, 2)
        query_row(i)

        @pl.when(second_chip)
        def _():
            kv_to_chip(i).wait_recv()
            kv_forward(i).start()

        @pl.when(second_core)
        def _():
            kv_to_partner(i).wait_recv()

        @pl.when(second_chip)
        def _():
            kv_forward(i).wait_recv()

        @pl.when(i >= 2)
        def _():
            dq_store(i - 2, par).wait()

            @pl.when(second_core)
            def _():
                part_copy(i - 2, par).wait_send()

            @pl.when(second_chip)
            def _():
                far_copy(i - 2, par).wait_send()

        @pl.when(jnp.logical_and(second_chip, i >= CHIP_BUFS))
        def _():
            chip_copy(i - CHIP_BUFS).wait_send()

        attend_row(i, par)
        o_start(i)
        dq_store(i, par).start()

        @pl.when(second_chip)
        def _():
            far_copy(i, par).start()

        @pl.when(second_core)
        def _():
            part_copy(i, par).start()

        @pl.when(i >= 1)
        def _():
            chip_sum(i - 1)

        @pl.when(i >= RELAY_LAG)
        def _():
            relay(i - RELAY_LAG)

        @pl.when(i == min(W_TWIN, batch - 1))
        def _():
            for d in range(1, tp):
                wz_wait(d)
                wx_copy(d).start()
                wp_copy(d).start()

        @pl.when(i == min(W_PARTNER, batch - 1))
        def _():
            for d in range(1, tp):
                wx_copy(d).wait_recv()
                wf_copy(d).start()

        return carry

    lax.fori_loop(0, batch, step, 0)
    chip_sum(batch - 1)
    lag = min(RELAY_LAG, batch)
    for k in range(lag):
        relay(batch - lag + k)

    def finish(b, carry):
        key_grads(b)
        return carry

    lax.fori_loop(0, batch, finish, 0)

    w_local.wait()
    for d in range(1, tp):
        wz_copy(d).wait_send()
        wx_copy(d).wait_send()
        for copy in (wp_copy(d), wf_copy(d)):
            copy.wait_send()
            copy.wait_recv()
    for b in range(batch):
        for which in range(2):
            dkv_store(b, which).wait()

        @pl.when(first_chip)
        def _(b=b):
            kv_to_chip(b).wait_send()

        @pl.when(first_core)
        def _(b=b):
            kv_to_partner(b).wait_send()

        @pl.when(second_chip)
        def _(b=b):
            kv_forward(b).wait_send()

        o_local_copy(b).wait()
        for k, step_, ok in hops:
            @pl.when(ok)
            def _(b=b, k=k, step_=step_):
                o_copy(b, k, step_).wait_send()

        @pl.when(jnp.logical_or(z == 1, z == tp - 2))
        def _(b=b):
            relay_copy(b, 0, tp - 1).wait_send()

        for src in range(tp):
            taken = jnp.logical_or(jnp.logical_and(z == tp - 2, src == 0), jnp.logical_and(z == 1, src == tp - 1))

            @pl.when(jnp.logical_and(z != src, jnp.logical_not(taken)))
            def _(b=b, src=src):
                o_arrived(src, b)

    for b in range(max(0, batch - 2), batch):
        dq_store(b, b % 2).wait()

        @pl.when(second_core)
        def _(b=b):
            part_copy(b, b % 2).wait_send()

        @pl.when(second_chip)
        def _(b=b):
            far_copy(b, b % 2).wait_send()

    for b in range(max(0, batch - CHIP_BUFS), batch):
        @pl.when(second_chip)
        def _(b=b):
            chip_copy(b).wait_send()


def front(x, dy, wq, wk, wv, wo, cos_t, sin_t, start, gain, seq, tp, cp):
    tokens, d_model = x.shape
    hidden = wq.shape[1]
    batch = tokens // seq
    tile = seq // 2
    hbm = pl.BlockSpec(memory_space=pl.ANY)
    vmem = pl.BlockSpec(memory_space=pltpu.VMEM)
    dma = pltpu.SemaphoreType.DMA
    bf = lambda *shape: pltpu.VMEM(shape, BF16)
    f32 = lambda *shape: pltpu.VMEM(shape, F32)
    return pl.pallas_call(
        functools.partial(front_kernel, batch, seq, tp, cp),
        in_specs=[hbm] * 6 + [vmem] * 4,
        out_specs=[hbm] * 5,
        out_shape=[
            jax.ShapeDtypeStruct((tokens, d_model), BF16),
            jax.ShapeDtypeStruct((tp, tokens, hidden), BF16),
            jax.ShapeDtypeStruct((tokens, hidden), BF16),
            jax.ShapeDtypeStruct((2, tokens, hidden), BF16),
            jax.ShapeDtypeStruct((tp, hidden, d_model), BF16),
        ],
        scratch_shapes=[
            bf(3, d_model, hidden), bf(hidden, d_model), bf(seq, hidden), bf(seq, hidden), bf(2, tile, d_model), bf(2, tile, d_model),
            bf(batch, 2, seq, hidden), bf(3, batch, 2, seq, hidden),
            f32(4, seq, seq), f32(4, seq, seq), f32(1, seq), f32(1, seq), f32(1, seq), f32(HEAD_DIM, seq), f32(HEAD_DIM, seq),
            bf(batch, seq, hidden), bf(2, seq, hidden),
            bf(2, 2, seq, hidden), bf(CHIP_BUFS, 2, seq, hidden), bf(2, 2, seq, hidden),
            bf(batch, 2, seq, hidden), bf(batch, 2, seq, hidden),
            dma((4,)), dma((1,)), dma((tp,)), dma((tp,)), dma((tp,)), dma((tp,)), dma((tp,)), dma((tp,)), dma((tp,)), dma((tp,)),
            dma((2, 2)), dma((2,)), dma((batch,)), dma((batch,)), dma((batch,)), dma((3, batch)),
            dma((batch,)), dma((4, batch)), dma((tp, batch)), dma((batch,)), dma((2,)),
            dma((2,)), dma((2,)), dma((CHIP_BUFS,)), dma((batch,)), dma((batch,)), dma((batch, 2)),
        ],
        compiler_params=pltpu.CompilerParams(collective_id=1, has_side_effects=True, vmem_limit_bytes=63 << 20),
        cost_estimate=pl.CostEstimate(flops=60 * tokens * seq * hidden, bytes_accessed=16 * tokens * d_model, transcendentals=4 * tokens * seq * (hidden // HEAD_DIM)),
        name="front",
    )(x, dy, wq, wk, wv, wo, cos_t, sin_t, start, gain)


PART_RING = 4
RS_RING = 5
FORWARD_LAG = 11
JOB_LAG = 5
OUT_LAG = 4
EARLY = 4


def back_kernel(groups, rows, tp, cp, dq_hbm, dkv_hbm, x_hbm, dy_hbm, o_hbm, n_hbm, wq_hbm, wk_hbm, wv_hbm, wo_hbm, gain_ref,
                gx_hbm, y_hbm, ga_hbm, gb_hbm, gg_ref,
                wq_ref, wk_ref, wv_ref, wo_ref, dq_all, dkv_all, o_t, part, rs_r, rs_l, send_r, send_l, tot, gx_buf,
                o_in, x_in, xo_in, dyo_in, y_buf, n_in, dy_in, away, part_in, mine, gain_all,
                w_sem, in_sem, fin_sem, job_sem, y_sem, own_sem, rss_r, rss_l, rsr_r, rsr_l, ag0_r, ag0_l, agf_r, agf_l, agr_r, agr_l,
                away_send, away_recv, mine_own, mine_part, mine_chip, ga_recv, chip_recv, gb_send, gb_recv, gs_sem, gr_sem):
    z = lax.axis_index("tp")
    r = lax.axis_index("cp")
    core = lax.rem(r, 2)
    chip = lax.div(r, 2)
    last = tp - 1
    slots = tp - 1
    span = tp * rows
    tokens, d_model = x_hbm.shape
    hidden = dq_hbm.shape[1]
    chunk = min(512, d_model)
    blocks = ga_hbm.shape[0]
    width = ga_hbm.shape[1]
    pairs = blocks // 2
    partner = {"cp": r + 1 - 2 * core}
    peer = {"cp": r + 2 - 4 * chip}

    head = min(EARLY, groups) * span
    weight_loads = [pltpu.make_async_copy(src, dst, w_sem.at[k]) for k, (src, dst) in enumerate((
        (dq_hbm.at[:head, :], dq_all.at[:head, :]), (dkv_hbm.at[:, :head, :], dkv_all.at[:, :head, :]), (wq_hbm, wq_ref), (wk_hbm, wk_ref), (wv_hbm, wv_ref)))]
    rest_loads = [] if head == tokens else [
        pltpu.make_async_copy(dq_hbm.at[head:, :], dq_all.at[head:, :], w_sem.at[6]),
        pltpu.make_async_copy(dkv_hbm.at[:, head:, :], dkv_all.at[:, head:, :], w_sem.at[7]),
    ]
    out_loads = [pltpu.make_async_copy(wo_hbm, wo_ref, w_sem.at[5])]
    for copy in weight_loads:
        copy.start()

    barrier = pltpu.get_barrier_semaphore()
    peers = [(dt, dc) for dt in range(tp) for dc in range(cp) if dt or dc]
    for dt, dc in peers:
        pl.semaphore_signal(barrier, inc=1, device_id={"tp": lax.rem(z + dt, tp), "cp": lax.rem(r + dc, cp)}, device_id_type=MESH)
    pl.semaphore_wait(barrier, len(peers))

    def remote(src, dst, ssem, rsem, dev):
        return pltpu.make_async_remote_copy(src_ref=src, dst_ref=dst, send_sem=ssem, recv_sem=rsem, device_id=dev, device_id_type=MESH)

    right = {"tp": jnp.where(z < last, z + 1, z)}
    left = {"tp": jnp.where(z > 0, z - 1, z)}

    def group_rows(i):
        return pl.ds(pl.multiple_of(i * span, span), span)

    def tile_rows(i, owner):
        return pl.ds(pl.multiple_of(i * span + owner * rows, rows), rows)

    def inputs(i, slot):
        g = group_rows(i)
        return [
            pltpu.make_async_copy(o_hbm.at[:, g, :], o_in.at[slot], in_sem.at[slot, 0]),
            pltpu.make_async_copy(x_hbm.at[g, :], x_in.at[slot], in_sem.at[slot, 1]),
        ]

    def final_inputs(i, slot):
        g = tile_rows(i, z)
        return [
            pltpu.make_async_copy(x_hbm.at[g, :], xo_in.at[slot], fin_sem.at[slot, 0]),
            pltpu.make_async_copy(dy_hbm.at[g, :], dyo_in.at[slot], fin_sem.at[slot, 1]),
        ]

    def y_copy(i, slot):
        return pltpu.make_async_copy(y_buf.at[slot], y_hbm.at[group_rows(i), :], y_sem.at[slot])

    def rs_copy(i, s, to_right):
        ring = lax.rem(i, RS_RING)
        if to_right:
            return remote(send_r.at[s], rs_r.at[ring, s], rss_r.at[s], rsr_r.at[ring, s], right)
        return remote(send_l.at[s], rs_l.at[ring, s], rss_l.at[s], rsr_l.at[ring, s], left)

    def rs_send(i, s):
        for to_right in (True, False):
            far = z if to_right else last - z
            owner = (z + slots - s) if to_right else (z - slots + s)
            buf, held = (send_r, rs_r) if to_right else (send_l, rs_l)

            @pl.when(jnp.logical_and(jnp.logical_and(i >= 0, i < groups), jnp.logical_and(far <= s, far < last)))
            def _(to_right=to_right, far=far, owner=owner, buf=buf, held=held):
                @pl.when(i > 0)
                def _():
                    rs_copy(i - 1, s, to_right).wait_send()

                cur = lax.rem(i, PART_RING)
                own = pl.ds(pl.multiple_of(owner * rows, rows), rows)
                if s == 0:
                    buf[s] = part[cur, own, :].astype(BF16)
                else:
                    @pl.when(far == 0)
                    def _():
                        buf[s] = part[cur, own, :].astype(BF16)

                    @pl.when(far > 0)
                    def _():
                        rs_copy(i, s - 1, to_right).wait_recv()
                        buf[s] = (part[cur, own, :] + held[lax.rem(i, RS_RING), s - 1].astype(F32)).astype(BF16)

                rs_copy(i, s, to_right).start()

    def ag_own(i, slot, to_right):
        src = gx_buf.at[slot]
        dst = gx_hbm.at[tile_rows(i, z), :]
        if to_right:
            return remote(src, dst, ag0_r.at[slot], agr_r.at[i, 0], right)
        return remote(src, dst, ag0_l.at[slot], agr_l.at[i, 0], left)

    def own_copy(i, slot):
        return pltpu.make_async_copy(gx_buf.at[slot], gx_hbm.at[tile_rows(i, z), :], own_sem.at[slot])

    def ag_forward(i, a, to_right):
        owner = z - a if to_right else z + a
        tile = gx_hbm.at[tile_rows(i, owner), :]
        if to_right:
            return remote(tile, tile, agf_r.at[a], agr_r.at[i, a], right)
        return remote(tile, tile, agf_l.at[a], agr_l.at[i, a], left)

    def ag_wait(i, a, to_right):
        tile = gx_hbm.at[tile_rows(i, 0), :]
        sem = agr_r.at[i, a] if to_right else agr_l.at[i, a]
        remote(tile, tile, agf_r.at[a], sem, right).wait_recv()

    def ag_step(i, a):
        for to_right in (True, False):
            far = z if to_right else last - z

            @pl.when(jnp.logical_and(jnp.logical_and(i >= 0, i < groups), far >= a))
            def _(to_right=to_right, far=far):
                ag_wait(i, a - 1, to_right)
                if a < slots:
                    @pl.when(far < last)
                    def _():
                        @pl.when(i > 0)
                        def _():
                            ag_forward(i - 1, a, to_right).wait_send()

                        ag_forward(i, a, to_right).start()

    def ag_first(i, slot):
        own_copy(i, slot).start()
        for to_right in (True, False):
            far = z if to_right else last - z

            @pl.when(far < last)
            def _(to_right=to_right):
                ag_own(i, slot, to_right).start()

    def ag_first_done(i, slot):
        own_copy(i, slot).wait()
        for to_right in (True, False):
            far = z if to_right else last - z

            @pl.when(far < last)
            def _(to_right=to_right):
                ag_own(i, slot, to_right).wait_send()

    def partial_norm(i):
        cur = lax.rem(i, PART_RING)
        g = group_rows(i)
        for c in range(0, d_model, chunk):
            cols = slice(c, c + chunk)
            part[cur, :, cols] = (
                dot_nt(dq_all[g, :], wq_ref[cols, :]) + dot_nt(dkv_all[0, g, :], wk_ref[cols, :]) + dot_nt(dkv_all[1, g, :], wv_ref[cols, :])
            )

    def project_out(cur):
        for c in range(0, d_model, chunk):
            cols = slice(c, c + chunk)
            acc = x_in[cur, :, cols].astype(F32)
            for t in range(tp):
                acc += dot_nn(o_in[cur, t], wo_ref[t, :, cols])
            y_buf[cur, :, cols] = acc.astype(BF16)

    def finalize(i):
        slot = lax.rem(i, 2)
        own = pl.ds(pl.multiple_of(z * rows, rows), rows)
        tot[...] = part[lax.rem(i, PART_RING), own, :]

        @pl.when(z > 0)
        def _():
            rs_copy(i, slots - 1, True).wait_recv()
            tot[...] += rs_r[lax.rem(i, RS_RING), slots - 1].astype(F32)

        @pl.when(z < last)
        def _():
            rs_copy(i, slots - 1, False).wait_recv()
            tot[...] += rs_l[lax.rem(i, RS_RING), slots - 1].astype(F32)

        @pl.when(i > 1)
        def _():
            ag_first_done(i - 2, slot)

        for copy in final_inputs(i, slot):
            copy.wait()
        x = xo_in[slot].astype(F32)
        centred = x - jnp.mean(x, axis=-1, keepdims=True)
        inv_std = lax.rsqrt(jnp.mean(centred * centred, axis=-1, keepdims=True) + LN_EPS)
        x_hat = centred * inv_std
        dn = tot[...]
        gg_ref[...] += jnp.sum(dn * x_hat, axis=0, keepdims=True)
        d_hat = dn * gain_ref[...]
        dx = inv_std * (d_hat - jnp.mean(d_hat, axis=-1, keepdims=True) - x_hat * jnp.mean(d_hat * x_hat, axis=-1, keepdims=True))
        gx_buf[slot] = (dyo_in[slot].astype(F32) + dx).astype(BF16)
        ag_first(i, slot)

    def block_of(t):
        return 2 * lax.div(t, 2) + jnp.where(lax.rem(t, 2) == 0, 1 - core, core)

    def job_loads(t, slot):
        cols = pl.ds(pl.multiple_of(block_of(t) * width, width), width)
        return [
            pltpu.make_async_copy(n_hbm.at[:, cols], n_in.at[slot], job_sem.at[slot, 0]),
            pltpu.make_async_copy(dy_hbm.at[:, cols], dy_in.at[slot], job_sem.at[slot, 1]),
        ]

    def away_copy(p):
        ring = lax.rem(p, 2)
        return remote(away, part_in.at[ring], away_send.at[0], away_recv.at[ring], partner)

    def job_block(t, put):
        slot = lax.rem(t, 2)
        n_t = n_in[slot].T
        put(0, hidden, dot_nn(n_t, dq_all[...]))
        put(hidden, hidden, dot_nn(n_t, dkv_all[0]))
        put(2 * hidden, hidden, dot_nn(n_t, dkv_all[1]))
        for k in range(hidden // width):
            put(3 * hidden + k * width, width, dot_nn(o_t[k * width:(k + 1) * width, :], dy_in[slot]))

    def mine_to_own(p, slot):
        return pltpu.make_async_copy(mine.at[slot], ga_hbm.at[2 * p + core], mine_own.at[slot])

    def mine_to_part(p, slot):
        return remote(mine.at[slot], ga_hbm.at[2 * p + core], mine_part.at[slot], ga_recv.at[p], partner)

    def mine_to_chip(p, slot):
        return remote(mine.at[slot], gb_hbm.at[2 * p + core], mine_chip.at[slot], chip_recv.at[p], peer)

    def mine_done(p, slot):
        mine_to_own(p, slot).wait()
        mine_to_part(p, slot).wait_send()
        mine_to_chip(p, slot).wait_send()

    def chip_forward(p):
        b = 2 * p + core
        return remote(gb_hbm.at[b], gb_hbm.at[b], gb_send.at[p], gb_recv.at[p], partner)

    def job(t):
        p = lax.div(t, 2)
        for copy in job_loads(t, lax.rem(t, 2)):
            copy.wait()

        @pl.when(t + 1 < blocks)
        def _():
            for copy in job_loads(t + 1, 1 - lax.rem(t, 2)):
                copy.start()

        @pl.when(lax.rem(t, 2) == 0)
        def _():
            @pl.when(p > 0)
            def _():
                away_copy(p - 1).wait_send()

            def put(at, size, value):
                away[:, at:at + size] = value

            job_block(t, put)
            away_copy(p).start()

        @pl.when(lax.rem(t, 2) == 1)
        def _():
            slot = lax.rem(p, 2)
            away_copy(p).wait_recv()

            @pl.when(p > 1)
            def _():
                mine_done(p - 2, slot)

            def put(at, size, value):
                mine[slot, :, at:at + size] = (value + part_in[slot, :, at:at + size]).astype(BF16)

            job_block(t, put)
            mine_to_chip(p, slot).start()
            mine_to_part(p, slot).start()
            mine_to_own(p, slot).start()

    gg_ref[...] = jnp.zeros_like(gg_ref)
    o_loads = [pltpu.make_async_copy(o_hbm.at[z, :, k * width:(k + 1) * width], n_in.at[k], job_sem.at[k, 0]) for k in range(hidden // width)]
    for copy in o_loads:
        copy.start()
    for copy in inputs(0, 0):
        copy.start()
    for copy in rest_loads + out_loads:
        copy.start()
    me = z * cp + r

    def gain_copy(dt, dc):
        to = {"tp": lax.rem(z + dt, tp), "cp": lax.rem(r + dc, cp)}
        return remote(gain_all.at[me], gain_all.at[me], gs_sem.at[dt * cp + dc], gr_sem.at[me], to)

    def gain_wait(dt, dc):
        sender = lax.rem(z + dt, tp) * cp + lax.rem(r + dc, cp)
        remote(gain_all.at[sender], gain_all.at[sender], gs_sem.at[0], gr_sem.at[sender], right).wait_recv()

    for copy in weight_loads:
        copy.wait()

    def step(i, carry):
        @pl.when(i == EARLY)
        def _():
            for copy in rest_loads:
                copy.wait()

        @pl.when(i < groups)
        def _():
            partial_norm(i)

        for a in range(1, slots + 1):
            ag_step(i - slots - a, a)
        for s in reversed(range(slots)):
            rs_send(i - s, s)

        @pl.when(jnp.logical_and(i >= slots, i < groups + slots))
        def _():
            finalize(i - slots)

        @pl.when(i == groups + slots - 1)
        def _():
            gain_all[me] = gg_ref[...]
            for dt, dc in peers:
                gain_copy(dt, dc).start()

        @pl.when(jnp.logical_and(i >= slots - 1, i < groups + slots - 1))
        def _():
            for copy in final_inputs(i - slots + 1, lax.rem(i - slots + 1, 2)):
                copy.start()

        @pl.when(i == JOB_LAG - 1)
        def _():
            for k, copy in enumerate(o_loads):
                copy.wait()
                o_t[k * width:(k + 1) * width, :] = n_in[k].T
            for copy in job_loads(0, 0):
                copy.start()

        @pl.when(i == OUT_LAG)
        def _():
            for copy in out_loads:
                copy.wait()

        @pl.when(jnp.logical_and(i >= OUT_LAG, i < groups + OUT_LAG))
        def _():
            j = i - OUT_LAG
            at = lax.rem(j, 2)
            for copy in inputs(j, at):
                copy.wait()

            @pl.when(j + 1 < groups)
            def _():
                for copy in inputs(j + 1, 1 - at):
                    copy.start()

            @pl.when(j >= 2)
            def _():
                y_copy(j - 2, at).wait()

            project_out(at)
            y_copy(j, at).start()

        @pl.when(jnp.logical_and(i >= JOB_LAG, i < JOB_LAG + blocks))
        def _():
            job(i - JOB_LAG)

        @pl.when(jnp.logical_and(lax.rem(i, 2) == 1, jnp.logical_and(i >= FORWARD_LAG, i < FORWARD_LAG + 2 * pairs)))
        def _():
            p = lax.div(i - FORWARD_LAG, 2)
            mine_to_chip(p, 0).wait_recv()
            chip_forward(p).start()

        return carry

    lax.fori_loop(0, max(groups + 2 * slots, groups + OUT_LAG, blocks + JOB_LAG, 2 * pairs + FORWARD_LAG - 1), step, 0)

    for i in (groups - 2, groups - 1):
        y_copy(i, i % 2).wait()
        ag_first_done(i, i % 2)
    for to_right in (True, False):
        far = z if to_right else last - z
        for s in range(slots):
            @pl.when(jnp.logical_and(far <= s, far < last))
            def _(s=s, to_right=to_right):
                rs_copy(groups - 1, s, to_right).wait_send()
        for a in range(1, slots):
            @pl.when(jnp.logical_and(far >= a, far < last))
            def _(a=a, to_right=to_right):
                ag_forward(groups - 1, a, to_right).wait_send()
    away_copy(pairs - 1).wait_send()
    for p in range(max(0, pairs - 2), pairs):
        mine_done(p, p % 2)
    for p in range(pairs):
        chip_forward(p).wait_send()
        chip_forward(p).wait_recv()
        mine_to_part(p, 0).wait_recv()
    for dt, dc in peers:
        gain_wait(dt, dc)
        gain_copy(dt, dc).wait_send()
    total = gain_all[0]
    for j in range(1, tp * cp):
        total += gain_all[j]
    gg_ref[...] = total


def backward_norm(dq, dkv, x, dy, o_all, normed, wq, wk, wv, wo_all, gain, rows, tp, cp):
    tokens, hidden = dq.shape
    d_model = x.shape[1]
    span = tp * rows
    groups = tokens // span
    slots = tp - 1
    width = WIDTH
    blocks = d_model // width
    pairs = blocks // 2
    hbm = pl.BlockSpec(memory_space=pl.ANY)
    vmem = pl.BlockSpec(memory_space=pltpu.VMEM)
    dma = pltpu.SemaphoreType.DMA
    bf = lambda *shape: pltpu.VMEM(shape, BF16)
    f32 = lambda *shape: pltpu.VMEM(shape, F32)
    return pl.pallas_call(
        functools.partial(back_kernel, groups, rows, tp, cp),
        in_specs=[hbm] * 10 + [vmem],
        out_specs=[hbm, hbm, hbm, hbm, vmem],
        out_shape=[
            jax.ShapeDtypeStruct((tokens, d_model), BF16),
            jax.ShapeDtypeStruct((tokens, d_model), BF16),
            jax.ShapeDtypeStruct((blocks, width, 4 * hidden), BF16),
            jax.ShapeDtypeStruct((blocks, width, 4 * hidden), BF16),
            jax.ShapeDtypeStruct((1, d_model), F32),
        ],
        scratch_shapes=[
            bf(d_model, hidden), bf(d_model, hidden), bf(d_model, hidden), bf(tp, hidden, d_model),
            bf(tokens, hidden), bf(2, tokens, hidden), bf(hidden, tokens),
            f32(PART_RING, span, d_model), bf(RS_RING, slots, rows, d_model), bf(RS_RING, slots, rows, d_model),
            bf(slots, rows, d_model), bf(slots, rows, d_model), f32(rows, d_model), bf(2, rows, d_model),
            bf(2, tp, span, hidden), bf(2, span, d_model), bf(2, rows, d_model), bf(2, rows, d_model), bf(2, span, d_model),
            bf(2, tokens, width), bf(2, tokens, width),
            f32(width, 4 * hidden), f32(2, width, 4 * hidden), bf(2, width, 4 * hidden), f32(tp * cp, 1, d_model),
            dma((8,)), dma((2, 2)), dma((2, 2)), dma((2, 2)), dma((2,)), dma((2,)),
            dma((slots,)), dma((slots,)), dma((RS_RING, slots)), dma((RS_RING, slots)),
            dma((2,)), dma((2,)), dma((slots,)), dma((slots,)), dma((groups, slots)), dma((groups, slots)),
            dma((1,)), dma((2,)), dma((2,)), dma((2,)), dma((2,)), dma((pairs,)), dma((pairs,)), dma((pairs,)), dma((pairs,)),
            dma((tp * cp,)), dma((tp * cp,)),
        ],
        compiler_params=pltpu.CompilerParams(collective_id=0, has_side_effects=True, vmem_limit_bytes=63 << 20),
        cost_estimate=pl.CostEstimate(flops=22 * tokens * hidden * d_model, bytes_accessed=16 * tokens * d_model, transcendentals=0),
        name="backward_norm",
    )(dq, dkv, x, dy, o_all, normed, wq, wk, wv, wo_all, gain)


def finish_kernel(y_ref, gx_ref, ga_ref, gb_ref, yo_ref, gxo_ref, wq_ref, wk_ref, wv_ref, wo_ref):
    yo_ref[...] = y_ref[...]
    gxo_ref[...] = gx_ref[...]
    width = ga_ref.shape[1]
    hidden = wq_ref.shape[1]
    for k, ref in enumerate((wq_ref, wk_ref, wv_ref)):
        cols = slice(k * hidden, (k + 1) * hidden)
        ref[...] = ga_ref[0, :, cols].astype(F32) + gb_ref[0, :, cols].astype(F32)
    for k in range(hidden // width):
        cols = slice(3 * hidden + k * width, 3 * hidden + (k + 1) * width)
        wo_ref[k * width:(k + 1) * width, :] = ga_ref[0, :, cols].astype(F32) + gb_ref[0, :, cols].astype(F32)


def finish(y, gx, ga, gb):
    tokens, d_model = y.shape
    blocks, width, packed = ga.shape
    hidden = packed // 4
    rows = tokens // blocks
    tile = pl.BlockSpec((rows, d_model), lambda j: (j, 0))
    block = pl.BlockSpec((1, width, packed), lambda j: (j, 0, 0))
    wide = pl.BlockSpec((width, hidden), lambda j: (j, 0))
    return pl.pallas_call(
        finish_kernel,
        grid=(blocks,),
        in_specs=[tile, tile, block, block],
        out_specs=[tile, tile, wide, wide, wide, pl.BlockSpec((hidden, width), lambda j: (0, j))],
        out_shape=[jax.ShapeDtypeStruct((tokens, d_model), BF16)] * 2 + [jax.ShapeDtypeStruct((d_model, hidden), F32)] * 3 + [jax.ShapeDtypeStruct((hidden, d_model), F32)],
        compiler_params=pltpu.CompilerParams(dimension_semantics=("arbitrary",), vmem_limit_bytes=48 << 20),
        cost_estimate=pl.CostEstimate(flops=8 * d_model * hidden, bytes_accessed=8 * tokens * d_model + 32 * d_model * hidden, transcendentals=0),
        name="finish",
    )(y, gx, ga, gb)


def solution(mesh):
    cp_size = mesh.shape["cp"]
    tp_size = mesh.shape["tp"]

    def device_step(x_in, segment_ids, positions, w_query, w_key, w_value, w_out, norm_gain, grad_out):
        batch, seq, d_model = x_in.shape
        tokens = batch * seq
        rank = lax.axis_index("cp")
        x = x_in.reshape(tokens, d_model)
        dy = grad_out.reshape(tokens, d_model)

        inv_freq = ROPE_THETA ** (-jnp.arange(0, HEAD_DIM, 2).astype(F32) / HEAD_DIM)
        angles = positions.reshape(tokens, 1).astype(F32) * jnp.repeat(inv_freq, 2)[None, :]
        cos_t, sin_t = jnp.cos(angles), jnp.sin(angles)
        start = (rank * seq + jnp.arange(seq, dtype=jnp.int32))[None, :] - positions

        gain = norm_gain.reshape(1, d_model)
        normed, o_all, dq, dkv, w_all = front(x, dy, w_query, w_key, w_value, w_out, cos_t, sin_t, start.reshape(batch, 1, seq), gain, seq, tp_size, cp_size)
        grad_x, y_out, sum_a, sum_b, grad_gain = backward_norm(dq, dkv, x, dy, o_all, normed, w_query, w_key, w_value, w_all, gain, ROWS, tp_size, cp_size)
        grad_gain = grad_gain.reshape(d_model)
        y_out, grad_x, grad_wq, grad_wk, grad_wv, grad_wo = finish(y_out, grad_x, sum_a, sum_b)
        return y_out.reshape(x_in.shape), grad_x.reshape(x_in.shape), grad_gain, grad_wq, grad_wk, grad_wv, grad_wo

    in_specs = (P("dp", "cp", None), P("dp", "cp"), P("dp", "cp"), P(None, "tp"), P(None, "tp"), P(None, "tp"), P("tp", None), P(None), P("dp", "cp", None))
    out_specs = (P("dp", "cp", None), P("dp", "cp", None), P("dp"), P("dp", "tp"), P("dp", "tp"), P("dp", "tp"), P(("dp", "tp"), None))
    return jax.shard_map(device_step, mesh=mesh, in_specs=in_specs, out_specs=out_specs, check_vma=False)
```

```python
import functools
import math

import jax
import jax.numpy as jnp
from jax import lax
from jax.experimental import pallas as pl
from jax.experimental.pallas import tpu as pltpu
from jax.sharding import PartitionSpec as P

HEAD_DIM = 128
ROPE_THETA = 8000000.0
LN_EPS = 1e-5
NEG_BIG = -1e30
SCALE = HEAD_DIM ** -0.5
EXP2_SCALE = SCALE * math.log2(math.e)
F32 = jnp.float32
BF16 = jnp.bfloat16
NT = (((1,), (1,)), ((), ()))


def dot_nn(a, b):
    return jnp.dot(a, b, preferred_element_type=F32)


def dot_nt(a, b):
    return lax.dot_general(a, b, NT, preferred_element_type=F32)


def dot_tn(a, b):
    return lax.dot_general(a, b, (((0,), (0,)), ((), ())), preferred_element_type=F32)


def swap_pairs(t, sign):
    lane = lax.broadcasted_iota(jnp.int32, t.shape, 1)
    even = (lane % 2) == 0
    up = pltpu.roll(t, HEAD_DIM - 1, 1)
    down = pltpu.roll(t, 1, 1)
    return jnp.where(even, -up, down) if sign > 0 else jnp.where(even, up, -down)


def rope(t, cos_t, sin_t, sign):
    return t * cos_t + swap_pairs(t, sign) * sin_t


def put_rope(dst, raw, cos_t, sin_t):
    for h in range(raw.shape[1] // HEAD_DIM):
        cols = slice(h * HEAD_DIM, (h + 1) * HEAD_DIM)
        dst[:, cols] = rope(raw[:, cols], cos_t, sin_t, 1.0).astype(BF16)


MESH = pl.DeviceIdType.MESH
SUB = 128
ROWS = 32
WIDTH = 256
HALVES = 2
RELAY_LAG = 4
CHIP_BUFS = 4
W_TWIN = 3
W_PARTNER = 6


def front_kernel(batch, seq, tp, cp, x_hbm, dy_hbm, wq_hbm, wk_hbm, wv_hbm, wo_hbm, cos_ref, sin_ref, start_ref, gain_ref,
                 n_hbm, o_all, dq_hbm, dkv_hbm, w_all,
                 big, wo_ref, q_row, do_row, a_in, b_in, kv_own, kvr, s_scr, dp_scr, m_scr, l_scr, d_scr, ot_scr, dqt_scr,
                 o_buf, dq_buf, g_part, g_chip, g_far, xin, part_in,
                 w_sem, wl_sem, wz_send, wz_recv, wx_send, wx_recv,
                 tile_sem, n_sem, kvs_part, kvs_chip, kvs_far, kv_recv, o_local, o_send, o_recv, relay_send, dq_sem,
                 far_send, part_send, chip_send, x_recv, part_recv, dkv_sem):
    z = lax.axis_index("tp")
    r = lax.axis_index("cp")
    dp = lax.axis_index("dp")
    core = lax.rem(r, 2)
    chip = lax.div(r, 2)
    d_model = x_hbm.shape[1]
    hidden = wq_hbm.shape[1]
    heads = hidden // HEAD_DIM
    first_chip, second_chip = chip == 0, chip == 1
    first_core, second_core = core == 0, core == 1
    partner = {"cp": r + 1 - 2 * core}
    peer = {"cp": r + 2 - 4 * chip}
    twin = {"dp": 1 - dp}

    weight_loads = [pltpu.make_async_copy(src, dst, w_sem.at[k]) for k, (src, dst) in enumerate(((wk_hbm, big.at[0]), (wv_hbm, big.at[1]), (wq_hbm, big.at[2]), (wo_hbm, wo_ref)))]
    for copy in weight_loads:
        copy.start()

    tile = a_in.shape[1]
    per_row = seq // tile
    tiles = batch * per_row

    def tile_rows(t):
        return pl.ds(pl.multiple_of(t * tile, tile), tile)

    def row(b):
        return pl.ds(pl.multiple_of(b * seq, seq), seq)

    def x_load(t, par):
        return pltpu.make_async_copy(x_hbm.at[tile_rows(t), :], a_in.at[par], tile_sem.at[par, 0])

    units = batch * HALVES
    half = hidden // HALVES

    def where(u):
        return lax.div(u, HALVES), lax.rem(u, HALVES)

    def half_cols(g):
        return pl.ds(pl.multiple_of(g * half, half), half)

    def n_load(t, par):
        return pltpu.make_async_copy(n_hbm.at[tile_rows(t), :], a_in.at[par], tile_sem.at[par, 0])

    def dy_load(t, par):
        return pltpu.make_async_copy(dy_hbm.at[tile_rows(t), :], b_in.at[par], tile_sem.at[par, 1])

    def n_store(t, par):
        return pltpu.make_async_copy(b_in.at[par], n_hbm.at[tile_rows(t), :], n_sem.at[par])

    x_load(0, 0).start()

    barrier = pltpu.get_barrier_semaphore()
    for dev in [partner, peer, twin] + [{"tp": lax.rem(z + dt, tp)} for dt in range(1, tp)]:
        pl.semaphore_signal(barrier, inc=1, device_id=dev, device_id_type=MESH)
    pl.semaphore_wait(barrier, tp + 2)

    def remote(src, dst, ssem, rsem, dev):
        return pltpu.make_async_remote_copy(src_ref=src, dst_ref=dst, send_sem=ssem, recv_sem=rsem, device_id=dev, device_id_type=MESH)

    share = hidden // 8

    def share_rows(y, c, g):
        return pl.ds(pl.multiple_of((4 * y + 2 * c + g) * share, share), share)

    mine, twins = share_rows(chip, core, dp), share_rows(chip, core, 1 - dp)
    peers, peer_twins = share_rows(1 - chip, core, dp), share_rows(1 - chip, core, 1 - dp)

    def wz_copy(d):
        return remote(wo_hbm.at[mine, :], w_all.at[z, mine, :], wz_send.at[d], wz_recv.at[z], {"tp": lax.rem(z + d, tp)})

    def wz_wait(d):
        src = lax.rem(z + d, tp)
        remote(wo_hbm.at[mine, :], w_all.at[src, mine, :], wz_send.at[d], wz_recv.at[src], partner).wait_recv()

    def w_copy(k, d, rows, dev):
        place = w_all.at[lax.rem(z + d, tp), rows, :]
        return remote(place, place, wx_send.at[k, d], wx_recv.at[k, d], dev)

    def w_move(k, d):
        rows, dev = ((mine, twin), (mine, partner), (twins, partner), (mine, peer), (twins, peer), (peers, partner), (peer_twins, partner))[k]
        return w_copy(k, d, rows, dev)

    w_steps = range(1, tp)

    for d in range(1, tp):
        wz_copy(d).start()

    def kv_to_partner(u):
        return remote(kv_own.at[u], kvr.at[0, u], kvs_part.at[u], kv_recv.at[0, u], partner)

    def kv_to_chip(u):
        return remote(kv_own.at[u], kvr.at[1, u], kvs_chip.at[u], kv_recv.at[1, u], peer)

    def kv_forward(u):
        return remote(kvr.at[1, u], kvr.at[2, u], kvs_far.at[u], kv_recv.at[2, u], partner)

    for copy in weight_loads:
        copy.wait()
    w_local = pltpu.make_async_copy(wo_ref, w_all.at[z], wl_sem.at[0])
    w_local.start()

    def key_tile(t, carry):
        par = lax.rem(t, 2)
        x_load(t, par).wait()

        @pl.when(t + 1 < tiles)
        def _():
            x_load(t + 1, 1 - par).start()

        @pl.when(t >= 2)
        def _():
            n_store(t - 2, par).wait()

        x = a_in[par].astype(F32)
        centred = x - jnp.mean(x, axis=-1, keepdims=True)
        inv_std = lax.rsqrt(jnp.mean(centred * centred, axis=-1, keepdims=True) + LN_EPS)
        normed = ((centred * inv_std) * gain_ref[...]).astype(BF16)
        b_in[par] = normed
        n_store(t, par).start()
        b = lax.div(t, per_row)
        part = lax.rem(t, per_row)
        inside = pl.ds(pl.multiple_of(part * tile, tile), tile)
        rows = tile_rows(t)
        for g in range(HALVES):
            u = b * HALVES + g
            cols = slice(g * half, (g + 1) * half)
            put_rope(kv_own.at[u, 0, inside, :], dot_nn(normed, big[0, :, cols]), cos_ref[rows, :], sin_ref[rows, :])
            kv_own[u, 1, inside, :] = dot_nn(normed, big[1, :, cols]).astype(BF16)

            @pl.when(part == per_row - 1)
            def _(u=u):
                @pl.when(first_chip)
                def _():
                    kv_to_chip(u).start()

                @pl.when(first_core)
                def _():
                    kv_to_partner(u).start()

        return carry

    lax.fori_loop(0, tiles, key_tile, 0)
    for t in range(tiles - 2, tiles):
        n_store(t, t % 2).wait()

    def query_loads(t, par):
        return [n_load(t, par), dy_load(t, par)]

    for copy in query_loads(0, 0):
        copy.start()

    def query_row(i):
        for k in range(per_row):
            t = i * per_row + k
            par = lax.rem(t, 2)
            for copy in query_loads(t, par):
                copy.wait()

            @pl.when(t + 1 < tiles)
            def _(t=t, par=par):
                for copy in query_loads(t + 1, 1 - par):
                    copy.start()

            rows = tile_rows(t)
            inside = slice(k * tile, (k + 1) * tile)
            put_rope(q_row.at[inside, :], dot_nn(a_in[par], big[2]), cos_ref[rows, :], sin_ref[rows, :])
            do_row[inside, :] = dot_nt(b_in[par], wo_ref[...]).astype(BF16)

    fit = d_model // seq

    def g_own(b, which, cols):
        k = 2 * b + which
        return big.at[lax.div(k, fit), pl.ds(pl.multiple_of(lax.rem(k, fit) * seq, seq), seq), cols]

    def o_place(src, u):
        b, g = where(u)
        return o_all.at[src, row(b), half_cols(g)]

    def o_local_copy(b):
        return pltpu.make_async_copy(o_buf.at[b], o_place(z, b), o_local.at[b])

    def o_copy(b, k, step):
        return remote(o_buf.at[b], o_place(z, b), o_send.at[k, b], o_recv.at[z, b], {"tp": jnp.clip(z + step, 0, tp - 1)})

    hops = [(k, step, jnp.logical_and(z + step >= 0, z + step < tp)) for k, step in enumerate((1, -1, 2, -2))]

    def o_start(b):
        o_local_copy(b).start()
        for k, step, ok in hops:
            @pl.when(ok)
            def _(k=k, step=step):
                o_copy(b, k, step).start()

    def o_arrived(src, b):
        remote(o_place(src, b), o_place(src, b), relay_send.at[b], o_recv.at[src, b], partner).wait_recv()

    def relay_copy(b, src, dst):
        return remote(o_place(src, b), o_place(src, b), relay_send.at[b], o_recv.at[src, b], {"tp": dst})

    def relay(b):
        @pl.when(z == tp - 2)
        def _():
            o_arrived(0, b)
            relay_copy(b, 0, tp - 1).start()

        @pl.when(z == 1)
        def _():
            o_arrived(tp - 1, b)
            relay_copy(b, tp - 1, 0).start()

    def far_copy(b, par):
        return remote(g_far.at[par], xin.at[b], far_send.at[par], x_recv.at[b], partner)

    def part_copy(b, par):
        return remote(g_part.at[par], part_in.at[b], part_send.at[par], part_recv.at[b], partner)

    def chip_copy(b):
        par = lax.rem(b, CHIP_BUFS)
        return remote(g_chip.at[par], xin.at[b], chip_send.at[par], x_recv.at[b], peer)

    def chip_sum(b):
        @pl.when(second_chip)
        def _():
            par = lax.rem(b, CHIP_BUFS)
            far_copy(b, 0).wait_recv()
            g_chip[par] = (g_chip[par].astype(F32) + xin[b].astype(F32)).astype(BF16)
            chip_copy(b).start()

    def own_half(u, which):
        b, g = where(u)
        return g_own(b, which, half_cols(g))

    def dkv_store(u, which):
        b, g = where(u)
        return pltpu.make_async_copy(own_half(u, which), dkv_hbm.at[which, row(b), half_cols(g)], dkv_sem.at[u, which])

    def key_grads(u):
        @pl.when(first_core)
        def _():
            part_copy(u, 0).wait_recv()

        @pl.when(first_chip)
        def _():
            chip_copy(u).wait_recv()

        b, g = where(u)
        rows = row(b)
        for which in range(2):
            for h in range(half // HEAD_DIM):
                cols = slice(h * HEAD_DIM, (h + 1) * HEAD_DIM)
                own = g_own(b, which, pl.ds(pl.multiple_of(g * half + h * HEAD_DIM, HEAD_DIM), HEAD_DIM))
                acc = own[...].astype(F32)
                acc = acc + jnp.where(first_core, part_in[u, which, :, cols].astype(F32), 0.0)
                acc = (acc + jnp.where(first_chip, xin[u, which, :, cols].astype(F32), 0.0)).astype(BF16)
                if which == 0:
                    acc = rope(acc.astype(F32), cos_ref[rows, :], sin_ref[rows, :], -1.0).astype(BF16)
                own[...] = acc
            dkv_store(u, which).start()

    def dq_store(b, par):
        return pltpu.make_async_copy(dq_buf.at[par], dq_hbm.at[row(where(b)[0]), half_cols(where(b)[1])], dq_sem.at[par])

    subs = range(0, seq, SUB)

    def attend_unit(i, par):
        b, g = where(i)
        rows = row(b)
        start = start_ref[b]
        chip_par = lax.rem(i, CHIP_BUFS)
        keys_of = [kv_own.at[i]] + [kvr.at[s, i] for s in range(3)]
        places = [g_part.at[par], g_chip.at[chip_par], g_far.at[par]]

        def grad(slot, which, cols, full):
            return places[slot - 1].at[which, :, cols] if slot else g_own(b, which, full)

        live = [None, second_core, second_chip, second_chip]
        piece = [r, r + 1 - 2 * core, r + 2 - 4 * chip, r + 3 - 2 * core - 4 * chip]

        def each(body):
            body(0)
            for slot in (1, 2, 3):
                pl.when(live[slot])(functools.partial(body, slot))

        def one_head(h, carry):
            cols = pl.ds(pl.multiple_of(h * HEAD_DIM, HEAD_DIM), HEAD_DIM)
            full = pl.ds(pl.multiple_of(g * half + h * HEAD_DIM, HEAD_DIM), HEAD_DIM)
            q = q_row[:, full]
            do = do_row[:, full]
            m_scr[...] = jnp.full(m_scr.shape, NEG_BIG, F32)
            l_scr[...] = jnp.zeros_like(l_scr)
            d_scr[...] = jnp.zeros_like(d_scr)
            ot_scr[...] = jnp.zeros_like(ot_scr)
            dqt_scr[...] = jnp.zeros_like(dqt_scr)

            def scores(slot):
                base = piece[slot] * seq
                for s in subs:
                    raw = dot_nt(keys_of[slot][0, s:s + SUB, cols], q)
                    local = lax.broadcasted_iota(jnp.int32, raw.shape, 0) + s
                    allowed = (local + base) >= start
                    if slot == 0:
                        allowed = jnp.logical_and(allowed, local <= lax.broadcasted_iota(jnp.int32, raw.shape, 1))
                    raw = jnp.where(allowed, raw, NEG_BIG)
                    s_scr[slot, s:s + SUB, :] = raw
                    m_scr[...] = jnp.maximum(m_scr[...], jnp.max(raw, axis=0, keepdims=True))

            def exps(slot):
                for s in subs:
                    e = jnp.exp2((s_scr[slot, s:s + SUB, :] - m_scr[...]) * EXP2_SCALE)
                    s_scr[slot, s:s + SUB, :] = e
                    l_scr[...] += jnp.sum(e, axis=0, keepdims=True)

            def values(slot):
                for s in subs:
                    v = keys_of[slot][1, s:s + SUB, cols]
                    prob = s_scr[slot, s:s + SUB, :] * l_scr[...]
                    low = prob.astype(BF16)
                    dp = dot_nt(v, do)
                    s_scr[slot, s:s + SUB, :] = prob
                    dp_scr[slot, s:s + SUB, :] = dp
                    d_scr[...] += jnp.sum(prob * dp, axis=0, keepdims=True)
                    grad(slot, 1, cols, full)[s:s + SUB, :] = dot_nn(low, do).astype(BF16)
                    ot_scr[...] += dot_nn(v.T, low)

            def keys(slot):
                for s in subs:
                    k = keys_of[slot][0, s:s + SUB, cols]
                    ds = (s_scr[slot, s:s + SUB, :] * (dp_scr[slot, s:s + SUB, :] - d_scr[...])).astype(BF16)
                    grad(slot, 0, cols, full)[s:s + SUB, :] = (dot_nn(ds, q) * SCALE).astype(BF16)
                    dqt_scr[...] += dot_nn(k.T, ds)

            each(scores)
            each(exps)
            l_scr[...] = 1.0 / l_scr[...]
            each(values)
            each(keys)
            o_buf[i, :, cols] = ot_scr[...].T.astype(BF16)
            dq_buf[par, :, cols] = rope(dqt_scr[...].T * SCALE, cos_ref[rows, :], sin_ref[rows, :], -1.0).astype(BF16)
            return carry

        lax.fori_loop(0, heads // HALVES, one_head, 0)

    def step(i, carry):
        par = lax.rem(i, 2)
        @pl.when(lax.rem(i, HALVES) == 0)
        def _():
            query_row(lax.div(i, HALVES))

        @pl.when(second_chip)
        def _():
            kv_to_chip(i).wait_recv()
            kv_forward(i).start()

        @pl.when(second_core)
        def _():
            kv_to_partner(i).wait_recv()

        @pl.when(second_chip)
        def _():
            kv_forward(i).wait_recv()

        @pl.when(i >= 2)
        def _():
            dq_store(i - 2, par).wait()

            @pl.when(second_core)
            def _():
                part_copy(i - 2, par).wait_send()

            @pl.when(second_chip)
            def _():
                far_copy(i - 2, par).wait_send()

        @pl.when(jnp.logical_and(second_chip, i >= CHIP_BUFS))
        def _():
            chip_copy(i - CHIP_BUFS).wait_send()

        attend_unit(i, par)
        o_start(i)
        dq_store(i, par).start()

        @pl.when(second_chip)
        def _():
            far_copy(i, par).start()

        @pl.when(second_core)
        def _():
            part_copy(i, par).start()

        @pl.when(i >= 1)
        def _():
            chip_sum(i - 1)

        @pl.when(i >= RELAY_LAG)
        def _():
            relay(i - RELAY_LAG)

        @pl.when(i == min(W_TWIN, units - 1))
        def _():
            for d in w_steps:
                wz_wait(d)
                w_move(0, d).start()
                w_move(1, d).start()

                @pl.when(second_chip)
                def _(d=d):
                    w_move(3, d).start()

        @pl.when(i == min(W_PARTNER, units - 1))
        def _():
            for d in w_steps:
                w_move(0, d).wait_recv()
                w_move(2, d).start()

                @pl.when(second_chip)
                def _(d=d):
                    w_move(4, d).start()

        return carry

    lax.fori_loop(0, units, step, 0)
    chip_sum(units - 1)

    @pl.when(first_chip)
    def _():
        for u in range(units):
            kv_to_chip(u).wait_send()
        for k in (3, 4):
            for d in w_steps:
                w_move(k, d).start()

    lag = min(RELAY_LAG, units)

    def finish(u, carry):
        @pl.when(u < lag)
        def _():
            relay(units - lag + u)

        key_grads(u)
        return carry

    lax.fori_loop(0, units, finish, 0)
    for k in (3, 4):
        for d in w_steps:
            w_move(k, d).wait_recv()
            w_move(k + 2, d).start()

    w_local.wait()
    for d in w_steps:
        wz_copy(d).wait_send()
        for k in range(7):
            w_move(k, d).wait_send()
            if k in (1, 2, 5, 6):
                w_move(k, d).wait_recv()

    def drain(b, carry):
        for which in range(2):
            dkv_store(b, which).wait()

        @pl.when(first_core)
        def _():
            kv_to_partner(b).wait_send()

        @pl.when(second_chip)
        def _():
            kv_forward(b).wait_send()

        o_local_copy(b).wait()
        for k, step_, ok in hops:
            @pl.when(ok)
            def _(k=k, step_=step_):
                o_copy(b, k, step_).wait_send()

        @pl.when(jnp.logical_or(z == 1, z == tp - 2))
        def _():
            relay_copy(b, 0, tp - 1).wait_send()

        for src in range(tp):
            taken = jnp.logical_or(jnp.logical_and(z == tp - 2, src == 0), jnp.logical_and(z == 1, src == tp - 1))

            @pl.when(jnp.logical_and(z != src, jnp.logical_not(taken)))
            def _(src=src):
                o_arrived(src, b)

        return carry

    lax.fori_loop(0, units, drain, 0)

    for b in range(max(0, units - 2), units):
        dq_store(b, b % 2).wait()

        @pl.when(second_core)
        def _(b=b):
            part_copy(b, b % 2).wait_send()

        @pl.when(second_chip)
        def _(b=b):
            far_copy(b, b % 2).wait_send()

    for b in range(max(0, units - CHIP_BUFS), units):
        @pl.when(second_chip)
        def _(b=b):
            chip_copy(b).wait_send()


def front(x, dy, wq, wk, wv, wo, cos_t, sin_t, start, gain, seq, tp, cp):
    tokens, d_model = x.shape
    hidden = wq.shape[1]
    batch = tokens // seq
    units = batch * HALVES
    half = hidden // HALVES
    tile = seq // 2
    hbm = pl.BlockSpec(memory_space=pl.ANY)
    vmem = pl.BlockSpec(memory_space=pltpu.VMEM)
    dma = pltpu.SemaphoreType.DMA
    bf = lambda *shape: pltpu.VMEM(shape, BF16)
    f32 = lambda *shape: pltpu.VMEM(shape, F32)
    return pl.pallas_call(
        functools.partial(front_kernel, batch, seq, tp, cp),
        in_specs=[hbm] * 6 + [vmem] * 4,
        out_specs=[hbm] * 5,
        out_shape=[
            jax.ShapeDtypeStruct((tokens, d_model), BF16),
            jax.ShapeDtypeStruct((tp, tokens, hidden), BF16),
            jax.ShapeDtypeStruct((tokens, hidden), BF16),
            jax.ShapeDtypeStruct((2, tokens, hidden), BF16),
            jax.ShapeDtypeStruct((tp, hidden, d_model), BF16),
        ],
        scratch_shapes=[
            bf(3, d_model, hidden), bf(hidden, d_model), bf(seq, hidden), bf(seq, hidden), bf(2, tile, d_model), bf(2, tile, d_model),
            bf(units, 2, seq, half), bf(3, units, 2, seq, half),
            f32(4, seq, seq), f32(4, seq, seq), f32(1, seq), f32(1, seq), f32(1, seq), f32(HEAD_DIM, seq), f32(HEAD_DIM, seq),
            bf(units, seq, half), bf(2, seq, half),
            bf(2, 2, seq, half), bf(CHIP_BUFS, 2, seq, half), bf(2, 2, seq, half),
            bf(units, 2, seq, half), bf(units, 2, seq, half),
            dma((4,)), dma((1,)), dma((tp,)), dma((tp,)), dma((7, tp)), dma((7, tp)),
            dma((2, 2)), dma((2,)), dma((units,)), dma((units,)), dma((units,)), dma((3, units)),
            dma((units,)), dma((4, units)), dma((tp, units)), dma((units,)), dma((2,)),
            dma((2,)), dma((2,)), dma((CHIP_BUFS,)), dma((units,)), dma((units,)), dma((units, 2)),
        ],
        compiler_params=pltpu.CompilerParams(collective_id=1, has_side_effects=True, vmem_limit_bytes=63 << 20),
        cost_estimate=pl.CostEstimate(flops=60 * tokens * seq * hidden, bytes_accessed=16 * tokens * d_model, transcendentals=4 * tokens * seq * (hidden // HEAD_DIM)),
        name="front",
    )(x, dy, wq, wk, wv, wo, cos_t, sin_t, start, gain)


PART_RING = 4
RS_RING = 5
FORWARD_LAG = 11
JOB_LAG = 5
OUT_LAG = 4
EARLY = 4


def back_kernel(groups, rows, tp, cp, dq_hbm, dkv_hbm, x_hbm, dy_hbm, o_hbm, n_hbm, wq_hbm, wk_hbm, wv_hbm, wo_hbm, gain_ref,
                gx_hbm, y_hbm, ga_hbm, gb_hbm, gg_ref,
                wq_ref, wk_ref, wv_ref, wo_ref, dq_all, dkv_all, o_t, part, rs_r, rs_l, send_r, send_l, tot, gx_buf,
                o_in, x_in, xo_in, dyo_in, y_buf, n_in, dy_in, away, part_in, mine, gain_all,
                w_sem, in_sem, fin_sem, job_sem, y_sem, own_sem, rss_r, rss_l, rsr_r, rsr_l, ag0_r, ag0_l, agf_r, agf_l, agr_r, agr_l,
                away_send, away_recv, mine_own, mine_part, mine_chip, ga_recv, chip_recv, gb_send, gb_recv, gs_sem, gr_sem):
    z = lax.axis_index("tp")
    r = lax.axis_index("cp")
    core = lax.rem(r, 2)
    chip = lax.div(r, 2)
    last = tp - 1
    slots = tp - 1
    span = tp * rows
    tokens, d_model = x_hbm.shape
    hidden = dq_hbm.shape[1]
    chunk = min(512, d_model)
    blocks = ga_hbm.shape[0]
    width = ga_hbm.shape[1]
    pairs = blocks // 2
    partner = {"cp": r + 1 - 2 * core}
    peer = {"cp": r + 2 - 4 * chip}

    head = min(EARLY, groups) * span
    weight_loads = [pltpu.make_async_copy(src, dst, w_sem.at[k]) for k, (src, dst) in enumerate((
        (dq_hbm.at[:head, :], dq_all.at[:head, :]), (dkv_hbm.at[:, :head, :], dkv_all.at[:, :head, :]), (wq_hbm, wq_ref), (wk_hbm, wk_ref), (wv_hbm, wv_ref)))]
    rest_loads = [] if head == tokens else [
        pltpu.make_async_copy(dq_hbm.at[head:, :], dq_all.at[head:, :], w_sem.at[6]),
        pltpu.make_async_copy(dkv_hbm.at[:, head:, :], dkv_all.at[:, head:, :], w_sem.at[7]),
    ]
    out_loads = [pltpu.make_async_copy(wo_hbm, wo_ref, w_sem.at[5])]
    for copy in weight_loads:
        copy.start()

    barrier = pltpu.get_barrier_semaphore()
    peers = [(dt, dc) for dt in range(tp) for dc in range(cp) if dt or dc]
    for dt, dc in peers:
        pl.semaphore_signal(barrier, inc=1, device_id={"tp": lax.rem(z + dt, tp), "cp": lax.rem(r + dc, cp)}, device_id_type=MESH)
    pl.semaphore_wait(barrier, len(peers))

    def remote(src, dst, ssem, rsem, dev):
        return pltpu.make_async_remote_copy(src_ref=src, dst_ref=dst, send_sem=ssem, recv_sem=rsem, device_id=dev, device_id_type=MESH)

    right = {"tp": jnp.where(z < last, z + 1, z)}
    left = {"tp": jnp.where(z > 0, z - 1, z)}

    def group_rows(i):
        return pl.ds(pl.multiple_of(i * span, span), span)

    def tile_rows(i, owner):
        return pl.ds(pl.multiple_of(i * span + owner * rows, rows), rows)

    def inputs(i, slot):
        g = group_rows(i)
        return [
            pltpu.make_async_copy(o_hbm.at[:, g, :], o_in.at[slot], in_sem.at[slot, 0]),
            pltpu.make_async_copy(x_hbm.at[g, :], x_in.at[slot], in_sem.at[slot, 1]),
        ]

    def final_inputs(i, slot):
        g = tile_rows(i, z)
        return [
            pltpu.make_async_copy(x_hbm.at[g, :], xo_in.at[slot], fin_sem.at[slot, 0]),
            pltpu.make_async_copy(dy_hbm.at[g, :], dyo_in.at[slot], fin_sem.at[slot, 1]),
        ]

    def y_copy(i, slot):
        return pltpu.make_async_copy(y_buf.at[slot], y_hbm.at[group_rows(i), :], y_sem.at[slot])

    def rs_copy(i, s, to_right):
        ring = lax.rem(i, RS_RING)
        if to_right:
            return remote(send_r.at[s], rs_r.at[ring, s], rss_r.at[s], rsr_r.at[ring, s], right)
        return remote(send_l.at[s], rs_l.at[ring, s], rss_l.at[s], rsr_l.at[ring, s], left)

    def rs_send(i, s):
        for to_right in (True, False):
            far = z if to_right else last - z
            owner = (z + slots - s) if to_right else (z - slots + s)
            buf, held = (send_r, rs_r) if to_right else (send_l, rs_l)

            @pl.when(jnp.logical_and(jnp.logical_and(i >= 0, i < groups), jnp.logical_and(far <= s, far < last)))
            def _(to_right=to_right, far=far, owner=owner, buf=buf, held=held):
                @pl.when(i > 0)
                def _():
                    rs_copy(i - 1, s, to_right).wait_send()

                cur = lax.rem(i, PART_RING)
                own = pl.ds(pl.multiple_of(owner * rows, rows), rows)
                if s == 0:
                    buf[s] = part[cur, own, :].astype(BF16)
                else:
                    @pl.when(far == 0)
                    def _():
                        buf[s] = part[cur, own, :].astype(BF16)

                    @pl.when(far > 0)
                    def _():
                        rs_copy(i, s - 1, to_right).wait_recv()
                        buf[s] = (part[cur, own, :] + held[lax.rem(i, RS_RING), s - 1].astype(F32)).astype(BF16)

                rs_copy(i, s, to_right).start()

    def ag_own(i, slot, to_right):
        src = gx_buf.at[slot]
        dst = gx_hbm.at[tile_rows(i, z), :]
        if to_right:
            return remote(src, dst, ag0_r.at[slot], agr_r.at[i, 0], right)
        return remote(src, dst, ag0_l.at[slot], agr_l.at[i, 0], left)

    def own_copy(i, slot):
        return pltpu.make_async_copy(gx_buf.at[slot], gx_hbm.at[tile_rows(i, z), :], own_sem.at[slot])

    def ag_forward(i, a, to_right):
        owner = z - a if to_right else z + a
        tile = gx_hbm.at[tile_rows(i, owner), :]
        if to_right:
            return remote(tile, tile, agf_r.at[a], agr_r.at[i, a], right)
        return remote(tile, tile, agf_l.at[a], agr_l.at[i, a], left)

    def ag_wait(i, a, to_right):
        tile = gx_hbm.at[tile_rows(i, 0), :]
        sem = agr_r.at[i, a] if to_right else agr_l.at[i, a]
        remote(tile, tile, agf_r.at[a], sem, right).wait_recv()

    def ag_step(i, a):
        for to_right in (True, False):
            far = z if to_right else last - z

            @pl.when(jnp.logical_and(jnp.logical_and(i >= 0, i < groups), far >= a))
            def _(to_right=to_right, far=far):
                ag_wait(i, a - 1, to_right)
                if a < slots:
                    @pl.when(far < last)
                    def _():
                        @pl.when(i > 0)
                        def _():
                            ag_forward(i - 1, a, to_right).wait_send()

                        ag_forward(i, a, to_right).start()

    def ag_first(i, slot):
        own_copy(i, slot).start()
        for to_right in (True, False):
            far = z if to_right else last - z

            @pl.when(far < last)
            def _(to_right=to_right):
                ag_own(i, slot, to_right).start()

    def ag_first_done(i, slot):
        own_copy(i, slot).wait()
        for to_right in (True, False):
            far = z if to_right else last - z

            @pl.when(far < last)
            def _(to_right=to_right):
                ag_own(i, slot, to_right).wait_send()

    def partial_norm(i):
        cur = lax.rem(i, PART_RING)
        g = group_rows(i)
        for c in range(0, d_model, chunk):
            cols = slice(c, c + chunk)
            part[cur, :, cols] = (
                dot_nt(dq_all[g, :], wq_ref[cols, :]) + dot_nt(dkv_all[0, g, :], wk_ref[cols, :]) + dot_nt(dkv_all[1, g, :], wv_ref[cols, :])
            )

    def project_out(cur):
        for c in range(0, d_model, chunk):
            cols = slice(c, c + chunk)
            acc = x_in[cur, :, cols].astype(F32)
            for t in range(tp):
                acc += dot_nn(o_in[cur, t], wo_ref[t, :, cols])
            y_buf[cur, :, cols] = acc.astype(BF16)

    def finalize(i):
        slot = lax.rem(i, 2)
        own = pl.ds(pl.multiple_of(z * rows, rows), rows)
        tot[...] = part[lax.rem(i, PART_RING), own, :]

        @pl.when(z > 0)
        def _():
            rs_copy(i, slots - 1, True).wait_recv()
            tot[...] += rs_r[lax.rem(i, RS_RING), slots - 1].astype(F32)

        @pl.when(z < last)
        def _():
            rs_copy(i, slots - 1, False).wait_recv()
            tot[...] += rs_l[lax.rem(i, RS_RING), slots - 1].astype(F32)

        @pl.when(i > 1)
        def _():
            ag_first_done(i - 2, slot)

        for copy in final_inputs(i, slot):
            copy.wait()
        x = xo_in[slot].astype(F32)
        centred = x - jnp.mean(x, axis=-1, keepdims=True)
        inv_std = lax.rsqrt(jnp.mean(centred * centred, axis=-1, keepdims=True) + LN_EPS)
        x_hat = centred * inv_std
        dn = tot[...]
        gg_ref[...] += jnp.sum(dn * x_hat, axis=0, keepdims=True)
        d_hat = dn * gain_ref[...]
        dx = inv_std * (d_hat - jnp.mean(d_hat, axis=-1, keepdims=True) - x_hat * jnp.mean(d_hat * x_hat, axis=-1, keepdims=True))
        gx_buf[slot] = (dyo_in[slot].astype(F32) + dx).astype(BF16)
        ag_first(i, slot)

    def block_of(t):
        return 2 * lax.div(t, 2) + jnp.where(lax.rem(t, 2) == 0, 1 - core, core)

    def job_loads(t, slot):
        cols = pl.ds(pl.multiple_of(block_of(t) * width, width), width)
        return [
            pltpu.make_async_copy(n_hbm.at[:, cols], n_in.at[slot], job_sem.at[slot, 0]),
            pltpu.make_async_copy(dy_hbm.at[:, cols], dy_in.at[slot], job_sem.at[slot, 1]),
        ]

    def away_copy(p):
        ring = lax.rem(p, 2)
        return remote(away, part_in.at[ring], away_send.at[0], away_recv.at[ring], partner)

    def job_block(t, put):
        slot = lax.rem(t, 2)
        n_t = n_in[slot].T
        put(0, hidden, dot_nn(n_t, dq_all[...]))
        put(hidden, hidden, dot_nn(n_t, dkv_all[0]))
        put(2 * hidden, hidden, dot_nn(n_t, dkv_all[1]))
        for k in range(hidden // width):
            put(3 * hidden + k * width, width, dot_nn(o_t[k * width:(k + 1) * width, :], dy_in[slot]))

    def mine_to_own(p, slot):
        return pltpu.make_async_copy(mine.at[slot], ga_hbm.at[2 * p + core], mine_own.at[slot])

    def mine_to_part(p, slot):
        return remote(mine.at[slot], ga_hbm.at[2 * p + core], mine_part.at[slot], ga_recv.at[p], partner)

    def mine_to_chip(p, slot):
        return remote(mine.at[slot], gb_hbm.at[2 * p + core], mine_chip.at[slot], chip_recv.at[p], peer)

    def mine_done(p, slot):
        mine_to_own(p, slot).wait()
        mine_to_part(p, slot).wait_send()
        mine_to_chip(p, slot).wait_send()

    def chip_forward(p):
        b = 2 * p + core
        return remote(gb_hbm.at[b], gb_hbm.at[b], gb_send.at[p], gb_recv.at[p], partner)

    def job(t):
        p = lax.div(t, 2)
        for copy in job_loads(t, lax.rem(t, 2)):
            copy.wait()

        @pl.when(t + 1 < blocks)
        def _():
            for copy in job_loads(t + 1, 1 - lax.rem(t, 2)):
                copy.start()

        @pl.when(lax.rem(t, 2) == 0)
        def _():
            @pl.when(p > 0)
            def _():
                away_copy(p - 1).wait_send()

            def put(at, size, value):
                away[:, at:at + size] = value

            job_block(t, put)
            away_copy(p).start()

        @pl.when(lax.rem(t, 2) == 1)
        def _():
            slot = lax.rem(p, 2)
            away_copy(p).wait_recv()

            @pl.when(p > 1)
            def _():
                mine_done(p - 2, slot)

            def put(at, size, value):
                mine[slot, :, at:at + size] = (value + part_in[slot, :, at:at + size]).astype(BF16)

            job_block(t, put)
            mine_to_chip(p, slot).start()
            mine_to_part(p, slot).start()
            mine_to_own(p, slot).start()

    gg_ref[...] = jnp.zeros_like(gg_ref)
    o_loads = [pltpu.make_async_copy(o_hbm.at[z, :, k * width:(k + 1) * width], n_in.at[k], job_sem.at[k, 0]) for k in range(hidden // width)]
    for copy in o_loads:
        copy.start()
    for copy in inputs(0, 0):
        copy.start()
    for copy in rest_loads + out_loads:
        copy.start()
    me = z * cp + r

    def gain_copy(dt, dc):
        to = {"tp": lax.rem(z + dt, tp), "cp": lax.rem(r + dc, cp)}
        return remote(gain_all.at[me], gain_all.at[me], gs_sem.at[dt * cp + dc], gr_sem.at[me], to)

    def gain_wait(dt, dc):
        sender = lax.rem(z + dt, tp) * cp + lax.rem(r + dc, cp)
        remote(gain_all.at[sender], gain_all.at[sender], gs_sem.at[0], gr_sem.at[sender], right).wait_recv()

    for copy in weight_loads:
        copy.wait()

    def step(i, carry):
        for k in reversed(range(1, slots)):
            rs_send(i - k, k)

        @pl.when(i == EARLY)
        def _():
            for copy in rest_loads:
                copy.wait()

        @pl.when(i < groups)
        def _():
            partial_norm(i)

        rs_send(i, 0)

        @pl.when(jnp.logical_and(i >= slots, i < groups + slots))
        def _():
            finalize(i - slots)

        for a in range(1, slots + 1):
            ag_step(i - slots - a, a)

        @pl.when(i == groups + slots - 1)
        def _():
            gain_all[me] = gg_ref[...]
            for dt, dc in peers:
                gain_copy(dt, dc).start()

        @pl.when(jnp.logical_and(i >= slots - 1, i < groups + slots - 1))
        def _():
            for copy in final_inputs(i - slots + 1, lax.rem(i - slots + 1, 2)):
                copy.start()

        @pl.when(i == JOB_LAG - 1)
        def _():
            for k, copy in enumerate(o_loads):
                copy.wait()
                o_t[k * width:(k + 1) * width, :] = n_in[k].T
            for copy in job_loads(0, 0):
                copy.start()

        @pl.when(i == OUT_LAG)
        def _():
            for copy in out_loads:
                copy.wait()

        @pl.when(jnp.logical_and(i >= OUT_LAG, i < groups + OUT_LAG))
        def _():
            j = i - OUT_LAG
            at = lax.rem(j, 2)
            for copy in inputs(j, at):
                copy.wait()

            @pl.when(j + 1 < groups)
            def _():
                for copy in inputs(j + 1, 1 - at):
                    copy.start()

            @pl.when(j >= 2)
            def _():
                y_copy(j - 2, at).wait()

            project_out(at)
            y_copy(j, at).start()

        @pl.when(jnp.logical_and(i >= JOB_LAG, i < JOB_LAG + blocks))
        def _():
            job(i - JOB_LAG)

        @pl.when(jnp.logical_and(lax.rem(i, 2) == 1, jnp.logical_and(i >= FORWARD_LAG, i < FORWARD_LAG + 2 * pairs)))
        def _():
            p = lax.div(i - FORWARD_LAG, 2)
            mine_to_chip(p, 0).wait_recv()
            chip_forward(p).start()

        return carry

    lax.fori_loop(0, max(groups + 2 * slots, groups + OUT_LAG, blocks + JOB_LAG, 2 * pairs + FORWARD_LAG - 1), step, 0)

    for i in (groups - 2, groups - 1):
        y_copy(i, i % 2).wait()
        ag_first_done(i, i % 2)
    for to_right in (True, False):
        far = z if to_right else last - z
        for s in range(slots):
            @pl.when(jnp.logical_and(far <= s, far < last))
            def _(s=s, to_right=to_right):
                rs_copy(groups - 1, s, to_right).wait_send()
        for a in range(1, slots):
            @pl.when(jnp.logical_and(far >= a, far < last))
            def _(a=a, to_right=to_right):
                ag_forward(groups - 1, a, to_right).wait_send()
    away_copy(pairs - 1).wait_send()
    for p in range(max(0, pairs - 2), pairs):
        mine_done(p, p % 2)
    for p in range(pairs):
        chip_forward(p).wait_send()
        chip_forward(p).wait_recv()
        mine_to_part(p, 0).wait_recv()
    for dt, dc in peers:
        gain_wait(dt, dc)
        gain_copy(dt, dc).wait_send()
    total = gain_all[0]
    for j in range(1, tp * cp):
        total += gain_all[j]
    gg_ref[...] = total


def backward_norm(dq, dkv, x, dy, o_all, normed, wq, wk, wv, wo_all, gain, rows, tp, cp):
    tokens, hidden = dq.shape
    d_model = x.shape[1]
    span = tp * rows
    groups = tokens // span
    slots = tp - 1
    width = WIDTH
    blocks = d_model // width
    pairs = blocks // 2
    hbm = pl.BlockSpec(memory_space=pl.ANY)
    vmem = pl.BlockSpec(memory_space=pltpu.VMEM)
    dma = pltpu.SemaphoreType.DMA
    bf = lambda *shape: pltpu.VMEM(shape, BF16)
    f32 = lambda *shape: pltpu.VMEM(shape, F32)
    return pl.pallas_call(
        functools.partial(back_kernel, groups, rows, tp, cp),
        in_specs=[hbm] * 10 + [vmem],
        out_specs=[hbm, hbm, hbm, hbm, vmem],
        out_shape=[
            jax.ShapeDtypeStruct((tokens, d_model), BF16),
            jax.ShapeDtypeStruct((tokens, d_model), BF16),
            jax.ShapeDtypeStruct((blocks, width, 4 * hidden), BF16),
            jax.ShapeDtypeStruct((blocks, width, 4 * hidden), BF16),
            jax.ShapeDtypeStruct((1, d_model), F32),
        ],
        scratch_shapes=[
            bf(d_model, hidden), bf(d_model, hidden), bf(d_model, hidden), bf(tp, hidden, d_model),
            bf(tokens, hidden), bf(2, tokens, hidden), bf(hidden, tokens),
            f32(PART_RING, span, d_model), bf(RS_RING, slots, rows, d_model), bf(RS_RING, slots, rows, d_model),
            bf(slots, rows, d_model), bf(slots, rows, d_model), f32(rows, d_model), bf(2, rows, d_model),
            bf(2, tp, span, hidden), bf(2, span, d_model), bf(2, rows, d_model), bf(2, rows, d_model), bf(2, span, d_model),
            bf(2, tokens, width), bf(2, tokens, width),
            f32(width, 4 * hidden), f32(2, width, 4 * hidden), bf(2, width, 4 * hidden), f32(tp * cp, 1, d_model),
            dma((8,)), dma((2, 2)), dma((2, 2)), dma((2, 2)), dma((2,)), dma((2,)),
            dma((slots,)), dma((slots,)), dma((RS_RING, slots)), dma((RS_RING, slots)),
            dma((2,)), dma((2,)), dma((slots,)), dma((slots,)), dma((groups, slots)), dma((groups, slots)),
            dma((1,)), dma((2,)), dma((2,)), dma((2,)), dma((2,)), dma((pairs,)), dma((pairs,)), dma((pairs,)), dma((pairs,)),
            dma((tp * cp,)), dma((tp * cp,)),
        ],
        compiler_params=pltpu.CompilerParams(collective_id=0, has_side_effects=True, vmem_limit_bytes=63 << 20),
        cost_estimate=pl.CostEstimate(flops=22 * tokens * hidden * d_model, bytes_accessed=16 * tokens * d_model, transcendentals=0),
        name="backward_norm",
    )(dq, dkv, x, dy, o_all, normed, wq, wk, wv, wo_all, gain)


def finish_kernel(y_ref, gx_ref, ga_ref, gb_ref, yo_ref, gxo_ref, wq_ref, wk_ref, wv_ref, wo_ref):
    yo_ref[...] = y_ref[...]
    gxo_ref[...] = gx_ref[...]
    width = ga_ref.shape[1]
    hidden = wq_ref.shape[1]
    for k, ref in enumerate((wq_ref, wk_ref, wv_ref)):
        cols = slice(k * hidden, (k + 1) * hidden)
        ref[...] = ga_ref[0, :, cols].astype(F32) + gb_ref[0, :, cols].astype(F32)
    for k in range(hidden // width):
        cols = slice(3 * hidden + k * width, 3 * hidden + (k + 1) * width)
        wo_ref[k * width:(k + 1) * width, :] = ga_ref[0, :, cols].astype(F32) + gb_ref[0, :, cols].astype(F32)


def finish(y, gx, ga, gb):
    tokens, d_model = y.shape
    blocks, width, packed = ga.shape
    hidden = packed // 4
    rows = tokens // blocks
    tile = pl.BlockSpec((rows, d_model), lambda j: (j, 0))
    block = pl.BlockSpec((1, width, packed), lambda j: (j, 0, 0))
    wide = pl.BlockSpec((width, hidden), lambda j: (j, 0))
    return pl.pallas_call(
        finish_kernel,
        grid=(blocks,),
        in_specs=[tile, tile, block, block],
        out_specs=[tile, tile, wide, wide, wide, pl.BlockSpec((hidden, width), lambda j: (0, j))],
        out_shape=[jax.ShapeDtypeStruct((tokens, d_model), BF16)] * 2 + [jax.ShapeDtypeStruct((d_model, hidden), F32)] * 3 + [jax.ShapeDtypeStruct((hidden, d_model), F32)],
        compiler_params=pltpu.CompilerParams(dimension_semantics=("arbitrary",), vmem_limit_bytes=48 << 20),
        cost_estimate=pl.CostEstimate(flops=8 * d_model * hidden, bytes_accessed=8 * tokens * d_model + 32 * d_model * hidden, transcendentals=0),
        name="finish",
    )(y, gx, ga, gb)


def solution(mesh):
    cp_size = mesh.shape["cp"]
    tp_size = mesh.shape["tp"]

    def device_step(x_in, segment_ids, positions, w_query, w_key, w_value, w_out, norm_gain, grad_out):
        batch, seq, d_model = x_in.shape
        tokens = batch * seq
        rank = lax.axis_index("cp")
        x = x_in.reshape(tokens, d_model)
        dy = grad_out.reshape(tokens, d_model)

        inv_freq = ROPE_THETA ** (-jnp.arange(0, HEAD_DIM, 2).astype(F32) / HEAD_DIM)
        angles = positions.reshape(tokens, 1).astype(F32) * jnp.repeat(inv_freq, 2)[None, :]
        cos_t, sin_t = jnp.cos(angles), jnp.sin(angles)
        start = (rank * seq + jnp.arange(seq, dtype=jnp.int32))[None, :] - positions

        gain = norm_gain.reshape(1, d_model)
        normed, o_all, dq, dkv, w_all = front(x, dy, w_query, w_key, w_value, w_out, cos_t, sin_t, start.reshape(batch, 1, seq), gain, seq, tp_size, cp_size)
        grad_x, y_out, sum_a, sum_b, grad_gain = backward_norm(dq, dkv, x, dy, o_all, normed, w_query, w_key, w_value, w_all, gain, ROWS, tp_size, cp_size)
        grad_gain = grad_gain.reshape(d_model)
        y_out, grad_x, grad_wq, grad_wk, grad_wv, grad_wo = finish(y_out, grad_x, sum_a, sum_b)
        return y_out.reshape(x_in.shape), grad_x.reshape(x_in.shape), grad_gain, grad_wq, grad_wk, grad_wv, grad_wo

    in_specs = (P("dp", "cp", None), P("dp", "cp"), P("dp", "cp"), P(None, "tp"), P(None, "tp"), P(None, "tp"), P("tp", None), P(None), P("dp", "cp", None))
    out_specs = (P("dp", "cp", None), P("dp", "cp", None), P("dp"), P("dp", "tp"), P("dp", "tp"), P("dp", "tp"), P(("dp", "tp"), None))
    return jax.shard_map(device_step, mesh=mesh, in_specs=in_specs, out_specs=out_specs, check_vma=False)
```

```python
import functools
import math

import jax
import jax.numpy as jnp
import numpy as np
from jax import lax
from jax.experimental import pallas as pl
from jax.experimental.pallas import tpu as pltpu
from jax.sharding import PartitionSpec as P

HEAD_DIM = 128
ROPE_THETA = 8000000.0
LN_EPS = 1e-5
NEG_BIG = -1e30
SCALE = HEAD_DIM ** -0.5
EXP2_SCALE = SCALE * math.log2(math.e)
F32 = jnp.float32
BF16 = jnp.bfloat16
NT = (((1,), (1,)), ((), ()))


def dot_nn(a, b):
    return jnp.dot(a, b, preferred_element_type=F32)


def dot_nt(a, b):
    return lax.dot_general(a, b, NT, preferred_element_type=F32)


def dot_tn(a, b):
    return lax.dot_general(a, b, (((0,), (0,)), ((), ())), preferred_element_type=F32)


def swap_pairs(t, sign):
    lane = lax.broadcasted_iota(jnp.int32, t.shape, 1)
    even = (lane % 2) == 0
    up = pltpu.roll(t, HEAD_DIM - 1, 1)
    down = pltpu.roll(t, 1, 1)
    return jnp.where(even, -up, down) if sign > 0 else jnp.where(even, up, -down)


def rope(t, cos_t, sin_t, sign):
    return t * cos_t + swap_pairs(t, sign) * sin_t


def angle_table():
    inv_freq = ROPE_THETA ** (-np.arange(0, HEAD_DIM, 2, dtype=np.float32) / np.float32(HEAD_DIM))
    freq = np.repeat(inv_freq.astype(np.float64), 2)[None, :]
    low = np.arange(POS_LOW)[:, None] * freq
    high = POS_LOW * np.arange(HEAD_DIM - POS_LOW)[:, None] * freq
    table = np.zeros((HEAD_DIM, 12 * HEAD_DIM), np.float32)
    for k, (first, value) in enumerate(((0, np.cos(low)), (0, np.sin(low)), (POS_LOW, np.cos(high)), (POS_LOW, np.sin(high)))):
        rest = value.astype(np.float32)
        for p in range(3):
            piece = rest.astype(BF16).astype(np.float32)
            at = (3 * k + p) * HEAD_DIM
            table[first:first + value.shape[0], at:at + HEAD_DIM] = piece
            rest = rest - piece
    return table


def put_rope(dst, raw, cos_t, sin_t):
    for h in range(raw.shape[1] // HEAD_DIM):
        cols = slice(h * HEAD_DIM, (h + 1) * HEAD_DIM)
        dst[:, cols] = rope(raw[:, cols], cos_t, sin_t, 1.0).astype(BF16)


MESH = pl.DeviceIdType.MESH
SUB = 128
ROWS = 16
WIDTH = 256
HALVES = 2
RELAY_LAG = 4
CHIP_BUFS = 4
OWN_RING = 6
Q_RING = 3
AHEAD = 2
POS_LOW = 64
W_TWIN = 3
W_PARTNER = 6


def front_kernel(batch, seq, tp, cp, x_hbm, dy_hbm, wq_hbm, wk_hbm, wv_hbm, wo_hbm, pos_ref, table_ref, gain_ref,
                 n_hbm, o_all, dq_hbm, dkv_hbm, w_all,
                 big, wo_ref, cos_ref, sin_ref, q_ring, do_ring, x_in, dy_in, n_buf, kv_own, kvr, s_scr, dp_scr, m_scr, l_scr, d_scr, ot_scr, dqt_scr,
                 o_buf, dq_buf, g_own, g_part, g_chip, g_far, xin, part_in,
                 w_sem, wl_sem, wz_send, wz_recv, wx_send, wx_recv,
                 x_sem, dy_sem, n_sem, kvs_part, kvs_chip, kvs_far, kv_recv, o_local, o_send, o_recv, relay_send, dq_sem,
                 far_send, part_send, chip_send, x_recv, part_recv, dkv_sem):
    z = lax.axis_index("tp")
    r = lax.axis_index("cp")
    dp = lax.axis_index("dp")
    core = lax.rem(r, 2)
    chip = lax.div(r, 2)
    d_model = x_hbm.shape[1]
    hidden = wq_hbm.shape[1]
    heads = hidden // HEAD_DIM
    first_chip, second_chip = chip == 0, chip == 1
    first_core, second_core = core == 0, core == 1
    partner = {"cp": r + 1 - 2 * core}
    peer = {"cp": r + 2 - 4 * chip}
    twin = {"dp": 1 - dp}

    tile = x_in.shape[1]
    per_row = seq // tile

    def row(b):
        return pl.ds(pl.multiple_of(b * seq, seq), seq)

    def tile_rows(b, k):
        return pl.ds(pl.multiple_of(b * seq + k * tile, tile), tile)

    def x_load(b, k):
        return pltpu.make_async_copy(x_hbm.at[tile_rows(b, k), :], x_in.at[k], x_sem.at[k])

    def dy_load(b, k):
        return pltpu.make_async_copy(dy_hbm.at[tile_rows(b, k), :], dy_in.at[k], dy_sem.at[k])

    def n_store(b, k):
        return pltpu.make_async_copy(n_buf.at[k], n_hbm.at[tile_rows(b, k), :], n_sem.at[k])

    weight_loads = [pltpu.make_async_copy(src, dst, w_sem.at[k]) for k, (src, dst) in enumerate(((wk_hbm, big.at[0]), (wv_hbm, big.at[1]), (wq_hbm, big.at[2]), (wo_hbm, wo_ref)))]
    x_load(0, 0).start()
    for copy in weight_loads[:2]:
        copy.start()
    for k in range(1, per_row):
        x_load(0, k).start()
    for copy in weight_loads[2:]:
        copy.start()
    for k in range(per_row):
        dy_load(0, k).start()

    units = batch * HALVES
    half = hidden // HALVES

    def where(u):
        return lax.div(u, HALVES), lax.rem(u, HALVES)

    def half_cols(g):
        return pl.ds(pl.multiple_of(g * half, half), half)

    barrier = pltpu.get_barrier_semaphore()
    for dev in [partner, peer, twin] + [{"tp": lax.rem(z + dt, tp)} for dt in range(1, tp)]:
        pl.semaphore_signal(barrier, inc=1, device_id=dev, device_id_type=MESH)
    pl.semaphore_wait(barrier, tp + 2)

    def remote(src, dst, ssem, rsem, dev):
        return pltpu.make_async_remote_copy(src_ref=src, dst_ref=dst, send_sem=ssem, recv_sem=rsem, device_id=dev, device_id_type=MESH)

    share = hidden // 8

    def share_rows(y, c, g):
        return pl.ds(pl.multiple_of((4 * y + 2 * c + g) * share, share), share)

    mine, twins = share_rows(chip, core, dp), share_rows(chip, core, 1 - dp)
    peers, peer_twins = share_rows(1 - chip, core, dp), share_rows(1 - chip, core, 1 - dp)

    def wz_copy(d):
        return remote(wo_hbm.at[mine, :], w_all.at[z, mine, :], wz_send.at[d], wz_recv.at[z], {"tp": lax.rem(z + d, tp)})

    def wz_wait(d):
        src = lax.rem(z + d, tp)
        remote(wo_hbm.at[mine, :], w_all.at[src, mine, :], wz_send.at[d], wz_recv.at[src], partner).wait_recv()

    def w_copy(k, d, rows, dev):
        place = w_all.at[lax.rem(z + d, tp), rows, :]
        return remote(place, place, wx_send.at[k, d], wx_recv.at[k, d], dev)

    def w_move(k, d):
        rows, dev = ((mine, twin), (mine, partner), (twins, partner), (mine, peer), (twins, peer), (peers, partner), (peer_twins, partner))[k]
        return w_copy(k, d, rows, dev)

    w_steps = range(1, tp)

    for d in range(1, tp):
        wz_copy(d).start()

    def kv_to_partner(u):
        return remote(kv_own.at[u], kvr.at[0, u], kvs_part.at[u], kv_recv.at[0, u], partner)

    def kv_to_chip(u):
        return remote(kv_own.at[u], kvr.at[1, u], kvs_chip.at[u], kv_recv.at[1, u], peer)

    def kv_forward(u):
        return remote(kvr.at[1, u], kvr.at[2, u], kvs_far.at[u], kv_recv.at[2, u], partner)

    w_local = pltpu.make_async_copy(wo_ref, w_all.at[z], wl_sem.at[0])
    for copy in weight_loads[:2]:
        copy.wait()

    def angles(b, k):
        rows = tile_rows(b, k)
        pos = jnp.broadcast_to(pos_ref[b, :, k * tile:(k + 1) * tile], (HEAD_DIM, tile)).T
        lane = lax.broadcasted_iota(jnp.int32, (tile, HEAD_DIM), 1)
        low = lane < POS_LOW
        pick = jnp.where(low, lax.rem(pos, POS_LOW), POS_LOW + lax.div(pos, POS_LOW)) == lane
        found = dot_nn(jnp.where(pick, 1.0, 0.0).astype(BF16), table_ref[...])

        def part(k):
            at = 3 * k * HEAD_DIM
            return found[:, at:at + HEAD_DIM] + found[:, at + HEAD_DIM:at + 2 * HEAD_DIM] + found[:, at + 2 * HEAD_DIM:at + 3 * HEAD_DIM]

        cos_b, sin_b, cos_a, sin_a = part(0), part(1), part(2), part(3)
        cos_ref[rows, :] = cos_a * cos_b - sin_a * sin_b
        sin_ref[rows, :] = sin_a * cos_b + cos_a * sin_b

    def project_row(b):
        ring = lax.rem(b, Q_RING)
        for k in range(per_row):
            rows = tile_rows(b, k)
            inside = slice(k * tile, (k + 1) * tile)
            x_load(b, k).wait()

            @pl.when(b > 0)
            def _(k=k):
                n_store(b - 1, k).wait()

            angles(b, k)
            x = x_in[k].astype(F32)
            centred = x - jnp.mean(x, axis=-1, keepdims=True)
            inv_std = lax.rsqrt(jnp.mean(centred * centred, axis=-1, keepdims=True) + LN_EPS)
            n_buf[k] = ((centred * inv_std) * gain_ref[...]).astype(BF16)
            n_store(b, k).start()

            @pl.when(b + 1 < batch)
            def _(k=k):
                x_load(b + 1, k).start()

            for g in range(HALVES):
                u = b * HALVES + g
                cols = slice(g * half, (g + 1) * half)
                put_rope(kv_own.at[u, 0, inside, :], dot_nn(n_buf[k], big[0, :, cols]), cos_ref[rows, :], sin_ref[rows, :])
                kv_own[u, 1, inside, :] = dot_nn(n_buf[k], big[1, :, cols]).astype(BF16)

        for g in range(HALVES):
            u = b * HALVES + g

            @pl.when(first_chip)
            def _(u=u):
                kv_to_chip(u).start()

            @pl.when(first_core)
            def _(u=u):
                kv_to_partner(u).start()

        @pl.when(b == 0)
        def _():
            for copy in weight_loads[2:]:
                copy.wait()
            w_local.start()

        for k in range(per_row):
            rows = tile_rows(b, k)
            inside = slice(k * tile, (k + 1) * tile)
            dy_load(b, k).wait()
            put_rope(q_ring.at[ring, inside, :], dot_nn(n_buf[k], big[2]), cos_ref[rows, :], sin_ref[rows, :])
            do_ring[ring, inside, :] = dot_nt(dy_in[k], wo_ref[...]).astype(BF16)

            @pl.when(b + 1 < batch)
            def _(k=k):
                dy_load(b + 1, k).start()

    def o_place(src, u):
        b, g = where(u)
        return o_all.at[src, row(b), half_cols(g)]

    def o_local_copy(b):
        return pltpu.make_async_copy(o_buf.at[b], o_place(z, b), o_local.at[b])

    def o_copy(b, k, step):
        return remote(o_buf.at[b], o_place(z, b), o_send.at[k, b], o_recv.at[z, b], {"tp": jnp.clip(z + step, 0, tp - 1)})

    hops = [(k, step, jnp.logical_and(z + step >= 0, z + step < tp)) for k, step in enumerate((1, -1, 2, -2))]

    def o_start(b):
        o_local_copy(b).start()
        for k, step, ok in hops:
            @pl.when(ok)
            def _(k=k, step=step):
                o_copy(b, k, step).start()

    def o_arrived(src, b):
        remote(o_place(src, b), o_place(src, b), relay_send.at[b], o_recv.at[src, b], partner).wait_recv()

    def relay_copy(b, src, dst):
        return remote(o_place(src, b), o_place(src, b), relay_send.at[b], o_recv.at[src, b], {"tp": dst})

    def relay(b):
        @pl.when(z == tp - 2)
        def _():
            o_arrived(0, b)
            relay_copy(b, 0, tp - 1).start()

        @pl.when(z == 1)
        def _():
            o_arrived(tp - 1, b)
            relay_copy(b, tp - 1, 0).start()

    def far_copy(b, par):
        return remote(g_far.at[par], xin.at[b], far_send.at[par], x_recv.at[b], partner)

    def part_copy(b, par):
        return remote(g_part.at[par], part_in.at[b], part_send.at[par], part_recv.at[b], partner)

    def chip_copy(b):
        par = lax.rem(b, CHIP_BUFS)
        return remote(g_chip.at[par], xin.at[b], chip_send.at[par], x_recv.at[b], peer)

    def chip_sum(b):
        @pl.when(second_chip)
        def _():
            par = lax.rem(b, CHIP_BUFS)
            far_copy(b, 0).wait_recv()
            g_chip[par] = (g_chip[par].astype(F32) + xin[b].astype(F32)).astype(BF16)
            chip_copy(b).start()

    def dkv_store(u, which):
        b, g = where(u)
        return pltpu.make_async_copy(g_own.at[lax.rem(u, OWN_RING), which], dkv_hbm.at[which, row(b), half_cols(g)], dkv_sem.at[u, which])

    def key_grads(u):
        @pl.when(first_core)
        def _():
            part_copy(u, 0).wait_recv()

        @pl.when(first_chip)
        def _():
            chip_copy(u).wait_recv()

        b, g = where(u)
        rows = row(b)
        for which in range(2):
            for h in range(half // HEAD_DIM):
                cols = slice(h * HEAD_DIM, (h + 1) * HEAD_DIM)
                own = g_own.at[lax.rem(u, OWN_RING), which, :, cols]
                acc = own[...].astype(F32)
                acc = acc + jnp.where(first_core, part_in[u, which, :, cols].astype(F32), 0.0)
                acc = (acc + jnp.where(first_chip, xin[u, which, :, cols].astype(F32), 0.0)).astype(BF16)
                if which == 0:
                    acc = rope(acc.astype(F32), cos_ref[rows, :], sin_ref[rows, :], -1.0).astype(BF16)
                own[...] = acc
            dkv_store(u, which).start()

    def dq_store(b, par):
        return pltpu.make_async_copy(dq_buf.at[par], dq_hbm.at[row(where(b)[0]), half_cols(where(b)[1])], dq_sem.at[par])

    subs = range(0, seq, SUB)

    def attend_unit(i, par):
        b, g = where(i)
        rows = row(b)
        ring = lax.rem(b, Q_RING)
        start = r * seq + lax.broadcasted_iota(jnp.int32, (1, seq), 1) - pos_ref[b]
        chip_par = lax.rem(i, CHIP_BUFS)
        keys_of = [kv_own.at[i]] + [kvr.at[s, i] for s in range(3)]
        places = [g_part.at[par], g_chip.at[chip_par], g_far.at[par]]

        def grad(slot, which, cols):
            return places[slot - 1].at[which, :, cols] if slot else g_own.at[lax.rem(i, OWN_RING), which, :, cols]

        live = [None, second_core, second_chip, second_chip]
        piece = [r, r + 1 - 2 * core, r + 2 - 4 * chip, r + 3 - 2 * core - 4 * chip]

        def each(body):
            body(0)
            for slot in (1, 2, 3):
                pl.when(live[slot])(functools.partial(body, slot))

        def one_head(h, carry):
            cols = pl.ds(pl.multiple_of(h * HEAD_DIM, HEAD_DIM), HEAD_DIM)
            full = pl.ds(pl.multiple_of(g * half + h * HEAD_DIM, HEAD_DIM), HEAD_DIM)
            q = q_ring[ring, :, full]
            do = do_ring[ring, :, full]
            m_scr[...] = jnp.full(m_scr.shape, NEG_BIG, F32)
            l_scr[...] = jnp.zeros_like(l_scr)
            d_scr[...] = jnp.zeros_like(d_scr)
            ot_scr[...] = jnp.zeros_like(ot_scr)
            dqt_scr[...] = jnp.zeros_like(dqt_scr)

            def scores(slot):
                base = piece[slot] * seq
                for s in subs:
                    raw = dot_nt(keys_of[slot][0, s:s + SUB, cols], q)
                    local = lax.broadcasted_iota(jnp.int32, raw.shape, 0) + s
                    allowed = (local + base) >= start
                    if slot == 0:
                        allowed = jnp.logical_and(allowed, local <= lax.broadcasted_iota(jnp.int32, raw.shape, 1))
                    raw = jnp.where(allowed, raw, NEG_BIG)
                    s_scr[slot, s:s + SUB, :] = raw
                    m_scr[...] = jnp.maximum(m_scr[...], jnp.max(raw, axis=0, keepdims=True))

            def exps(slot):
                for s in subs:
                    e = jnp.exp2((s_scr[slot, s:s + SUB, :] - m_scr[...]) * EXP2_SCALE)
                    s_scr[slot, s:s + SUB, :] = e
                    l_scr[...] += jnp.sum(e, axis=0, keepdims=True)

            def values(slot):
                for s in subs:
                    v = keys_of[slot][1, s:s + SUB, cols]
                    prob = s_scr[slot, s:s + SUB, :] * l_scr[...]
                    low = prob.astype(BF16)
                    dp = dot_nt(v, do)
                    s_scr[slot, s:s + SUB, :] = prob
                    dp_scr[slot, s:s + SUB, :] = dp
                    d_scr[...] += jnp.sum(prob * dp, axis=0, keepdims=True)
                    grad(slot, 1, cols)[s:s + SUB, :] = dot_nn(low, do).astype(BF16)
                    ot_scr[...] += dot_nn(v.T, low)

            def keys(slot):
                for s in subs:
                    k = keys_of[slot][0, s:s + SUB, cols]
                    ds = (s_scr[slot, s:s + SUB, :] * (dp_scr[slot, s:s + SUB, :] - d_scr[...])).astype(BF16)
                    grad(slot, 0, cols)[s:s + SUB, :] = (dot_nn(ds, q) * SCALE).astype(BF16)
                    dqt_scr[...] += dot_nn(k.T, ds)

            each(scores)
            each(exps)
            l_scr[...] = 1.0 / l_scr[...]
            each(values)
            each(keys)
            o_buf[i, :, cols] = ot_scr[...].T.astype(BF16)
            dq_buf[par, :, cols] = rope(dqt_scr[...].T * SCALE, cos_ref[rows, :], sin_ref[rows, :], -1.0).astype(BF16)
            return carry

        lax.fori_loop(0, heads // HALVES, one_head, 0)

    def step(i, carry):
        par = lax.rem(i, 2)
        @pl.when(jnp.logical_and(lax.rem(i, HALVES) == 0, lax.div(i, HALVES) + AHEAD < batch))
        def _():
            project_row(lax.div(i, HALVES) + AHEAD)

        @pl.when(i >= OWN_RING)
        def _():
            for which in range(2):
                dkv_store(i - OWN_RING, which).wait()

        @pl.when(second_chip)
        def _():
            kv_to_chip(i).wait_recv()
            kv_forward(i).start()

        @pl.when(second_core)
        def _():
            kv_to_partner(i).wait_recv()

        @pl.when(second_chip)
        def _():
            kv_forward(i).wait_recv()

        @pl.when(i >= 2)
        def _():
            dq_store(i - 2, par).wait()

            @pl.when(second_core)
            def _():
                part_copy(i - 2, par).wait_send()

            @pl.when(second_chip)
            def _():
                far_copy(i - 2, par).wait_send()

        @pl.when(jnp.logical_and(second_chip, i >= CHIP_BUFS))
        def _():
            chip_copy(i - CHIP_BUFS).wait_send()

        attend_unit(i, par)
        o_start(i)
        dq_store(i, par).start()

        @pl.when(second_chip)
        def _():
            far_copy(i, par).start()

        @pl.when(second_core)
        def _():
            part_copy(i, par).start()

        @pl.when(i >= 1)
        def _():
            chip_sum(i - 1)

        @pl.when(i >= RELAY_LAG)
        def _():
            key_grads(i - RELAY_LAG)
            relay(i - RELAY_LAG)

        @pl.when(i == min(W_TWIN, units - 1))
        def _():
            for d in w_steps:
                wz_wait(d)
                w_move(0, d).start()
                w_move(1, d).start()

                @pl.when(second_chip)
                def _(d=d):
                    w_move(3, d).start()

        @pl.when(i == min(W_PARTNER, units - 1))
        def _():
            for d in w_steps:
                w_move(0, d).wait_recv()
                w_move(2, d).start()

                @pl.when(second_chip)
                def _(d=d):
                    w_move(4, d).start()

        return carry

    for b in range(min(AHEAD, batch)):
        project_row(b)
    lax.fori_loop(0, units, step, 0)
    chip_sum(units - 1)

    @pl.when(first_chip)
    def _():
        for u in range(units):
            kv_to_chip(u).wait_send()
        for k in (3, 4):
            for d in w_steps:
                w_move(k, d).start()

    lag = min(RELAY_LAG, units)
    for u in range(lag):
        key_grads(units - lag + u)
        relay(units - lag + u)
        if u == min(1, lag - 1):
            for k in (3, 4):
                for d in w_steps:
                    w_move(k, d).wait_recv()
                    w_move(k + 2, d).start()

    w_local.wait()
    for d in w_steps:
        wz_copy(d).wait_send()
        for k in range(7):
            w_move(k, d).wait_send()
            if k in (1, 2, 5, 6):
                w_move(k, d).wait_recv()

    for k in range(per_row):
        n_store(batch - 1, k).wait()
    for u in range(max(0, units - OWN_RING), units):
        for which in range(2):
            dkv_store(u, which).wait()

    def drain(b, carry):
        @pl.when(first_core)
        def _():
            kv_to_partner(b).wait_send()

        @pl.when(second_chip)
        def _():
            kv_forward(b).wait_send()

        o_local_copy(b).wait()
        for k, step_, ok in hops:
            @pl.when(ok)
            def _(k=k, step_=step_):
                o_copy(b, k, step_).wait_send()

        @pl.when(jnp.logical_or(z == 1, z == tp - 2))
        def _():
            relay_copy(b, 0, tp - 1).wait_send()

        for src in range(tp):
            taken = jnp.logical_or(jnp.logical_and(z == tp - 2, src == 0), jnp.logical_and(z == 1, src == tp - 1))

            @pl.when(jnp.logical_and(z != src, jnp.logical_not(taken)))
            def _(src=src):
                o_arrived(src, b)

        return carry

    lax.fori_loop(0, units, drain, 0)

    for b in range(max(0, units - 2), units):
        dq_store(b, b % 2).wait()

        @pl.when(second_core)
        def _(b=b):
            part_copy(b, b % 2).wait_send()

        @pl.when(second_chip)
        def _(b=b):
            far_copy(b, b % 2).wait_send()

    for b in range(max(0, units - CHIP_BUFS), units):
        @pl.when(second_chip)
        def _(b=b):
            chip_copy(b).wait_send()


def front(x, dy, wq, wk, wv, wo, pos, table, gain, seq, tp, cp):
    tokens, d_model = x.shape
    hidden = wq.shape[1]
    batch = tokens // seq
    units = batch * HALVES
    half = hidden // HALVES
    tile = seq // 2
    hbm = pl.BlockSpec(memory_space=pl.ANY)
    vmem = pl.BlockSpec(memory_space=pltpu.VMEM)
    dma = pltpu.SemaphoreType.DMA
    bf = lambda *shape: pltpu.VMEM(shape, BF16)
    f32 = lambda *shape: pltpu.VMEM(shape, F32)
    return pl.pallas_call(
        functools.partial(front_kernel, batch, seq, tp, cp),
        in_specs=[hbm] * 6 + [vmem] * 3,
        out_specs=[hbm] * 5,
        out_shape=[
            jax.ShapeDtypeStruct((tokens, d_model), BF16),
            jax.ShapeDtypeStruct((tp, tokens, hidden), BF16),
            jax.ShapeDtypeStruct((tokens, hidden), BF16),
            jax.ShapeDtypeStruct((2, tokens, hidden), BF16),
            jax.ShapeDtypeStruct((tp, hidden, d_model), BF16),
        ],
        scratch_shapes=[
            bf(3, d_model, hidden), bf(hidden, d_model), f32(tokens, HEAD_DIM), f32(tokens, HEAD_DIM),
            bf(Q_RING, seq, hidden), bf(Q_RING, seq, hidden), bf(2, tile, d_model), bf(2, tile, d_model), bf(2, tile, d_model),
            bf(units, 2, seq, half), bf(3, units, 2, seq, half),
            f32(4, seq, seq), f32(4, seq, seq), f32(1, seq), f32(1, seq), f32(1, seq), f32(HEAD_DIM, seq), f32(HEAD_DIM, seq),
            bf(units, seq, half), bf(2, seq, half),
            bf(OWN_RING, 2, seq, half), bf(2, 2, seq, half), bf(CHIP_BUFS, 2, seq, half), bf(2, 2, seq, half),
            bf(units, 2, seq, half), bf(units, 2, seq, half),
            dma((4,)), dma((1,)), dma((tp,)), dma((tp,)), dma((7, tp)), dma((7, tp)),
            dma((2,)), dma((2,)), dma((2,)), dma((units,)), dma((units,)), dma((units,)), dma((3, units)),
            dma((units,)), dma((4, units)), dma((tp, units)), dma((units,)), dma((2,)),
            dma((2,)), dma((2,)), dma((CHIP_BUFS,)), dma((units,)), dma((units,)), dma((units, 2)),
        ],
        compiler_params=pltpu.CompilerParams(collective_id=1, has_side_effects=True, vmem_limit_bytes=63 << 20),
        cost_estimate=pl.CostEstimate(flops=60 * tokens * seq * hidden, bytes_accessed=16 * tokens * d_model, transcendentals=4 * tokens * seq * (hidden // HEAD_DIM)),
        name="front",
    )(x, dy, wq, wk, wv, wo, pos, table, gain)


PART_RING = 4
RS_RING = 5
FORWARD_LAG = 11
JOB_LAG = 5
OUT_LAG = 4
EARLY = 4


def back_kernel(groups, rows, tp, cp, dq_hbm, dkv_hbm, x_hbm, dy_hbm, o_hbm, n_hbm, wq_hbm, wk_hbm, wv_hbm, wo_hbm, gain_ref,
                gx_hbm, y_hbm, ga_hbm, gb_hbm, gg_ref,
                wq_ref, wk_ref, wv_ref, wo_ref, dq_all, dkv_all, o_t, part, rs_r, rs_l, send_r, send_l, tot, gx_buf,
                o_in, x_in, xo_in, dyo_in, y_buf, n_in, dy_in, away, part_in, mine, gain_all,
                w_sem, in_sem, fin_sem, job_sem, y_sem, own_sem, rss_r, rss_l, rsr_r, rsr_l, ag0_r, ag0_l, agf_r, agf_l, agr_r, agr_l,
                away_send, away_recv, mine_own, mine_part, mine_chip, ga_recv, chip_recv, gb_send, gb_recv, gs_sem, gr_sem):
    z = lax.axis_index("tp")
    r = lax.axis_index("cp")
    core = lax.rem(r, 2)
    chip = lax.div(r, 2)
    last = tp - 1
    slots = tp - 1
    span = tp * rows
    tokens, d_model = x_hbm.shape
    hidden = dq_hbm.shape[1]
    chunk = min(512, d_model)
    blocks = ga_hbm.shape[0]
    width = ga_hbm.shape[1]
    pairs = blocks // 2
    partner = {"cp": r + 1 - 2 * core}
    peer = {"cp": r + 2 - 4 * chip}

    head = min(EARLY, groups) * span
    weight_loads = [pltpu.make_async_copy(src, dst, w_sem.at[k]) for k, (src, dst) in enumerate((
        (dq_hbm.at[:head, :], dq_all.at[:head, :]), (dkv_hbm.at[:, :head, :], dkv_all.at[:, :head, :]), (wq_hbm, wq_ref), (wk_hbm, wk_ref), (wv_hbm, wv_ref)))]
    rest_loads = [] if head == tokens else [
        pltpu.make_async_copy(dq_hbm.at[head:, :], dq_all.at[head:, :], w_sem.at[6]),
        pltpu.make_async_copy(dkv_hbm.at[:, head:, :], dkv_all.at[:, head:, :], w_sem.at[7]),
    ]
    out_loads = [pltpu.make_async_copy(wo_hbm, wo_ref, w_sem.at[5])]
    for copy in weight_loads:
        copy.start()

    barrier = pltpu.get_barrier_semaphore()
    peers = [(dt, dc) for dt in range(tp) for dc in range(cp) if dt or dc]
    for dt, dc in peers:
        pl.semaphore_signal(barrier, inc=1, device_id={"tp": lax.rem(z + dt, tp), "cp": lax.rem(r + dc, cp)}, device_id_type=MESH)
    pl.semaphore_wait(barrier, len(peers))

    def remote(src, dst, ssem, rsem, dev):
        return pltpu.make_async_remote_copy(src_ref=src, dst_ref=dst, send_sem=ssem, recv_sem=rsem, device_id=dev, device_id_type=MESH)

    right = {"tp": jnp.where(z < last, z + 1, z)}
    left = {"tp": jnp.where(z > 0, z - 1, z)}

    def group_rows(i):
        return pl.ds(pl.multiple_of(i * span, span), span)

    def tile_rows(i, owner):
        return pl.ds(pl.multiple_of(i * span + owner * rows, rows), rows)

    def inputs(i, slot):
        g = group_rows(i)
        return [
            pltpu.make_async_copy(o_hbm.at[:, g, :], o_in.at[slot], in_sem.at[slot, 0]),
            pltpu.make_async_copy(x_hbm.at[g, :], x_in.at[slot], in_sem.at[slot, 1]),
        ]

    def final_inputs(i, slot):
        g = tile_rows(i, z)
        return [
            pltpu.make_async_copy(x_hbm.at[g, :], xo_in.at[slot], fin_sem.at[slot, 0]),
            pltpu.make_async_copy(dy_hbm.at[g, :], dyo_in.at[slot], fin_sem.at[slot, 1]),
        ]

    def y_copy(i, slot):
        return pltpu.make_async_copy(y_buf.at[slot], y_hbm.at[group_rows(i), :], y_sem.at[slot])

    def rs_copy(i, s, to_right):
        ring = lax.rem(i, RS_RING)
        if to_right:
            return remote(send_r.at[s], rs_r.at[ring, s], rss_r.at[s], rsr_r.at[ring, s], right)
        return remote(send_l.at[s], rs_l.at[ring, s], rss_l.at[s], rsr_l.at[ring, s], left)

    def rs_send(i, s):
        for to_right in (True, False):
            far = z if to_right else last - z
            owner = (z + slots - s) if to_right else (z - slots + s)
            buf, held = (send_r, rs_r) if to_right else (send_l, rs_l)

            @pl.when(jnp.logical_and(jnp.logical_and(i >= 0, i < groups), jnp.logical_and(far <= s, far < last)))
            def _(to_right=to_right, far=far, owner=owner, buf=buf, held=held):
                @pl.when(i > 0)
                def _():
                    rs_copy(i - 1, s, to_right).wait_send()

                cur = lax.rem(i, PART_RING)
                own = pl.ds(pl.multiple_of(owner * rows, rows), rows)
                if s == 0:
                    buf[s] = part[cur, own, :].astype(BF16)
                else:
                    @pl.when(far == 0)
                    def _():
                        buf[s] = part[cur, own, :].astype(BF16)

                    @pl.when(far > 0)
                    def _():
                        rs_copy(i, s - 1, to_right).wait_recv()
                        buf[s] = (part[cur, own, :] + held[lax.rem(i, RS_RING), s - 1].astype(F32)).astype(BF16)

                rs_copy(i, s, to_right).start()

    def ag_own(i, slot, to_right):
        src = gx_buf.at[slot]
        dst = gx_hbm.at[tile_rows(i, z), :]
        if to_right:
            return remote(src, dst, ag0_r.at[slot], agr_r.at[i, 0], right)
        return remote(src, dst, ag0_l.at[slot], agr_l.at[i, 0], left)

    def own_copy(i, slot):
        return pltpu.make_async_copy(gx_buf.at[slot], gx_hbm.at[tile_rows(i, z), :], own_sem.at[slot])

    def ag_forward(i, a, to_right):
        owner = z - a if to_right else z + a
        tile = gx_hbm.at[tile_rows(i, owner), :]
        if to_right:
            return remote(tile, tile, agf_r.at[a], agr_r.at[i, a], right)
        return remote(tile, tile, agf_l.at[a], agr_l.at[i, a], left)

    def ag_wait(i, a, to_right):
        tile = gx_hbm.at[tile_rows(i, 0), :]
        sem = agr_r.at[i, a] if to_right else agr_l.at[i, a]
        remote(tile, tile, agf_r.at[a], sem, right).wait_recv()

    def ag_step(i, a):
        for to_right in (True, False):
            far = z if to_right else last - z

            @pl.when(jnp.logical_and(jnp.logical_and(i >= 0, i < groups), far >= a))
            def _(to_right=to_right, far=far):
                ag_wait(i, a - 1, to_right)
                if a < slots:
                    @pl.when(far < last)
                    def _():
                        @pl.when(i > 0)
                        def _():
                            ag_forward(i - 1, a, to_right).wait_send()

                        ag_forward(i, a, to_right).start()

    def ag_first(i, slot):
        own_copy(i, slot).start()
        for to_right in (True, False):
            far = z if to_right else last - z

            @pl.when(far < last)
            def _(to_right=to_right):
                ag_own(i, slot, to_right).start()

    def ag_first_done(i, slot):
        own_copy(i, slot).wait()
        for to_right in (True, False):
            far = z if to_right else last - z

            @pl.when(far < last)
            def _(to_right=to_right):
                ag_own(i, slot, to_right).wait_send()

    def partial_norm(i):
        cur = lax.rem(i, PART_RING)
        g = group_rows(i)
        for c in range(0, d_model, chunk):
            cols = slice(c, c + chunk)
            part[cur, :, cols] = (
                dot_nt(dq_all[g, :], wq_ref[cols, :]) + dot_nt(dkv_all[0, g, :], wk_ref[cols, :]) + dot_nt(dkv_all[1, g, :], wv_ref[cols, :])
            )

    def project_out(cur):
        for c in range(0, d_model, chunk):
            cols = slice(c, c + chunk)
            acc = x_in[cur, :, cols].astype(F32)
            for t in range(tp):
                acc += dot_nn(o_in[cur, t], wo_ref[t, :, cols])
            y_buf[cur, :, cols] = acc.astype(BF16)

    def finalize(i):
        slot = lax.rem(i, 2)
        own = pl.ds(pl.multiple_of(z * rows, rows), rows)
        tot[...] = part[lax.rem(i, PART_RING), own, :]

        @pl.when(z > 0)
        def _():
            rs_copy(i, slots - 1, True).wait_recv()
            tot[...] += rs_r[lax.rem(i, RS_RING), slots - 1].astype(F32)

        @pl.when(z < last)
        def _():
            rs_copy(i, slots - 1, False).wait_recv()
            tot[...] += rs_l[lax.rem(i, RS_RING), slots - 1].astype(F32)

        @pl.when(i > 1)
        def _():
            ag_first_done(i - 2, slot)

        for copy in final_inputs(i, slot):
            copy.wait()
        x = xo_in[slot].astype(F32)
        centred = x - jnp.mean(x, axis=-1, keepdims=True)
        inv_std = lax.rsqrt(jnp.mean(centred * centred, axis=-1, keepdims=True) + LN_EPS)
        x_hat = centred * inv_std
        dn = tot[...]
        gg_ref[...] += jnp.sum(dn * x_hat, axis=0, keepdims=True)
        d_hat = dn * gain_ref[...]
        dx = inv_std * (d_hat - jnp.mean(d_hat, axis=-1, keepdims=True) - x_hat * jnp.mean(d_hat * x_hat, axis=-1, keepdims=True))
        gx_buf[slot] = (dyo_in[slot].astype(F32) + dx).astype(BF16)
        ag_first(i, slot)

    def block_of(t):
        return 2 * lax.div(t, 2) + jnp.where(lax.rem(t, 2) == 0, 1 - core, core)

    def job_loads(t, slot):
        cols = pl.ds(pl.multiple_of(block_of(t) * width, width), width)
        return [
            pltpu.make_async_copy(n_hbm.at[:, cols], n_in.at[slot], job_sem.at[slot, 0]),
            pltpu.make_async_copy(dy_hbm.at[:, cols], dy_in.at[slot], job_sem.at[slot, 1]),
        ]

    def away_copy(p):
        ring = lax.rem(p, 2)
        return remote(away, part_in.at[ring], away_send.at[0], away_recv.at[ring], partner)

    def job_block(t, put):
        slot = lax.rem(t, 2)
        n_t = n_in[slot].T
        put(0, hidden, dot_nn(n_t, dq_all[...]))
        put(hidden, hidden, dot_nn(n_t, dkv_all[0]))
        put(2 * hidden, hidden, dot_nn(n_t, dkv_all[1]))
        for k in range(hidden // width):
            put(3 * hidden + k * width, width, dot_nn(o_t[k * width:(k + 1) * width, :], dy_in[slot]))

    def mine_to_own(p, slot):
        return pltpu.make_async_copy(mine.at[slot], ga_hbm.at[2 * p + core], mine_own.at[slot])

    def mine_to_part(p, slot):
        return remote(mine.at[slot], ga_hbm.at[2 * p + core], mine_part.at[slot], ga_recv.at[p], partner)

    def mine_to_chip(p, slot):
        return remote(mine.at[slot], gb_hbm.at[2 * p + core], mine_chip.at[slot], chip_recv.at[p], peer)

    def mine_done(p, slot):
        mine_to_own(p, slot).wait()
        mine_to_part(p, slot).wait_send()
        mine_to_chip(p, slot).wait_send()

    def chip_forward(p):
        b = 2 * p + core
        return remote(gb_hbm.at[b], gb_hbm.at[b], gb_send.at[p], gb_recv.at[p], partner)

    def job(t):
        p = lax.div(t, 2)
        for copy in job_loads(t, lax.rem(t, 2)):
            copy.wait()

        @pl.when(t + 1 < blocks)
        def _():
            for copy in job_loads(t + 1, 1 - lax.rem(t, 2)):
                copy.start()

        @pl.when(lax.rem(t, 2) == 0)
        def _():
            @pl.when(p > 0)
            def _():
                away_copy(p - 1).wait_send()

            def put(at, size, value):
                away[:, at:at + size] = value

            job_block(t, put)
            away_copy(p).start()

        @pl.when(lax.rem(t, 2) == 1)
        def _():
            slot = lax.rem(p, 2)
            away_copy(p).wait_recv()

            @pl.when(p > 1)
            def _():
                mine_done(p - 2, slot)

            def put(at, size, value):
                mine[slot, :, at:at + size] = (value + part_in[slot, :, at:at + size]).astype(BF16)

            job_block(t, put)
            mine_to_chip(p, slot).start()
            mine_to_part(p, slot).start()
            mine_to_own(p, slot).start()

    gg_ref[...] = jnp.zeros_like(gg_ref)
    o_loads = [pltpu.make_async_copy(o_hbm.at[z, :, k * width:(k + 1) * width], n_in.at[k], job_sem.at[k, 0]) for k in range(hidden // width)]
    for copy in o_loads:
        copy.start()
    for copy in inputs(0, 0):
        copy.start()
    for copy in rest_loads + out_loads:
        copy.start()
    me = z * cp + r

    def gain_copy(dt, dc):
        to = {"tp": lax.rem(z + dt, tp), "cp": lax.rem(r + dc, cp)}
        return remote(gain_all.at[me], gain_all.at[me], gs_sem.at[dt * cp + dc], gr_sem.at[me], to)

    def gain_wait(dt, dc):
        sender = lax.rem(z + dt, tp) * cp + lax.rem(r + dc, cp)
        remote(gain_all.at[sender], gain_all.at[sender], gs_sem.at[0], gr_sem.at[sender], right).wait_recv()

    for copy in weight_loads:
        copy.wait()

    def step(i, carry):
        for k in reversed(range(1, slots)):
            rs_send(i - k, k)

        @pl.when(i == EARLY)
        def _():
            for copy in rest_loads:
                copy.wait()

        @pl.when(i < groups)
        def _():
            partial_norm(i)

        rs_send(i, 0)

        @pl.when(jnp.logical_and(i >= slots, i < groups + slots))
        def _():
            finalize(i - slots)

        for a in range(1, slots + 1):
            ag_step(i - slots - a, a)

        @pl.when(i == groups + slots - 1)
        def _():
            gain_all[me] = gg_ref[...]
            for dt, dc in peers:
                gain_copy(dt, dc).start()

        @pl.when(jnp.logical_and(i >= slots - 1, i < groups + slots - 1))
        def _():
            for copy in final_inputs(i - slots + 1, lax.rem(i - slots + 1, 2)):
                copy.start()

        @pl.when(i == JOB_LAG - 1)
        def _():
            for k, copy in enumerate(o_loads):
                copy.wait()
                o_t[k * width:(k + 1) * width, :] = n_in[k].T
            for copy in job_loads(0, 0):
                copy.start()

        @pl.when(i == OUT_LAG)
        def _():
            for copy in out_loads:
                copy.wait()

        @pl.when(jnp.logical_and(i >= OUT_LAG, i < groups + OUT_LAG))
        def _():
            j = i - OUT_LAG
            at = lax.rem(j, 2)
            for copy in inputs(j, at):
                copy.wait()

            @pl.when(j + 1 < groups)
            def _():
                for copy in inputs(j + 1, 1 - at):
                    copy.start()

            @pl.when(j >= 2)
            def _():
                y_copy(j - 2, at).wait()

            project_out(at)
            y_copy(j, at).start()

        @pl.when(jnp.logical_and(i >= JOB_LAG, i < JOB_LAG + blocks))
        def _():
            job(i - JOB_LAG)

        @pl.when(jnp.logical_and(lax.rem(i, 2) == 1, jnp.logical_and(i >= FORWARD_LAG, i < FORWARD_LAG + 2 * pairs)))
        def _():
            p = lax.div(i - FORWARD_LAG, 2)
            mine_to_chip(p, 0).wait_recv()
            chip_forward(p).start()

        return carry

    lax.fori_loop(0, max(groups + 2 * slots, groups + OUT_LAG, blocks + JOB_LAG, 2 * pairs + FORWARD_LAG - 1), step, 0)

    for i in (groups - 2, groups - 1):
        y_copy(i, i % 2).wait()
        ag_first_done(i, i % 2)
    for to_right in (True, False):
        far = z if to_right else last - z
        for s in range(slots):
            @pl.when(jnp.logical_and(far <= s, far < last))
            def _(s=s, to_right=to_right):
                rs_copy(groups - 1, s, to_right).wait_send()
        for a in range(1, slots):
            @pl.when(jnp.logical_and(far >= a, far < last))
            def _(a=a, to_right=to_right):
                ag_forward(groups - 1, a, to_right).wait_send()
    away_copy(pairs - 1).wait_send()
    for p in range(max(0, pairs - 2), pairs):
        mine_done(p, p % 2)
    for p in range(pairs):
        chip_forward(p).wait_send()
        chip_forward(p).wait_recv()
        mine_to_part(p, 0).wait_recv()
    for dt, dc in peers:
        gain_wait(dt, dc)
        gain_copy(dt, dc).wait_send()
    total = gain_all[0]
    for j in range(1, tp * cp):
        total += gain_all[j]
    gg_ref[...] = total


def backward_norm(dq, dkv, x, dy, o_all, normed, wq, wk, wv, wo_all, gain, rows, tp, cp):
    tokens, hidden = dq.shape
    d_model = x.shape[1]
    span = tp * rows
    groups = tokens // span
    slots = tp - 1
    width = WIDTH
    blocks = d_model // width
    pairs = blocks // 2
    hbm = pl.BlockSpec(memory_space=pl.ANY)
    vmem = pl.BlockSpec(memory_space=pltpu.VMEM)
    dma = pltpu.SemaphoreType.DMA
    bf = lambda *shape: pltpu.VMEM(shape, BF16)
    f32 = lambda *shape: pltpu.VMEM(shape, F32)
    return pl.pallas_call(
        functools.partial(back_kernel, groups, rows, tp, cp),
        in_specs=[hbm] * 10 + [vmem],
        out_specs=[hbm, hbm, hbm, hbm, vmem],
        out_shape=[
            jax.ShapeDtypeStruct((tokens, d_model), BF16),
            jax.ShapeDtypeStruct((tokens, d_model), BF16),
            jax.ShapeDtypeStruct((blocks, width, 4 * hidden), BF16),
            jax.ShapeDtypeStruct((blocks, width, 4 * hidden), BF16),
            jax.ShapeDtypeStruct((1, d_model), F32),
        ],
        scratch_shapes=[
            bf(d_model, hidden), bf(d_model, hidden), bf(d_model, hidden), bf(tp, hidden, d_model),
            bf(tokens, hidden), bf(2, tokens, hidden), bf(hidden, tokens),
            f32(PART_RING, span, d_model), bf(RS_RING, slots, rows, d_model), bf(RS_RING, slots, rows, d_model),
            bf(slots, rows, d_model), bf(slots, rows, d_model), f32(rows, d_model), bf(2, rows, d_model),
            bf(2, tp, span, hidden), bf(2, span, d_model), bf(2, rows, d_model), bf(2, rows, d_model), bf(2, span, d_model),
            bf(2, tokens, width), bf(2, tokens, width),
            f32(width, 4 * hidden), f32(2, width, 4 * hidden), bf(2, width, 4 * hidden), f32(tp * cp, 1, d_model),
            dma((8,)), dma((2, 2)), dma((2, 2)), dma((2, 2)), dma((2,)), dma((2,)),
            dma((slots,)), dma((slots,)), dma((RS_RING, slots)), dma((RS_RING, slots)),
            dma((2,)), dma((2,)), dma((slots,)), dma((slots,)), dma((groups, slots)), dma((groups, slots)),
            dma((1,)), dma((2,)), dma((2,)), dma((2,)), dma((2,)), dma((pairs,)), dma((pairs,)), dma((pairs,)), dma((pairs,)),
            dma((tp * cp,)), dma((tp * cp,)),
        ],
        compiler_params=pltpu.CompilerParams(collective_id=0, has_side_effects=True, vmem_limit_bytes=63 << 20),
        cost_estimate=pl.CostEstimate(flops=22 * tokens * hidden * d_model, bytes_accessed=16 * tokens * d_model, transcendentals=0),
        name="backward_norm",
    )(dq, dkv, x, dy, o_all, normed, wq, wk, wv, wo_all, gain)


def finish_kernel(y_ref, gx_ref, ga_ref, gb_ref, yo_ref, gxo_ref, wq_ref, wk_ref, wv_ref, wo_ref):
    yo_ref[...] = y_ref[...]
    gxo_ref[...] = gx_ref[...]
    width = ga_ref.shape[1]
    hidden = wq_ref.shape[1]
    for k, ref in enumerate((wq_ref, wk_ref, wv_ref)):
        cols = slice(k * hidden, (k + 1) * hidden)
        ref[...] = ga_ref[0, :, cols].astype(F32) + gb_ref[0, :, cols].astype(F32)
    for k in range(hidden // width):
        cols = slice(3 * hidden + k * width, 3 * hidden + (k + 1) * width)
        wo_ref[k * width:(k + 1) * width, :] = ga_ref[0, :, cols].astype(F32) + gb_ref[0, :, cols].astype(F32)


def finish(y, gx, ga, gb):
    tokens, d_model = y.shape
    blocks, width, packed = ga.shape
    hidden = packed // 4
    rows = tokens // blocks
    tile = pl.BlockSpec((rows, d_model), lambda j: (j, 0))
    block = pl.BlockSpec((1, width, packed), lambda j: (j, 0, 0))
    wide = pl.BlockSpec((width, hidden), lambda j: (j, 0))
    return pl.pallas_call(
        finish_kernel,
        grid=(blocks,),
        in_specs=[tile, tile, block, block],
        out_specs=[tile, tile, wide, wide, wide, pl.BlockSpec((hidden, width), lambda j: (0, j))],
        out_shape=[jax.ShapeDtypeStruct((tokens, d_model), BF16)] * 2 + [jax.ShapeDtypeStruct((d_model, hidden), F32)] * 3 + [jax.ShapeDtypeStruct((hidden, d_model), F32)],
        compiler_params=pltpu.CompilerParams(dimension_semantics=("arbitrary",), vmem_limit_bytes=48 << 20),
        cost_estimate=pl.CostEstimate(flops=8 * d_model * hidden, bytes_accessed=8 * tokens * d_model + 32 * d_model * hidden, transcendentals=0),
        name="finish",
    )(y, gx, ga, gb)


def solution(mesh):
    cp_size = mesh.shape["cp"]
    tp_size = mesh.shape["tp"]

    def device_step(x_in, segment_ids, positions, w_query, w_key, w_value, w_out, norm_gain, grad_out):
        batch, seq, d_model = x_in.shape
        tokens = batch * seq
        x = x_in.reshape(tokens, d_model)
        dy = grad_out.reshape(tokens, d_model)

        gain = norm_gain.reshape(1, d_model)
        normed, o_all, dq, dkv, w_all = front(x, dy, w_query, w_key, w_value, w_out, positions.reshape(batch, 1, seq), jnp.asarray(angle_table(), BF16), gain, seq, tp_size, cp_size)
        grad_x, y_out, sum_a, sum_b, grad_gain = backward_norm(dq, dkv, x, dy, o_all, normed, w_query, w_key, w_value, w_all, gain, ROWS, tp_size, cp_size)
        grad_gain = grad_gain.reshape(d_model)
        y_out, grad_x, grad_wq, grad_wk, grad_wv, grad_wo = finish(y_out, grad_x, sum_a, sum_b)
        return y_out.reshape(x_in.shape), grad_x.reshape(x_in.shape), grad_gain, grad_wq, grad_wk, grad_wv, grad_wo

    in_specs = (P("dp", "cp", None), P("dp", "cp"), P("dp", "cp"), P(None, "tp"), P(None, "tp"), P(None, "tp"), P("tp", None), P(None), P("dp", "cp", None))
    out_specs = (P("dp", "cp", None), P("dp", "cp", None), P("dp"), P("dp", "tp"), P("dp", "tp"), P("dp", "tp"), P(("dp", "tp"), None))
    return jax.shard_map(device_step, mesh=mesh, in_specs=in_specs, out_specs=out_specs, check_vma=False)
```

```python
import functools
import math

import jax
import jax.numpy as jnp
import numpy as np
from jax import lax
from jax.experimental import pallas as pl
from jax.experimental.pallas import tpu as pltpu
from jax.sharding import PartitionSpec as P

HEAD_DIM = 128
ROPE_THETA = 8000000.0
LN_EPS = 1e-5
NEG_BIG = -1e30
SCALE = HEAD_DIM ** -0.5
EXP2_SCALE = SCALE * math.log2(math.e)
F32 = jnp.float32
BF16 = jnp.bfloat16
NT = (((1,), (1,)), ((), ()))


def dot_nn(a, b):
    return jnp.dot(a, b, preferred_element_type=F32)


def dot_nt(a, b):
    return lax.dot_general(a, b, NT, preferred_element_type=F32)


def dot_tn(a, b):
    return lax.dot_general(a, b, (((0,), (0,)), ((), ())), preferred_element_type=F32)


def swap_pairs(t, sign):
    lane = lax.broadcasted_iota(jnp.int32, t.shape, 1)
    even = (lane % 2) == 0
    up = pltpu.roll(t, HEAD_DIM - 1, 1)
    down = pltpu.roll(t, 1, 1)
    return jnp.where(even, -up, down) if sign > 0 else jnp.where(even, up, -down)


def rope(t, cos_t, sin_t, sign):
    return t * cos_t + swap_pairs(t, sign) * sin_t


def angle_table():
    inv_freq = ROPE_THETA ** (-np.arange(0, HEAD_DIM, 2, dtype=np.float32) / np.float32(HEAD_DIM))
    freq = np.repeat(inv_freq.astype(np.float64), 2)[None, :]
    low = np.arange(POS_LOW)[:, None] * freq
    high = POS_LOW * np.arange(HEAD_DIM - POS_LOW)[:, None] * freq
    table = np.zeros((HEAD_DIM, 12 * HEAD_DIM), np.float32)
    for k, (first, value) in enumerate(((0, np.cos(low)), (0, np.sin(low)), (POS_LOW, np.cos(high)), (POS_LOW, np.sin(high)))):
        rest = value.astype(np.float32)
        for p in range(3):
            piece = rest.astype(BF16).astype(np.float32)
            at = (3 * k + p) * HEAD_DIM
            table[first:first + value.shape[0], at:at + HEAD_DIM] = piece
            rest = rest - piece
    return table


def put_rope(dst, raw, cos_t, sin_t):
    for h in range(raw.shape[1] // HEAD_DIM):
        cols = slice(h * HEAD_DIM, (h + 1) * HEAD_DIM)
        dst[:, cols] = rope(raw[:, cols], cos_t, sin_t, 1.0).astype(BF16)


MESH = pl.DeviceIdType.MESH
SUB = 128
ROWS = 32
WIDTH = 256
HALVES = 2
RELAY_LAG = 2
SUM_LAG = 4
CHIP_BUFS = 4
OWN_RING = 6
Q_RING = 3
AHEAD = 2
POS_LOW = 64
W_TWIN = 3
W_PARTNER = 6


def front_kernel(batch, seq, tp, cp, x_hbm, dy_hbm, wq_hbm, wk_hbm, wv_hbm, wo_hbm, pos_ref, table_ref, gain_ref,
                 n_hbm, o_all, dq_hbm, dkv_hbm, w_all,
                 big, wo_ref, cos_ref, sin_ref, q_ring, do_ring, x_in, dy_in, n_buf, kv_own, kvr, s_scr, dp_scr, m_scr, l_scr, d_scr, ot_scr, dqt_scr,
                 o_buf, dq_buf, g_own, g_part, g_chip, g_far, xin, part_in,
                 w_sem, wl_sem, wz_send, wz_recv, wx_send, wx_recv,
                 x_sem, dy_sem, n_sem, kvs_part, kvs_chip, kvs_far, kv_recv, o_local, o_send, o_recv, relay_send, dq_sem,
                 far_send, part_send, chip_send, x_recv, part_recv, dkv_sem):
    z = lax.axis_index("tp")
    r = lax.axis_index("cp")
    dp = lax.axis_index("dp")
    core = lax.rem(r, 2)
    chip = lax.div(r, 2)
    d_model = x_hbm.shape[1]
    hidden = wq_hbm.shape[1]
    heads = hidden // HEAD_DIM
    first_chip, second_chip = chip == 0, chip == 1
    first_core, second_core = core == 0, core == 1
    partner = {"cp": r + 1 - 2 * core}
    peer = {"cp": r + 2 - 4 * chip}
    twin = {"dp": 1 - dp}

    tile = x_in.shape[1]
    per_row = seq // tile

    def row(b):
        return pl.ds(pl.multiple_of(b * seq, seq), seq)

    def tile_rows(b, k):
        return pl.ds(pl.multiple_of(b * seq + k * tile, tile), tile)

    def x_load(b, k):
        return pltpu.make_async_copy(x_hbm.at[tile_rows(b, k), :], x_in.at[k], x_sem.at[k])

    def dy_load(b, k):
        return pltpu.make_async_copy(dy_hbm.at[tile_rows(b, k), :], dy_in.at[k], dy_sem.at[k])

    def n_store(b, k):
        return pltpu.make_async_copy(n_buf.at[k], n_hbm.at[tile_rows(b, k), :], n_sem.at[k])

    weight_loads = [pltpu.make_async_copy(src, dst, w_sem.at[k]) for k, (src, dst) in enumerate(((wk_hbm, big.at[0]), (wv_hbm, big.at[1]), (wq_hbm, big.at[2]), (wo_hbm, wo_ref)))]
    x_load(0, 0).start()
    for copy in weight_loads[:2]:
        copy.start()
    for k in range(1, per_row):
        x_load(0, k).start()
    for copy in weight_loads[2:]:
        copy.start()
    for k in range(per_row):
        dy_load(0, k).start()

    units = batch * HALVES
    half = hidden // HALVES

    def where(u):
        return lax.div(u, HALVES), lax.rem(u, HALVES)

    def half_cols(g):
        return pl.ds(pl.multiple_of(g * half, half), half)

    barrier = pltpu.get_barrier_semaphore()
    for dev in [partner, peer, twin] + [{"tp": lax.rem(z + dt, tp)} for dt in range(1, tp)]:
        pl.semaphore_signal(barrier, inc=1, device_id=dev, device_id_type=MESH)
    pl.semaphore_wait(barrier, tp + 2)

    def remote(src, dst, ssem, rsem, dev):
        return pltpu.make_async_remote_copy(src_ref=src, dst_ref=dst, send_sem=ssem, recv_sem=rsem, device_id=dev, device_id_type=MESH)

    share = hidden // 8

    def share_rows(y, c, g):
        return pl.ds(pl.multiple_of((4 * y + 2 * c + g) * share, share), share)

    mine, twins = share_rows(chip, core, dp), share_rows(chip, core, 1 - dp)
    peers, peer_twins = share_rows(1 - chip, core, dp), share_rows(1 - chip, core, 1 - dp)

    def wz_copy(d):
        return remote(wo_hbm.at[mine, :], w_all.at[z, mine, :], wz_send.at[d], wz_recv.at[z], {"tp": lax.rem(z + d, tp)})

    def wz_wait(d):
        src = lax.rem(z + d, tp)
        remote(wo_hbm.at[mine, :], w_all.at[src, mine, :], wz_send.at[d], wz_recv.at[src], partner).wait_recv()

    def w_copy(k, d, rows, dev):
        place = w_all.at[lax.rem(z + d, tp), rows, :]
        return remote(place, place, wx_send.at[k, d], wx_recv.at[k, d], dev)

    def w_move(k, d):
        rows, dev = ((mine, twin), (mine, partner), (twins, partner), (mine, peer), (twins, peer), (peers, partner), (peer_twins, partner))[k]
        return w_copy(k, d, rows, dev)

    w_steps = range(1, tp)

    for d in range(1, tp):
        wz_copy(d).start()

    def kv_to_partner(u):
        return remote(kv_own.at[u], kvr.at[0, u], kvs_part.at[u], kv_recv.at[0, u], partner)

    def kv_to_chip(u):
        return remote(kv_own.at[u], kvr.at[1, u], kvs_chip.at[u], kv_recv.at[1, u], peer)

    def kv_forward(u):
        return remote(kvr.at[1, u], kvr.at[2, u], kvs_far.at[u], kv_recv.at[2, u], partner)

    w_local = pltpu.make_async_copy(wo_ref, w_all.at[z], wl_sem.at[0])
    for copy in weight_loads[:2]:
        copy.wait()

    def angles(b, k):
        rows = tile_rows(b, k)
        pos = jnp.broadcast_to(pos_ref[pl.ds(b, 1), k * tile:(k + 1) * tile], (HEAD_DIM, tile)).T
        lane = lax.broadcasted_iota(jnp.int32, (tile, HEAD_DIM), 1)
        low = lane < POS_LOW
        pick = jnp.where(low, lax.rem(pos, POS_LOW), POS_LOW + lax.div(pos, POS_LOW)) == lane
        found = dot_nn(jnp.where(pick, 1.0, 0.0).astype(BF16), table_ref[...])

        def part(k):
            at = 3 * k * HEAD_DIM
            return found[:, at:at + HEAD_DIM] + found[:, at + HEAD_DIM:at + 2 * HEAD_DIM] + found[:, at + 2 * HEAD_DIM:at + 3 * HEAD_DIM]

        cos_b, sin_b, cos_a, sin_a = part(0), part(1), part(2), part(3)
        cos_ref[rows, :] = cos_a * cos_b - sin_a * sin_b
        sin_ref[rows, :] = sin_a * cos_b + cos_a * sin_b

    def project_row(b):
        ring = lax.rem(b, Q_RING)
        for k in range(per_row):
            rows = tile_rows(b, k)
            inside = slice(k * tile, (k + 1) * tile)
            x_load(b, k).wait()

            @pl.when(b > 0)
            def _(k=k):
                n_store(b - 1, k).wait()

            angles(b, k)
            x = x_in[k].astype(F32)
            centred = x - jnp.mean(x, axis=-1, keepdims=True)
            inv_std = lax.rsqrt(jnp.mean(centred * centred, axis=-1, keepdims=True) + LN_EPS)
            n_buf[k] = ((centred * inv_std) * gain_ref[...]).astype(BF16)
            n_store(b, k).start()

            @pl.when(b + 1 < batch)
            def _(k=k):
                x_load(b + 1, k).start()

            for g in range(HALVES):
                u = b * HALVES + g
                cols = slice(g * half, (g + 1) * half)
                put_rope(kv_own.at[u, 0, inside, :], dot_nn(n_buf[k], big[0, :, cols]), cos_ref[rows, :], sin_ref[rows, :])
                kv_own[u, 1, inside, :] = dot_nn(n_buf[k], big[1, :, cols]).astype(BF16)

        for g in range(HALVES):
            u = b * HALVES + g

            @pl.when(first_chip)
            def _(u=u):
                kv_to_chip(u).start()

            @pl.when(first_core)
            def _(u=u):
                kv_to_partner(u).start()

        @pl.when(b == 0)
        def _():
            for copy in weight_loads[2:]:
                copy.wait()
            w_local.start()

        for k in range(per_row):
            rows = tile_rows(b, k)
            inside = slice(k * tile, (k + 1) * tile)
            dy_load(b, k).wait()
            put_rope(q_ring.at[ring, inside, :], dot_nn(n_buf[k], big[2]), cos_ref[rows, :], sin_ref[rows, :])
            do_ring[ring, inside, :] = dot_nt(dy_in[k], wo_ref[...]).astype(BF16)

            @pl.when(b + 1 < batch)
            def _(k=k):
                dy_load(b + 1, k).start()

    def o_place(src, u):
        b, g = where(u)
        return o_all.at[src, row(b), half_cols(g)]

    def o_local_copy(b):
        return pltpu.make_async_copy(o_buf.at[b], o_place(z, b), o_local.at[b])

    def o_copy(b, k, step):
        return remote(o_buf.at[b], o_place(z, b), o_send.at[k, b], o_recv.at[z, b], {"tp": jnp.clip(z + step, 0, tp - 1)})

    hops = [(k, step, jnp.logical_and(z + step >= 0, z + step < tp)) for k, step in enumerate((1, -1))]

    def o_start(b):
        o_local_copy(b).start()
        for k, step, ok in hops:
            @pl.when(ok)
            def _(k=k, step=step):
                o_copy(b, k, step).start()

    def o_arrived(src, b):
        remote(o_place(src, b), o_place(src, b), relay_send.at[0, 0, b], o_recv.at[src, b], partner).wait_recv()

    def relay_copy(b, age, step):
        src = jnp.clip(z - age * step, 0, tp - 1)
        return remote(o_place(src, b), o_place(src, b), relay_send.at[age - 1, (1 - step) // 2, b], o_recv.at[src, b], {"tp": jnp.clip(z + step, 0, tp - 1)})

    def relays(age, step):
        far = z if step > 0 else tp - 1 - z
        return jnp.logical_and(far >= age, far < tp - 1)

    def relay(b, age):
        for step in (1, -1):
            @pl.when(relays(age, step))
            def _(step=step):
                o_arrived(jnp.clip(z - age * step, 0, tp - 1), b)
                relay_copy(b, age, step).start()

    def far_copy(b, par):
        return remote(g_far.at[par], xin.at[b], far_send.at[par], x_recv.at[b], partner)

    def part_copy(b, par):
        return remote(g_part.at[par], part_in.at[b], part_send.at[par], part_recv.at[b], partner)

    def chip_copy(b):
        par = lax.rem(b, CHIP_BUFS)
        return remote(g_chip.at[par], xin.at[b], chip_send.at[par], x_recv.at[b], peer)

    def chip_sum(b):
        @pl.when(second_chip)
        def _():
            par = lax.rem(b, CHIP_BUFS)
            far_copy(b, 0).wait_recv()
            g_chip[par] = (g_chip[par].astype(F32) + xin[b].astype(F32)).astype(BF16)
            chip_copy(b).start()

    def dkv_store(u, which):
        b, g = where(u)
        return pltpu.make_async_copy(g_own.at[lax.rem(u, OWN_RING), which], dkv_hbm.at[which, row(b), half_cols(g)], dkv_sem.at[u, which])

    def key_grads(u):
        @pl.when(first_core)
        def _():
            part_copy(u, 0).wait_recv()

        @pl.when(first_chip)
        def _():
            chip_copy(u).wait_recv()

        b, g = where(u)
        rows = row(b)
        for which in range(2):
            for h in range(half // HEAD_DIM):
                cols = slice(h * HEAD_DIM, (h + 1) * HEAD_DIM)
                own = g_own.at[lax.rem(u, OWN_RING), which, :, cols]
                acc = own[...].astype(F32)
                acc = acc + jnp.where(first_core, part_in[u, which, :, cols].astype(F32), 0.0)
                acc = (acc + jnp.where(first_chip, xin[u, which, :, cols].astype(F32), 0.0)).astype(BF16)
                if which == 0:
                    acc = rope(acc.astype(F32), cos_ref[rows, :], sin_ref[rows, :], -1.0).astype(BF16)
                own[...] = acc
            dkv_store(u, which).start()

    def dq_store(b, par):
        return pltpu.make_async_copy(dq_buf.at[par], dq_hbm.at[row(where(b)[0]), half_cols(where(b)[1])], dq_sem.at[par])

    subs = range(0, seq, SUB)

    def attend_unit(i, par):
        b, g = where(i)
        rows = row(b)
        ring = lax.rem(b, Q_RING)
        start = r * seq + lax.broadcasted_iota(jnp.int32, (1, seq), 1) - pos_ref[pl.ds(b, 1), :]
        chip_par = lax.rem(i, CHIP_BUFS)
        keys_of = [kv_own.at[i]] + [kvr.at[s, i] for s in range(3)]
        places = [g_part.at[par], g_chip.at[chip_par], g_far.at[par]]

        def grad(slot, which, cols):
            return places[slot - 1].at[which, :, cols] if slot else g_own.at[lax.rem(i, OWN_RING), which, :, cols]

        live = [None, second_core, second_chip, second_chip]
        piece = [r, r + 1 - 2 * core, r + 2 - 4 * chip, r + 3 - 2 * core - 4 * chip]

        def each(body):
            body(0)
            for slot in (1, 2, 3):
                pl.when(live[slot])(functools.partial(body, slot))

        def one_head(h, carry):
            cols = pl.ds(pl.multiple_of(h * HEAD_DIM, HEAD_DIM), HEAD_DIM)
            full = pl.ds(pl.multiple_of(g * half + h * HEAD_DIM, HEAD_DIM), HEAD_DIM)
            q = q_ring[ring, :, full]
            do = do_ring[ring, :, full]
            m_scr[...] = jnp.full(m_scr.shape, NEG_BIG, F32)
            l_scr[...] = jnp.zeros_like(l_scr)
            d_scr[...] = jnp.zeros_like(d_scr)
            ot_scr[...] = jnp.zeros_like(ot_scr)
            dqt_scr[...] = jnp.zeros_like(dqt_scr)

            def scores(slot):
                base = piece[slot] * seq
                for s in subs:
                    raw = dot_nt(keys_of[slot][0, s:s + SUB, cols], q)
                    local = lax.broadcasted_iota(jnp.int32, raw.shape, 0) + s
                    allowed = (local + base) >= start
                    if slot == 0:
                        allowed = jnp.logical_and(allowed, local <= lax.broadcasted_iota(jnp.int32, raw.shape, 1))
                    raw = jnp.where(allowed, raw, NEG_BIG)
                    s_scr[slot, s:s + SUB, :] = raw
                    m_scr[...] = jnp.maximum(m_scr[...], jnp.max(raw, axis=0, keepdims=True))

            def exps(slot):
                for s in subs:
                    e = jnp.exp2((s_scr[slot, s:s + SUB, :] - m_scr[...]) * EXP2_SCALE)
                    s_scr[slot, s:s + SUB, :] = e
                    l_scr[...] += jnp.sum(e, axis=0, keepdims=True)

            def values(slot):
                for s in subs:
                    v = keys_of[slot][1, s:s + SUB, cols]
                    prob = s_scr[slot, s:s + SUB, :] * l_scr[...]
                    low = prob.astype(BF16)
                    dp = dot_nt(v, do)
                    s_scr[slot, s:s + SUB, :] = prob
                    dp_scr[slot, s:s + SUB, :] = dp
                    d_scr[...] += jnp.sum(prob * dp, axis=0, keepdims=True)
                    grad(slot, 1, cols)[s:s + SUB, :] = dot_nn(low, do).astype(BF16)
                    ot_scr[...] += dot_nn(v.T, low)

            def keys(slot):
                for s in subs:
                    k = keys_of[slot][0, s:s + SUB, cols]
                    ds = (s_scr[slot, s:s + SUB, :] * (dp_scr[slot, s:s + SUB, :] - d_scr[...])).astype(BF16)
                    grad(slot, 0, cols)[s:s + SUB, :] = (dot_nn(ds, q) * SCALE).astype(BF16)
                    dqt_scr[...] += dot_nn(k.T, ds)

            each(scores)
            each(exps)
            l_scr[...] = 1.0 / l_scr[...]
            each(values)
            each(keys)
            o_buf[i, :, cols] = ot_scr[...].T.astype(BF16)
            dq_buf[par, :, cols] = rope(dqt_scr[...].T * SCALE, cos_ref[rows, :], sin_ref[rows, :], -1.0).astype(BF16)
            return carry

        lax.fori_loop(0, heads // HALVES, one_head, 0)

    def step(i, carry):
        par = lax.rem(i, 2)
        @pl.when(jnp.logical_and(lax.rem(i, HALVES) == 0, lax.div(i, HALVES) + AHEAD < batch))
        def _():
            project_row(lax.div(i, HALVES) + AHEAD)

        @pl.when(i >= OWN_RING)
        def _():
            for which in range(2):
                dkv_store(i - OWN_RING, which).wait()

        @pl.when(second_chip)
        def _():
            kv_to_chip(i).wait_recv()
            kv_forward(i).start()

        @pl.when(second_core)
        def _():
            kv_to_partner(i).wait_recv()

        @pl.when(second_chip)
        def _():
            kv_forward(i).wait_recv()

        @pl.when(i >= 2)
        def _():
            dq_store(i - 2, par).wait()

            @pl.when(second_core)
            def _():
                part_copy(i - 2, par).wait_send()

            @pl.when(second_chip)
            def _():
                far_copy(i - 2, par).wait_send()

        @pl.when(jnp.logical_and(second_chip, i >= CHIP_BUFS))
        def _():
            chip_copy(i - CHIP_BUFS).wait_send()

        attend_unit(i, par)
        o_start(i)
        dq_store(i, par).start()

        @pl.when(second_chip)
        def _():
            far_copy(i, par).start()

        @pl.when(second_core)
        def _():
            part_copy(i, par).start()

        @pl.when(i >= 1)
        def _():
            chip_sum(i - 1)

        for age in range(1, tp - 1):
            @pl.when(i >= age * RELAY_LAG)
            def _(age=age):
                relay(i - age * RELAY_LAG, age)

        @pl.when(i >= SUM_LAG)
        def _():
            key_grads(i - SUM_LAG)

        @pl.when(i == min(W_TWIN, units - 1))
        def _():
            for d in w_steps:
                wz_wait(d)
                w_move(0, d).start()
                w_move(1, d).start()

                @pl.when(second_chip)
                def _(d=d):
                    w_move(3, d).start()

        @pl.when(i == min(W_PARTNER, units - 1))
        def _():
            for d in w_steps:
                w_move(0, d).wait_recv()
                w_move(2, d).start()

                @pl.when(second_chip)
                def _(d=d):
                    w_move(4, d).start()

        return carry

    for b in range(min(AHEAD, batch)):
        project_row(b)
    lax.fori_loop(0, units, step, 0)
    chip_sum(units - 1)

    @pl.when(first_chip)
    def _():
        for u in range(units):
            kv_to_chip(u).wait_send()
        for k in (3, 4):
            for d in w_steps:
                w_move(k, d).start()

    for i in range(units, units + max(SUM_LAG, (tp - 2) * RELAY_LAG)):
        for age in range(1, tp - 1):
            if 0 <= i - age * RELAY_LAG < units:
                relay(i - age * RELAY_LAG, age)
        if 0 <= i - SUM_LAG < units:
            key_grads(i - SUM_LAG)
        if i == units + 1:
            for k in (3, 4):
                for d in w_steps:
                    w_move(k, d).wait_recv()
                    w_move(k + 2, d).start()

    w_local.wait()
    for d in w_steps:
        wz_copy(d).wait_send()
        for k in range(7):
            w_move(k, d).wait_send()
            if k in (1, 2, 5, 6):
                w_move(k, d).wait_recv()

    for k in range(per_row):
        n_store(batch - 1, k).wait()
    for u in range(max(0, units - OWN_RING), units):
        for which in range(2):
            dkv_store(u, which).wait()

    def drain(b, carry):
        @pl.when(first_core)
        def _():
            kv_to_partner(b).wait_send()

        @pl.when(second_chip)
        def _():
            kv_forward(b).wait_send()

        o_local_copy(b).wait()
        for k, step_, ok in hops:
            @pl.when(ok)
            def _(k=k, step_=step_):
                o_copy(b, k, step_).wait_send()

        for age in range(1, tp - 1):
            for step_ in (1, -1):
                @pl.when(relays(age, step_))
                def _(age=age, step_=step_):
                    relay_copy(b, age, step_).wait_send()

        for src in range(tp):
            way = jnp.where(z > src, 1, -1)
            gone = jnp.abs(z - src)
            far = jnp.where(way > 0, z, tp - 1 - z)
            taken = jnp.logical_and(gone <= tp - 2, far < tp - 1)

            @pl.when(jnp.logical_and(z != src, jnp.logical_not(taken)))
            def _(src=src):
                o_arrived(src, b)

        return carry

    lax.fori_loop(0, units, drain, 0)

    for b in range(max(0, units - 2), units):
        dq_store(b, b % 2).wait()

        @pl.when(second_core)
        def _(b=b):
            part_copy(b, b % 2).wait_send()

        @pl.when(second_chip)
        def _(b=b):
            far_copy(b, b % 2).wait_send()

    for b in range(max(0, units - CHIP_BUFS), units):
        @pl.when(second_chip)
        def _(b=b):
            chip_copy(b).wait_send()


def front(x, dy, wq, wk, wv, wo, pos, table, gain, seq, tp, cp):
    tokens, d_model = x.shape
    hidden = wq.shape[1]
    batch = tokens // seq
    units = batch * HALVES
    half = hidden // HALVES
    tile = seq // 2
    hbm = pl.BlockSpec(memory_space=pl.ANY)
    vmem = pl.BlockSpec(memory_space=pltpu.VMEM)
    dma = pltpu.SemaphoreType.DMA
    bf = lambda *shape: pltpu.VMEM(shape, BF16)
    f32 = lambda *shape: pltpu.VMEM(shape, F32)
    return pl.pallas_call(
        functools.partial(front_kernel, batch, seq, tp, cp),
        in_specs=[hbm] * 6 + [vmem] * 3,
        out_specs=[hbm] * 5,
        out_shape=[
            jax.ShapeDtypeStruct((tokens, d_model), BF16),
            jax.ShapeDtypeStruct((tp, tokens, hidden), BF16),
            jax.ShapeDtypeStruct((tokens, hidden), BF16),
            jax.ShapeDtypeStruct((2, tokens, hidden), BF16),
            jax.ShapeDtypeStruct((tp, hidden, d_model), BF16),
        ],
        scratch_shapes=[
            bf(3, d_model, hidden), bf(hidden, d_model), f32(tokens, HEAD_DIM), f32(tokens, HEAD_DIM),
            bf(Q_RING, seq, hidden), bf(Q_RING, seq, hidden), bf(2, tile, d_model), bf(2, tile, d_model), bf(2, tile, d_model),
            bf(units, 2, seq, half), bf(3, units, 2, seq, half),
            f32(4, seq, seq), f32(4, seq, seq), f32(1, seq), f32(1, seq), f32(1, seq), f32(HEAD_DIM, seq), f32(HEAD_DIM, seq),
            bf(units, seq, half), bf(2, seq, half),
            bf(OWN_RING, 2, seq, half), bf(2, 2, seq, half), bf(CHIP_BUFS, 2, seq, half), bf(2, 2, seq, half),
            bf(units, 2, seq, half), bf(units, 2, seq, half),
            dma((4,)), dma((1,)), dma((tp,)), dma((tp,)), dma((7, tp)), dma((7, tp)),
            dma((2,)), dma((2,)), dma((2,)), dma((units,)), dma((units,)), dma((units,)), dma((3, units)),
            dma((units,)), dma((2, units)), dma((tp, units)), dma((2, 2, units)), dma((2,)),
            dma((2,)), dma((2,)), dma((CHIP_BUFS,)), dma((units,)), dma((units,)), dma((units, 2)),
        ],
        compiler_params=pltpu.CompilerParams(collective_id=1, has_side_effects=True, vmem_limit_bytes=63 << 20),
        cost_estimate=pl.CostEstimate(flops=60 * tokens * seq * hidden, bytes_accessed=16 * tokens * d_model, transcendentals=4 * tokens * seq * (hidden // HEAD_DIM)),
        name="front",
    )(x, dy, wq, wk, wv, wo, pos, table, gain)


PART_RING = 4
RS_RING = 5
FORWARD_LAG = 11
JOB_LAG = 5
OUT_LAG = 4
EARLY = 4


def back_kernel(groups, rows, tp, cp, dq_hbm, dkv_hbm, x_hbm, dy_hbm, o_hbm, n_hbm, wq_hbm, wk_hbm, wv_hbm, wo_hbm, gain_ref,
                gx_hbm, y_hbm, ga_hbm, gb_hbm, gg_ref,
                wq_ref, wk_ref, wv_ref, wo_ref, dq_all, dkv_all, o_t, part, rs_r, rs_l, send_r, send_l, tot, gx_buf,
                o_in, x_in, xo_in, dyo_in, y_buf, n_in, dy_in, away, part_in, mine, gain_all,
                w_sem, in_sem, fin_sem, job_sem, y_sem, own_sem, rss_r, rss_l, rsr_r, rsr_l, ag0_r, ag0_l, agf_r, agf_l, agr_r, agr_l,
                away_send, away_recv, mine_own, mine_part, mine_chip, ga_recv, chip_recv, gb_send, gb_recv, gs_sem, gr_sem):
    z = lax.axis_index("tp")
    r = lax.axis_index("cp")
    core = lax.rem(r, 2)
    chip = lax.div(r, 2)
    last = tp - 1
    slots = tp - 1
    span = tp * rows
    tokens, d_model = x_hbm.shape
    hidden = dq_hbm.shape[1]
    chunk = min(512, d_model)
    blocks = ga_hbm.shape[0]
    width = ga_hbm.shape[1]
    pairs = blocks // 2
    partner = {"cp": r + 1 - 2 * core}
    peer = {"cp": r + 2 - 4 * chip}

    head = min(EARLY, groups) * span
    weight_loads = [pltpu.make_async_copy(src, dst, w_sem.at[k]) for k, (src, dst) in enumerate((
        (dq_hbm.at[:head, :], dq_all.at[:head, :]), (dkv_hbm.at[:, :head, :], dkv_all.at[:, :head, :]), (wq_hbm, wq_ref), (wk_hbm, wk_ref), (wv_hbm, wv_ref)))]
    rest_loads = [] if head == tokens else [
        pltpu.make_async_copy(dq_hbm.at[head:, :], dq_all.at[head:, :], w_sem.at[6]),
        pltpu.make_async_copy(dkv_hbm.at[:, head:, :], dkv_all.at[:, head:, :], w_sem.at[7]),
    ]
    out_loads = [pltpu.make_async_copy(wo_hbm, wo_ref, w_sem.at[5])]
    for copy in weight_loads:
        copy.start()

    barrier = pltpu.get_barrier_semaphore()
    peers = [(dt, dc) for dt in range(tp) for dc in range(cp) if dt or dc]
    for dt, dc in peers:
        pl.semaphore_signal(barrier, inc=1, device_id={"tp": lax.rem(z + dt, tp), "cp": lax.rem(r + dc, cp)}, device_id_type=MESH)
    pl.semaphore_wait(barrier, len(peers))

    def remote(src, dst, ssem, rsem, dev):
        return pltpu.make_async_remote_copy(src_ref=src, dst_ref=dst, send_sem=ssem, recv_sem=rsem, device_id=dev, device_id_type=MESH)

    right = {"tp": jnp.where(z < last, z + 1, z)}
    left = {"tp": jnp.where(z > 0, z - 1, z)}

    def group_rows(i):
        return pl.ds(pl.multiple_of(i * span, span), span)

    def tile_rows(i, owner):
        return pl.ds(pl.multiple_of(i * span + owner * rows, rows), rows)

    def inputs(i, slot):
        g = group_rows(i)
        return [
            pltpu.make_async_copy(o_hbm.at[:, g, :], o_in.at[slot], in_sem.at[slot, 0]),
            pltpu.make_async_copy(x_hbm.at[g, :], x_in.at[slot], in_sem.at[slot, 1]),
        ]

    def final_inputs(i, slot):
        g = tile_rows(i, z)
        return [
            pltpu.make_async_copy(x_hbm.at[g, :], xo_in.at[slot], fin_sem.at[slot, 0]),
            pltpu.make_async_copy(dy_hbm.at[g, :], dyo_in.at[slot], fin_sem.at[slot, 1]),
        ]

    def y_copy(i, slot):
        return pltpu.make_async_copy(y_buf.at[slot], y_hbm.at[group_rows(i), :], y_sem.at[slot])

    def rs_copy(i, s, to_right):
        ring = lax.rem(i, RS_RING)
        if to_right:
            return remote(send_r.at[s], rs_r.at[ring, s], rss_r.at[s], rsr_r.at[ring, s], right)
        return remote(send_l.at[s], rs_l.at[ring, s], rss_l.at[s], rsr_l.at[ring, s], left)

    def rs_send(i, s):
        for to_right in (True, False):
            far = z if to_right else last - z
            owner = (z + slots - s) if to_right else (z - slots + s)
            buf, held = (send_r, rs_r) if to_right else (send_l, rs_l)

            @pl.when(jnp.logical_and(jnp.logical_and(i >= 0, i < groups), jnp.logical_and(far <= s, far < last)))
            def _(to_right=to_right, far=far, owner=owner, buf=buf, held=held):
                @pl.when(i > 0)
                def _():
                    rs_copy(i - 1, s, to_right).wait_send()

                cur = lax.rem(i, PART_RING)
                own = pl.ds(pl.multiple_of(owner * rows, rows), rows)
                if s == 0:
                    buf[s] = part[cur, own, :].astype(BF16)
                else:
                    @pl.when(far == 0)
                    def _():
                        buf[s] = part[cur, own, :].astype(BF16)

                    @pl.when(far > 0)
                    def _():
                        rs_copy(i, s - 1, to_right).wait_recv()
                        buf[s] = (part[cur, own, :] + held[lax.rem(i, RS_RING), s - 1].astype(F32)).astype(BF16)

                rs_copy(i, s, to_right).start()

    def ag_own(i, slot, to_right):
        src = gx_buf.at[slot]
        dst = gx_hbm.at[tile_rows(i, z), :]
        if to_right:
            return remote(src, dst, ag0_r.at[slot], agr_r.at[i, 0], right)
        return remote(src, dst, ag0_l.at[slot], agr_l.at[i, 0], left)

    def own_copy(i, slot):
        return pltpu.make_async_copy(gx_buf.at[slot], gx_hbm.at[tile_rows(i, z), :], own_sem.at[slot])

    def ag_forward(i, a, to_right):
        owner = z - a if to_right else z + a
        tile = gx_hbm.at[tile_rows(i, owner), :]
        if to_right:
            return remote(tile, tile, agf_r.at[a], agr_r.at[i, a], right)
        return remote(tile, tile, agf_l.at[a], agr_l.at[i, a], left)

    def ag_wait(i, a, to_right):
        tile = gx_hbm.at[tile_rows(i, 0), :]
        sem = agr_r.at[i, a] if to_right else agr_l.at[i, a]
        remote(tile, tile, agf_r.at[a], sem, right).wait_recv()

    def ag_step(i, a):
        for to_right in (True, False):
            far = z if to_right else last - z

            @pl.when(jnp.logical_and(jnp.logical_and(i >= 0, i < groups), far >= a))
            def _(to_right=to_right, far=far):
                ag_wait(i, a - 1, to_right)
                if a < slots:
                    @pl.when(far < last)
                    def _():
                        @pl.when(i > 0)
                        def _():
                            ag_forward(i - 1, a, to_right).wait_send()

                        ag_forward(i, a, to_right).start()

    def ag_first(i, slot):
        own_copy(i, slot).start()
        for to_right in (True, False):
            far = z if to_right else last - z

            @pl.when(far < last)
            def _(to_right=to_right):
                ag_own(i, slot, to_right).start()

    def ag_first_done(i, slot):
        own_copy(i, slot).wait()
        for to_right in (True, False):
            far = z if to_right else last - z

            @pl.when(far < last)
            def _(to_right=to_right):
                ag_own(i, slot, to_right).wait_send()

    def partial_norm(i):
        cur = lax.rem(i, PART_RING)
        g = group_rows(i)
        for c in range(0, d_model, chunk):
            cols = slice(c, c + chunk)
            part[cur, :, cols] = (
                dot_nt(dq_all[g, :], wq_ref[cols, :]) + dot_nt(dkv_all[0, g, :], wk_ref[cols, :]) + dot_nt(dkv_all[1, g, :], wv_ref[cols, :])
            )

    def project_out(cur):
        for c in range(0, d_model, chunk):
            cols = slice(c, c + chunk)
            acc = x_in[cur, :, cols].astype(F32)
            for t in range(tp):
                acc += dot_nn(o_in[cur, t], wo_ref[t, :, cols])
            y_buf[cur, :, cols] = acc.astype(BF16)

    def finalize(i):
        slot = lax.rem(i, 2)
        own = pl.ds(pl.multiple_of(z * rows, rows), rows)
        tot[...] = part[lax.rem(i, PART_RING), own, :]

        @pl.when(z > 0)
        def _():
            rs_copy(i, slots - 1, True).wait_recv()
            tot[...] += rs_r[lax.rem(i, RS_RING), slots - 1].astype(F32)

        @pl.when(z < last)
        def _():
            rs_copy(i, slots - 1, False).wait_recv()
            tot[...] += rs_l[lax.rem(i, RS_RING), slots - 1].astype(F32)

        @pl.when(i > 1)
        def _():
            ag_first_done(i - 2, slot)

        for copy in final_inputs(i, slot):
            copy.wait()
        x = xo_in[slot].astype(F32)
        centred = x - jnp.mean(x, axis=-1, keepdims=True)
        inv_std = lax.rsqrt(jnp.mean(centred * centred, axis=-1, keepdims=True) + LN_EPS)
        x_hat = centred * inv_std
        dn = tot[...]
        gg_ref[...] += jnp.sum(dn * x_hat, axis=0, keepdims=True)
        d_hat = dn * gain_ref[...]
        dx = inv_std * (d_hat - jnp.mean(d_hat, axis=-1, keepdims=True) - x_hat * jnp.mean(d_hat * x_hat, axis=-1, keepdims=True))
        gx_buf[slot] = (dyo_in[slot].astype(F32) + dx).astype(BF16)
        ag_first(i, slot)

    def block_of(t):
        return 2 * lax.div(t, 2) + jnp.where(lax.rem(t, 2) == 0, 1 - core, core)

    def job_loads(t, slot):
        cols = pl.ds(pl.multiple_of(block_of(t) * width, width), width)
        return [
            pltpu.make_async_copy(n_hbm.at[:, cols], n_in.at[slot], job_sem.at[slot, 0]),
            pltpu.make_async_copy(dy_hbm.at[:, cols], dy_in.at[slot], job_sem.at[slot, 1]),
        ]

    def away_copy(p):
        ring = lax.rem(p, 2)
        return remote(away, part_in.at[ring], away_send.at[0], away_recv.at[ring], partner)

    def job_block(t, put):
        slot = lax.rem(t, 2)
        n_t = n_in[slot].T
        put(0, hidden, dot_nn(n_t, dq_all[...]))
        put(hidden, hidden, dot_nn(n_t, dkv_all[0]))
        put(2 * hidden, hidden, dot_nn(n_t, dkv_all[1]))
        for k in range(hidden // width):
            put(3 * hidden + k * width, width, dot_nn(o_t[k * width:(k + 1) * width, :], dy_in[slot]))

    def mine_to_own(p, slot):
        return pltpu.make_async_copy(mine.at[slot], ga_hbm.at[2 * p + core], mine_own.at[slot])

    def mine_to_part(p, slot):
        return remote(mine.at[slot], ga_hbm.at[2 * p + core], mine_part.at[slot], ga_recv.at[p], partner)

    def mine_to_chip(p, slot):
        return remote(mine.at[slot], gb_hbm.at[2 * p + core], mine_chip.at[slot], chip_recv.at[p], peer)

    def mine_done(p, slot):
        mine_to_own(p, slot).wait()
        mine_to_part(p, slot).wait_send()
        mine_to_chip(p, slot).wait_send()

    def chip_forward(p):
        b = 2 * p + core
        return remote(gb_hbm.at[b], gb_hbm.at[b], gb_send.at[p], gb_recv.at[p], partner)

    def job(t):
        p = lax.div(t, 2)
        for copy in job_loads(t, lax.rem(t, 2)):
            copy.wait()

        @pl.when(t + 1 < blocks)
        def _():
            for copy in job_loads(t + 1, 1 - lax.rem(t, 2)):
                copy.start()

        @pl.when(lax.rem(t, 2) == 0)
        def _():
            @pl.when(p > 0)
            def _():
                away_copy(p - 1).wait_send()

            def put(at, size, value):
                away[:, at:at + size] = value

            job_block(t, put)
            away_copy(p).start()

        @pl.when(lax.rem(t, 2) == 1)
        def _():
            slot = lax.rem(p, 2)
            away_copy(p).wait_recv()

            @pl.when(p > 1)
            def _():
                mine_done(p - 2, slot)

            def put(at, size, value):
                mine[slot, :, at:at + size] = (value + part_in[slot, :, at:at + size]).astype(BF16)

            job_block(t, put)
            mine_to_chip(p, slot).start()
            mine_to_part(p, slot).start()
            mine_to_own(p, slot).start()

    gg_ref[...] = jnp.zeros_like(gg_ref)
    o_loads = [pltpu.make_async_copy(o_hbm.at[z, :, k * width:(k + 1) * width], n_in.at[k], job_sem.at[k, 0]) for k in range(hidden // width)]
    for copy in o_loads:
        copy.start()
    for copy in inputs(0, 0):
        copy.start()
    for copy in rest_loads + out_loads:
        copy.start()
    me = z * cp + r

    def gain_copy(dt, dc):
        to = {"tp": lax.rem(z + dt, tp), "cp": lax.rem(r + dc, cp)}
        return remote(gain_all.at[me], gain_all.at[me], gs_sem.at[dt * cp + dc], gr_sem.at[me], to)

    def gain_wait(dt, dc):
        sender = lax.rem(z + dt, tp) * cp + lax.rem(r + dc, cp)
        remote(gain_all.at[sender], gain_all.at[sender], gs_sem.at[0], gr_sem.at[sender], right).wait_recv()

    for copy in weight_loads:
        copy.wait()

    def step(i, carry):
        for k in reversed(range(1, slots)):
            rs_send(i - k, k)

        @pl.when(i == EARLY)
        def _():
            for copy in rest_loads:
                copy.wait()

        @pl.when(i < groups)
        def _():
            partial_norm(i)

        rs_send(i, 0)

        @pl.when(jnp.logical_and(i >= slots, i < groups + slots))
        def _():
            finalize(i - slots)

        for a in range(1, slots + 1):
            ag_step(i - slots - a, a)

        @pl.when(i == groups + slots - 1)
        def _():
            gain_all[me] = gg_ref[...]
            for dt, dc in peers:
                gain_copy(dt, dc).start()

        @pl.when(jnp.logical_and(i >= slots - 1, i < groups + slots - 1))
        def _():
            for copy in final_inputs(i - slots + 1, lax.rem(i - slots + 1, 2)):
                copy.start()

        @pl.when(i == JOB_LAG - 1)
        def _():
            for k, copy in enumerate(o_loads):
                copy.wait()
                o_t[k * width:(k + 1) * width, :] = n_in[k].T
            for copy in job_loads(0, 0):
                copy.start()

        @pl.when(i == OUT_LAG)
        def _():
            for copy in out_loads:
                copy.wait()

        @pl.when(jnp.logical_and(i >= OUT_LAG, i < groups + OUT_LAG))
        def _():
            j = i - OUT_LAG
            at = lax.rem(j, 2)
            for copy in inputs(j, at):
                copy.wait()

            @pl.when(j + 1 < groups)
            def _():
                for copy in inputs(j + 1, 1 - at):
                    copy.start()

            @pl.when(j >= 2)
            def _():
                y_copy(j - 2, at).wait()

            project_out(at)
            y_copy(j, at).start()

        @pl.when(jnp.logical_and(i >= JOB_LAG, i < JOB_LAG + blocks))
        def _():
            job(i - JOB_LAG)

        @pl.when(jnp.logical_and(lax.rem(i, 2) == 1, jnp.logical_and(i >= FORWARD_LAG, i < FORWARD_LAG + 2 * pairs)))
        def _():
            p = lax.div(i - FORWARD_LAG, 2)
            mine_to_chip(p, 0).wait_recv()
            chip_forward(p).start()

        return carry

    lax.fori_loop(0, max(groups + 2 * slots, groups + OUT_LAG, blocks + JOB_LAG, 2 * pairs + FORWARD_LAG - 1), step, 0)

    for i in (groups - 2, groups - 1):
        y_copy(i, i % 2).wait()
        ag_first_done(i, i % 2)
    for to_right in (True, False):
        far = z if to_right else last - z
        for s in range(slots):
            @pl.when(jnp.logical_and(far <= s, far < last))
            def _(s=s, to_right=to_right):
                rs_copy(groups - 1, s, to_right).wait_send()
        for a in range(1, slots):
            @pl.when(jnp.logical_and(far >= a, far < last))
            def _(a=a, to_right=to_right):
                ag_forward(groups - 1, a, to_right).wait_send()
    away_copy(pairs - 1).wait_send()
    for p in range(max(0, pairs - 2), pairs):
        mine_done(p, p % 2)
    for p in range(pairs):
        chip_forward(p).wait_send()
        chip_forward(p).wait_recv()
        mine_to_part(p, 0).wait_recv()
    for dt, dc in peers:
        gain_wait(dt, dc)
        gain_copy(dt, dc).wait_send()
    total = gain_all[0]
    for j in range(1, tp * cp):
        total += gain_all[j]
    gg_ref[...] = total


def backward_norm(dq, dkv, x, dy, o_all, normed, wq, wk, wv, wo_all, gain, rows, tp, cp):
    tokens, hidden = dq.shape
    d_model = x.shape[1]
    span = tp * rows
    groups = tokens // span
    slots = tp - 1
    width = WIDTH
    blocks = d_model // width
    pairs = blocks // 2
    hbm = pl.BlockSpec(memory_space=pl.ANY)
    vmem = pl.BlockSpec(memory_space=pltpu.VMEM)
    dma = pltpu.SemaphoreType.DMA
    bf = lambda *shape: pltpu.VMEM(shape, BF16)
    f32 = lambda *shape: pltpu.VMEM(shape, F32)
    return pl.pallas_call(
        functools.partial(back_kernel, groups, rows, tp, cp),
        in_specs=[hbm] * 10 + [vmem],
        out_specs=[hbm, hbm, hbm, hbm, vmem],
        out_shape=[
            jax.ShapeDtypeStruct((tokens, d_model), BF16),
            jax.ShapeDtypeStruct((tokens, d_model), BF16),
            jax.ShapeDtypeStruct((blocks, width, 4 * hidden), BF16),
            jax.ShapeDtypeStruct((blocks, width, 4 * hidden), BF16),
            jax.ShapeDtypeStruct((1, d_model), F32),
        ],
        scratch_shapes=[
            bf(d_model, hidden), bf(d_model, hidden), bf(d_model, hidden), bf(tp, hidden, d_model),
            bf(tokens, hidden), bf(2, tokens, hidden), bf(hidden, tokens),
            f32(PART_RING, span, d_model), bf(RS_RING, slots, rows, d_model), bf(RS_RING, slots, rows, d_model),
            bf(slots, rows, d_model), bf(slots, rows, d_model), f32(rows, d_model), bf(2, rows, d_model),
            bf(2, tp, span, hidden), bf(2, span, d_model), bf(2, rows, d_model), bf(2, rows, d_model), bf(2, span, d_model),
            bf(2, tokens, width), bf(2, tokens, width),
            f32(width, 4 * hidden), f32(2, width, 4 * hidden), bf(2, width, 4 * hidden), f32(tp * cp, 1, d_model),
            dma((8,)), dma((2, 2)), dma((2, 2)), dma((2, 2)), dma((2,)), dma((2,)),
            dma((slots,)), dma((slots,)), dma((RS_RING, slots)), dma((RS_RING, slots)),
            dma((2,)), dma((2,)), dma((slots,)), dma((slots,)), dma((groups, slots)), dma((groups, slots)),
            dma((1,)), dma((2,)), dma((2,)), dma((2,)), dma((2,)), dma((pairs,)), dma((pairs,)), dma((pairs,)), dma((pairs,)),
            dma((tp * cp,)), dma((tp * cp,)),
        ],
        compiler_params=pltpu.CompilerParams(collective_id=0, has_side_effects=True, vmem_limit_bytes=63 << 20),
        cost_estimate=pl.CostEstimate(flops=22 * tokens * hidden * d_model, bytes_accessed=16 * tokens * d_model, transcendentals=0),
        name="backward_norm",
    )(dq, dkv, x, dy, o_all, normed, wq, wk, wv, wo_all, gain)


def finish_kernel(y_ref, gx_ref, ga_ref, gb_ref, yo_ref, gxo_ref, wq_ref, wk_ref, wv_ref, wo_ref):
    yo_ref[...] = y_ref[...]
    gxo_ref[...] = gx_ref[...]
    width = ga_ref.shape[1]
    hidden = wq_ref.shape[1]
    for k, ref in enumerate((wq_ref, wk_ref, wv_ref)):
        cols = slice(k * hidden, (k + 1) * hidden)
        ref[...] = ga_ref[0, :, cols].astype(F32) + gb_ref[0, :, cols].astype(F32)
    for k in range(hidden // width):
        cols = slice(3 * hidden + k * width, 3 * hidden + (k + 1) * width)
        wo_ref[k * width:(k + 1) * width, :] = ga_ref[0, :, cols].astype(F32) + gb_ref[0, :, cols].astype(F32)


def finish(y, gx, ga, gb):
    tokens, d_model = y.shape
    blocks, width, packed = ga.shape
    hidden = packed // 4
    rows = tokens // blocks
    tile = pl.BlockSpec((rows, d_model), lambda j: (j, 0))
    block = pl.BlockSpec((1, width, packed), lambda j: (j, 0, 0))
    wide = pl.BlockSpec((width, hidden), lambda j: (j, 0))
    return pl.pallas_call(
        finish_kernel,
        grid=(blocks,),
        in_specs=[tile, tile, block, block],
        out_specs=[tile, tile, wide, wide, wide, pl.BlockSpec((hidden, width), lambda j: (0, j))],
        out_shape=[jax.ShapeDtypeStruct((tokens, d_model), BF16)] * 2 + [jax.ShapeDtypeStruct((d_model, hidden), F32)] * 3 + [jax.ShapeDtypeStruct((hidden, d_model), F32)],
        compiler_params=pltpu.CompilerParams(dimension_semantics=("arbitrary",), vmem_limit_bytes=48 << 20),
        cost_estimate=pl.CostEstimate(flops=8 * d_model * hidden, bytes_accessed=8 * tokens * d_model + 32 * d_model * hidden, transcendentals=0),
        name="finish",
    )(y, gx, ga, gb)


def solution(mesh):
    cp_size = mesh.shape["cp"]
    tp_size = mesh.shape["tp"]

    def device_step(x_in, segment_ids, positions, w_query, w_key, w_value, w_out, norm_gain, grad_out):
        batch, seq, d_model = x_in.shape
        tokens = batch * seq
        x = x_in.reshape(tokens, d_model)
        dy = grad_out.reshape(tokens, d_model)

        gain = norm_gain.reshape(1, d_model)
        normed, o_all, dq, dkv, w_all = front(x, dy, w_query, w_key, w_value, w_out, positions, jnp.asarray(angle_table(), BF16), gain, seq, tp_size, cp_size)
        grad_x, y_out, sum_a, sum_b, grad_gain = backward_norm(dq, dkv, x, dy, o_all, normed, w_query, w_key, w_value, w_all, gain, ROWS, tp_size, cp_size)
        grad_gain = grad_gain.reshape(d_model)
        y_out, grad_x, grad_wq, grad_wk, grad_wv, grad_wo = finish(y_out, grad_x, sum_a, sum_b)
        return y_out.reshape(x_in.shape), grad_x.reshape(x_in.shape), grad_gain, grad_wq, grad_wk, grad_wv, grad_wo

    in_specs = (P("dp", "cp", None), P("dp", "cp"), P("dp", "cp"), P(None, "tp"), P(None, "tp"), P(None, "tp"), P("tp", None), P(None), P("dp", "cp", None))
    out_specs = (P("dp", "cp", None), P("dp", "cp", None), P("dp"), P("dp", "tp"), P("dp", "tp"), P("dp", "tp"), P(("dp", "tp"), None))
    return jax.shard_map(device_step, mesh=mesh, in_specs=in_specs, out_specs=out_specs, check_vma=False)
```

```python
import functools
import math

import jax
import jax.numpy as jnp
import numpy as np
from jax import lax
from jax.experimental import pallas as pl
from jax.experimental.pallas import tpu as pltpu
from jax.sharding import PartitionSpec as P

HEAD_DIM = 128
ROPE_THETA = 8000000.0
LN_EPS = 1e-5
NEG_BIG = -1e30
SCALE = HEAD_DIM ** -0.5
EXP2_SCALE = SCALE * math.log2(math.e)
F32 = jnp.float32
BF16 = jnp.bfloat16
NT = (((1,), (1,)), ((), ()))


def dot_nn(a, b):
    return jnp.dot(a, b, preferred_element_type=F32)


def dot_nt(a, b):
    return lax.dot_general(a, b, NT, preferred_element_type=F32)


def dot_tn(a, b):
    return lax.dot_general(a, b, (((0,), (0,)), ((), ())), preferred_element_type=F32)


def swap_pairs(t, sign):
    lane = lax.broadcasted_iota(jnp.int32, t.shape, 1)
    even = (lane % 2) == 0
    up = pltpu.roll(t, HEAD_DIM - 1, 1)
    down = pltpu.roll(t, 1, 1)
    return jnp.where(even, -up, down) if sign > 0 else jnp.where(even, up, -down)


def rope(t, cos_t, sin_t, sign):
    return t * cos_t + swap_pairs(t, sign) * sin_t


def angle_table():
    inv_freq = ROPE_THETA ** (-np.arange(0, HEAD_DIM, 2, dtype=np.float32) / np.float32(HEAD_DIM))
    freq = np.repeat(inv_freq.astype(np.float64), 2)[None, :]
    low = np.arange(POS_LOW)[:, None] * freq
    high = POS_LOW * np.arange(HEAD_DIM - POS_LOW)[:, None] * freq
    table = np.zeros((HEAD_DIM, 12 * HEAD_DIM), np.float32)
    for k, (first, value) in enumerate(((0, np.cos(low)), (0, np.sin(low)), (POS_LOW, np.cos(high)), (POS_LOW, np.sin(high)))):
        rest = value.astype(np.float32)
        for p in range(3):
            piece = rest.astype(BF16).astype(np.float32)
            at = (3 * k + p) * HEAD_DIM
            table[first:first + value.shape[0], at:at + HEAD_DIM] = piece
            rest = rest - piece
    return table


def put_rope(dst, raw, cos_t, sin_t):
    for h in range(raw.shape[1] // HEAD_DIM):
        cols = slice(h * HEAD_DIM, (h + 1) * HEAD_DIM)
        dst[:, cols] = rope(raw[:, cols], cos_t, sin_t, 1.0).astype(BF16)


MESH = pl.DeviceIdType.MESH
SUB = 128
ROWS = 32
WIDTH = 256
HALVES = 2
RELAY_LAG = 2
SUM_LAG = 4
CHIP_BUFS = 4
OWN_RING = 6
Q_RING = 3
AHEAD = 2
POS_LOW = 64
W_TWIN = 0
W_PARTNER = 4
W_CHIP = 7


def front_kernel(batch, seq, tp, cp, x_hbm, dy_hbm, wq_hbm, wk_hbm, wv_hbm, wo_hbm, pos_ref, table_ref, gain_ref,
                 n_hbm, o_all, dq_hbm, dkv_hbm, w_all,
                 big, wo_ref, cos_ref, sin_ref, q_ring, do_ring, x_in, dy_in, n_buf, kv_own, kvr, s_scr, dp_scr, m_scr, l_scr, d_scr, ot_scr, dqt_scr,
                 o_buf, dq_buf, g_own, g_part, g_chip, g_far, xin, part_in,
                 w_sem, wl_sem, wz_send, wz_recv, wx_send, wx_recv,
                 x_sem, dy_sem, n_sem, kvs_part, kvs_chip, kvs_far, kv_recv, o_local, o_send, o_recv, relay_send, dq_sem,
                 far_send, part_send, chip_send, x_recv, part_recv, dkv_sem):
    z = lax.axis_index("tp")
    r = lax.axis_index("cp")
    dp = lax.axis_index("dp")
    core = lax.rem(r, 2)
    chip = lax.div(r, 2)
    d_model = x_hbm.shape[1]
    hidden = wq_hbm.shape[1]
    heads = hidden // HEAD_DIM
    first_chip, second_chip = chip == 0, chip == 1
    first_core, second_core = core == 0, core == 1
    partner = {"cp": r + 1 - 2 * core}
    peer = {"cp": r + 2 - 4 * chip}
    twin = {"dp": 1 - dp}

    tile = x_in.shape[1]
    per_row = seq // tile

    def row(b):
        return pl.ds(pl.multiple_of(b * seq, seq), seq)

    def tile_rows(b, k):
        return pl.ds(pl.multiple_of(b * seq + k * tile, tile), tile)

    def x_load(b, k):
        return pltpu.make_async_copy(x_hbm.at[tile_rows(b, k), :], x_in.at[k], x_sem.at[k])

    def dy_load(b, k):
        return pltpu.make_async_copy(dy_hbm.at[tile_rows(b, k), :], dy_in.at[k], dy_sem.at[k])

    def n_store(b, k):
        return pltpu.make_async_copy(n_buf.at[k], n_hbm.at[tile_rows(b, k), :], n_sem.at[k])

    weight_loads = [pltpu.make_async_copy(src, dst, w_sem.at[k]) for k, (src, dst) in enumerate(((wk_hbm, big.at[0]), (wv_hbm, big.at[1]), (wq_hbm, big.at[2]), (wo_hbm, wo_ref)))]
    x_load(0, 0).start()
    for copy in weight_loads[:2]:
        copy.start()
    for k in range(1, per_row):
        x_load(0, k).start()
    for copy in weight_loads[2:]:
        copy.start()
    for k in range(per_row):
        dy_load(0, k).start()

    units = batch * HALVES
    half = hidden // HALVES

    def where(u):
        return lax.div(u, HALVES), lax.rem(u, HALVES)

    def half_cols(g):
        return pl.ds(pl.multiple_of(g * half, half), half)

    barrier = pltpu.get_barrier_semaphore()
    for dev in [partner, peer, twin] + [{"tp": lax.rem(z + dt, tp)} for dt in range(1, tp)]:
        pl.semaphore_signal(barrier, inc=1, device_id=dev, device_id_type=MESH)
    pl.semaphore_wait(barrier, tp + 2)

    def remote(src, dst, ssem, rsem, dev):
        return pltpu.make_async_remote_copy(src_ref=src, dst_ref=dst, send_sem=ssem, recv_sem=rsem, device_id=dev, device_id_type=MESH)

    share = hidden // 8

    def share_rows(y, c, g):
        return pl.ds(pl.multiple_of((4 * y + 2 * c + g) * share, share), share)

    mine, twins = share_rows(chip, core, dp), share_rows(chip, core, 1 - dp)
    peers, peer_twins = share_rows(1 - chip, core, dp), share_rows(1 - chip, core, 1 - dp)

    def wz_copy(d):
        return remote(wo_hbm.at[mine, :], w_all.at[z, mine, :], wz_send.at[d], wz_recv.at[z], {"tp": lax.rem(z + d, tp)})

    def wz_wait(d):
        src = lax.rem(z + d, tp)
        remote(wo_hbm.at[mine, :], w_all.at[src, mine, :], wz_send.at[d], wz_recv.at[src], partner).wait_recv()

    def w_copy(k, d, rows, dev):
        place = w_all.at[lax.rem(z + d, tp), rows, :]
        return remote(place, place, wx_send.at[k, d], wx_recv.at[k, d], dev)

    def w_move(k, d):
        rows, dev = ((mine, twin), (mine, partner), (twins, partner), (mine, peer), (twins, peer), (peers, partner), (peer_twins, partner))[k]
        return w_copy(k, d, rows, dev)

    w_steps = range(1, tp)

    for d in range(1, tp):
        wz_copy(d).start()

    def kv_to_partner(u):
        return remote(kv_own.at[u], kvr.at[0, u], kvs_part.at[u], kv_recv.at[0, u], partner)

    def kv_to_chip(u):
        return remote(kv_own.at[u], kvr.at[1, u], kvs_chip.at[u], kv_recv.at[1, u], peer)

    def kv_forward(u):
        return remote(kvr.at[1, u], kvr.at[2, u], kvs_far.at[u], kv_recv.at[2, u], partner)

    w_local = pltpu.make_async_copy(wo_ref, w_all.at[z], wl_sem.at[0])
    for copy in weight_loads[:2]:
        copy.wait()

    def angles(b, k):
        rows = tile_rows(b, k)
        pos = jnp.broadcast_to(pos_ref[pl.ds(b, 1), k * tile:(k + 1) * tile], (HEAD_DIM, tile)).T
        lane = lax.broadcasted_iota(jnp.int32, (tile, HEAD_DIM), 1)
        low = lane < POS_LOW
        pick = jnp.where(low, lax.rem(pos, POS_LOW), POS_LOW + lax.div(pos, POS_LOW)) == lane
        found = dot_nn(jnp.where(pick, 1.0, 0.0).astype(BF16), table_ref[...])

        def part(k):
            at = 3 * k * HEAD_DIM
            return found[:, at:at + HEAD_DIM] + found[:, at + HEAD_DIM:at + 2 * HEAD_DIM] + found[:, at + 2 * HEAD_DIM:at + 3 * HEAD_DIM]

        cos_b, sin_b, cos_a, sin_a = part(0), part(1), part(2), part(3)
        cos_ref[rows, :] = cos_a * cos_b - sin_a * sin_b
        sin_ref[rows, :] = sin_a * cos_b + cos_a * sin_b

    def project_row(b):
        ring = lax.rem(b, Q_RING)
        for k in range(per_row):
            rows = tile_rows(b, k)
            inside = slice(k * tile, (k + 1) * tile)
            x_load(b, k).wait()

            @pl.when(b > 0)
            def _(k=k):
                n_store(b - 1, k).wait()

            angles(b, k)
            x = x_in[k].astype(F32)
            centred = x - jnp.mean(x, axis=-1, keepdims=True)
            inv_std = lax.rsqrt(jnp.mean(centred * centred, axis=-1, keepdims=True) + LN_EPS)
            n_buf[k] = ((centred * inv_std) * gain_ref[...]).astype(BF16)
            n_store(b, k).start()

            @pl.when(b + 1 < batch)
            def _(k=k):
                x_load(b + 1, k).start()

            for g in range(HALVES):
                u = b * HALVES + g
                cols = slice(g * half, (g + 1) * half)
                put_rope(kv_own.at[u, 0, inside, :], dot_nn(n_buf[k], big[0, :, cols]), cos_ref[rows, :], sin_ref[rows, :])
                kv_own[u, 1, inside, :] = dot_nn(n_buf[k], big[1, :, cols]).astype(BF16)

        for g in range(HALVES):
            u = b * HALVES + g

            @pl.when(first_chip)
            def _(u=u):
                kv_to_chip(u).start()

            @pl.when(first_core)
            def _(u=u):
                kv_to_partner(u).start()

        @pl.when(b == 0)
        def _():
            for copy in weight_loads[2:]:
                copy.wait()
            w_local.start()

        for k in range(per_row):
            rows = tile_rows(b, k)
            inside = slice(k * tile, (k + 1) * tile)
            dy_load(b, k).wait()
            put_rope(q_ring.at[ring, inside, :], dot_nn(n_buf[k], big[2]), cos_ref[rows, :], sin_ref[rows, :])
            do_ring[ring, inside, :] = dot_nt(dy_in[k], wo_ref[...]).astype(BF16)

            @pl.when(b + 1 < batch)
            def _(k=k):
                dy_load(b + 1, k).start()

    def o_place(src, u):
        b, g = where(u)
        return o_all.at[src, row(b), half_cols(g)]

    def o_local_copy(b):
        return pltpu.make_async_copy(o_buf.at[b], o_place(z, b), o_local.at[b])

    def o_copy(b, k, step):
        return remote(o_buf.at[b], o_place(z, b), o_send.at[k, b], o_recv.at[z, b], {"tp": jnp.clip(z + step, 0, tp - 1)})

    hops = [(k, step, jnp.logical_and(z + step >= 0, z + step < tp)) for k, step in enumerate((1, -1))]

    def o_start(b):
        o_local_copy(b).start()
        for k, step, ok in hops:
            @pl.when(ok)
            def _(k=k, step=step):
                o_copy(b, k, step).start()

    def o_arrived(src, b):
        remote(o_place(src, b), o_place(src, b), relay_send.at[0, 0, b], o_recv.at[src, b], partner).wait_recv()

    def relay_copy(b, age, step):
        src = jnp.clip(z - age * step, 0, tp - 1)
        return remote(o_place(src, b), o_place(src, b), relay_send.at[age - 1, (1 - step) // 2, b], o_recv.at[src, b], {"tp": jnp.clip(z + step, 0, tp - 1)})

    def relays(age, step):
        far = z if step > 0 else tp - 1 - z
        return jnp.logical_and(far >= age, far < tp - 1)

    def relay(b, age):
        for step in (1, -1):
            @pl.when(relays(age, step))
            def _(step=step):
                o_arrived(jnp.clip(z - age * step, 0, tp - 1), b)
                relay_copy(b, age, step).start()

    def far_copy(b, par):
        return remote(g_far.at[par], xin.at[b], far_send.at[par], x_recv.at[b], partner)

    def part_copy(b, par):
        return remote(g_part.at[par], part_in.at[b], part_send.at[par], part_recv.at[b], partner)

    def chip_copy(b):
        par = lax.rem(b, CHIP_BUFS)
        return remote(g_chip.at[par], xin.at[b], chip_send.at[par], x_recv.at[b], peer)

    def chip_sum(b):
        @pl.when(second_chip)
        def _():
            par = lax.rem(b, CHIP_BUFS)
            far_copy(b, 0).wait_recv()
            g_chip[par] = (g_chip[par].astype(F32) + xin[b].astype(F32)).astype(BF16)
            chip_copy(b).start()

    def dkv_store(u, which):
        b, g = where(u)
        return pltpu.make_async_copy(g_own.at[lax.rem(u, OWN_RING), which], dkv_hbm.at[which, row(b), half_cols(g)], dkv_sem.at[u, which])

    def key_grads(u):
        @pl.when(first_core)
        def _():
            part_copy(u, 0).wait_recv()

        @pl.when(first_chip)
        def _():
            chip_copy(u).wait_recv()

        b, g = where(u)
        rows = row(b)
        for which in range(2):
            for h in range(half // HEAD_DIM):
                cols = slice(h * HEAD_DIM, (h + 1) * HEAD_DIM)
                own = g_own.at[lax.rem(u, OWN_RING), which, :, cols]
                acc = own[...].astype(F32)
                acc = acc + jnp.where(first_core, part_in[u, which, :, cols].astype(F32), 0.0)
                acc = (acc + jnp.where(first_chip, xin[u, which, :, cols].astype(F32), 0.0)).astype(BF16)
                if which == 0:
                    acc = rope(acc.astype(F32), cos_ref[rows, :], sin_ref[rows, :], -1.0).astype(BF16)
                own[...] = acc
            dkv_store(u, which).start()

    def dq_store(b, par):
        return pltpu.make_async_copy(dq_buf.at[par], dq_hbm.at[row(where(b)[0]), half_cols(where(b)[1])], dq_sem.at[par])

    subs = range(0, seq, SUB)

    def attend_unit(i, par):
        b, g = where(i)
        rows = row(b)
        ring = lax.rem(b, Q_RING)
        start = r * seq + lax.broadcasted_iota(jnp.int32, (1, seq), 1) - pos_ref[pl.ds(b, 1), :]
        chip_par = lax.rem(i, CHIP_BUFS)
        keys_of = [kv_own.at[i]] + [kvr.at[s, i] for s in range(3)]
        places = [g_part.at[par], g_chip.at[chip_par], g_far.at[par]]

        def grad(slot, which, cols):
            return places[slot - 1].at[which, :, cols] if slot else g_own.at[lax.rem(i, OWN_RING), which, :, cols]

        live = [None, second_core, second_chip, second_chip]
        piece = [r, r + 1 - 2 * core, r + 2 - 4 * chip, r + 3 - 2 * core - 4 * chip]

        def each(body):
            body(0)
            for slot in (1, 2, 3):
                pl.when(live[slot])(functools.partial(body, slot))

        def one_head(h, carry):
            cols = pl.ds(pl.multiple_of(h * HEAD_DIM, HEAD_DIM), HEAD_DIM)
            full = pl.ds(pl.multiple_of(g * half + h * HEAD_DIM, HEAD_DIM), HEAD_DIM)
            q = q_ring[ring, :, full]
            do = do_ring[ring, :, full]
            m_scr[...] = jnp.full(m_scr.shape, NEG_BIG, F32)
            l_scr[...] = jnp.zeros_like(l_scr)
            d_scr[...] = jnp.zeros_like(d_scr)
            ot_scr[...] = jnp.zeros_like(ot_scr)
            dqt_scr[...] = jnp.zeros_like(dqt_scr)

            def scores(slot):
                base = piece[slot] * seq
                for s in subs:
                    raw = dot_nt(keys_of[slot][0, s:s + SUB, cols], q)
                    local = lax.broadcasted_iota(jnp.int32, raw.shape, 0) + s
                    allowed = (local + base) >= start
                    if slot == 0:
                        allowed = jnp.logical_and(allowed, local <= lax.broadcasted_iota(jnp.int32, raw.shape, 1))
                    raw = jnp.where(allowed, raw, NEG_BIG)
                    s_scr[slot, s:s + SUB, :] = raw
                    m_scr[...] = jnp.maximum(m_scr[...], jnp.max(raw, axis=0, keepdims=True))

            def exps(slot):
                for s in subs:
                    e = jnp.exp2((s_scr[slot, s:s + SUB, :] - m_scr[...]) * EXP2_SCALE)
                    s_scr[slot, s:s + SUB, :] = e
                    l_scr[...] += jnp.sum(e, axis=0, keepdims=True)

            def values(slot):
                for s in subs:
                    v = keys_of[slot][1, s:s + SUB, cols]
                    prob = s_scr[slot, s:s + SUB, :] * l_scr[...]
                    low = prob.astype(BF16)
                    dp = dot_nt(v, do)
                    s_scr[slot, s:s + SUB, :] = prob
                    dp_scr[slot, s:s + SUB, :] = dp
                    d_scr[...] += jnp.sum(prob * dp, axis=0, keepdims=True)
                    grad(slot, 1, cols)[s:s + SUB, :] = dot_nn(low, do).astype(BF16)
                    ot_scr[...] += dot_nn(v.T, low)

            def keys(slot):
                for s in subs:
                    k = keys_of[slot][0, s:s + SUB, cols]
                    ds = (s_scr[slot, s:s + SUB, :] * (dp_scr[slot, s:s + SUB, :] - d_scr[...])).astype(BF16)
                    grad(slot, 0, cols)[s:s + SUB, :] = (dot_nn(ds, q) * SCALE).astype(BF16)
                    dqt_scr[...] += dot_nn(k.T, ds)

            each(scores)
            each(exps)
            l_scr[...] = 1.0 / l_scr[...]
            each(values)
            each(keys)
            o_buf[i, :, cols] = ot_scr[...].T.astype(BF16)
            dq_buf[par, :, cols] = rope(dqt_scr[...].T * SCALE, cos_ref[rows, :], sin_ref[rows, :], -1.0).astype(BF16)
            return carry

        lax.fori_loop(0, heads // HALVES, one_head, 0)

    def step(i, carry):
        par = lax.rem(i, 2)
        @pl.when(jnp.logical_and(lax.rem(i, HALVES) == 0, lax.div(i, HALVES) + AHEAD < batch))
        def _():
            project_row(lax.div(i, HALVES) + AHEAD)

        @pl.when(i >= OWN_RING)
        def _():
            for which in range(2):
                dkv_store(i - OWN_RING, which).wait()

        @pl.when(second_chip)
        def _():
            kv_to_chip(i).wait_recv()
            kv_forward(i).start()

        @pl.when(second_core)
        def _():
            kv_to_partner(i).wait_recv()

        @pl.when(second_chip)
        def _():
            kv_forward(i).wait_recv()

        @pl.when(i >= 2)
        def _():
            dq_store(i - 2, par).wait()

            @pl.when(second_core)
            def _():
                part_copy(i - 2, par).wait_send()

            @pl.when(second_chip)
            def _():
                far_copy(i - 2, par).wait_send()

        @pl.when(jnp.logical_and(second_chip, i >= CHIP_BUFS))
        def _():
            chip_copy(i - CHIP_BUFS).wait_send()

        attend_unit(i, par)
        o_start(i)
        dq_store(i, par).start()

        @pl.when(second_chip)
        def _():
            far_copy(i, par).start()

        @pl.when(second_core)
        def _():
            part_copy(i, par).start()

        @pl.when(i >= 1)
        def _():
            chip_sum(i - 1)

        for age in range(1, tp - 1):
            @pl.when(i >= age * RELAY_LAG)
            def _(age=age):
                relay(i - age * RELAY_LAG, age)

        @pl.when(i >= SUM_LAG)
        def _():
            key_grads(i - SUM_LAG)

        @pl.when(i == min(W_TWIN, units - 1))
        def _():
            for d in w_steps:
                wz_wait(d)
                w_move(0, d).start()
                w_move(1, d).start()

                @pl.when(second_chip)
                def _(d=d):
                    w_move(3, d).start()

        @pl.when(i == min(W_PARTNER, units - 1))
        def _():
            for d in w_steps:
                w_move(0, d).wait_recv()
                w_move(2, d).start()

        @pl.when(jnp.logical_and(first_chip, i == min(W_CHIP, units - 1)))
        def _():
            for k in (3, 4):
                for d in w_steps:
                    w_move(k, d).start()

        return carry

    for b in range(min(AHEAD, batch)):
        project_row(b)
    lax.fori_loop(0, units, step, 0)
    chip_sum(units - 1)

    @pl.when(second_chip)
    def _():
        for d in w_steps:
            w_move(4, d).start()

    end = units + max(SUM_LAG, (tp - 2) * RELAY_LAG)
    for i in range(units, end):
        for age in range(1, tp - 1):
            if 0 <= i - age * RELAY_LAG < units:
                relay(i - age * RELAY_LAG, age)
        if 0 <= i - SUM_LAG < units:
            key_grads(i - SUM_LAG)
        if i == end - 1:
            for k in (3, 4):
                for d in w_steps:
                    w_move(k, d).wait_recv()
                    w_move(k + 2, d).start()

    w_local.wait()
    for d in w_steps:
        wz_copy(d).wait_send()
        for k in range(7):
            w_move(k, d).wait_send()
            if k in (1, 2, 5, 6):
                w_move(k, d).wait_recv()

    for k in range(per_row):
        n_store(batch - 1, k).wait()
    for u in range(max(0, units - OWN_RING), units):
        for which in range(2):
            dkv_store(u, which).wait()

    def drain(b, carry):
        @pl.when(first_chip)
        def _():
            kv_to_chip(b).wait_send()

        @pl.when(first_core)
        def _():
            kv_to_partner(b).wait_send()

        @pl.when(second_chip)
        def _():
            kv_forward(b).wait_send()

        o_local_copy(b).wait()
        for k, step_, ok in hops:
            @pl.when(ok)
            def _(k=k, step_=step_):
                o_copy(b, k, step_).wait_send()

        for age in range(1, tp - 1):
            for step_ in (1, -1):
                @pl.when(relays(age, step_))
                def _(age=age, step_=step_):
                    relay_copy(b, age, step_).wait_send()

        for src in range(tp):
            way = jnp.where(z > src, 1, -1)
            gone = jnp.abs(z - src)
            far = jnp.where(way > 0, z, tp - 1 - z)
            taken = jnp.logical_and(gone <= tp - 2, far < tp - 1)

            @pl.when(jnp.logical_and(z != src, jnp.logical_not(taken)))
            def _(src=src):
                o_arrived(src, b)

        return carry

    lax.fori_loop(0, units, drain, 0)

    for b in range(max(0, units - 2), units):
        dq_store(b, b % 2).wait()

        @pl.when(second_core)
        def _(b=b):
            part_copy(b, b % 2).wait_send()

        @pl.when(second_chip)
        def _(b=b):
            far_copy(b, b % 2).wait_send()

    for b in range(max(0, units - CHIP_BUFS), units):
        @pl.when(second_chip)
        def _(b=b):
            chip_copy(b).wait_send()


def front(x, dy, wq, wk, wv, wo, pos, table, gain, seq, tp, cp):
    tokens, d_model = x.shape
    hidden = wq.shape[1]
    batch = tokens // seq
    units = batch * HALVES
    half = hidden // HALVES
    tile = seq // 2
    hbm = pl.BlockSpec(memory_space=pl.ANY)
    vmem = pl.BlockSpec(memory_space=pltpu.VMEM)
    dma = pltpu.SemaphoreType.DMA
    bf = lambda *shape: pltpu.VMEM(shape, BF16)
    f32 = lambda *shape: pltpu.VMEM(shape, F32)
    return pl.pallas_call(
        functools.partial(front_kernel, batch, seq, tp, cp),
        in_specs=[hbm] * 6 + [vmem] * 3,
        out_specs=[hbm] * 5,
        out_shape=[
            jax.ShapeDtypeStruct((tokens, d_model), BF16),
            jax.ShapeDtypeStruct((tp, tokens, hidden), BF16),
            jax.ShapeDtypeStruct((tokens, hidden), BF16),
            jax.ShapeDtypeStruct((2, tokens, hidden), BF16),
            jax.ShapeDtypeStruct((tp, hidden, d_model), BF16),
        ],
        scratch_shapes=[
            bf(3, d_model, hidden), bf(hidden, d_model), f32(tokens, HEAD_DIM), f32(tokens, HEAD_DIM),
            bf(Q_RING, seq, hidden), bf(Q_RING, seq, hidden), bf(2, tile, d_model), bf(2, tile, d_model), bf(2, tile, d_model),
            bf(units, 2, seq, half), bf(3, units, 2, seq, half),
            f32(4, seq, seq), f32(4, seq, seq), f32(1, seq), f32(1, seq), f32(1, seq), f32(HEAD_DIM, seq), f32(HEAD_DIM, seq),
            bf(units, seq, half), bf(2, seq, half),
            bf(OWN_RING, 2, seq, half), bf(2, 2, seq, half), bf(CHIP_BUFS, 2, seq, half), bf(2, 2, seq, half),
            bf(units, 2, seq, half), bf(units, 2, seq, half),
            dma((4,)), dma((1,)), dma((tp,)), dma((tp,)), dma((7, tp)), dma((7, tp)),
            dma((2,)), dma((2,)), dma((2,)), dma((units,)), dma((units,)), dma((units,)), dma((3, units)),
            dma((units,)), dma((2, units)), dma((tp, units)), dma((2, 2, units)), dma((2,)),
            dma((2,)), dma((2,)), dma((CHIP_BUFS,)), dma((units,)), dma((units,)), dma((units, 2)),
        ],
        compiler_params=pltpu.CompilerParams(collective_id=1, has_side_effects=True, vmem_limit_bytes=63 << 20),
        cost_estimate=pl.CostEstimate(flops=60 * tokens * seq * hidden, bytes_accessed=16 * tokens * d_model, transcendentals=4 * tokens * seq * (hidden // HEAD_DIM)),
        name="front",
    )(x, dy, wq, wk, wv, wo, pos, table, gain)


PART_RING = 4
RS_RING = 5
FORWARD_LAG = 11
JOB_LAG = 5
OUT_LAG = 4
EARLY = 4


def back_kernel(groups, rows, tp, cp, dq_hbm, dkv_hbm, x_hbm, dy_hbm, o_hbm, n_hbm, wq_hbm, wk_hbm, wv_hbm, wo_hbm, gain_ref,
                gx_hbm, y_hbm, ga_hbm, gb_hbm, gg_ref,
                wq_ref, wk_ref, wv_ref, wo_ref, dq_all, dkv_all, o_t, part, rs_r, rs_l, send_r, send_l, tot, gx_buf,
                o_in, x_in, xo_in, dyo_in, y_buf, n_in, dy_in, away, part_in, mine, gain_all,
                w_sem, in_sem, fin_sem, job_sem, y_sem, own_sem, rss_r, rss_l, rsr_r, rsr_l, ag0_r, ag0_l, agf_r, agf_l, agr_r, agr_l,
                away_send, away_recv, mine_own, mine_part, mine_chip, ga_recv, chip_recv, gb_send, gb_recv, gs_sem, gr_sem):
    z = lax.axis_index("tp")
    r = lax.axis_index("cp")
    core = lax.rem(r, 2)
    chip = lax.div(r, 2)
    last = tp - 1
    slots = tp - 1
    span = tp * rows
    tokens, d_model = x_hbm.shape
    hidden = dq_hbm.shape[1]
    chunk = min(512, d_model)
    blocks = ga_hbm.shape[0]
    width = ga_hbm.shape[1]
    pairs = blocks // 2
    partner = {"cp": r + 1 - 2 * core}
    peer = {"cp": r + 2 - 4 * chip}

    head = min(EARLY, groups) * span
    weight_loads = [pltpu.make_async_copy(src, dst, w_sem.at[k]) for k, (src, dst) in enumerate((
        (dq_hbm.at[:head, :], dq_all.at[:head, :]), (dkv_hbm.at[:, :head, :], dkv_all.at[:, :head, :]), (wq_hbm, wq_ref), (wk_hbm, wk_ref), (wv_hbm, wv_ref)))]
    rest_loads = [] if head == tokens else [
        pltpu.make_async_copy(dq_hbm.at[head:, :], dq_all.at[head:, :], w_sem.at[6]),
        pltpu.make_async_copy(dkv_hbm.at[:, head:, :], dkv_all.at[:, head:, :], w_sem.at[7]),
    ]
    out_loads = [pltpu.make_async_copy(wo_hbm, wo_ref, w_sem.at[5])]
    for copy in weight_loads:
        copy.start()

    barrier = pltpu.get_barrier_semaphore()
    peers = [(dt, dc) for dt in range(tp) for dc in range(cp) if dt or dc]
    for dt, dc in peers:
        pl.semaphore_signal(barrier, inc=1, device_id={"tp": lax.rem(z + dt, tp), "cp": lax.rem(r + dc, cp)}, device_id_type=MESH)
    pl.semaphore_wait(barrier, len(peers))

    def remote(src, dst, ssem, rsem, dev):
        return pltpu.make_async_remote_copy(src_ref=src, dst_ref=dst, send_sem=ssem, recv_sem=rsem, device_id=dev, device_id_type=MESH)

    right = {"tp": jnp.where(z < last, z + 1, z)}
    left = {"tp": jnp.where(z > 0, z - 1, z)}

    def group_rows(i):
        return pl.ds(pl.multiple_of(i * span, span), span)

    def tile_rows(i, owner):
        return pl.ds(pl.multiple_of(i * span + owner * rows, rows), rows)

    def inputs(i, slot):
        g = group_rows(i)
        return [
            pltpu.make_async_copy(o_hbm.at[:, g, :], o_in.at[slot], in_sem.at[slot, 0]),
            pltpu.make_async_copy(x_hbm.at[g, :], x_in.at[slot], in_sem.at[slot, 1]),
        ]

    def final_inputs(i, slot):
        g = tile_rows(i, z)
        return [
            pltpu.make_async_copy(x_hbm.at[g, :], xo_in.at[slot], fin_sem.at[slot, 0]),
            pltpu.make_async_copy(dy_hbm.at[g, :], dyo_in.at[slot], fin_sem.at[slot, 1]),
        ]

    def y_copy(i, slot):
        return pltpu.make_async_copy(y_buf.at[slot], y_hbm.at[group_rows(i), :], y_sem.at[slot])

    def rs_copy(i, s, to_right):
        ring = lax.rem(i, RS_RING)
        if to_right:
            return remote(send_r.at[s], rs_r.at[ring, s], rss_r.at[s], rsr_r.at[ring, s], right)
        return remote(send_l.at[s], rs_l.at[ring, s], rss_l.at[s], rsr_l.at[ring, s], left)

    def rs_send(i, s):
        for to_right in (True, False):
            far = z if to_right else last - z
            owner = (z + slots - s) if to_right else (z - slots + s)
            buf, held = (send_r, rs_r) if to_right else (send_l, rs_l)

            @pl.when(jnp.logical_and(jnp.logical_and(i >= 0, i < groups), jnp.logical_and(far <= s, far < last)))
            def _(to_right=to_right, far=far, owner=owner, buf=buf, held=held):
                @pl.when(i > 0)
                def _():
                    rs_copy(i - 1, s, to_right).wait_send()

                cur = lax.rem(i, PART_RING)
                own = pl.ds(pl.multiple_of(owner * rows, rows), rows)
                if s == 0:
                    buf[s] = part[cur, own, :].astype(BF16)
                else:
                    @pl.when(far == 0)
                    def _():
                        buf[s] = part[cur, own, :].astype(BF16)

                    @pl.when(far > 0)
                    def _():
                        rs_copy(i, s - 1, to_right).wait_recv()
                        buf[s] = (part[cur, own, :] + held[lax.rem(i, RS_RING), s - 1].astype(F32)).astype(BF16)

                rs_copy(i, s, to_right).start()

    def ag_own(i, slot, to_right):
        src = gx_buf.at[slot]
        dst = gx_hbm.at[tile_rows(i, z), :]
        if to_right:
            return remote(src, dst, ag0_r.at[slot], agr_r.at[i, 0], right)
        return remote(src, dst, ag0_l.at[slot], agr_l.at[i, 0], left)

    def own_copy(i, slot):
        return pltpu.make_async_copy(gx_buf.at[slot], gx_hbm.at[tile_rows(i, z), :], own_sem.at[slot])

    def ag_forward(i, a, to_right):
        owner = z - a if to_right else z + a
        tile = gx_hbm.at[tile_rows(i, owner), :]
        if to_right:
            return remote(tile, tile, agf_r.at[a], agr_r.at[i, a], right)
        return remote(tile, tile, agf_l.at[a], agr_l.at[i, a], left)

    def ag_wait(i, a, to_right):
        tile = gx_hbm.at[tile_rows(i, 0), :]
        sem = agr_r.at[i, a] if to_right else agr_l.at[i, a]
        remote(tile, tile, agf_r.at[a], sem, right).wait_recv()

    def ag_step(i, a):
        for to_right in (True, False):
            far = z if to_right else last - z

            @pl.when(jnp.logical_and(jnp.logical_and(i >= 0, i < groups), far >= a))
            def _(to_right=to_right, far=far):
                ag_wait(i, a - 1, to_right)
                if a < slots:
                    @pl.when(far < last)
                    def _():
                        @pl.when(i > 0)
                        def _():
                            ag_forward(i - 1, a, to_right).wait_send()

                        ag_forward(i, a, to_right).start()

    def ag_first(i, slot):
        own_copy(i, slot).start()
        for to_right in (True, False):
            far = z if to_right else last - z

            @pl.when(far < last)
            def _(to_right=to_right):
                ag_own(i, slot, to_right).start()

    def ag_first_done(i, slot):
        own_copy(i, slot).wait()
        for to_right in (True, False):
            far = z if to_right else last - z

            @pl.when(far < last)
            def _(to_right=to_right):
                ag_own(i, slot, to_right).wait_send()

    def partial_norm(i):
        cur = lax.rem(i, PART_RING)
        g = group_rows(i)
        for c in range(0, d_model, chunk):
            cols = slice(c, c + chunk)
            part[cur, :, cols] = (
                dot_nt(dq_all[g, :], wq_ref[cols, :]) + dot_nt(dkv_all[0, g, :], wk_ref[cols, :]) + dot_nt(dkv_all[1, g, :], wv_ref[cols, :])
            )

    def project_out(cur):
        for c in range(0, d_model, chunk):
            cols = slice(c, c + chunk)
            acc = x_in[cur, :, cols].astype(F32)
            for t in range(tp):
                acc += dot_nn(o_in[cur, t], wo_ref[t, :, cols])
            y_buf[cur, :, cols] = acc.astype(BF16)

    def finalize(i):
        slot = lax.rem(i, 2)
        own = pl.ds(pl.multiple_of(z * rows, rows), rows)
        tot[...] = part[lax.rem(i, PART_RING), own, :]

        @pl.when(z > 0)
        def _():
            rs_copy(i, slots - 1, True).wait_recv()
            tot[...] += rs_r[lax.rem(i, RS_RING), slots - 1].astype(F32)

        @pl.when(z < last)
        def _():
            rs_copy(i, slots - 1, False).wait_recv()
            tot[...] += rs_l[lax.rem(i, RS_RING), slots - 1].astype(F32)

        @pl.when(i > 1)
        def _():
            ag_first_done(i - 2, slot)

        for copy in final_inputs(i, slot):
            copy.wait()
        x = xo_in[slot].astype(F32)
        centred = x - jnp.mean(x, axis=-1, keepdims=True)
        inv_std = lax.rsqrt(jnp.mean(centred * centred, axis=-1, keepdims=True) + LN_EPS)
        x_hat = centred * inv_std
        dn = tot[...]
        gg_ref[...] += jnp.sum(dn * x_hat, axis=0, keepdims=True)
        d_hat = dn * gain_ref[...]
        dx = inv_std * (d_hat - jnp.mean(d_hat, axis=-1, keepdims=True) - x_hat * jnp.mean(d_hat * x_hat, axis=-1, keepdims=True))
        gx_buf[slot] = (dyo_in[slot].astype(F32) + dx).astype(BF16)
        ag_first(i, slot)

    def block_of(t):
        return 2 * lax.div(t, 2) + jnp.where(lax.rem(t, 2) == 0, 1 - core, core)

    def job_loads(t, slot):
        cols = pl.ds(pl.multiple_of(block_of(t) * width, width), width)
        return [
            pltpu.make_async_copy(n_hbm.at[:, cols], n_in.at[slot], job_sem.at[slot, 0]),
            pltpu.make_async_copy(dy_hbm.at[:, cols], dy_in.at[slot], job_sem.at[slot, 1]),
        ]

    def away_copy(p):
        ring = lax.rem(p, 2)
        return remote(away, part_in.at[ring], away_send.at[0], away_recv.at[ring], partner)

    def job_block(t, put):
        slot = lax.rem(t, 2)
        n_t = n_in[slot].T
        put(0, hidden, dot_nn(n_t, dq_all[...]))
        put(hidden, hidden, dot_nn(n_t, dkv_all[0]))
        put(2 * hidden, hidden, dot_nn(n_t, dkv_all[1]))
        for k in range(hidden // width):
            put(3 * hidden + k * width, width, dot_nn(o_t[k * width:(k + 1) * width, :], dy_in[slot]))

    def mine_to_own(p, slot):
        return pltpu.make_async_copy(mine.at[slot], ga_hbm.at[2 * p + core], mine_own.at[slot])

    def mine_to_part(p, slot):
        return remote(mine.at[slot], ga_hbm.at[2 * p + core], mine_part.at[slot], ga_recv.at[p], partner)

    def mine_to_chip(p, slot):
        return remote(mine.at[slot], gb_hbm.at[2 * p + core], mine_chip.at[slot], chip_recv.at[p], peer)

    def mine_done(p, slot):
        mine_to_own(p, slot).wait()
        mine_to_part(p, slot).wait_send()
        mine_to_chip(p, slot).wait_send()

    def chip_forward(p):
        b = 2 * p + core
        return remote(gb_hbm.at[b], gb_hbm.at[b], gb_send.at[p], gb_recv.at[p], partner)

    def job(t):
        p = lax.div(t, 2)
        for copy in job_loads(t, lax.rem(t, 2)):
            copy.wait()

        @pl.when(t + 1 < blocks)
        def _():
            for copy in job_loads(t + 1, 1 - lax.rem(t, 2)):
                copy.start()

        @pl.when(lax.rem(t, 2) == 0)
        def _():
            @pl.when(p > 0)
            def _():
                away_copy(p - 1).wait_send()

            def put(at, size, value):
                away[:, at:at + size] = value

            job_block(t, put)
            away_copy(p).start()

        @pl.when(lax.rem(t, 2) == 1)
        def _():
            slot = lax.rem(p, 2)
            away_copy(p).wait_recv()

            @pl.when(p > 1)
            def _():
                mine_done(p - 2, slot)

            def put(at, size, value):
                mine[slot, :, at:at + size] = (value + part_in[slot, :, at:at + size]).astype(BF16)

            job_block(t, put)
            mine_to_chip(p, slot).start()
            mine_to_part(p, slot).start()
            mine_to_own(p, slot).start()

    gg_ref[...] = jnp.zeros_like(gg_ref)
    o_loads = [pltpu.make_async_copy(o_hbm.at[z, :, k * width:(k + 1) * width], n_in.at[k], job_sem.at[k, 0]) for k in range(hidden // width)]
    for copy in o_loads:
        copy.start()
    for copy in inputs(0, 0):
        copy.start()
    for copy in rest_loads + out_loads:
        copy.start()
    me = z * cp + r

    def gain_copy(dt, dc):
        to = {"tp": lax.rem(z + dt, tp), "cp": lax.rem(r + dc, cp)}
        return remote(gain_all.at[me], gain_all.at[me], gs_sem.at[dt * cp + dc], gr_sem.at[me], to)

    def gain_wait(dt, dc):
        sender = lax.rem(z + dt, tp) * cp + lax.rem(r + dc, cp)
        remote(gain_all.at[sender], gain_all.at[sender], gs_sem.at[0], gr_sem.at[sender], right).wait_recv()

    for copy in weight_loads:
        copy.wait()

    def step(i, carry):
        for k in reversed(range(1, slots)):
            rs_send(i - k, k)

        @pl.when(i == EARLY)
        def _():
            for copy in rest_loads:
                copy.wait()

        @pl.when(i < groups)
        def _():
            partial_norm(i)

        rs_send(i, 0)

        @pl.when(jnp.logical_and(i >= slots, i < groups + slots))
        def _():
            finalize(i - slots)

        for a in range(1, slots + 1):
            ag_step(i - slots - a, a)

        @pl.when(i == groups + slots - 1)
        def _():
            gain_all[me] = gg_ref[...]
            for dt, dc in peers:
                gain_copy(dt, dc).start()

        @pl.when(jnp.logical_and(i >= slots - 1, i < groups + slots - 1))
        def _():
            for copy in final_inputs(i - slots + 1, lax.rem(i - slots + 1, 2)):
                copy.start()

        @pl.when(i == JOB_LAG - 1)
        def _():
            for k, copy in enumerate(o_loads):
                copy.wait()
                o_t[k * width:(k + 1) * width, :] = n_in[k].T
            for copy in job_loads(0, 0):
                copy.start()

        @pl.when(i == OUT_LAG)
        def _():
            for copy in out_loads:
                copy.wait()

        @pl.when(jnp.logical_and(i >= OUT_LAG, i < groups + OUT_LAG))
        def _():
            j = i - OUT_LAG
            at = lax.rem(j, 2)
            for copy in inputs(j, at):
                copy.wait()

            @pl.when(j + 1 < groups)
            def _():
                for copy in inputs(j + 1, 1 - at):
                    copy.start()

            @pl.when(j >= 2)
            def _():
                y_copy(j - 2, at).wait()

            project_out(at)
            y_copy(j, at).start()

        @pl.when(jnp.logical_and(i >= JOB_LAG, i < JOB_LAG + blocks))
        def _():
            job(i - JOB_LAG)

        @pl.when(jnp.logical_and(lax.rem(i, 2) == 1, jnp.logical_and(i >= FORWARD_LAG, i < FORWARD_LAG + 2 * pairs)))
        def _():
            p = lax.div(i - FORWARD_LAG, 2)
            mine_to_chip(p, 0).wait_recv()
            chip_forward(p).start()

        return carry

    lax.fori_loop(0, max(groups + 2 * slots, groups + OUT_LAG, blocks + JOB_LAG, 2 * pairs + FORWARD_LAG - 1), step, 0)

    for i in (groups - 2, groups - 1):
        y_copy(i, i % 2).wait()
        ag_first_done(i, i % 2)
    for to_right in (True, False):
        far = z if to_right else last - z
        for s in range(slots):
            @pl.when(jnp.logical_and(far <= s, far < last))
            def _(s=s, to_right=to_right):
                rs_copy(groups - 1, s, to_right).wait_send()
        for a in range(1, slots):
            @pl.when(jnp.logical_and(far >= a, far < last))
            def _(a=a, to_right=to_right):
                ag_forward(groups - 1, a, to_right).wait_send()
    away_copy(pairs - 1).wait_send()
    for p in range(max(0, pairs - 2), pairs):
        mine_done(p, p % 2)
    for p in range(pairs):
        chip_forward(p).wait_send()
        chip_forward(p).wait_recv()
        mine_to_part(p, 0).wait_recv()
    for dt, dc in peers:
        gain_wait(dt, dc)
        gain_copy(dt, dc).wait_send()
    total = gain_all[0]
    for j in range(1, tp * cp):
        total += gain_all[j]
    gg_ref[...] = total


def backward_norm(dq, dkv, x, dy, o_all, normed, wq, wk, wv, wo_all, gain, rows, tp, cp):
    tokens, hidden = dq.shape
    d_model = x.shape[1]
    span = tp * rows
    groups = tokens // span
    slots = tp - 1
    width = WIDTH
    blocks = d_model // width
    pairs = blocks // 2
    hbm = pl.BlockSpec(memory_space=pl.ANY)
    vmem = pl.BlockSpec(memory_space=pltpu.VMEM)
    dma = pltpu.SemaphoreType.DMA
    bf = lambda *shape: pltpu.VMEM(shape, BF16)
    f32 = lambda *shape: pltpu.VMEM(shape, F32)
    return pl.pallas_call(
        functools.partial(back_kernel, groups, rows, tp, cp),
        in_specs=[hbm] * 10 + [vmem],
        out_specs=[hbm, hbm, hbm, hbm, vmem],
        out_shape=[
            jax.ShapeDtypeStruct((tokens, d_model), BF16),
            jax.ShapeDtypeStruct((tokens, d_model), BF16),
            jax.ShapeDtypeStruct((blocks, width, 4 * hidden), BF16),
            jax.ShapeDtypeStruct((blocks, width, 4 * hidden), BF16),
            jax.ShapeDtypeStruct((1, d_model), F32),
        ],
        scratch_shapes=[
            bf(d_model, hidden), bf(d_model, hidden), bf(d_model, hidden), bf(tp, hidden, d_model),
            bf(tokens, hidden), bf(2, tokens, hidden), bf(hidden, tokens),
            f32(PART_RING, span, d_model), bf(RS_RING, slots, rows, d_model), bf(RS_RING, slots, rows, d_model),
            bf(slots, rows, d_model), bf(slots, rows, d_model), f32(rows, d_model), bf(2, rows, d_model),
            bf(2, tp, span, hidden), bf(2, span, d_model), bf(2, rows, d_model), bf(2, rows, d_model), bf(2, span, d_model),
            bf(2, tokens, width), bf(2, tokens, width),
            f32(width, 4 * hidden), f32(2, width, 4 * hidden), bf(2, width, 4 * hidden), f32(tp * cp, 1, d_model),
            dma((8,)), dma((2, 2)), dma((2, 2)), dma((2, 2)), dma((2,)), dma((2,)),
            dma((slots,)), dma((slots,)), dma((RS_RING, slots)), dma((RS_RING, slots)),
            dma((2,)), dma((2,)), dma((slots,)), dma((slots,)), dma((groups, slots)), dma((groups, slots)),
            dma((1,)), dma((2,)), dma((2,)), dma((2,)), dma((2,)), dma((pairs,)), dma((pairs,)), dma((pairs,)), dma((pairs,)),
            dma((tp * cp,)), dma((tp * cp,)),
        ],
        compiler_params=pltpu.CompilerParams(collective_id=0, has_side_effects=True, vmem_limit_bytes=63 << 20),
        cost_estimate=pl.CostEstimate(flops=22 * tokens * hidden * d_model, bytes_accessed=16 * tokens * d_model, transcendentals=0),
        name="backward_norm",
    )(dq, dkv, x, dy, o_all, normed, wq, wk, wv, wo_all, gain)


def finish_kernel(y_ref, gx_ref, ga_ref, gb_ref, yo_ref, gxo_ref, wq_ref, wk_ref, wv_ref, wo_ref):
    yo_ref[...] = y_ref[...]
    gxo_ref[...] = gx_ref[...]
    width = ga_ref.shape[1]
    hidden = wq_ref.shape[1]
    for k, ref in enumerate((wq_ref, wk_ref, wv_ref)):
        cols = slice(k * hidden, (k + 1) * hidden)
        ref[...] = ga_ref[0, :, cols].astype(F32) + gb_ref[0, :, cols].astype(F32)
    for k in range(hidden // width):
        cols = slice(3 * hidden + k * width, 3 * hidden + (k + 1) * width)
        wo_ref[k * width:(k + 1) * width, :] = ga_ref[0, :, cols].astype(F32) + gb_ref[0, :, cols].astype(F32)


def finish(y, gx, ga, gb):
    tokens, d_model = y.shape
    blocks, width, packed = ga.shape
    hidden = packed // 4
    rows = tokens // blocks
    tile = pl.BlockSpec((rows, d_model), lambda j: (j, 0))
    block = pl.BlockSpec((1, width, packed), lambda j: (j, 0, 0))
    wide = pl.BlockSpec((width, hidden), lambda j: (j, 0))
    return pl.pallas_call(
        finish_kernel,
        grid=(blocks,),
        in_specs=[tile, tile, block, block],
        out_specs=[tile, tile, wide, wide, wide, pl.BlockSpec((hidden, width), lambda j: (0, j))],
        out_shape=[jax.ShapeDtypeStruct((tokens, d_model), BF16)] * 2 + [jax.ShapeDtypeStruct((d_model, hidden), F32)] * 3 + [jax.ShapeDtypeStruct((hidden, d_model), F32)],
        compiler_params=pltpu.CompilerParams(dimension_semantics=("arbitrary",), vmem_limit_bytes=48 << 20),
        cost_estimate=pl.CostEstimate(flops=8 * d_model * hidden, bytes_accessed=8 * tokens * d_model + 32 * d_model * hidden, transcendentals=0),
        name="finish",
    )(y, gx, ga, gb)


def solution(mesh):
    cp_size = mesh.shape["cp"]
    tp_size = mesh.shape["tp"]

    def device_step(x_in, segment_ids, positions, w_query, w_key, w_value, w_out, norm_gain, grad_out):
        batch, seq, d_model = x_in.shape
        tokens = batch * seq
        x = x_in.reshape(tokens, d_model)
        dy = grad_out.reshape(tokens, d_model)

        gain = norm_gain.reshape(1, d_model)
        normed, o_all, dq, dkv, w_all = front(x, dy, w_query, w_key, w_value, w_out, positions, jnp.asarray(angle_table(), BF16), gain, seq, tp_size, cp_size)
        grad_x, y_out, sum_a, sum_b, grad_gain = backward_norm(dq, dkv, x, dy, o_all, normed, w_query, w_key, w_value, w_all, gain, ROWS, tp_size, cp_size)
        grad_gain = grad_gain.reshape(d_model)
        y_out, grad_x, grad_wq, grad_wk, grad_wv, grad_wo = finish(y_out, grad_x, sum_a, sum_b)
        return y_out.reshape(x_in.shape), grad_x.reshape(x_in.shape), grad_gain, grad_wq, grad_wk, grad_wv, grad_wo

    in_specs = (P("dp", "cp", None), P("dp", "cp"), P("dp", "cp"), P(None, "tp"), P(None, "tp"), P(None, "tp"), P("tp", None), P(None), P("dp", "cp", None))
    out_specs = (P("dp", "cp", None), P("dp", "cp", None), P("dp"), P("dp", "tp"), P("dp", "tp"), P("dp", "tp"), P(("dp", "tp"), None))
    return jax.shard_map(device_step, mesh=mesh, in_specs=in_specs, out_specs=out_specs, check_vma=False)
```

```python
import functools
import math

import jax
import jax.numpy as jnp
import numpy as np
from jax import lax
from jax.experimental import pallas as pl
from jax.experimental.pallas import tpu as pltpu
from jax.sharding import PartitionSpec as P

HEAD_DIM = 128
ROPE_THETA = 8000000.0
LN_EPS = 1e-5
NEG_BIG = -1e30
SCALE = HEAD_DIM ** -0.5
EXP2_SCALE = SCALE * math.log2(math.e)
F32 = jnp.float32
BF16 = jnp.bfloat16
NT = (((1,), (1,)), ((), ()))


def dot_nn(a, b):
    return jnp.dot(a, b, preferred_element_type=F32)


def dot_nt(a, b):
    return lax.dot_general(a, b, NT, preferred_element_type=F32)


def dot_tn(a, b):
    return lax.dot_general(a, b, (((0,), (0,)), ((), ())), preferred_element_type=F32)


def swap_pairs(t, sign):
    lane = lax.broadcasted_iota(jnp.int32, t.shape, 1)
    even = (lane % 2) == 0
    up = pltpu.roll(t, HEAD_DIM - 1, 1)
    down = pltpu.roll(t, 1, 1)
    return jnp.where(even, -up, down) if sign > 0 else jnp.where(even, up, -down)


def rope(t, cos_t, sin_t, sign):
    return t * cos_t + swap_pairs(t, sign) * sin_t


def angle_table():
    inv_freq = ROPE_THETA ** (-np.arange(0, HEAD_DIM, 2, dtype=np.float32) / np.float32(HEAD_DIM))
    freq = np.repeat(inv_freq.astype(np.float64), 2)[None, :]
    low = np.arange(POS_LOW)[:, None] * freq
    high = POS_LOW * np.arange(HEAD_DIM - POS_LOW)[:, None] * freq
    table = np.zeros((HEAD_DIM, 12 * HEAD_DIM), np.float32)
    for k, (first, value) in enumerate(((0, np.cos(low)), (0, np.sin(low)), (POS_LOW, np.cos(high)), (POS_LOW, np.sin(high)))):
        rest = value.astype(np.float32)
        for p in range(3):
            piece = rest.astype(BF16).astype(np.float32)
            at = (3 * k + p) * HEAD_DIM
            table[first:first + value.shape[0], at:at + HEAD_DIM] = piece
            rest = rest - piece
    return table


def put_rope(dst, raw, cos_t, sin_t):
    for h in range(raw.shape[1] // HEAD_DIM):
        cols = slice(h * HEAD_DIM, (h + 1) * HEAD_DIM)
        dst[:, cols] = rope(raw[:, cols], cos_t, sin_t, 1.0).astype(BF16)


MESH = pl.DeviceIdType.MESH
SUB = 128
ROWS = 32
WIDTH = 256
HALVES = 2
RELAY_LAG = 1
LATE = 3
SUM_LAG = 4
CHIP_BUFS = 4
OWN_RING = 6
Q_RING = 3
AHEAD = 2
POS_LOW = 64
W_TWIN = 1
W_PARTNER = 3
W_CHIP = 7


def front_kernel(batch, seq, tp, cp, x_hbm, dy_hbm, wq_hbm, wk_hbm, wv_hbm, wo_hbm, pos_ref, table_ref, gain_ref,
                 n_hbm, o_all, dq_hbm, dkv_hbm, w_all,
                 big, wo_ref, cos_ref, sin_ref, q_ring, do_ring, x_in, dy_in, n_buf, kv_own, kvr, s_scr, dp_scr, m_scr, l_scr, d_scr, ot_scr, dqt_scr,
                 o_buf, dq_buf, g_own, g_part, g_chip, g_far, xin, part_in,
                 w_sem, wl_sem, wz_send, wz_recv, wx_send, wx_recv,
                 x_sem, dy_sem, n_sem, kvs_part, kvs_chip, kvs_far, kv_recv, o_local, o_send, o_recv, relay_send, dq_sem,
                 far_send, part_send, chip_send, x_recv, part_recv, dkv_sem):
    z = lax.axis_index("tp")
    r = lax.axis_index("cp")
    dp = lax.axis_index("dp")
    core = lax.rem(r, 2)
    chip = lax.div(r, 2)
    d_model = x_hbm.shape[1]
    hidden = wq_hbm.shape[1]
    heads = hidden // HEAD_DIM
    first_chip, second_chip = chip == 0, chip == 1
    first_core, second_core = core == 0, core == 1
    partner = {"cp": r + 1 - 2 * core}
    peer = {"cp": r + 2 - 4 * chip}
    twin = {"dp": 1 - dp}

    tile = x_in.shape[1]
    per_row = seq // tile

    def row(b):
        return pl.ds(pl.multiple_of(b * seq, seq), seq)

    def tile_rows(b, k):
        return pl.ds(pl.multiple_of(b * seq + k * tile, tile), tile)

    def x_load(b, k):
        return pltpu.make_async_copy(x_hbm.at[tile_rows(b, k), :], x_in.at[k], x_sem.at[k])

    def dy_load(b, k):
        return pltpu.make_async_copy(dy_hbm.at[tile_rows(b, k), :], dy_in.at[k], dy_sem.at[k])

    def n_store(b, k):
        return pltpu.make_async_copy(n_buf.at[k], n_hbm.at[tile_rows(b, k), :], n_sem.at[k])

    weight_loads = [pltpu.make_async_copy(src, dst, w_sem.at[k]) for k, (src, dst) in enumerate(((wk_hbm, big.at[0]), (wv_hbm, big.at[1]), (wq_hbm, big.at[2]), (wo_hbm, wo_ref)))]
    x_load(0, 0).start()
    for copy in weight_loads[:2]:
        copy.start()
    for k in range(1, per_row):
        x_load(0, k).start()
    for copy in weight_loads[2:]:
        copy.start()
    for k in range(per_row):
        dy_load(0, k).start()

    units = batch * HALVES
    half = hidden // HALVES

    def where(u):
        return lax.div(u, HALVES), lax.rem(u, HALVES)

    def half_cols(g):
        return pl.ds(pl.multiple_of(g * half, half), half)

    barrier = pltpu.get_barrier_semaphore()
    for dev in [partner, peer, twin] + [{"tp": lax.rem(z + dt, tp)} for dt in range(1, tp)]:
        pl.semaphore_signal(barrier, inc=1, device_id=dev, device_id_type=MESH)
    pl.semaphore_wait(barrier, tp + 2)

    def remote(src, dst, ssem, rsem, dev):
        return pltpu.make_async_remote_copy(src_ref=src, dst_ref=dst, send_sem=ssem, recv_sem=rsem, device_id=dev, device_id_type=MESH)

    share = hidden // 8

    def share_rows(y, c, g):
        return pl.ds(pl.multiple_of((4 * y + 2 * c + g) * share, share), share)

    mine, twins = share_rows(chip, core, dp), share_rows(chip, core, 1 - dp)
    peers, peer_twins = share_rows(1 - chip, core, dp), share_rows(1 - chip, core, 1 - dp)

    def wz_copy(d):
        return remote(wo_hbm.at[mine, :], w_all.at[z, mine, :], wz_send.at[d], wz_recv.at[z], {"tp": lax.rem(z + d, tp)})

    def wz_wait(d):
        src = lax.rem(z + d, tp)
        remote(wo_hbm.at[mine, :], w_all.at[src, mine, :], wz_send.at[d], wz_recv.at[src], partner).wait_recv()

    def w_copy(k, d, rows, dev):
        place = w_all.at[lax.rem(z + d, tp), rows, :]
        return remote(place, place, wx_send.at[k, d], wx_recv.at[k, d], dev)

    def w_move(k, d):
        rows, dev = ((mine, twin), (mine, partner), (twins, partner), (mine, peer), (twins, peer), (peers, partner), (peer_twins, partner))[k]
        return w_copy(k, d, rows, dev)

    w_steps = range(1, tp)

    for d in range(1, tp):
        wz_copy(d).start()

    def kv_to_partner(u):
        return remote(kv_own.at[u], kvr.at[0, u], kvs_part.at[u], kv_recv.at[0, u], partner)

    def kv_to_chip(u):
        return remote(kv_own.at[u], kvr.at[1, u], kvs_chip.at[u], kv_recv.at[1, u], peer)

    def kv_forward(u):
        return remote(kvr.at[1, u], kvr.at[2, u], kvs_far.at[u], kv_recv.at[2, u], partner)

    w_local = pltpu.make_async_copy(wo_ref, w_all.at[z], wl_sem.at[0])
    for copy in weight_loads[:2]:
        copy.wait()

    def angles(b, k):
        rows = tile_rows(b, k)
        pos = jnp.broadcast_to(pos_ref[pl.ds(b, 1), k * tile:(k + 1) * tile], (HEAD_DIM, tile)).T
        lane = lax.broadcasted_iota(jnp.int32, (tile, HEAD_DIM), 1)
        low = lane < POS_LOW
        pick = jnp.where(low, lax.rem(pos, POS_LOW), POS_LOW + lax.div(pos, POS_LOW)) == lane
        found = dot_nn(jnp.where(pick, 1.0, 0.0).astype(BF16), table_ref[...])

        def part(k):
            at = 3 * k * HEAD_DIM
            return found[:, at:at + HEAD_DIM] + found[:, at + HEAD_DIM:at + 2 * HEAD_DIM] + found[:, at + 2 * HEAD_DIM:at + 3 * HEAD_DIM]

        cos_b, sin_b, cos_a, sin_a = part(0), part(1), part(2), part(3)
        cos_ref[rows, :] = cos_a * cos_b - sin_a * sin_b
        sin_ref[rows, :] = sin_a * cos_b + cos_a * sin_b

    def project_row(b):
        ring = lax.rem(b, Q_RING)
        for k in range(per_row):
            rows = tile_rows(b, k)
            inside = slice(k * tile, (k + 1) * tile)
            x_load(b, k).wait()

            @pl.when(b > 0)
            def _(k=k):
                n_store(b - 1, k).wait()

            angles(b, k)
            x = x_in[k].astype(F32)
            centred = x - jnp.mean(x, axis=-1, keepdims=True)
            inv_std = lax.rsqrt(jnp.mean(centred * centred, axis=-1, keepdims=True) + LN_EPS)
            n_buf[k] = ((centred * inv_std) * gain_ref[...]).astype(BF16)
            n_store(b, k).start()

            @pl.when(b + 1 < batch)
            def _(k=k):
                x_load(b + 1, k).start()

            for g in range(HALVES):
                u = b * HALVES + g
                cols = slice(g * half, (g + 1) * half)
                put_rope(kv_own.at[u, 0, inside, :], dot_nn(n_buf[k], big[0, :, cols]), cos_ref[rows, :], sin_ref[rows, :])
                kv_own[u, 1, inside, :] = dot_nn(n_buf[k], big[1, :, cols]).astype(BF16)

        for g in range(HALVES):
            u = b * HALVES + g

            @pl.when(first_chip)
            def _(u=u):
                kv_to_chip(u).start()

            @pl.when(first_core)
            def _(u=u):
                kv_to_partner(u).start()

        @pl.when(b == 0)
        def _():
            for copy in weight_loads[2:]:
                copy.wait()
            w_local.start()

        for k in range(per_row):
            rows = tile_rows(b, k)
            inside = slice(k * tile, (k + 1) * tile)
            dy_load(b, k).wait()
            put_rope(q_ring.at[ring, inside, :], dot_nn(n_buf[k], big[2]), cos_ref[rows, :], sin_ref[rows, :])
            do_ring[ring, inside, :] = dot_nt(dy_in[k], wo_ref[...]).astype(BF16)

            @pl.when(b + 1 < batch)
            def _(k=k):
                dy_load(b + 1, k).start()

    def o_place(src, u):
        b, g = where(u)
        return o_all.at[src, row(b), half_cols(g)]

    def o_local_copy(b):
        return pltpu.make_async_copy(o_buf.at[b], o_place(z, b), o_local.at[b])

    def o_copy(b, k, step):
        return remote(o_buf.at[b], o_place(z, b), o_send.at[k, b], o_recv.at[z, b], {"tp": jnp.clip(z + step, 0, tp - 1)})

    hops = [(k, step, jnp.logical_and(z + step >= 0, z + step < tp)) for k, step in enumerate((1, -1))]

    def far_from_end(step):
        return jnp.logical_and(z + step != 0, z + step != tp - 1)

    def o_start(b):
        o_local_copy(b).start()
        for k, step, ok in hops:
            @pl.when(jnp.logical_and(ok, jnp.logical_or(b < units - LATE, far_from_end(step))))
            def _(k=k, step=step):
                o_copy(b, k, step).start()

    def o_arrived(src, b):
        remote(o_place(src, b), o_place(src, b), relay_send.at[0, 0, b], o_recv.at[src, b], partner).wait_recv()

    def relay_copy(b, age, step):
        src = jnp.clip(z - age * step, 0, tp - 1)
        return remote(o_place(src, b), o_place(src, b), relay_send.at[age - 1, (1 - step) // 2, b], o_recv.at[src, b], {"tp": jnp.clip(z + step, 0, tp - 1)})

    def relays(age, step):
        far = z if step > 0 else tp - 1 - z
        return jnp.logical_and(far >= age, far < tp - 1)

    def relay(b, age):
        for step in (1, -1):
            @pl.when(relays(age, step))
            def _(step=step):
                o_arrived(jnp.clip(z - age * step, 0, tp - 1), b)
                relay_copy(b, age, step).start()

    def far_copy(b, par):
        return remote(g_far.at[par], xin.at[b], far_send.at[par], x_recv.at[b], partner)

    def part_copy(b, par):
        return remote(g_part.at[par], part_in.at[b], part_send.at[par], part_recv.at[b], partner)

    def chip_copy(b):
        par = lax.rem(b, CHIP_BUFS)
        return remote(g_chip.at[par], xin.at[b], chip_send.at[par], x_recv.at[b], peer)

    def chip_sum(b):
        @pl.when(second_chip)
        def _():
            par = lax.rem(b, CHIP_BUFS)
            far_copy(b, 0).wait_recv()
            g_chip[par] = (g_chip[par].astype(F32) + xin[b].astype(F32)).astype(BF16)
            chip_copy(b).start()

    def dkv_store(u, which):
        b, g = where(u)
        return pltpu.make_async_copy(g_own.at[lax.rem(u, OWN_RING), which], dkv_hbm.at[which, row(b), half_cols(g)], dkv_sem.at[u, which])

    def key_grads(u):
        @pl.when(first_core)
        def _():
            part_copy(u, 0).wait_recv()

        @pl.when(first_chip)
        def _():
            chip_copy(u).wait_recv()

        b, g = where(u)
        rows = row(b)
        for which in range(2):
            for h in range(half // HEAD_DIM):
                cols = slice(h * HEAD_DIM, (h + 1) * HEAD_DIM)
                own = g_own.at[lax.rem(u, OWN_RING), which, :, cols]
                acc = own[...].astype(F32)
                acc = acc + jnp.where(first_core, part_in[u, which, :, cols].astype(F32), 0.0)
                acc = (acc + jnp.where(first_chip, xin[u, which, :, cols].astype(F32), 0.0)).astype(BF16)
                if which == 0:
                    acc = rope(acc.astype(F32), cos_ref[rows, :], sin_ref[rows, :], -1.0).astype(BF16)
                own[...] = acc
            dkv_store(u, which).start()

    def dq_store(b, par):
        return pltpu.make_async_copy(dq_buf.at[par], dq_hbm.at[row(where(b)[0]), half_cols(where(b)[1])], dq_sem.at[par])

    subs = range(0, seq, SUB)

    def attend_unit(i, par):
        b, g = where(i)
        rows = row(b)
        ring = lax.rem(b, Q_RING)
        start = r * seq + lax.broadcasted_iota(jnp.int32, (1, seq), 1) - pos_ref[pl.ds(b, 1), :]
        chip_par = lax.rem(i, CHIP_BUFS)
        keys_of = [kv_own.at[i]] + [kvr.at[s, i] for s in range(3)]
        places = [g_part.at[par], g_chip.at[chip_par], g_far.at[par]]

        def grad(slot, which, cols):
            return places[slot - 1].at[which, :, cols] if slot else g_own.at[lax.rem(i, OWN_RING), which, :, cols]

        live = [None, second_core, second_chip, second_chip]
        piece = [r, r + 1 - 2 * core, r + 2 - 4 * chip, r + 3 - 2 * core - 4 * chip]

        def each(body):
            body(0)
            for slot in (1, 2, 3):
                pl.when(live[slot])(functools.partial(body, slot))

        def one_head(h, carry):
            cols = pl.ds(pl.multiple_of(h * HEAD_DIM, HEAD_DIM), HEAD_DIM)
            full = pl.ds(pl.multiple_of(g * half + h * HEAD_DIM, HEAD_DIM), HEAD_DIM)
            q = q_ring[ring, :, full]
            do = do_ring[ring, :, full]
            m_scr[...] = jnp.full(m_scr.shape, NEG_BIG, F32)
            l_scr[...] = jnp.zeros_like(l_scr)
            d_scr[...] = jnp.zeros_like(d_scr)
            ot_scr[...] = jnp.zeros_like(ot_scr)
            dqt_scr[...] = jnp.zeros_like(dqt_scr)

            def scores(slot):
                base = piece[slot] * seq
                for s in subs:
                    raw = dot_nt(keys_of[slot][0, s:s + SUB, cols], q)
                    local = lax.broadcasted_iota(jnp.int32, raw.shape, 0) + s
                    allowed = (local + base) >= start
                    if slot == 0:
                        allowed = jnp.logical_and(allowed, local <= lax.broadcasted_iota(jnp.int32, raw.shape, 1))
                    raw = jnp.where(allowed, raw, NEG_BIG)
                    s_scr[slot, s:s + SUB, :] = raw
                    m_scr[...] = jnp.maximum(m_scr[...], jnp.max(raw, axis=0, keepdims=True))

            def exps(slot):
                for s in subs:
                    e = jnp.exp2((s_scr[slot, s:s + SUB, :] - m_scr[...]) * EXP2_SCALE)
                    s_scr[slot, s:s + SUB, :] = e
                    l_scr[...] += jnp.sum(e, axis=0, keepdims=True)

            def values(slot):
                for s in subs:
                    v = keys_of[slot][1, s:s + SUB, cols]
                    prob = s_scr[slot, s:s + SUB, :] * l_scr[...]
                    low = prob.astype(BF16)
                    dp = dot_nt(v, do)
                    s_scr[slot, s:s + SUB, :] = prob
                    dp_scr[slot, s:s + SUB, :] = dp
                    d_scr[...] += jnp.sum(prob * dp, axis=0, keepdims=True)
                    grad(slot, 1, cols)[s:s + SUB, :] = dot_nn(low, do).astype(BF16)
                    ot_scr[...] += dot_nn(v.T, low)

            def keys(slot):
                for s in subs:
                    k = keys_of[slot][0, s:s + SUB, cols]
                    ds = (s_scr[slot, s:s + SUB, :] * (dp_scr[slot, s:s + SUB, :] - d_scr[...])).astype(BF16)
                    grad(slot, 0, cols)[s:s + SUB, :] = (dot_nn(ds, q) * SCALE).astype(BF16)
                    dqt_scr[...] += dot_nn(k.T, ds)

            each(scores)
            each(exps)
            l_scr[...] = 1.0 / l_scr[...]
            each(values)
            each(keys)
            o_buf[i, :, cols] = ot_scr[...].T.astype(BF16)
            dq_buf[par, :, cols] = rope(dqt_scr[...].T * SCALE, cos_ref[rows, :], sin_ref[rows, :], -1.0).astype(BF16)
            return carry

        lax.fori_loop(0, heads // HALVES, one_head, 0)

    def step(i, carry):
        par = lax.rem(i, 2)
        @pl.when(jnp.logical_and(lax.rem(i, HALVES) == 0, lax.div(i, HALVES) + AHEAD < batch))
        def _():
            project_row(lax.div(i, HALVES) + AHEAD)

        @pl.when(i >= OWN_RING)
        def _():
            for which in range(2):
                dkv_store(i - OWN_RING, which).wait()

        @pl.when(second_chip)
        def _():
            kv_to_chip(i).wait_recv()
            kv_forward(i).start()

        @pl.when(second_core)
        def _():
            kv_to_partner(i).wait_recv()

        @pl.when(second_chip)
        def _():
            kv_forward(i).wait_recv()

        @pl.when(i >= 2)
        def _():
            dq_store(i - 2, par).wait()

            @pl.when(second_core)
            def _():
                part_copy(i - 2, par).wait_send()

            @pl.when(second_chip)
            def _():
                far_copy(i - 2, par).wait_send()

        @pl.when(jnp.logical_and(second_chip, i >= CHIP_BUFS))
        def _():
            chip_copy(i - CHIP_BUFS).wait_send()

        attend_unit(i, par)
        o_start(i)
        dq_store(i, par).start()

        @pl.when(second_chip)
        def _():
            far_copy(i, par).start()

        @pl.when(second_core)
        def _():
            part_copy(i, par).start()

        @pl.when(i >= 1)
        def _():
            chip_sum(i - 1)

        for age in range(1, tp - 1):
            @pl.when(i >= age * RELAY_LAG)
            def _(age=age):
                relay(i - age * RELAY_LAG, age)

        @pl.when(i >= SUM_LAG)
        def _():
            key_grads(i - SUM_LAG)

        @pl.when(i == min(W_TWIN, units - 1))
        def _():
            for d in w_steps:
                wz_wait(d)
                w_move(0, d).start()
                w_move(1, d).start()

                @pl.when(second_chip)
                def _(d=d):
                    w_move(3, d).start()

        @pl.when(i == min(W_PARTNER, units - 1))
        def _():
            for d in w_steps:
                w_move(0, d).wait_recv()
                w_move(2, d).start()

                @pl.when(second_chip)
                def _(d=d):
                    w_move(4, d).start()

        @pl.when(jnp.logical_and(first_chip, i == min(W_CHIP, units - 1)))
        def _():
            for k in (3, 4):
                for d in w_steps:
                    w_move(k, d).start()

        return carry

    for b in range(min(AHEAD, batch)):
        project_row(b)
    lax.fori_loop(0, units, step, 0)
    chip_sum(units - 1)

    end = units + max(SUM_LAG, (tp - 2) * RELAY_LAG)
    for i in range(units, end):
        for age in range(1, tp - 1):
            if 0 <= i - age * RELAY_LAG < units:
                relay(i - age * RELAY_LAG, age)
        if 0 <= i - SUM_LAG < units:
            key_grads(i - SUM_LAG)
        if i == end - 1:
            for k in (3, 4):
                for d in w_steps:
                    w_move(k, d).wait_recv()
                    w_move(k + 2, d).start()

    w_local.wait()
    for d in w_steps:
        wz_copy(d).wait_send()
        for k in range(7):
            w_move(k, d).wait_send()
            if k in (1, 2, 5, 6):
                w_move(k, d).wait_recv()

    for k in range(per_row):
        n_store(batch - 1, k).wait()
    for u in range(max(0, units - OWN_RING), units):
        for which in range(2):
            dkv_store(u, which).wait()

    def drain(b, carry):
        @pl.when(first_chip)
        def _():
            kv_to_chip(b).wait_send()

        @pl.when(first_core)
        def _():
            kv_to_partner(b).wait_send()

        @pl.when(second_chip)
        def _():
            kv_forward(b).wait_send()

        o_local_copy(b).wait()
        for k, step_, ok in hops:
            @pl.when(jnp.logical_and(ok, jnp.logical_or(b < units - LATE, far_from_end(step_))))
            def _(k=k, step_=step_):
                o_copy(b, k, step_).wait_send()

        for age in range(1, tp - 1):
            for step_ in (1, -1):
                @pl.when(relays(age, step_))
                def _(age=age, step_=step_):
                    relay_copy(b, age, step_).wait_send()

        for src in range(tp):
            way = jnp.where(z > src, 1, -1)
            gone = jnp.abs(z - src)
            far = jnp.where(way > 0, z, tp - 1 - z)
            taken = jnp.logical_and(gone <= tp - 2, far < tp - 1)
            late = jnp.logical_and(b >= units - LATE, jnp.logical_and(gone == 1, far == tp - 1))

            @pl.when(jnp.logical_and(z != src, jnp.logical_not(jnp.logical_or(taken, late))))
            def _(src=src):
                o_arrived(src, b)

        return carry

    lax.fori_loop(0, units, drain, 0)

    for b in range(max(0, units - 2), units):
        dq_store(b, b % 2).wait()

        @pl.when(second_core)
        def _(b=b):
            part_copy(b, b % 2).wait_send()

        @pl.when(second_chip)
        def _(b=b):
            far_copy(b, b % 2).wait_send()

    for b in range(max(0, units - CHIP_BUFS), units):
        @pl.when(second_chip)
        def _(b=b):
            chip_copy(b).wait_send()


def front(x, dy, wq, wk, wv, wo, pos, table, gain, seq, tp, cp):
    tokens, d_model = x.shape
    hidden = wq.shape[1]
    batch = tokens // seq
    units = batch * HALVES
    half = hidden // HALVES
    tile = seq // 2
    hbm = pl.BlockSpec(memory_space=pl.ANY)
    vmem = pl.BlockSpec(memory_space=pltpu.VMEM)
    dma = pltpu.SemaphoreType.DMA
    bf = lambda *shape: pltpu.VMEM(shape, BF16)
    f32 = lambda *shape: pltpu.VMEM(shape, F32)
    return pl.pallas_call(
        functools.partial(front_kernel, batch, seq, tp, cp),
        in_specs=[hbm] * 6 + [vmem] * 3,
        out_specs=[hbm] * 5,
        out_shape=[
            jax.ShapeDtypeStruct((tokens, d_model), BF16),
            jax.ShapeDtypeStruct((tp, tokens, hidden), BF16),
            jax.ShapeDtypeStruct((tokens, hidden), BF16),
            jax.ShapeDtypeStruct((2, tokens, hidden), BF16),
            jax.ShapeDtypeStruct((tp, hidden, d_model), BF16),
        ],
        scratch_shapes=[
            bf(3, d_model, hidden), bf(hidden, d_model), f32(tokens, HEAD_DIM), f32(tokens, HEAD_DIM),
            bf(Q_RING, seq, hidden), bf(Q_RING, seq, hidden), bf(2, tile, d_model), bf(2, tile, d_model), bf(2, tile, d_model),
            bf(units, 2, seq, half), bf(3, units, 2, seq, half),
            f32(4, seq, seq), f32(4, seq, seq), f32(1, seq), f32(1, seq), f32(1, seq), f32(HEAD_DIM, seq), f32(HEAD_DIM, seq),
            bf(units, seq, half), bf(2, seq, half),
            bf(OWN_RING, 2, seq, half), bf(2, 2, seq, half), bf(CHIP_BUFS, 2, seq, half), bf(2, 2, seq, half),
            bf(units, 2, seq, half), bf(units, 2, seq, half),
            dma((4,)), dma((1,)), dma((tp,)), dma((tp,)), dma((7, tp)), dma((7, tp)),
            dma((2,)), dma((2,)), dma((2,)), dma((units,)), dma((units,)), dma((units,)), dma((3, units)),
            dma((units,)), dma((2, units)), dma((tp, units)), dma((2, 2, units)), dma((2,)),
            dma((2,)), dma((2,)), dma((CHIP_BUFS,)), dma((units,)), dma((units,)), dma((units, 2)),
        ],
        compiler_params=pltpu.CompilerParams(collective_id=1, has_side_effects=True, vmem_limit_bytes=63 << 20),
        cost_estimate=pl.CostEstimate(flops=60 * tokens * seq * hidden, bytes_accessed=16 * tokens * d_model, transcendentals=4 * tokens * seq * (hidden // HEAD_DIM)),
        name="front",
    )(x, dy, wq, wk, wv, wo, pos, table, gain)


PART_RING = 4
RS_RING = 5
FORWARD_LAG = 11
JOB_LAG = 5
OUT_LAG = 4
EARLY = 4


def back_kernel(groups, rows, tp, cp, seq, dq_hbm, dkv_hbm, x_hbm, dy_hbm, o_old, n_hbm, wq_hbm, wk_hbm, wv_hbm, wo_hbm, gain_ref,
                gx_hbm, y_hbm, ga_hbm, gb_hbm, gg_ref, o_out,
                wq_ref, wk_ref, wv_ref, wo_ref, dq_all, dkv_all, o_t, part, rs_r, rs_l, send_r, send_l, tot, gx_buf,
                o_in, x_in, xo_in, dyo_in, y_buf, n_in, dy_in, away, part_in, mine, gain_all,
                w_sem, in_sem, fin_sem, job_sem, y_sem, own_sem, rss_r, rss_l, rsr_r, rsr_l, ag0_r, ag0_l, agf_r, agf_l, agr_r, agr_l,
                away_send, away_recv, mine_own, mine_part, mine_chip, ga_recv, chip_recv, gb_send, gb_recv, gs_sem, gr_sem, late_send, late_recv):
    o_hbm = o_out
    z = lax.axis_index("tp")
    r = lax.axis_index("cp")
    core = lax.rem(r, 2)
    chip = lax.div(r, 2)
    last = tp - 1
    slots = tp - 1
    span = tp * rows
    tokens, d_model = x_hbm.shape
    hidden = dq_hbm.shape[1]
    chunk = min(512, d_model)
    blocks = ga_hbm.shape[0]
    width = ga_hbm.shape[1]
    pairs = blocks // 2
    partner = {"cp": r + 1 - 2 * core}
    peer = {"cp": r + 2 - 4 * chip}

    head = min(EARLY, groups) * span
    weight_loads = [pltpu.make_async_copy(src, dst, w_sem.at[k]) for k, (src, dst) in enumerate((
        (dq_hbm.at[:head, :], dq_all.at[:head, :]), (dkv_hbm.at[:, :head, :], dkv_all.at[:, :head, :]), (wq_hbm, wq_ref), (wk_hbm, wk_ref), (wv_hbm, wv_ref)))]
    rest_loads = [] if head == tokens else [
        pltpu.make_async_copy(dq_hbm.at[head:, :], dq_all.at[head:, :], w_sem.at[6]),
        pltpu.make_async_copy(dkv_hbm.at[:, head:, :], dkv_all.at[:, head:, :], w_sem.at[7]),
    ]
    out_loads = [pltpu.make_async_copy(wo_hbm, wo_ref, w_sem.at[5])]
    for copy in weight_loads:
        copy.start()

    barrier = pltpu.get_barrier_semaphore()
    peers = [(dt, dc) for dt in range(tp) for dc in range(cp) if dt or dc]
    for dt, dc in peers:
        pl.semaphore_signal(barrier, inc=1, device_id={"tp": lax.rem(z + dt, tp), "cp": lax.rem(r + dc, cp)}, device_id_type=MESH)
    pl.semaphore_wait(barrier, len(peers))

    def remote(src, dst, ssem, rsem, dev):
        return pltpu.make_async_remote_copy(src_ref=src, dst_ref=dst, send_sem=ssem, recv_sem=rsem, device_id=dev, device_id_type=MESH)

    right = {"tp": jnp.where(z < last, z + 1, z)}
    left = {"tp": jnp.where(z > 0, z - 1, z)}

    def group_rows(i):
        return pl.ds(pl.multiple_of(i * span, span), span)

    def tile_rows(i, owner):
        return pl.ds(pl.multiple_of(i * span + owner * rows, rows), rows)

    def inputs(i, slot):
        g = group_rows(i)
        return [
            pltpu.make_async_copy(o_hbm.at[:, g, :], o_in.at[slot], in_sem.at[slot, 0]),
            pltpu.make_async_copy(x_hbm.at[g, :], x_in.at[slot], in_sem.at[slot, 1]),
        ]

    def final_inputs(i, slot):
        g = tile_rows(i, z)
        return [
            pltpu.make_async_copy(x_hbm.at[g, :], xo_in.at[slot], fin_sem.at[slot, 0]),
            pltpu.make_async_copy(dy_hbm.at[g, :], dyo_in.at[slot], fin_sem.at[slot, 1]),
        ]

    def y_copy(i, slot):
        return pltpu.make_async_copy(y_buf.at[slot], y_hbm.at[group_rows(i), :], y_sem.at[slot])

    def rs_copy(i, s, to_right):
        ring = lax.rem(i, RS_RING)
        if to_right:
            return remote(send_r.at[s], rs_r.at[ring, s], rss_r.at[s], rsr_r.at[ring, s], right)
        return remote(send_l.at[s], rs_l.at[ring, s], rss_l.at[s], rsr_l.at[ring, s], left)

    def rs_send(i, s):
        for to_right in (True, False):
            far = z if to_right else last - z
            owner = (z + slots - s) if to_right else (z - slots + s)
            buf, held = (send_r, rs_r) if to_right else (send_l, rs_l)

            @pl.when(jnp.logical_and(jnp.logical_and(i >= 0, i < groups), jnp.logical_and(far <= s, far < last)))
            def _(to_right=to_right, far=far, owner=owner, buf=buf, held=held):
                @pl.when(i > 0)
                def _():
                    rs_copy(i - 1, s, to_right).wait_send()

                cur = lax.rem(i, PART_RING)
                own = pl.ds(pl.multiple_of(owner * rows, rows), rows)
                if s == 0:
                    buf[s] = part[cur, own, :].astype(BF16)
                else:
                    @pl.when(far == 0)
                    def _():
                        buf[s] = part[cur, own, :].astype(BF16)

                    @pl.when(far > 0)
                    def _():
                        rs_copy(i, s - 1, to_right).wait_recv()
                        buf[s] = (part[cur, own, :] + held[lax.rem(i, RS_RING), s - 1].astype(F32)).astype(BF16)

                rs_copy(i, s, to_right).start()

    def ag_own(i, slot, to_right):
        src = gx_buf.at[slot]
        dst = gx_hbm.at[tile_rows(i, z), :]
        if to_right:
            return remote(src, dst, ag0_r.at[slot], agr_r.at[i, 0], right)
        return remote(src, dst, ag0_l.at[slot], agr_l.at[i, 0], left)

    def own_copy(i, slot):
        return pltpu.make_async_copy(gx_buf.at[slot], gx_hbm.at[tile_rows(i, z), :], own_sem.at[slot])

    def ag_forward(i, a, to_right):
        owner = z - a if to_right else z + a
        tile = gx_hbm.at[tile_rows(i, owner), :]
        if to_right:
            return remote(tile, tile, agf_r.at[a], agr_r.at[i, a], right)
        return remote(tile, tile, agf_l.at[a], agr_l.at[i, a], left)

    def ag_wait(i, a, to_right):
        tile = gx_hbm.at[tile_rows(i, 0), :]
        sem = agr_r.at[i, a] if to_right else agr_l.at[i, a]
        remote(tile, tile, agf_r.at[a], sem, right).wait_recv()

    def ag_step(i, a):
        for to_right in (True, False):
            far = z if to_right else last - z

            @pl.when(jnp.logical_and(jnp.logical_and(i >= 0, i < groups), far >= a))
            def _(to_right=to_right, far=far):
                ag_wait(i, a - 1, to_right)
                if a < slots:
                    @pl.when(far < last)
                    def _():
                        @pl.when(i > 0)
                        def _():
                            ag_forward(i - 1, a, to_right).wait_send()

                        ag_forward(i, a, to_right).start()

    def ag_first(i, slot):
        own_copy(i, slot).start()
        for to_right in (True, False):
            far = z if to_right else last - z

            @pl.when(far < last)
            def _(to_right=to_right):
                ag_own(i, slot, to_right).start()

    def ag_first_done(i, slot):
        own_copy(i, slot).wait()
        for to_right in (True, False):
            far = z if to_right else last - z

            @pl.when(far < last)
            def _(to_right=to_right):
                ag_own(i, slot, to_right).wait_send()

    def partial_norm(i):
        cur = lax.rem(i, PART_RING)
        g = group_rows(i)
        for c in range(0, d_model, chunk):
            cols = slice(c, c + chunk)
            part[cur, :, cols] = (
                dot_nt(dq_all[g, :], wq_ref[cols, :]) + dot_nt(dkv_all[0, g, :], wk_ref[cols, :]) + dot_nt(dkv_all[1, g, :], wv_ref[cols, :])
            )

    def project_out(cur):
        for c in range(0, d_model, chunk):
            cols = slice(c, c + chunk)
            acc = x_in[cur, :, cols].astype(F32)
            for t in range(tp):
                acc += dot_nn(o_in[cur, t], wo_ref[t, :, cols])
            y_buf[cur, :, cols] = acc.astype(BF16)

    def finalize(i):
        slot = lax.rem(i, 2)
        own = pl.ds(pl.multiple_of(z * rows, rows), rows)
        tot[...] = part[lax.rem(i, PART_RING), own, :]

        @pl.when(z > 0)
        def _():
            rs_copy(i, slots - 1, True).wait_recv()
            tot[...] += rs_r[lax.rem(i, RS_RING), slots - 1].astype(F32)

        @pl.when(z < last)
        def _():
            rs_copy(i, slots - 1, False).wait_recv()
            tot[...] += rs_l[lax.rem(i, RS_RING), slots - 1].astype(F32)

        @pl.when(i > 1)
        def _():
            ag_first_done(i - 2, slot)

        for copy in final_inputs(i, slot):
            copy.wait()
        x = xo_in[slot].astype(F32)
        centred = x - jnp.mean(x, axis=-1, keepdims=True)
        inv_std = lax.rsqrt(jnp.mean(centred * centred, axis=-1, keepdims=True) + LN_EPS)
        x_hat = centred * inv_std
        dn = tot[...]
        gg_ref[...] += jnp.sum(dn * x_hat, axis=0, keepdims=True)
        d_hat = dn * gain_ref[...]
        dx = inv_std * (d_hat - jnp.mean(d_hat, axis=-1, keepdims=True) - x_hat * jnp.mean(d_hat * x_hat, axis=-1, keepdims=True))
        gx_buf[slot] = (dyo_in[slot].astype(F32) + dx).astype(BF16)
        ag_first(i, slot)

    def block_of(t):
        return 2 * lax.div(t, 2) + jnp.where(lax.rem(t, 2) == 0, 1 - core, core)

    def job_loads(t, slot):
        cols = pl.ds(pl.multiple_of(block_of(t) * width, width), width)
        return [
            pltpu.make_async_copy(n_hbm.at[:, cols], n_in.at[slot], job_sem.at[slot, 0]),
            pltpu.make_async_copy(dy_hbm.at[:, cols], dy_in.at[slot], job_sem.at[slot, 1]),
        ]

    def away_copy(p):
        ring = lax.rem(p, 2)
        return remote(away, part_in.at[ring], away_send.at[0], away_recv.at[ring], partner)

    def job_block(t, put):
        slot = lax.rem(t, 2)
        n_t = n_in[slot].T
        put(0, hidden, dot_nn(n_t, dq_all[...]))
        put(hidden, hidden, dot_nn(n_t, dkv_all[0]))
        put(2 * hidden, hidden, dot_nn(n_t, dkv_all[1]))
        for k in range(hidden // width):
            put(3 * hidden + k * width, width, dot_nn(o_t[k * width:(k + 1) * width, :], dy_in[slot]))

    def mine_to_own(p, slot):
        return pltpu.make_async_copy(mine.at[slot], ga_hbm.at[2 * p + core], mine_own.at[slot])

    def mine_to_part(p, slot):
        return remote(mine.at[slot], ga_hbm.at[2 * p + core], mine_part.at[slot], ga_recv.at[p], partner)

    def mine_to_chip(p, slot):
        return remote(mine.at[slot], gb_hbm.at[2 * p + core], mine_chip.at[slot], chip_recv.at[p], peer)

    def mine_done(p, slot):
        mine_to_own(p, slot).wait()
        mine_to_part(p, slot).wait_send()
        mine_to_chip(p, slot).wait_send()

    def chip_forward(p):
        b = 2 * p + core
        return remote(gb_hbm.at[b], gb_hbm.at[b], gb_send.at[p], gb_recv.at[p], partner)

    def job(t):
        p = lax.div(t, 2)
        for copy in job_loads(t, lax.rem(t, 2)):
            copy.wait()

        @pl.when(t + 1 < blocks)
        def _():
            for copy in job_loads(t + 1, 1 - lax.rem(t, 2)):
                copy.start()

        @pl.when(lax.rem(t, 2) == 0)
        def _():
            @pl.when(p > 0)
            def _():
                away_copy(p - 1).wait_send()

            def put(at, size, value):
                away[:, at:at + size] = value

            job_block(t, put)
            away_copy(p).start()

        @pl.when(lax.rem(t, 2) == 1)
        def _():
            slot = lax.rem(p, 2)
            away_copy(p).wait_recv()

            @pl.when(p > 1)
            def _():
                mine_done(p - 2, slot)

            def put(at, size, value):
                mine[slot, :, at:at + size] = (value + part_in[slot, :, at:at + size]).astype(BF16)

            job_block(t, put)
            mine_to_chip(p, slot).start()
            mine_to_part(p, slot).start()
            mine_to_own(p, slot).start()

    gg_ref[...] = jnp.zeros_like(gg_ref)
    o_loads = [pltpu.make_async_copy(o_hbm.at[z, :, k * width:(k + 1) * width], n_in.at[k], job_sem.at[k, 0]) for k in range(hidden // width)]
    for copy in o_loads:
        copy.start()
    for copy in inputs(0, 0):
        copy.start()
    for copy in rest_loads + out_loads:
        copy.start()
    me = z * cp + r

    def gain_copy(dt, dc):
        to = {"tp": lax.rem(z + dt, tp), "cp": lax.rem(r + dc, cp)}
        return remote(gain_all.at[me], gain_all.at[me], gs_sem.at[dt * cp + dc], gr_sem.at[me], to)

    def gain_wait(dt, dc):
        sender = lax.rem(z + dt, tp) * cp + lax.rem(r + dc, cp)
        remote(gain_all.at[sender], gain_all.at[sender], gs_sem.at[0], gr_sem.at[sender], right).wait_recv()

    units = tokens // seq * HALVES
    half = hidden // HALVES
    late_units = range(max(0, units - LATE), units)
    late_wait = max(0, late_units[0] // HALVES * seq // span + OUT_LAG - 2)
    sends_late = jnp.logical_or(z == 1, z == last - 1)
    gets_late = jnp.logical_or(z == 0, z == last)

    def late_copy(n, src, dst):
        u = late_units[n]
        place = o_out.at[src, u // HALVES * seq:(u // HALVES + 1) * seq, u % HALVES * half:(u % HALVES + 1) * half]
        return remote(place, place, late_send.at[n], late_recv.at[n], {"tp": dst})

    def late_move(n):
        return late_copy(n, z, jnp.where(z == 1, 0, last))

    for n in range(len(late_units)):
        @pl.when(sends_late)
        def _(n=n):
            late_move(n).start()

    for copy in weight_loads:
        copy.wait()

    def step(i, carry):
        @pl.when(jnp.logical_and(gets_late, i == late_wait))
        def _():
            for n in range(len(late_units)):
                late_copy(n, jnp.where(z == 0, 1, last - 1), z).wait_recv()

        for a in reversed(range(1, slots + 1)):
            ag_step(i - slots - a, a)

        @pl.when(i == OUT_LAG)
        def _():
            for copy in out_loads:
                copy.wait()

        @pl.when(jnp.logical_and(i >= OUT_LAG, i < groups + OUT_LAG))
        def _():
            j = i - OUT_LAG
            at = lax.rem(j, 2)
            for copy in inputs(j, at):
                copy.wait()

            @pl.when(j + 1 < groups)
            def _():
                for copy in inputs(j + 1, 1 - at):
                    copy.start()

            @pl.when(j >= 2)
            def _():
                y_copy(j - 2, at).wait()

            project_out(at)
            y_copy(j, at).start()

        @pl.when(jnp.logical_and(i >= slots, i < groups + slots))
        def _():
            finalize(i - slots)

        @pl.when(i == groups + slots - 1)
        def _():
            gain_all[me] = gg_ref[...]
            for dt, dc in peers:
                gain_copy(dt, dc).start()

        @pl.when(jnp.logical_and(i >= slots - 1, i < groups + slots - 1))
        def _():
            for copy in final_inputs(i - slots + 1, lax.rem(i - slots + 1, 2)):
                copy.start()

        @pl.when(i == EARLY)
        def _():
            for copy in rest_loads:
                copy.wait()

        @pl.when(i < groups)
        def _():
            partial_norm(i)

        @pl.when(i == JOB_LAG - 1)
        def _():
            for k, copy in enumerate(o_loads):
                copy.wait()
                o_t[k * width:(k + 1) * width, :] = n_in[k].T
            for copy in job_loads(0, 0):
                copy.start()

        @pl.when(jnp.logical_and(i >= JOB_LAG, i < JOB_LAG + blocks))
        def _():
            job(i - JOB_LAG)

        for k in reversed(range(slots)):
            rs_send(i - k, k)

        @pl.when(jnp.logical_and(lax.rem(i, 2) == 1, jnp.logical_and(i >= FORWARD_LAG, i < FORWARD_LAG + 2 * pairs)))
        def _():
            p = lax.div(i - FORWARD_LAG, 2)
            mine_to_chip(p, 0).wait_recv()
            chip_forward(p).start()

        return carry

    lax.fori_loop(0, max(groups + 2 * slots, groups + OUT_LAG, blocks + JOB_LAG, 2 * pairs + FORWARD_LAG - 1), step, 0)

    for i in (groups - 2, groups - 1):
        y_copy(i, i % 2).wait()
        ag_first_done(i, i % 2)
    for to_right in (True, False):
        far = z if to_right else last - z
        for s in range(slots):
            @pl.when(jnp.logical_and(far <= s, far < last))
            def _(s=s, to_right=to_right):
                rs_copy(groups - 1, s, to_right).wait_send()
        for a in range(1, slots):
            @pl.when(jnp.logical_and(far >= a, far < last))
            def _(a=a, to_right=to_right):
                ag_forward(groups - 1, a, to_right).wait_send()
    for n in range(len(late_units)):
        @pl.when(sends_late)
        def _(n=n):
            late_move(n).wait_send()

    away_copy(pairs - 1).wait_send()
    for p in range(max(0, pairs - 2), pairs):
        mine_done(p, p % 2)
    for p in range(pairs):
        chip_forward(p).wait_send()
        chip_forward(p).wait_recv()
        mine_to_part(p, 0).wait_recv()
    for dt, dc in peers:
        gain_wait(dt, dc)
        gain_copy(dt, dc).wait_send()
    total = gain_all[0]
    for j in range(1, tp * cp):
        total += gain_all[j]
    gg_ref[...] = total


def backward_norm(dq, dkv, x, dy, o_all, normed, wq, wk, wv, wo_all, gain, rows, seq, tp, cp):
    tokens, hidden = dq.shape
    d_model = x.shape[1]
    span = tp * rows
    groups = tokens // span
    slots = tp - 1
    width = WIDTH
    blocks = d_model // width
    pairs = blocks // 2
    hbm = pl.BlockSpec(memory_space=pl.ANY)
    vmem = pl.BlockSpec(memory_space=pltpu.VMEM)
    dma = pltpu.SemaphoreType.DMA
    bf = lambda *shape: pltpu.VMEM(shape, BF16)
    f32 = lambda *shape: pltpu.VMEM(shape, F32)
    return pl.pallas_call(
        functools.partial(back_kernel, groups, rows, tp, cp, seq),
        in_specs=[hbm] * 10 + [vmem],
        out_specs=[hbm, hbm, hbm, hbm, vmem, hbm],
        input_output_aliases={4: 5},
        out_shape=[
            jax.ShapeDtypeStruct((tokens, d_model), BF16),
            jax.ShapeDtypeStruct((tokens, d_model), BF16),
            jax.ShapeDtypeStruct((blocks, width, 4 * hidden), BF16),
            jax.ShapeDtypeStruct((blocks, width, 4 * hidden), BF16),
            jax.ShapeDtypeStruct((1, d_model), F32),
            jax.ShapeDtypeStruct(o_all.shape, BF16),
        ],
        scratch_shapes=[
            bf(d_model, hidden), bf(d_model, hidden), bf(d_model, hidden), bf(tp, hidden, d_model),
            bf(tokens, hidden), bf(2, tokens, hidden), bf(hidden, tokens),
            f32(PART_RING, span, d_model), bf(RS_RING, slots, rows, d_model), bf(RS_RING, slots, rows, d_model),
            bf(slots, rows, d_model), bf(slots, rows, d_model), f32(rows, d_model), bf(2, rows, d_model),
            bf(2, tp, span, hidden), bf(2, span, d_model), bf(2, rows, d_model), bf(2, rows, d_model), bf(2, span, d_model),
            bf(2, tokens, width), bf(2, tokens, width),
            f32(width, 4 * hidden), f32(2, width, 4 * hidden), bf(2, width, 4 * hidden), f32(tp * cp, 1, d_model),
            dma((8,)), dma((2, 2)), dma((2, 2)), dma((2, 2)), dma((2,)), dma((2,)),
            dma((slots,)), dma((slots,)), dma((RS_RING, slots)), dma((RS_RING, slots)),
            dma((2,)), dma((2,)), dma((slots,)), dma((slots,)), dma((groups, slots)), dma((groups, slots)),
            dma((1,)), dma((2,)), dma((2,)), dma((2,)), dma((2,)), dma((pairs,)), dma((pairs,)), dma((pairs,)), dma((pairs,)),
            dma((tp * cp,)), dma((tp * cp,)), dma((max(LATE, 1),)), dma((max(LATE, 1),)),
        ],
        compiler_params=pltpu.CompilerParams(collective_id=0, has_side_effects=True, vmem_limit_bytes=63 << 20),
        cost_estimate=pl.CostEstimate(flops=22 * tokens * hidden * d_model, bytes_accessed=16 * tokens * d_model, transcendentals=0),
        name="backward_norm",
    )(dq, dkv, x, dy, o_all, normed, wq, wk, wv, wo_all, gain)


def finish_kernel(y_ref, gx_ref, ga_ref, gb_ref, yo_ref, gxo_ref, wq_ref, wk_ref, wv_ref, wo_ref):
    yo_ref[...] = y_ref[...]
    gxo_ref[...] = gx_ref[...]
    width = ga_ref.shape[1]
    hidden = wq_ref.shape[1]
    for k, ref in enumerate((wq_ref, wk_ref, wv_ref)):
        cols = slice(k * hidden, (k + 1) * hidden)
        ref[...] = ga_ref[0, :, cols].astype(F32) + gb_ref[0, :, cols].astype(F32)
    for k in range(hidden // width):
        cols = slice(3 * hidden + k * width, 3 * hidden + (k + 1) * width)
        wo_ref[k * width:(k + 1) * width, :] = ga_ref[0, :, cols].astype(F32) + gb_ref[0, :, cols].astype(F32)


def finish(y, gx, ga, gb):
    tokens, d_model = y.shape
    blocks, width, packed = ga.shape
    hidden = packed // 4
    rows = tokens // blocks
    tile = pl.BlockSpec((rows, d_model), lambda j: (j, 0))
    block = pl.BlockSpec((1, width, packed), lambda j: (j, 0, 0))
    wide = pl.BlockSpec((width, hidden), lambda j: (j, 0))
    return pl.pallas_call(
        finish_kernel,
        grid=(blocks,),
        in_specs=[tile, tile, block, block],
        out_specs=[tile, tile, wide, wide, wide, pl.BlockSpec((hidden, width), lambda j: (0, j))],
        out_shape=[jax.ShapeDtypeStruct((tokens, d_model), BF16)] * 2 + [jax.ShapeDtypeStruct((d_model, hidden), F32)] * 3 + [jax.ShapeDtypeStruct((hidden, d_model), F32)],
        compiler_params=pltpu.CompilerParams(dimension_semantics=("arbitrary",), vmem_limit_bytes=48 << 20),
        cost_estimate=pl.CostEstimate(flops=8 * d_model * hidden, bytes_accessed=8 * tokens * d_model + 32 * d_model * hidden, transcendentals=0),
        name="finish",
    )(y, gx, ga, gb)


def solution(mesh):
    cp_size = mesh.shape["cp"]
    tp_size = mesh.shape["tp"]

    def device_step(x_in, segment_ids, positions, w_query, w_key, w_value, w_out, norm_gain, grad_out):
        batch, seq, d_model = x_in.shape
        tokens = batch * seq
        x = x_in.reshape(tokens, d_model)
        dy = grad_out.reshape(tokens, d_model)

        gain = norm_gain.reshape(1, d_model)
        normed, o_all, dq, dkv, w_all = front(x, dy, w_query, w_key, w_value, w_out, positions, jnp.asarray(angle_table(), BF16), gain, seq, tp_size, cp_size)
        grad_x, y_out, sum_a, sum_b, grad_gain, _ = backward_norm(dq, dkv, x, dy, o_all, normed, w_query, w_key, w_value, w_all, gain, ROWS, seq, tp_size, cp_size)
        grad_gain = grad_gain.reshape(d_model)
        y_out, grad_x, grad_wq, grad_wk, grad_wv, grad_wo = finish(y_out, grad_x, sum_a, sum_b)
        return y_out.reshape(x_in.shape), grad_x.reshape(x_in.shape), grad_gain, grad_wq, grad_wk, grad_wv, grad_wo

    in_specs = (P("dp", "cp", None), P("dp", "cp"), P("dp", "cp"), P(None, "tp"), P(None, "tp"), P(None, "tp"), P("tp", None), P(None), P("dp", "cp", None))
    out_specs = (P("dp", "cp", None), P("dp", "cp", None), P("dp"), P("dp", "tp"), P("dp", "tp"), P("dp", "tp"), P(("dp", "tp"), None))
    return jax.shard_map(device_step, mesh=mesh, in_specs=in_specs, out_specs=out_specs, check_vma=False)
```

```python
import functools
import math

import jax
import jax.numpy as jnp
import numpy as np
from jax import lax
from jax.experimental import pallas as pl
from jax.experimental.pallas import tpu as pltpu
from jax.sharding import PartitionSpec as P

HEAD_DIM = 128
ROPE_THETA = 8000000.0
LN_EPS = 1e-5
NEG_BIG = -1e30
SCALE = HEAD_DIM ** -0.5
EXP2_SCALE = SCALE * math.log2(math.e)
F32 = jnp.float32
BF16 = jnp.bfloat16
NT = (((1,), (1,)), ((), ()))


def dot_nn(a, b):
    return jnp.dot(a, b, preferred_element_type=F32)


def dot_nt(a, b):
    return lax.dot_general(a, b, NT, preferred_element_type=F32)


def dot_tn(a, b):
    return lax.dot_general(a, b, (((0,), (0,)), ((), ())), preferred_element_type=F32)


def swap_pairs(t, sign):
    lane = lax.broadcasted_iota(jnp.int32, t.shape, 1)
    even = (lane % 2) == 0
    up = pltpu.roll(t, HEAD_DIM - 1, 1)
    down = pltpu.roll(t, 1, 1)
    return jnp.where(even, -up, down) if sign > 0 else jnp.where(even, up, -down)


def rope(t, cos_t, sin_t, sign):
    return t * cos_t + swap_pairs(t, sign) * sin_t


def angle_table():
    inv_freq = ROPE_THETA ** (-np.arange(0, HEAD_DIM, 2, dtype=np.float32) / np.float32(HEAD_DIM))
    freq = np.repeat(inv_freq.astype(np.float64), 2)[None, :]
    low = np.arange(POS_LOW)[:, None] * freq
    high = POS_LOW * np.arange(HEAD_DIM - POS_LOW)[:, None] * freq
    table = np.zeros((HEAD_DIM, 12 * HEAD_DIM), np.float32)
    for k, (first, value) in enumerate(((0, np.cos(low)), (0, np.sin(low)), (POS_LOW, np.cos(high)), (POS_LOW, np.sin(high)))):
        rest = value.astype(np.float32)
        for p in range(3):
            piece = rest.astype(BF16).astype(np.float32)
            at = (3 * k + p) * HEAD_DIM
            table[first:first + value.shape[0], at:at + HEAD_DIM] = piece
            rest = rest - piece
    return table


def put_rope(dst, raw, cos_t, sin_t):
    for h in range(raw.shape[1] // HEAD_DIM):
        cols = slice(h * HEAD_DIM, (h + 1) * HEAD_DIM)
        dst[:, cols] = rope(raw[:, cols], cos_t, sin_t, 1.0).astype(BF16)


MESH = pl.DeviceIdType.MESH
SUB = 384
ROWS = 32
WIDTH = 256
PARTS = 2
HALVES = 2
RELAY_LAG = 1
LATE = 3
SUM_LAG = 4
CHIP_BUFS = 4
OWN_RING = 6
Q_RING = 3
AHEAD = 2
POS_LOW = 64
W_TWIN = 1
W_PARTNER = 3
W_CHIP = 7


def front_kernel(batch, seq, tp, cp, x_hbm, dy_hbm, wq_hbm, wk_hbm, wv_hbm, wo_hbm, pos_ref, table_ref, gain_ref,
                 n_hbm, o_all, dq_hbm, dkv_hbm, w_all,
                 big, wo_ref, cos_ref, sin_ref, q_ring, do_ring, x_in, dy_in, n_buf, kv_own, kvr, s_scr, dp_scr, m_scr, l_scr, d_scr, ot_scr, dqt_scr,
                 o_buf, dq_buf, g_own, g_part, g_chip, g_far, xin, part_in,
                 w_sem, wl_sem, wz_send, wz_recv, wx_send, wx_recv,
                 x_sem, dy_sem, n_sem, kvs_part, kvs_chip, kvs_far, kv_recv, o_local, o_send, o_recv, relay_send, dq_sem,
                 far_send, part_send, chip_send, x_recv, part_recv, dkv_sem):
    z = lax.axis_index("tp")
    r = lax.axis_index("cp")
    dp = lax.axis_index("dp")
    core = lax.rem(r, 2)
    chip = lax.div(r, 2)
    d_model = x_hbm.shape[1]
    hidden = wq_hbm.shape[1]
    heads = hidden // HEAD_DIM
    first_chip, second_chip = chip == 0, chip == 1
    first_core, second_core = core == 0, core == 1
    partner = {"cp": r + 1 - 2 * core}
    peer = {"cp": r + 2 - 4 * chip}
    twin = {"dp": 1 - dp}

    tile = x_in.shape[1]
    per_row = seq // tile

    def row(b):
        return pl.ds(pl.multiple_of(b * seq, seq), seq)

    def tile_rows(b, k):
        return pl.ds(pl.multiple_of(b * seq + k * tile, tile), tile)

    def x_load(b, k):
        return pltpu.make_async_copy(x_hbm.at[tile_rows(b, k), :], x_in.at[k], x_sem.at[k])

    def dy_load(b, k):
        return pltpu.make_async_copy(dy_hbm.at[tile_rows(b, k), :], dy_in.at[k], dy_sem.at[k])

    def n_store(b, k):
        return pltpu.make_async_copy(n_buf.at[k], n_hbm.at[tile_rows(b, k), :], n_sem.at[k])

    weight_loads = [pltpu.make_async_copy(src, dst, w_sem.at[k]) for k, (src, dst) in enumerate(((wk_hbm, big.at[0]), (wv_hbm, big.at[1]), (wq_hbm, big.at[2]), (wo_hbm, wo_ref)))]
    x_load(0, 0).start()
    for copy in weight_loads[:2]:
        copy.start()
    for k in range(1, per_row):
        x_load(0, k).start()
    for copy in weight_loads[2:]:
        copy.start()
    for k in range(per_row):
        dy_load(0, k).start()

    units = batch * HALVES
    half = hidden // HALVES

    def where(u):
        return lax.div(u, HALVES), lax.rem(u, HALVES)

    def half_cols(g):
        return pl.ds(pl.multiple_of(g * half, half), half)

    barrier = pltpu.get_barrier_semaphore()
    for dev in [partner, peer, twin] + [{"tp": lax.rem(z + dt, tp)} for dt in range(1, tp)]:
        pl.semaphore_signal(barrier, inc=1, device_id=dev, device_id_type=MESH)
    pl.semaphore_wait(barrier, tp + 2)

    def remote(src, dst, ssem, rsem, dev):
        return pltpu.make_async_remote_copy(src_ref=src, dst_ref=dst, send_sem=ssem, recv_sem=rsem, device_id=dev, device_id_type=MESH)

    share = hidden // 8

    def share_rows(y, c, g):
        return pl.ds(pl.multiple_of((4 * y + 2 * c + g) * share, share), share)

    mine, twins = share_rows(chip, core, dp), share_rows(chip, core, 1 - dp)
    peers, peer_twins = share_rows(1 - chip, core, dp), share_rows(1 - chip, core, 1 - dp)

    def wz_copy(d):
        return remote(wo_hbm.at[mine, :], w_all.at[z, mine, :], wz_send.at[d], wz_recv.at[z], {"tp": lax.rem(z + d, tp)})

    def wz_wait(d):
        src = lax.rem(z + d, tp)
        remote(wo_hbm.at[mine, :], w_all.at[src, mine, :], wz_send.at[d], wz_recv.at[src], partner).wait_recv()

    def w_copy(k, d, rows, dev):
        place = w_all.at[lax.rem(z + d, tp), rows, :]
        return remote(place, place, wx_send.at[k, d], wx_recv.at[k, d], dev)

    def w_move(k, d):
        rows, dev = ((mine, twin), (mine, partner), (twins, partner), (mine, peer), (twins, peer), (peers, partner), (peer_twins, partner))[k]
        return w_copy(k, d, rows, dev)

    w_steps = range(1, tp)

    for d in range(1, tp):
        wz_copy(d).start()

    def kv_to_partner(u):
        return remote(kv_own.at[u], kvr.at[0, u], kvs_part.at[u], kv_recv.at[0, u], partner)

    def kv_to_chip(u):
        return remote(kv_own.at[u], kvr.at[1, u], kvs_chip.at[u], kv_recv.at[1, u], peer)

    def kv_forward(u):
        return remote(kvr.at[1, u], kvr.at[2, u], kvs_far.at[u], kv_recv.at[2, u], partner)

    w_local = pltpu.make_async_copy(wo_ref, w_all.at[z], wl_sem.at[0])
    for copy in weight_loads[:2]:
        copy.wait()

    def angles(b, k):
        rows = tile_rows(b, k)
        pos = jnp.broadcast_to(pos_ref[pl.ds(b, 1), k * tile:(k + 1) * tile], (HEAD_DIM, tile)).T
        lane = lax.broadcasted_iota(jnp.int32, (tile, HEAD_DIM), 1)
        low = lane < POS_LOW
        pick = jnp.where(low, lax.rem(pos, POS_LOW), POS_LOW + lax.div(pos, POS_LOW)) == lane
        found = dot_nn(jnp.where(pick, 1.0, 0.0).astype(BF16), table_ref[...])

        def part(k):
            at = 3 * k * HEAD_DIM
            return found[:, at:at + HEAD_DIM] + found[:, at + HEAD_DIM:at + 2 * HEAD_DIM] + found[:, at + 2 * HEAD_DIM:at + 3 * HEAD_DIM]

        cos_b, sin_b, cos_a, sin_a = part(0), part(1), part(2), part(3)
        cos_ref[rows, :] = cos_a * cos_b - sin_a * sin_b
        sin_ref[rows, :] = sin_a * cos_b + cos_a * sin_b

    def project_row(b):
        ring = lax.rem(b, Q_RING)
        for k in range(per_row):
            rows = tile_rows(b, k)
            inside = slice(k * tile, (k + 1) * tile)
            x_load(b, k).wait()

            @pl.when(b > 0)
            def _(k=k):
                n_store(b - 1, k).wait()

            angles(b, k)
            x = x_in[k].astype(F32)
            centred = x - jnp.mean(x, axis=-1, keepdims=True)
            inv_std = lax.rsqrt(jnp.mean(centred * centred, axis=-1, keepdims=True) + LN_EPS)
            n_buf[k] = ((centred * inv_std) * gain_ref[...]).astype(BF16)
            n_store(b, k).start()

            @pl.when(b + 1 < batch)
            def _(k=k):
                x_load(b + 1, k).start()

            for g in range(HALVES):
                u = b * HALVES + g
                cols = slice(g * half, (g + 1) * half)
                put_rope(kv_own.at[u, 0, inside, :], dot_nn(n_buf[k], big[0, :, cols]), cos_ref[rows, :], sin_ref[rows, :])
                kv_own[u, 1, inside, :] = dot_nn(n_buf[k], big[1, :, cols]).astype(BF16)

        for g in range(HALVES):
            u = b * HALVES + g

            @pl.when(first_chip)
            def _(u=u):
                kv_to_chip(u).start()

            @pl.when(first_core)
            def _(u=u):
                kv_to_partner(u).start()

        @pl.when(b == 0)
        def _():
            for copy in weight_loads[2:]:
                copy.wait()
            w_local.start()

        for k in range(per_row):
            rows = tile_rows(b, k)
            inside = slice(k * tile, (k + 1) * tile)
            dy_load(b, k).wait()
            put_rope(q_ring.at[ring, inside, :], dot_nn(n_buf[k], big[2]), cos_ref[rows, :], sin_ref[rows, :])
            do_ring[ring, inside, :] = dot_nt(dy_in[k], wo_ref[...]).astype(BF16)

            @pl.when(b + 1 < batch)
            def _(k=k):
                dy_load(b + 1, k).start()

    def o_place(src, u):
        b, g = where(u)
        return o_all.at[src, row(b), half_cols(g)]

    def o_local_copy(b):
        return pltpu.make_async_copy(o_buf.at[b], o_place(z, b), o_local.at[b])

    def o_copy(b, k, step):
        return remote(o_buf.at[b], o_place(z, b), o_send.at[k, b], o_recv.at[z, b], {"tp": jnp.clip(z + step, 0, tp - 1)})

    hops = [(k, step, jnp.logical_and(z + step >= 0, z + step < tp)) for k, step in enumerate((1, -1))]

    def far_from_end(step):
        return jnp.logical_and(z + step != 0, z + step != tp - 1)

    def o_start(b):
        o_local_copy(b).start()
        for k, step, ok in hops:
            @pl.when(jnp.logical_and(ok, jnp.logical_or(b < units - LATE, far_from_end(step))))
            def _(k=k, step=step):
                o_copy(b, k, step).start()

    def o_arrived(src, b):
        remote(o_place(src, b), o_place(src, b), relay_send.at[0, 0, b], o_recv.at[src, b], partner).wait_recv()

    def relay_copy(b, age, step):
        src = jnp.clip(z - age * step, 0, tp - 1)
        return remote(o_place(src, b), o_place(src, b), relay_send.at[age - 1, (1 - step) // 2, b], o_recv.at[src, b], {"tp": jnp.clip(z + step, 0, tp - 1)})

    def relays(age, step):
        far = z if step > 0 else tp - 1 - z
        return jnp.logical_and(far >= age, far < tp - 1)

    def relay(b, age):
        for step in (1, -1):
            @pl.when(relays(age, step))
            def _(step=step):
                o_arrived(jnp.clip(z - age * step, 0, tp - 1), b)
                relay_copy(b, age, step).start()

    def far_copy(b, par):
        return remote(g_far.at[par], xin.at[b], far_send.at[par], x_recv.at[b], partner)

    def part_copy(b, par):
        return remote(g_part.at[par], part_in.at[b], part_send.at[par], part_recv.at[b], partner)

    def chip_copy(b):
        par = lax.rem(b, CHIP_BUFS)
        return remote(g_chip.at[par], xin.at[b], chip_send.at[par], x_recv.at[b], peer)

    def chip_sum(b):
        @pl.when(second_chip)
        def _():
            par = lax.rem(b, CHIP_BUFS)
            far_copy(b, 0).wait_recv()
            g_chip[par] = (g_chip[par].astype(F32) + xin[b].astype(F32)).astype(BF16)
            chip_copy(b).start()

    def dkv_store(u, which):
        b, g = where(u)
        return pltpu.make_async_copy(g_own.at[lax.rem(u, OWN_RING), which], dkv_hbm.at[which, row(b), half_cols(g)], dkv_sem.at[u, which])

    def key_grads(u):
        @pl.when(first_core)
        def _():
            part_copy(u, 0).wait_recv()

        @pl.when(first_chip)
        def _():
            chip_copy(u).wait_recv()

        b, g = where(u)
        rows = row(b)
        for which in range(2):
            for h in range(half // HEAD_DIM):
                cols = slice(h * HEAD_DIM, (h + 1) * HEAD_DIM)
                own = g_own.at[lax.rem(u, OWN_RING), which, :, cols]
                acc = own[...].astype(F32)
                acc = acc + jnp.where(first_core, part_in[u, which, :, cols].astype(F32), 0.0)
                acc = (acc + jnp.where(first_chip, xin[u, which, :, cols].astype(F32), 0.0)).astype(BF16)
                if which == 0:
                    acc = rope(acc.astype(F32), cos_ref[rows, :], sin_ref[rows, :], -1.0).astype(BF16)
                own[...] = acc
            dkv_store(u, which).start()

    def dq_store(b, par):
        return pltpu.make_async_copy(dq_buf.at[par], dq_hbm.at[row(where(b)[0]), half_cols(where(b)[1])], dq_sem.at[par])

    subs = range(0, seq, SUB)

    def attend_unit(i, par):
        b, g = where(i)
        rows = row(b)
        ring = lax.rem(b, Q_RING)
        start = r * seq + lax.broadcasted_iota(jnp.int32, (1, seq), 1) - pos_ref[pl.ds(b, 1), :]
        chip_par = lax.rem(i, CHIP_BUFS)
        keys_of = [kv_own.at[i]] + [kvr.at[s, i] for s in range(3)]
        places = [g_part.at[par], g_chip.at[chip_par], g_far.at[par]]

        def grad(slot, which, cols):
            return places[slot - 1].at[which, :, cols] if slot else g_own.at[lax.rem(i, OWN_RING), which, :, cols]

        live = [None, second_core, second_chip, second_chip]
        piece = [r, r + 1 - 2 * core, r + 2 - 4 * chip, r + 3 - 2 * core - 4 * chip]

        def each(body):
            body(0)
            for slot in (1, 2, 3):
                pl.when(live[slot])(functools.partial(body, slot))

        def one_head(h, carry):
            cols = pl.ds(pl.multiple_of(h * HEAD_DIM, HEAD_DIM), HEAD_DIM)
            full = pl.ds(pl.multiple_of(g * half + h * HEAD_DIM, HEAD_DIM), HEAD_DIM)
            q = q_ring[ring, :, full]
            do = do_ring[ring, :, full]
            m_scr[...] = jnp.full(m_scr.shape, NEG_BIG, F32)
            l_scr[...] = jnp.zeros_like(l_scr)
            d_scr[...] = jnp.zeros_like(d_scr)
            ot_scr[...] = jnp.zeros_like(ot_scr)
            dqt_scr[...] = jnp.zeros_like(dqt_scr)

            def scores(slot):
                base = piece[slot] * seq
                top = None
                for s in subs:
                    raw = dot_nt(keys_of[slot][0, s:s + SUB, cols], q)
                    local = lax.broadcasted_iota(jnp.int32, raw.shape, 0) + s
                    allowed = (local + base) >= start
                    if slot == 0:
                        allowed = jnp.logical_and(allowed, local <= lax.broadcasted_iota(jnp.int32, raw.shape, 1))
                    raw = jnp.where(allowed, raw, NEG_BIG)
                    s_scr[slot, s:s + SUB, :] = raw
                    high = jnp.max(raw, axis=0, keepdims=True)
                    top = high if top is None else jnp.maximum(top, high)
                m_scr[...] = jnp.maximum(m_scr[...], top)

            def exps(slot):
                top = m_scr[...]
                total = None
                for s in subs:
                    e = jnp.exp2((s_scr[slot, s:s + SUB, :] - top) * EXP2_SCALE)
                    s_scr[slot, s:s + SUB, :] = e
                    part = jnp.sum(e, axis=0, keepdims=True)
                    total = part if total is None else total + part
                l_scr[...] += total

            def values(slot):
                inv = l_scr[...]
                total, out = None, None
                for s in subs:
                    v = keys_of[slot][1, s:s + SUB, cols]
                    prob = s_scr[slot, s:s + SUB, :] * inv
                    low = prob.astype(BF16)
                    dp = dot_nt(v, do)
                    dp_scr[slot, s:s + SUB, :] = dp
                    part = jnp.sum(prob * dp, axis=0, keepdims=True)
                    total = part if total is None else total + part
                    grad(slot, 1, cols)[s:s + SUB, :] = dot_nn(low, do).astype(BF16)
                    piece_out = dot_nn(v.T, low)
                    out = piece_out if out is None else out + piece_out
                d_scr[...] += total
                ot_scr[...] += out

            def keys(slot):
                inv, mean = l_scr[...], d_scr[...]
                out = None
                for s in subs:
                    k = keys_of[slot][0, s:s + SUB, cols]
                    ds = ((s_scr[slot, s:s + SUB, :] * inv) * (dp_scr[slot, s:s + SUB, :] - mean)).astype(BF16)
                    grad(slot, 0, cols)[s:s + SUB, :] = (dot_nn(ds, q) * SCALE).astype(BF16)
                    piece_out = dot_nn(k.T, ds)
                    out = piece_out if out is None else out + piece_out
                dqt_scr[...] += out

            each(scores)
            each(exps)
            l_scr[...] = 1.0 / l_scr[...]
            each(values)
            each(keys)
            o_buf[i, :, cols] = ot_scr[...].T.astype(BF16)
            dq_buf[par, :, cols] = rope(dqt_scr[...].T * SCALE, cos_ref[rows, :], sin_ref[rows, :], -1.0).astype(BF16)
            return carry

        lax.fori_loop(0, heads // HALVES, one_head, 0)

    def step(i, carry):
        par = lax.rem(i, 2)
        @pl.when(jnp.logical_and(lax.rem(i, HALVES) == 0, lax.div(i, HALVES) + AHEAD < batch))
        def _():
            project_row(lax.div(i, HALVES) + AHEAD)

        @pl.when(i >= OWN_RING)
        def _():
            for which in range(2):
                dkv_store(i - OWN_RING, which).wait()

        @pl.when(second_chip)
        def _():
            kv_to_chip(i).wait_recv()
            kv_forward(i).start()

        @pl.when(second_core)
        def _():
            kv_to_partner(i).wait_recv()

        @pl.when(second_chip)
        def _():
            kv_forward(i).wait_recv()

        @pl.when(i >= 2)
        def _():
            dq_store(i - 2, par).wait()

            @pl.when(second_core)
            def _():
                part_copy(i - 2, par).wait_send()

            @pl.when(second_chip)
            def _():
                far_copy(i - 2, par).wait_send()

        @pl.when(jnp.logical_and(second_chip, i >= CHIP_BUFS))
        def _():
            chip_copy(i - CHIP_BUFS).wait_send()

        attend_unit(i, par)
        o_start(i)
        dq_store(i, par).start()

        @pl.when(second_chip)
        def _():
            far_copy(i, par).start()

        @pl.when(second_core)
        def _():
            part_copy(i, par).start()

        @pl.when(i >= 1)
        def _():
            chip_sum(i - 1)

        for age in range(1, tp - 1):
            @pl.when(i >= age * RELAY_LAG)
            def _(age=age):
                relay(i - age * RELAY_LAG, age)

        @pl.when(i >= SUM_LAG)
        def _():
            key_grads(i - SUM_LAG)

        @pl.when(i == min(W_TWIN, units - 1))
        def _():
            for d in w_steps:
                wz_wait(d)
                w_move(0, d).start()
                w_move(1, d).start()

                @pl.when(second_chip)
                def _(d=d):
                    w_move(3, d).start()

        @pl.when(i == min(W_PARTNER, units - 1))
        def _():
            for d in w_steps:
                w_move(0, d).wait_recv()
                w_move(2, d).start()

                @pl.when(second_chip)
                def _(d=d):
                    w_move(4, d).start()

        @pl.when(jnp.logical_and(first_chip, i == min(W_CHIP, units - 1)))
        def _():
            for k in (3, 4):
                for d in w_steps:
                    w_move(k, d).start()

        return carry

    for b in range(min(AHEAD, batch)):
        project_row(b)
    lax.fori_loop(0, units, step, 0)
    chip_sum(units - 1)

    end = units + max(SUM_LAG, (tp - 2) * RELAY_LAG)
    for i in range(units, end):
        for age in range(1, tp - 1):
            if 0 <= i - age * RELAY_LAG < units:
                relay(i - age * RELAY_LAG, age)
        if 0 <= i - SUM_LAG < units:
            key_grads(i - SUM_LAG)
        if i == end - 1:
            for k in (3, 4):
                for d in w_steps:
                    w_move(k, d).wait_recv()
                    w_move(k + 2, d).start()

    w_local.wait()
    for d in w_steps:
        wz_copy(d).wait_send()
        for k in range(7):
            w_move(k, d).wait_send()
            if k in (1, 2, 5, 6):
                w_move(k, d).wait_recv()

    for k in range(per_row):
        n_store(batch - 1, k).wait()
    for u in range(max(0, units - OWN_RING), units):
        for which in range(2):
            dkv_store(u, which).wait()

    def drain(b, carry):
        @pl.when(first_chip)
        def _():
            kv_to_chip(b).wait_send()

        @pl.when(first_core)
        def _():
            kv_to_partner(b).wait_send()

        @pl.when(second_chip)
        def _():
            kv_forward(b).wait_send()

        o_local_copy(b).wait()
        for k, step_, ok in hops:
            @pl.when(jnp.logical_and(ok, jnp.logical_or(b < units - LATE, far_from_end(step_))))
            def _(k=k, step_=step_):
                o_copy(b, k, step_).wait_send()

        for age in range(1, tp - 1):
            for step_ in (1, -1):
                @pl.when(relays(age, step_))
                def _(age=age, step_=step_):
                    relay_copy(b, age, step_).wait_send()

        for src in range(tp):
            way = jnp.where(z > src, 1, -1)
            gone = jnp.abs(z - src)
            far = jnp.where(way > 0, z, tp - 1 - z)
            taken = jnp.logical_and(gone <= tp - 2, far < tp - 1)
            late = jnp.logical_and(b >= units - LATE, jnp.logical_and(gone == 1, far == tp - 1))

            @pl.when(jnp.logical_and(z != src, jnp.logical_not(jnp.logical_or(taken, late))))
            def _(src=src):
                o_arrived(src, b)

        return carry

    lax.fori_loop(0, units, drain, 0)

    for b in range(max(0, units - 2), units):
        dq_store(b, b % 2).wait()

        @pl.when(second_core)
        def _(b=b):
            part_copy(b, b % 2).wait_send()

        @pl.when(second_chip)
        def _(b=b):
            far_copy(b, b % 2).wait_send()

    for b in range(max(0, units - CHIP_BUFS), units):
        @pl.when(second_chip)
        def _(b=b):
            chip_copy(b).wait_send()


def front(x, dy, wq, wk, wv, wo, pos, table, gain, seq, tp, cp):
    tokens, d_model = x.shape
    hidden = wq.shape[1]
    batch = tokens // seq
    units = batch * HALVES
    half = hidden // HALVES
    tile = seq // 2
    hbm = pl.BlockSpec(memory_space=pl.ANY)
    vmem = pl.BlockSpec(memory_space=pltpu.VMEM)
    dma = pltpu.SemaphoreType.DMA
    bf = lambda *shape: pltpu.VMEM(shape, BF16)
    f32 = lambda *shape: pltpu.VMEM(shape, F32)
    return pl.pallas_call(
        functools.partial(front_kernel, batch, seq, tp, cp),
        in_specs=[hbm] * 6 + [vmem] * 3,
        out_specs=[hbm] * 5,
        out_shape=[
            jax.ShapeDtypeStruct((tokens, d_model), BF16),
            jax.ShapeDtypeStruct((tp, tokens, hidden), BF16),
            jax.ShapeDtypeStruct((tokens, hidden), BF16),
            jax.ShapeDtypeStruct((2, tokens, hidden), BF16),
            jax.ShapeDtypeStruct((tp, hidden, d_model), BF16),
        ],
        scratch_shapes=[
            bf(3, d_model, hidden), bf(hidden, d_model), f32(tokens, HEAD_DIM), f32(tokens, HEAD_DIM),
            bf(Q_RING, seq, hidden), bf(Q_RING, seq, hidden), bf(2, tile, d_model), bf(2, tile, d_model), bf(2, tile, d_model),
            bf(units, 2, seq, half), bf(3, units, 2, seq, half),
            f32(4, seq, seq), f32(4, seq, seq), f32(1, seq), f32(1, seq), f32(1, seq), f32(HEAD_DIM, seq), f32(HEAD_DIM, seq),
            bf(units, seq, half), bf(2, seq, half),
            bf(OWN_RING, 2, seq, half), bf(2, 2, seq, half), bf(CHIP_BUFS, 2, seq, half), bf(2, 2, seq, half),
            bf(units, 2, seq, half), bf(units, 2, seq, half),
            dma((4,)), dma((1,)), dma((tp,)), dma((tp,)), dma((7, tp)), dma((7, tp)),
            dma((2,)), dma((2,)), dma((2,)), dma((units,)), dma((units,)), dma((units,)), dma((3, units)),
            dma((units,)), dma((2, units)), dma((tp, units)), dma((2, 2, units)), dma((2,)),
            dma((2,)), dma((2,)), dma((CHIP_BUFS,)), dma((units,)), dma((units,)), dma((units, 2)),
        ],
        compiler_params=pltpu.CompilerParams(collective_id=1, has_side_effects=True, vmem_limit_bytes=63 << 20),
        cost_estimate=pl.CostEstimate(flops=60 * tokens * seq * hidden, bytes_accessed=16 * tokens * d_model, transcendentals=4 * tokens * seq * (hidden // HEAD_DIM)),
        name="front",
    )(x, dy, wq, wk, wv, wo, pos, table, gain)


PART_RING = 4
RS_RING = 5
FORWARD_LAG = 11
JOB_LAG = 5
OUT_LAG = 4
EARLY = 4


def back_kernel(groups, rows, tp, cp, seq, dq_hbm, dkv_hbm, x_hbm, dy_hbm, o_old, n_hbm, wq_hbm, wk_hbm, wv_hbm, wo_hbm, gain_ref,
                gx_hbm, y_hbm, ga_hbm, gb_hbm, gg_ref, o_out,
                wq_ref, wk_ref, wv_ref, wo_ref, dq_all, dkv_all, o_t, part, rs_r, rs_l, send_r, send_l, tot, gx_buf,
                o_in, x_in, xo_in, dyo_in, y_buf, n_in, dy_in, away, part_in, mine, gain_all,
                w_sem, in_sem, fin_sem, job_sem, y_sem, own_sem, rss_r, rss_l, rsr_r, rsr_l, ag0_r, ag0_l, agf_r, agf_l, agr_r, agr_l,
                away_send, away_recv, mine_own, mine_part, mine_chip, ga_recv, chip_recv, gb_send, gb_recv, gs_sem, gr_sem, late_send, late_recv):
    o_hbm = o_out
    z = lax.axis_index("tp")
    r = lax.axis_index("cp")
    core = lax.rem(r, 2)
    chip = lax.div(r, 2)
    last = tp - 1
    slots = tp - 1
    span = tp * rows
    tokens, d_model = x_hbm.shape
    hidden = dq_hbm.shape[1]
    chunk = min(512, d_model)
    blocks = ga_hbm.shape[0]
    width = ga_hbm.shape[1]
    pairs = blocks // 2
    partner = {"cp": r + 1 - 2 * core}
    peer = {"cp": r + 2 - 4 * chip}

    head = min(EARLY, groups) * span
    weight_loads = [pltpu.make_async_copy(src, dst, w_sem.at[k]) for k, (src, dst) in enumerate((
        (dq_hbm.at[:head, :], dq_all.at[:head, :]), (dkv_hbm.at[:, :head, :], dkv_all.at[:, :head, :]), (wq_hbm, wq_ref), (wk_hbm, wk_ref), (wv_hbm, wv_ref)))]
    rest_loads = [] if head == tokens else [
        pltpu.make_async_copy(dq_hbm.at[head:, :], dq_all.at[head:, :], w_sem.at[6]),
        pltpu.make_async_copy(dkv_hbm.at[:, head:, :], dkv_all.at[:, head:, :], w_sem.at[7]),
    ]
    out_loads = [pltpu.make_async_copy(wo_hbm, wo_ref, w_sem.at[5])]
    for copy in weight_loads:
        copy.start()

    barrier = pltpu.get_barrier_semaphore()
    peers = [(dt, dc) for dt in range(tp) for dc in range(cp) if dt or dc]
    for dt, dc in peers:
        pl.semaphore_signal(barrier, inc=1, device_id={"tp": lax.rem(z + dt, tp), "cp": lax.rem(r + dc, cp)}, device_id_type=MESH)
    pl.semaphore_wait(barrier, len(peers))

    def remote(src, dst, ssem, rsem, dev):
        return pltpu.make_async_remote_copy(src_ref=src, dst_ref=dst, send_sem=ssem, recv_sem=rsem, device_id=dev, device_id_type=MESH)

    right = {"tp": jnp.where(z < last, z + 1, z)}
    left = {"tp": jnp.where(z > 0, z - 1, z)}

    def group_rows(i):
        return pl.ds(pl.multiple_of(i * span, span), span)

    def tile_rows(i, owner):
        return pl.ds(pl.multiple_of(i * span + owner * rows, rows), rows)

    def inputs(i, slot):
        g = group_rows(i)
        return [
            pltpu.make_async_copy(o_hbm.at[:, g, :], o_in.at[slot], in_sem.at[slot, 0]),
            pltpu.make_async_copy(x_hbm.at[g, :], x_in.at[slot], in_sem.at[slot, 1]),
        ]

    def final_inputs(i, slot):
        g = tile_rows(i, z)
        return [
            pltpu.make_async_copy(x_hbm.at[g, :], xo_in.at[slot], fin_sem.at[slot, 0]),
            pltpu.make_async_copy(dy_hbm.at[g, :], dyo_in.at[slot], fin_sem.at[slot, 1]),
        ]

    def y_copy(i, slot):
        return pltpu.make_async_copy(y_buf.at[slot], y_hbm.at[group_rows(i), :], y_sem.at[slot])

    def rs_copy(i, s, to_right):
        ring = lax.rem(i, RS_RING)
        if to_right:
            return remote(send_r.at[s], rs_r.at[ring, s], rss_r.at[s], rsr_r.at[ring, s], right)
        return remote(send_l.at[s], rs_l.at[ring, s], rss_l.at[s], rsr_l.at[ring, s], left)

    def rs_send(i, s):
        for to_right in (True, False):
            far = z if to_right else last - z
            owner = (z + slots - s) if to_right else (z - slots + s)
            buf, held = (send_r, rs_r) if to_right else (send_l, rs_l)

            @pl.when(jnp.logical_and(jnp.logical_and(i >= 0, i < groups), jnp.logical_and(far <= s, far < last)))
            def _(to_right=to_right, far=far, owner=owner, buf=buf, held=held):
                @pl.when(i > 0)
                def _():
                    rs_copy(i - 1, s, to_right).wait_send()

                cur = lax.rem(i, PART_RING)
                own = pl.ds(pl.multiple_of(owner * rows, rows), rows)
                if s == 0:
                    buf[s] = part[cur, own, :].astype(BF16)
                else:
                    @pl.when(far == 0)
                    def _():
                        buf[s] = part[cur, own, :].astype(BF16)

                    @pl.when(far > 0)
                    def _():
                        rs_copy(i, s - 1, to_right).wait_recv()
                        buf[s] = (part[cur, own, :] + held[lax.rem(i, RS_RING), s - 1].astype(F32)).astype(BF16)

                rs_copy(i, s, to_right).start()

    def ag_own(i, slot, to_right):
        src = gx_buf.at[slot]
        dst = gx_hbm.at[tile_rows(i, z), :]
        if to_right:
            return remote(src, dst, ag0_r.at[slot], agr_r.at[i, 0], right)
        return remote(src, dst, ag0_l.at[slot], agr_l.at[i, 0], left)

    def own_copy(i, slot):
        return pltpu.make_async_copy(gx_buf.at[slot], gx_hbm.at[tile_rows(i, z), :], own_sem.at[slot])

    def ag_forward(i, a, to_right):
        owner = z - a if to_right else z + a
        tile = gx_hbm.at[tile_rows(i, owner), :]
        if to_right:
            return remote(tile, tile, agf_r.at[a], agr_r.at[i, a], right)
        return remote(tile, tile, agf_l.at[a], agr_l.at[i, a], left)

    def ag_wait(i, a, to_right):
        tile = gx_hbm.at[tile_rows(i, 0), :]
        sem = agr_r.at[i, a] if to_right else agr_l.at[i, a]
        remote(tile, tile, agf_r.at[a], sem, right).wait_recv()

    def ag_step(i, a):
        for to_right in (True, False):
            far = z if to_right else last - z

            @pl.when(jnp.logical_and(jnp.logical_and(i >= 0, i < groups), far >= a))
            def _(to_right=to_right, far=far):
                ag_wait(i, a - 1, to_right)
                if a < slots:
                    @pl.when(far < last)
                    def _():
                        @pl.when(i > 0)
                        def _():
                            ag_forward(i - 1, a, to_right).wait_send()

                        ag_forward(i, a, to_right).start()

    def ag_first(i, slot):
        own_copy(i, slot).start()
        for to_right in (True, False):
            far = z if to_right else last - z

            @pl.when(far < last)
            def _(to_right=to_right):
                ag_own(i, slot, to_right).start()

    def ag_first_done(i, slot):
        own_copy(i, slot).wait()
        for to_right in (True, False):
            far = z if to_right else last - z

            @pl.when(far < last)
            def _(to_right=to_right):
                ag_own(i, slot, to_right).wait_send()

    def partial_norm(i):
        cur = lax.rem(i, PART_RING)
        g = group_rows(i)
        for c in range(0, d_model, chunk):
            cols = slice(c, c + chunk)
            part[cur, :, cols] = (
                dot_nt(dq_all[g, :], wq_ref[cols, :]) + dot_nt(dkv_all[0, g, :], wk_ref[cols, :]) + dot_nt(dkv_all[1, g, :], wv_ref[cols, :])
            )

    def project_out(cur):
        for c in range(0, d_model, chunk):
            cols = slice(c, c + chunk)
            acc = x_in[cur, :, cols].astype(F32)
            for t in range(tp):
                acc += dot_nn(o_in[cur, t], wo_ref[t, :, cols])
            y_buf[cur, :, cols] = acc.astype(BF16)

    def finalize(i):
        slot = lax.rem(i, 2)
        own = pl.ds(pl.multiple_of(z * rows, rows), rows)
        tot[...] = part[lax.rem(i, PART_RING), own, :]

        @pl.when(z > 0)
        def _():
            rs_copy(i, slots - 1, True).wait_recv()
            tot[...] += rs_r[lax.rem(i, RS_RING), slots - 1].astype(F32)

        @pl.when(z < last)
        def _():
            rs_copy(i, slots - 1, False).wait_recv()
            tot[...] += rs_l[lax.rem(i, RS_RING), slots - 1].astype(F32)

        @pl.when(i > 1)
        def _():
            ag_first_done(i - 2, slot)

        for copy in final_inputs(i, slot):
            copy.wait()
        x = xo_in[slot].astype(F32)
        centred = x - jnp.mean(x, axis=-1, keepdims=True)
        inv_std = lax.rsqrt(jnp.mean(centred * centred, axis=-1, keepdims=True) + LN_EPS)
        x_hat = centred * inv_std
        dn = tot[...]
        gg_ref[...] += jnp.sum(dn * x_hat, axis=0, keepdims=True)
        d_hat = dn * gain_ref[...]
        dx = inv_std * (d_hat - jnp.mean(d_hat, axis=-1, keepdims=True) - x_hat * jnp.mean(d_hat * x_hat, axis=-1, keepdims=True))
        gx_buf[slot] = (dyo_in[slot].astype(F32) + dx).astype(BF16)
        ag_first(i, slot)

    def block_of(t):
        return 2 * lax.div(t, 2) + jnp.where(lax.rem(t, 2) == 0, 1 - core, core)

    def job_loads(t, slot):
        cols = pl.ds(pl.multiple_of(block_of(t) * width, width), width)
        return [
            pltpu.make_async_copy(n_hbm.at[:, cols], n_in.at[slot], job_sem.at[slot, 0]),
            pltpu.make_async_copy(dy_hbm.at[:, cols], dy_in.at[slot], job_sem.at[slot, 1]),
        ]

    def away_copy(p):
        ring = lax.rem(p, 2)
        return remote(away, part_in.at[ring], away_send.at[0], away_recv.at[ring], partner)

    def job_block(t, put):
        slot = lax.rem(t, 2)
        n_t = n_in[slot].T
        put(0, hidden, dot_nn(n_t, dq_all[...]))
        put(hidden, hidden, dot_nn(n_t, dkv_all[0]))
        put(2 * hidden, hidden, dot_nn(n_t, dkv_all[1]))
        for k in range(hidden // width):
            put(3 * hidden + k * width, width, dot_nn(o_t[k * width:(k + 1) * width, :], dy_in[slot]))

    def mine_to_own(p, slot):
        return pltpu.make_async_copy(mine.at[slot], ga_hbm.at[2 * p + core], mine_own.at[slot])

    def mine_to_part(p, slot):
        return remote(mine.at[slot], ga_hbm.at[2 * p + core], mine_part.at[slot], ga_recv.at[p], partner)

    def mine_to_chip(p, slot):
        return remote(mine.at[slot], gb_hbm.at[2 * p + core], mine_chip.at[slot], chip_recv.at[p], peer)

    def mine_done(p, slot):
        mine_to_own(p, slot).wait()
        mine_to_part(p, slot).wait_send()
        mine_to_chip(p, slot).wait_send()

    def chip_forward(p):
        b = 2 * p + core
        return remote(gb_hbm.at[b], gb_hbm.at[b], gb_send.at[p], gb_recv.at[p], partner)

    def job(t):
        p = lax.div(t, 2)
        for copy in job_loads(t, lax.rem(t, 2)):
            copy.wait()

        @pl.when(t + 1 < blocks)
        def _():
            for copy in job_loads(t + 1, 1 - lax.rem(t, 2)):
                copy.start()

        @pl.when(lax.rem(t, 2) == 0)
        def _():
            @pl.when(p > 0)
            def _():
                away_copy(p - 1).wait_send()

            def put(at, size, value):
                away[:, at:at + size] = value

            job_block(t, put)
            away_copy(p).start()

        @pl.when(lax.rem(t, 2) == 1)
        def _():
            slot = lax.rem(p, 2)
            away_copy(p).wait_recv()

            @pl.when(p > 1)
            def _():
                mine_done(p - 2, slot)

            def put(at, size, value):
                mine[slot, :, at:at + size] = (value + part_in[slot, :, at:at + size]).astype(BF16)

            job_block(t, put)
            mine_to_chip(p, slot).start()
            mine_to_part(p, slot).start()
            mine_to_own(p, slot).start()

    gg_ref[...] = jnp.zeros_like(gg_ref)
    o_loads = [pltpu.make_async_copy(o_hbm.at[z, :, k * width:(k + 1) * width], n_in.at[k], job_sem.at[k, 0]) for k in range(hidden // width)]
    for copy in o_loads:
        copy.start()
    for copy in inputs(0, 0):
        copy.start()
    for copy in rest_loads + out_loads:
        copy.start()
    me = z * cp + r

    def gain_copy(dt, dc):
        to = {"tp": lax.rem(z + dt, tp), "cp": lax.rem(r + dc, cp)}
        return remote(gain_all.at[me], gain_all.at[me], gs_sem.at[dt * cp + dc], gr_sem.at[me], to)

    def gain_wait(dt, dc):
        sender = lax.rem(z + dt, tp) * cp + lax.rem(r + dc, cp)
        remote(gain_all.at[sender], gain_all.at[sender], gs_sem.at[0], gr_sem.at[sender], right).wait_recv()

    units = tokens // seq * HALVES
    half = hidden // HALVES
    late_units = range(max(0, units - LATE), units)
    late_wait = max(0, late_units[0] // HALVES * seq // span + OUT_LAG - 2)
    sends_late = jnp.logical_or(z == 1, z == last - 1)
    gets_late = jnp.logical_or(z == 0, z == last)

    def late_copy(n, src, dst):
        u = late_units[n]
        place = o_out.at[src, u // HALVES * seq:(u // HALVES + 1) * seq, u % HALVES * half:(u % HALVES + 1) * half]
        return remote(place, place, late_send.at[n], late_recv.at[n], {"tp": dst})

    def late_move(n):
        return late_copy(n, z, jnp.where(z == 1, 0, last))

    for n in range(len(late_units)):
        @pl.when(sends_late)
        def _(n=n):
            late_move(n).start()

    for copy in weight_loads:
        copy.wait()

    def step(i, carry):
        @pl.when(jnp.logical_and(gets_late, i == late_wait))
        def _():
            for n in range(len(late_units)):
                late_copy(n, jnp.where(z == 0, 1, last - 1), z).wait_recv()

        for a in reversed(range(1, slots + 1)):
            ag_step(i - slots - a, a)

        @pl.when(i == OUT_LAG)
        def _():
            for copy in out_loads:
                copy.wait()

        @pl.when(jnp.logical_and(i >= OUT_LAG, i < groups + OUT_LAG))
        def _():
            j = i - OUT_LAG
            at = lax.rem(j, 2)
            for copy in inputs(j, at):
                copy.wait()

            @pl.when(j + 1 < groups)
            def _():
                for copy in inputs(j + 1, 1 - at):
                    copy.start()

            @pl.when(j >= 2)
            def _():
                y_copy(j - 2, at).wait()

            project_out(at)
            y_copy(j, at).start()

        @pl.when(jnp.logical_and(i >= slots, i < groups + slots))
        def _():
            finalize(i - slots)

        @pl.when(i == groups + slots - 1)
        def _():
            gain_all[me] = gg_ref[...]
            for dt, dc in peers:
                gain_copy(dt, dc).start()

        @pl.when(jnp.logical_and(i >= slots - 1, i < groups + slots - 1))
        def _():
            for copy in final_inputs(i - slots + 1, lax.rem(i - slots + 1, 2)):
                copy.start()

        @pl.when(i == EARLY)
        def _():
            for copy in rest_loads:
                copy.wait()

        @pl.when(i < groups)
        def _():
            partial_norm(i)

        @pl.when(i == JOB_LAG - 1)
        def _():
            for k, copy in enumerate(o_loads):
                copy.wait()
                o_t[k * width:(k + 1) * width, :] = n_in[k].T
            for copy in job_loads(0, 0):
                copy.start()

        @pl.when(jnp.logical_and(i >= JOB_LAG, i < JOB_LAG + blocks))
        def _():
            job(i - JOB_LAG)

        for k in reversed(range(slots)):
            rs_send(i - k, k)

        @pl.when(jnp.logical_and(lax.rem(i, 2) == 1, jnp.logical_and(i >= FORWARD_LAG, i < FORWARD_LAG + 2 * pairs)))
        def _():
            p = lax.div(i - FORWARD_LAG, 2)
            mine_to_chip(p, 0).wait_recv()
            chip_forward(p).start()

        return carry

    lax.fori_loop(0, max(groups + 2 * slots, groups + OUT_LAG, blocks + JOB_LAG, 2 * pairs + FORWARD_LAG - 1), step, 0)

    for i in (groups - 2, groups - 1):
        y_copy(i, i % 2).wait()
        ag_first_done(i, i % 2)
    for to_right in (True, False):
        far = z if to_right else last - z
        for s in range(slots):
            @pl.when(jnp.logical_and(far <= s, far < last))
            def _(s=s, to_right=to_right):
                rs_copy(groups - 1, s, to_right).wait_send()
        for a in range(1, slots):
            @pl.when(jnp.logical_and(far >= a, far < last))
            def _(a=a, to_right=to_right):
                ag_forward(groups - 1, a, to_right).wait_send()
    for n in range(len(late_units)):
        @pl.when(sends_late)
        def _(n=n):
            late_move(n).wait_send()

    away_copy(pairs - 1).wait_send()
    for p in range(max(0, pairs - 2), pairs):
        mine_done(p, p % 2)
    for p in range(pairs):
        chip_forward(p).wait_send()
        chip_forward(p).wait_recv()
        mine_to_part(p, 0).wait_recv()
    for dt, dc in peers:
        gain_wait(dt, dc)
        gain_copy(dt, dc).wait_send()
    total = gain_all[0]
    for j in range(1, tp * cp):
        total += gain_all[j]
    gg_ref[...] = total


def backward_norm(dq, dkv, x, dy, o_all, normed, wq, wk, wv, wo_all, gain, rows, seq, tp, cp):
    tokens, hidden = dq.shape
    d_model = x.shape[1]
    span = tp * rows
    groups = tokens // span
    slots = tp - 1
    width = WIDTH
    blocks = d_model // width
    pairs = blocks // 2
    hbm = pl.BlockSpec(memory_space=pl.ANY)
    vmem = pl.BlockSpec(memory_space=pltpu.VMEM)
    dma = pltpu.SemaphoreType.DMA
    bf = lambda *shape: pltpu.VMEM(shape, BF16)
    f32 = lambda *shape: pltpu.VMEM(shape, F32)
    return pl.pallas_call(
        functools.partial(back_kernel, groups, rows, tp, cp, seq),
        in_specs=[hbm] * 10 + [vmem],
        out_specs=[hbm, hbm, hbm, hbm, vmem, hbm],
        input_output_aliases={4: 5},
        out_shape=[
            jax.ShapeDtypeStruct((tokens, d_model), BF16),
            jax.ShapeDtypeStruct((tokens, d_model), BF16),
            jax.ShapeDtypeStruct((blocks, width, 4 * hidden), BF16),
            jax.ShapeDtypeStruct((blocks, width, 4 * hidden), BF16),
            jax.ShapeDtypeStruct((1, d_model), F32),
            jax.ShapeDtypeStruct(o_all.shape, BF16),
        ],
        scratch_shapes=[
            bf(d_model, hidden), bf(d_model, hidden), bf(d_model, hidden), bf(tp, hidden, d_model),
            bf(tokens, hidden), bf(2, tokens, hidden), bf(hidden, tokens),
            f32(PART_RING, span, d_model), bf(RS_RING, slots, rows, d_model), bf(RS_RING, slots, rows, d_model),
            bf(slots, rows, d_model), bf(slots, rows, d_model), f32(rows, d_model), bf(2, rows, d_model),
            bf(2, tp, span, hidden), bf(2, span, d_model), bf(2, rows, d_model), bf(2, rows, d_model), bf(2, span, d_model),
            bf(2, tokens, width), bf(2, tokens, width),
            f32(width, 4 * hidden), f32(2, width, 4 * hidden), bf(2, width, 4 * hidden), f32(tp * cp, 1, d_model),
            dma((8,)), dma((2, 2)), dma((2, 2)), dma((2, 2)), dma((2,)), dma((2,)),
            dma((slots,)), dma((slots,)), dma((RS_RING, slots)), dma((RS_RING, slots)),
            dma((2,)), dma((2,)), dma((slots,)), dma((slots,)), dma((groups, slots)), dma((groups, slots)),
            dma((1,)), dma((2,)), dma((2,)), dma((2,)), dma((2,)), dma((pairs,)), dma((pairs,)), dma((pairs,)), dma((pairs,)),
            dma((tp * cp,)), dma((tp * cp,)), dma((max(LATE, 1),)), dma((max(LATE, 1),)),
        ],
        compiler_params=pltpu.CompilerParams(collective_id=0, has_side_effects=True, vmem_limit_bytes=63 << 20),
        cost_estimate=pl.CostEstimate(flops=22 * tokens * hidden * d_model, bytes_accessed=16 * tokens * d_model, transcendentals=0),
        name="backward_norm",
    )(dq, dkv, x, dy, o_all, normed, wq, wk, wv, wo_all, gain)


def finish_kernel(y_ref, gx_ref, ga_ref, gb_ref, yo_ref, gxo_ref, wq_ref, wk_ref, wv_ref, wo_ref):
    yo_ref[...] = y_ref[...]
    gxo_ref[...] = gx_ref[...]
    rows = ga_ref.shape[1]
    width = rows * PARTS
    hidden = wq_ref.shape[1]
    for k, ref in enumerate((wq_ref, wk_ref, wv_ref)):
        cols = slice(k * hidden, (k + 1) * hidden)
        ref[...] = ga_ref[0, :, cols].astype(F32) + gb_ref[0, :, cols].astype(F32)
    for k in range(hidden // width):
        cols = slice(3 * hidden + k * width, 3 * hidden + (k + 1) * width)
        at = k * width + lax.rem(pl.program_id(0), PARTS) * rows
        wo_ref[pl.ds(pl.multiple_of(at, rows), rows), :] = ga_ref[0, :, cols].astype(F32) + gb_ref[0, :, cols].astype(F32)


def finish(y, gx, ga, gb):
    tokens, d_model = y.shape
    blocks, width, packed = ga.shape
    hidden = packed // 4
    steps = blocks * PARTS
    tile = pl.BlockSpec((tokens // steps, d_model), lambda j: (j, 0))
    block = pl.BlockSpec((1, width // PARTS, packed), lambda j: (j // PARTS, j % PARTS, 0))
    wide = pl.BlockSpec((width // PARTS, hidden), lambda j: (j, 0))
    return pl.pallas_call(
        finish_kernel,
        grid=(steps,),
        in_specs=[tile, tile, block, block],
        out_specs=[tile, tile, wide, wide, wide, pl.BlockSpec((hidden, width), lambda j: (0, j // PARTS))],
        out_shape=[jax.ShapeDtypeStruct((tokens, d_model), BF16)] * 2 + [jax.ShapeDtypeStruct((d_model, hidden), F32)] * 3 + [jax.ShapeDtypeStruct((hidden, d_model), F32)],
        compiler_params=pltpu.CompilerParams(dimension_semantics=("arbitrary",), vmem_limit_bytes=48 << 20),
        cost_estimate=pl.CostEstimate(flops=8 * d_model * hidden, bytes_accessed=8 * tokens * d_model + 32 * d_model * hidden, transcendentals=0),
        name="finish",
    )(y, gx, ga, gb)


def solution(mesh):
    cp_size = mesh.shape["cp"]
    tp_size = mesh.shape["tp"]

    def device_step(x_in, segment_ids, positions, w_query, w_key, w_value, w_out, norm_gain, grad_out):
        batch, seq, d_model = x_in.shape
        tokens = batch * seq
        x = x_in.reshape(tokens, d_model)
        dy = grad_out.reshape(tokens, d_model)

        gain = norm_gain.reshape(1, d_model)
        normed, o_all, dq, dkv, w_all = front(x, dy, w_query, w_key, w_value, w_out, positions, jnp.asarray(angle_table(), BF16), gain, seq, tp_size, cp_size)
        grad_x, y_out, sum_a, sum_b, grad_gain, _ = backward_norm(dq, dkv, x, dy, o_all, normed, w_query, w_key, w_value, w_all, gain, ROWS, seq, tp_size, cp_size)
        grad_gain = grad_gain.reshape(d_model)
        y_out, grad_x, grad_wq, grad_wk, grad_wv, grad_wo = finish(y_out, grad_x, sum_a, sum_b)
        return y_out.reshape(x_in.shape), grad_x.reshape(x_in.shape), grad_gain, grad_wq, grad_wk, grad_wv, grad_wo

    in_specs = (P("dp", "cp", None), P("dp", "cp"), P("dp", "cp"), P(None, "tp"), P(None, "tp"), P(None, "tp"), P("tp", None), P(None), P("dp", "cp", None))
    out_specs = (P("dp", "cp", None), P("dp", "cp", None), P("dp"), P("dp", "tp"), P("dp", "tp"), P("dp", "tp"), P(("dp", "tp"), None))
    return jax.shard_map(device_step, mesh=mesh, in_specs=in_specs, out_specs=out_specs, check_vma=False)
```

```python
import functools
import math

import jax
import jax.numpy as jnp
import numpy as np
from jax import lax
from jax.experimental import pallas as pl
from jax.experimental.pallas import tpu as pltpu
from jax.sharding import PartitionSpec as P

HEAD_DIM = 128
ROPE_THETA = 8000000.0
LN_EPS = 1e-5
NEG_BIG = -1e30
SCALE = HEAD_DIM ** -0.5
EXP2_SCALE = SCALE * math.log2(math.e)
F32 = jnp.float32
BF16 = jnp.bfloat16
NT = (((1,), (1,)), ((), ()))


def dot_nn(a, b):
    return jnp.dot(a, b, preferred_element_type=F32)


def dot_nt(a, b):
    return lax.dot_general(a, b, NT, preferred_element_type=F32)


def dot_tn(a, b):
    return lax.dot_general(a, b, (((0,), (0,)), ((), ())), preferred_element_type=F32)


def swap_pairs(t, sign):
    lane = lax.broadcasted_iota(jnp.int32, t.shape, 1)
    even = (lane % 2) == 0
    up = pltpu.roll(t, HEAD_DIM - 1, 1)
    down = pltpu.roll(t, 1, 1)
    return jnp.where(even, -up, down) if sign > 0 else jnp.where(even, up, -down)


def rope(t, cos_t, sin_t, sign):
    return t * cos_t + swap_pairs(t, sign) * sin_t


def angle_table():
    inv_freq = ROPE_THETA ** (-np.arange(0, HEAD_DIM, 2, dtype=np.float32) / np.float32(HEAD_DIM))
    freq = np.repeat(inv_freq.astype(np.float64), 2)[None, :]
    low = np.arange(POS_LOW)[:, None] * freq
    high = POS_LOW * np.arange(HEAD_DIM - POS_LOW)[:, None] * freq
    table = np.zeros((HEAD_DIM, 12 * HEAD_DIM), np.float32)
    for k, (first, value) in enumerate(((0, np.cos(low)), (0, np.sin(low)), (POS_LOW, np.cos(high)), (POS_LOW, np.sin(high)))):
        rest = value.astype(np.float32)
        for p in range(3):
            piece = rest.astype(BF16).astype(np.float32)
            at = (3 * k + p) * HEAD_DIM
            table[first:first + value.shape[0], at:at + HEAD_DIM] = piece
            rest = rest - piece
    return table


def put_rope(dst, raw, cos_t, sin_t):
    for h in range(raw.shape[1] // HEAD_DIM):
        cols = slice(h * HEAD_DIM, (h + 1) * HEAD_DIM)
        dst[:, cols] = rope(raw[:, cols], cos_t, sin_t, 1.0).astype(BF16)


MESH = pl.DeviceIdType.MESH
SUB = 384
ROWS = 32
WIDTH = 256
PARTS = 1
HALVES = 2
RELAY_LAG = 1
LATE = 3
SUM_LAG = 4
CHIP_BUFS = 4
OWN_RING = 6
Q_RING = 3
AHEAD = 2
POS_LOW = 64
W_TWIN = 1
W_PARTNER = 3
W_CHIP = 7


def front_kernel(batch, seq, tp, cp, x_hbm, dy_hbm, wq_hbm, wk_hbm, wv_hbm, wo_hbm, pos_ref, table_ref, gain_ref,
                 n_hbm, o_all, dq_hbm, dkv_hbm, w_all,
                 big, wo_ref, cos_ref, sin_ref, q_ring, do_ring, x_in, dy_in, n_buf, kv_own, kvr, s_scr, dp_scr, m_scr, l_scr, d_scr, ot_scr, dqt_scr,
                 o_buf, dq_buf, g_own, g_part, g_chip, g_far, xin, part_in,
                 w_sem, wl_sem, wz_send, wz_recv, wx_send, wx_recv,
                 x_sem, dy_sem, n_sem, kvs_part, kvs_chip, kvs_far, kv_recv, o_local, o_send, o_recv, relay_send, dq_sem,
                 far_send, part_send, chip_send, x_recv, part_recv, dkv_sem):
    z = lax.axis_index("tp")
    r = lax.axis_index("cp")
    dp = lax.axis_index("dp")
    core = lax.rem(r, 2)
    chip = lax.div(r, 2)
    d_model = x_hbm.shape[1]
    hidden = wq_hbm.shape[1]
    heads = hidden // HEAD_DIM
    first_chip, second_chip = chip == 0, chip == 1
    first_core, second_core = core == 0, core == 1
    partner = {"cp": r + 1 - 2 * core}
    peer = {"cp": r + 2 - 4 * chip}
    twin = {"dp": 1 - dp}

    tile = x_in.shape[1]
    per_row = seq // tile

    def row(b):
        return pl.ds(pl.multiple_of(b * seq, seq), seq)

    def tile_rows(b, k):
        return pl.ds(pl.multiple_of(b * seq + k * tile, tile), tile)

    def x_load(b, k):
        return pltpu.make_async_copy(x_hbm.at[tile_rows(b, k), :], x_in.at[k], x_sem.at[k])

    def dy_load(b, k):
        return pltpu.make_async_copy(dy_hbm.at[tile_rows(b, k), :], dy_in.at[k], dy_sem.at[k])

    def n_store(b, k):
        return pltpu.make_async_copy(n_buf.at[k], n_hbm.at[tile_rows(b, k), :], n_sem.at[k])

    weight_loads = [pltpu.make_async_copy(src, dst, w_sem.at[k]) for k, (src, dst) in enumerate(((wk_hbm, big.at[0]), (wv_hbm, big.at[1]), (wq_hbm, big.at[2]), (wo_hbm, wo_ref)))]
    x_load(0, 0).start()
    for copy in weight_loads[:2]:
        copy.start()
    for k in range(1, per_row):
        x_load(0, k).start()
    for copy in weight_loads[2:]:
        copy.start()
    for k in range(per_row):
        dy_load(0, k).start()

    units = batch * HALVES
    half = hidden // HALVES

    def where(u):
        return lax.div(u, HALVES), lax.rem(u, HALVES)

    def half_cols(g):
        return pl.ds(pl.multiple_of(g * half, half), half)

    barrier = pltpu.get_barrier_semaphore()
    for dev in [partner, peer, twin] + [{"tp": lax.rem(z + dt, tp)} for dt in range(1, tp)]:
        pl.semaphore_signal(barrier, inc=1, device_id=dev, device_id_type=MESH)

    def remote(src, dst, ssem, rsem, dev):
        return pltpu.make_async_remote_copy(src_ref=src, dst_ref=dst, send_sem=ssem, recv_sem=rsem, device_id=dev, device_id_type=MESH)

    share = hidden // 8

    def share_rows(y, c, g):
        return pl.ds(pl.multiple_of((4 * y + 2 * c + g) * share, share), share)

    mine, twins = share_rows(chip, core, dp), share_rows(chip, core, 1 - dp)
    peers, peer_twins = share_rows(1 - chip, core, dp), share_rows(1 - chip, core, 1 - dp)

    def wz_copy(d):
        return remote(wo_hbm.at[mine, :], w_all.at[z, mine, :], wz_send.at[d], wz_recv.at[z], {"tp": lax.rem(z + d, tp)})

    def wz_wait(d):
        src = lax.rem(z + d, tp)
        remote(wo_hbm.at[mine, :], w_all.at[src, mine, :], wz_send.at[d], wz_recv.at[src], partner).wait_recv()

    def w_copy(k, d, rows, dev):
        place = w_all.at[lax.rem(z + d, tp), rows, :]
        return remote(place, place, wx_send.at[k, d], wx_recv.at[k, d], dev)

    def w_move(k, d):
        rows, dev = ((mine, twin), (mine, partner), (twins, partner), (mine, peer), (twins, peer), (peers, partner), (peer_twins, partner))[k]
        return w_copy(k, d, rows, dev)

    w_steps = range(1, tp)

    def kv_to_partner(u):
        return remote(kv_own.at[u], kvr.at[0, u], kvs_part.at[u], kv_recv.at[0, u], partner)

    def kv_to_chip(u):
        return remote(kv_own.at[u], kvr.at[1, u], kvs_chip.at[u], kv_recv.at[1, u], peer)

    def kv_forward(u):
        return remote(kvr.at[1, u], kvr.at[2, u], kvs_far.at[u], kv_recv.at[2, u], partner)

    w_local = pltpu.make_async_copy(wo_ref, w_all.at[z], wl_sem.at[0])

    def angles(b, k):
        rows = tile_rows(b, k)
        pos = jnp.broadcast_to(pos_ref[pl.ds(b, 1), k * tile:(k + 1) * tile], (HEAD_DIM, tile)).T
        lane = lax.broadcasted_iota(jnp.int32, (tile, HEAD_DIM), 1)
        low = lane < POS_LOW
        pick = jnp.where(low, lax.rem(pos, POS_LOW), POS_LOW + lax.div(pos, POS_LOW)) == lane
        found = dot_nn(jnp.where(pick, 1.0, 0.0).astype(BF16), table_ref[...])

        def part(k):
            at = 3 * k * HEAD_DIM
            return found[:, at:at + HEAD_DIM] + found[:, at + HEAD_DIM:at + 2 * HEAD_DIM] + found[:, at + 2 * HEAD_DIM:at + 3 * HEAD_DIM]

        cos_b, sin_b, cos_a, sin_a = part(0), part(1), part(2), part(3)
        cos_ref[rows, :] = cos_a * cos_b - sin_a * sin_b
        sin_ref[rows, :] = sin_a * cos_b + cos_a * sin_b

    def project_row(b, first=False):
        ring = lax.rem(b, Q_RING)
        for k in range(per_row):
            rows = tile_rows(b, k)
            inside = slice(k * tile, (k + 1) * tile)
            x_load(b, k).wait()

            @pl.when(b > 0)
            def _(k=k):
                n_store(b - 1, k).wait()

            angles(b, k)
            x = x_in[k].astype(F32)
            centred = x - jnp.mean(x, axis=-1, keepdims=True)
            inv_std = lax.rsqrt(jnp.mean(centred * centred, axis=-1, keepdims=True) + LN_EPS)
            n_buf[k] = ((centred * inv_std) * gain_ref[...]).astype(BF16)
            n_store(b, k).start()

            @pl.when(b + 1 < batch)
            def _(k=k):
                x_load(b + 1, k).start()

            if first and k == 0:
                for copy in weight_loads[:2]:
                    copy.wait()
            for g in range(HALVES):
                u = b * HALVES + g
                cols = slice(g * half, (g + 1) * half)
                put_rope(kv_own.at[u, 0, inside, :], dot_nn(n_buf[k], big[0, :, cols]), cos_ref[rows, :], sin_ref[rows, :])
                kv_own[u, 1, inside, :] = dot_nn(n_buf[k], big[1, :, cols]).astype(BF16)

        if first:
            pl.semaphore_wait(barrier, tp + 2)
        for g in range(HALVES):
            u = b * HALVES + g

            @pl.when(first_chip)
            def _(u=u):
                kv_to_chip(u).start()

            @pl.when(first_core)
            def _(u=u):
                kv_to_partner(u).start()

        if first:
            for d in range(1, tp):
                wz_copy(d).start()
            for copy in weight_loads[2:]:
                copy.wait()
            w_local.start()

        for k in range(per_row):
            rows = tile_rows(b, k)
            inside = slice(k * tile, (k + 1) * tile)
            dy_load(b, k).wait()
            put_rope(q_ring.at[ring, inside, :], dot_nn(n_buf[k], big[2]), cos_ref[rows, :], sin_ref[rows, :])
            do_ring[ring, inside, :] = dot_nt(dy_in[k], wo_ref[...]).astype(BF16)

            @pl.when(b + 1 < batch)
            def _(k=k):
                dy_load(b + 1, k).start()

    def o_place(src, u):
        b, g = where(u)
        return o_all.at[src, row(b), half_cols(g)]

    def o_local_copy(b):
        return pltpu.make_async_copy(o_buf.at[b], o_place(z, b), o_local.at[b])

    def o_copy(b, k, step):
        return remote(o_buf.at[b], o_place(z, b), o_send.at[k, b], o_recv.at[z, b], {"tp": jnp.clip(z + step, 0, tp - 1)})

    hops = [(k, step, jnp.logical_and(z + step >= 0, z + step < tp)) for k, step in enumerate((1, -1))]

    def far_from_end(step):
        return jnp.logical_and(z + step != 0, z + step != tp - 1)

    def o_start(b):
        o_local_copy(b).start()
        for k, step, ok in hops:
            @pl.when(jnp.logical_and(ok, jnp.logical_or(b < units - LATE, far_from_end(step))))
            def _(k=k, step=step):
                o_copy(b, k, step).start()

    def o_arrived(src, b):
        remote(o_place(src, b), o_place(src, b), relay_send.at[0, 0, b], o_recv.at[src, b], partner).wait_recv()

    def relay_copy(b, age, step):
        src = jnp.clip(z - age * step, 0, tp - 1)
        return remote(o_place(src, b), o_place(src, b), relay_send.at[age - 1, (1 - step) // 2, b], o_recv.at[src, b], {"tp": jnp.clip(z + step, 0, tp - 1)})

    def relays(age, step):
        far = z if step > 0 else tp - 1 - z
        return jnp.logical_and(far >= age, far < tp - 1)

    def relay(b, age):
        for step in (1, -1):
            @pl.when(relays(age, step))
            def _(step=step):
                o_arrived(jnp.clip(z - age * step, 0, tp - 1), b)
                relay_copy(b, age, step).start()

    def far_copy(b, par):
        return remote(g_far.at[par], xin.at[b], far_send.at[par], x_recv.at[b], partner)

    def part_copy(b, par):
        return remote(g_part.at[par], part_in.at[b], part_send.at[par], part_recv.at[b], partner)

    def chip_copy(b):
        par = lax.rem(b, CHIP_BUFS)
        return remote(g_chip.at[par], xin.at[b], chip_send.at[par], x_recv.at[b], peer)

    def chip_sum(b):
        @pl.when(second_chip)
        def _():
            par = lax.rem(b, CHIP_BUFS)
            far_copy(b, 0).wait_recv()
            g_chip[par] = (g_chip[par].astype(F32) + xin[b].astype(F32)).astype(BF16)
            chip_copy(b).start()

    def dkv_store(u, which):
        b, g = where(u)
        return pltpu.make_async_copy(g_own.at[lax.rem(u, OWN_RING), which], dkv_hbm.at[which, row(b), half_cols(g)], dkv_sem.at[u, which])

    def key_grads(u):
        @pl.when(first_core)
        def _():
            part_copy(u, 0).wait_recv()

        @pl.when(first_chip)
        def _():
            chip_copy(u).wait_recv()

        b, g = where(u)
        rows = row(b)
        for which in range(2):
            for h in range(half // HEAD_DIM):
                cols = slice(h * HEAD_DIM, (h + 1) * HEAD_DIM)
                own = g_own.at[lax.rem(u, OWN_RING), which, :, cols]
                acc = own[...].astype(F32)
                acc = acc + jnp.where(first_core, part_in[u, which, :, cols].astype(F32), 0.0)
                acc = (acc + jnp.where(first_chip, xin[u, which, :, cols].astype(F32), 0.0)).astype(BF16)
                if which == 0:
                    acc = rope(acc.astype(F32), cos_ref[rows, :], sin_ref[rows, :], -1.0).astype(BF16)
                own[...] = acc
            dkv_store(u, which).start()

    def dq_store(b, par):
        return pltpu.make_async_copy(dq_buf.at[par], dq_hbm.at[row(where(b)[0]), half_cols(where(b)[1])], dq_sem.at[par])

    subs = range(0, seq, SUB)

    def attend_unit(i, par):
        b, g = where(i)
        rows = row(b)
        ring = lax.rem(b, Q_RING)
        start = r * seq + lax.broadcasted_iota(jnp.int32, (1, seq), 1) - pos_ref[pl.ds(b, 1), :]
        chip_par = lax.rem(i, CHIP_BUFS)
        keys_of = [kv_own.at[i]] + [kvr.at[s, i] for s in range(3)]
        places = [g_part.at[par], g_chip.at[chip_par], g_far.at[par]]

        def grad(slot, which, cols):
            return places[slot - 1].at[which, :, cols] if slot else g_own.at[lax.rem(i, OWN_RING), which, :, cols]

        live = [None, second_core, second_chip, second_chip]
        piece = [r, r + 1 - 2 * core, r + 2 - 4 * chip, r + 3 - 2 * core - 4 * chip]

        def each(body):
            body(0)
            for slot in (1, 2, 3):
                pl.when(live[slot])(functools.partial(body, slot))

        def one_head(h, carry):
            cols = pl.ds(pl.multiple_of(h * HEAD_DIM, HEAD_DIM), HEAD_DIM)
            full = pl.ds(pl.multiple_of(g * half + h * HEAD_DIM, HEAD_DIM), HEAD_DIM)
            q = q_ring[ring, :, full]
            do = do_ring[ring, :, full]
            m_scr[...] = jnp.full(m_scr.shape, NEG_BIG, F32)
            l_scr[...] = jnp.zeros_like(l_scr)
            d_scr[...] = jnp.zeros_like(d_scr)
            ot_scr[...] = jnp.zeros_like(ot_scr)
            dqt_scr[...] = jnp.zeros_like(dqt_scr)

            def scores(slot):
                base = piece[slot] * seq
                top = None
                for s in subs:
                    raw = dot_nt(keys_of[slot][0, s:s + SUB, cols], q)
                    local = lax.broadcasted_iota(jnp.int32, raw.shape, 0) + s
                    allowed = (local + base) >= start
                    if slot == 0:
                        allowed = jnp.logical_and(allowed, local <= lax.broadcasted_iota(jnp.int32, raw.shape, 1))
                    raw = jnp.where(allowed, raw, NEG_BIG)
                    s_scr[slot, s:s + SUB, :] = raw
                    high = jnp.max(raw, axis=0, keepdims=True)
                    top = high if top is None else jnp.maximum(top, high)
                m_scr[...] = jnp.maximum(m_scr[...], top)

            def exps(slot):
                top = m_scr[...]
                total = None
                for s in subs:
                    e = jnp.exp2((s_scr[slot, s:s + SUB, :] - top) * EXP2_SCALE)
                    s_scr[slot, s:s + SUB, :] = e
                    part = jnp.sum(e, axis=0, keepdims=True)
                    total = part if total is None else total + part
                l_scr[...] += total

            def values(slot):
                inv = l_scr[...]
                total, out = None, None
                for s in subs:
                    v = keys_of[slot][1, s:s + SUB, cols]
                    prob = s_scr[slot, s:s + SUB, :] * inv
                    low = prob.astype(BF16)
                    dp = dot_nt(v, do)
                    dp_scr[slot, s:s + SUB, :] = dp
                    part = jnp.sum(prob * dp, axis=0, keepdims=True)
                    total = part if total is None else total + part
                    grad(slot, 1, cols)[s:s + SUB, :] = dot_nn(low, do).astype(BF16)
                    piece_out = dot_nn(v.T, low)
                    out = piece_out if out is None else out + piece_out
                d_scr[...] += total
                ot_scr[...] += out

            def keys(slot):
                inv, mean = l_scr[...], d_scr[...]
                out = None
                for s in subs:
                    k = keys_of[slot][0, s:s + SUB, cols]
                    ds = ((s_scr[slot, s:s + SUB, :] * inv) * (dp_scr[slot, s:s + SUB, :] - mean)).astype(BF16)
                    grad(slot, 0, cols)[s:s + SUB, :] = (dot_nn(ds, q) * SCALE).astype(BF16)
                    piece_out = dot_nn(k.T, ds)
                    out = piece_out if out is None else out + piece_out
                dqt_scr[...] += out

            each(scores)
            each(exps)
            l_scr[...] = 1.0 / l_scr[...]
            each(values)
            each(keys)
            o_buf[i, :, cols] = ot_scr[...].T.astype(BF16)
            dq_buf[par, :, cols] = rope(dqt_scr[...].T * SCALE, cos_ref[rows, :], sin_ref[rows, :], -1.0).astype(BF16)
            return carry

        lax.fori_loop(0, heads // HALVES, one_head, 0)

    def step(i, carry):
        par = lax.rem(i, 2)
        @pl.when(jnp.logical_and(lax.rem(i, HALVES) == 0, lax.div(i, HALVES) + AHEAD < batch))
        def _():
            project_row(lax.div(i, HALVES) + AHEAD)

        @pl.when(i >= OWN_RING)
        def _():
            for which in range(2):
                dkv_store(i - OWN_RING, which).wait()

        @pl.when(second_chip)
        def _():
            kv_to_chip(i).wait_recv()
            kv_forward(i).start()

        @pl.when(second_core)
        def _():
            kv_to_partner(i).wait_recv()

        @pl.when(second_chip)
        def _():
            kv_forward(i).wait_recv()

        @pl.when(i >= 2)
        def _():
            dq_store(i - 2, par).wait()

            @pl.when(second_core)
            def _():
                part_copy(i - 2, par).wait_send()

            @pl.when(second_chip)
            def _():
                far_copy(i - 2, par).wait_send()

        @pl.when(jnp.logical_and(second_chip, i >= CHIP_BUFS))
        def _():
            chip_copy(i - CHIP_BUFS).wait_send()

        attend_unit(i, par)
        o_start(i)
        dq_store(i, par).start()

        @pl.when(second_chip)
        def _():
            far_copy(i, par).start()

        @pl.when(second_core)
        def _():
            part_copy(i, par).start()

        @pl.when(i >= 1)
        def _():
            chip_sum(i - 1)

        for age in range(1, tp - 1):
            @pl.when(i >= age * RELAY_LAG)
            def _(age=age):
                relay(i - age * RELAY_LAG, age)

        @pl.when(i >= SUM_LAG)
        def _():
            key_grads(i - SUM_LAG)

        @pl.when(i == min(W_TWIN, units - 1))
        def _():
            for d in w_steps:
                wz_wait(d)
                w_move(0, d).start()
                w_move(1, d).start()

                @pl.when(second_chip)
                def _(d=d):
                    w_move(3, d).start()

        @pl.when(i == min(W_PARTNER, units - 1))
        def _():
            for d in w_steps:
                w_move(0, d).wait_recv()
                w_move(2, d).start()

                @pl.when(second_chip)
                def _(d=d):
                    w_move(4, d).start()

        @pl.when(jnp.logical_and(first_chip, i == min(W_CHIP, units - 1)))
        def _():
            for k in (3, 4):
                for d in w_steps:
                    w_move(k, d).start()

        return carry

    for b in range(min(AHEAD, batch)):
        project_row(b, b == 0)
    lax.fori_loop(0, units, step, 0)
    chip_sum(units - 1)

    end = units + max(SUM_LAG, (tp - 2) * RELAY_LAG)
    for i in range(units, end):
        for age in range(1, tp - 1):
            if 0 <= i - age * RELAY_LAG < units:
                relay(i - age * RELAY_LAG, age)
        if 0 <= i - SUM_LAG < units:
            key_grads(i - SUM_LAG)
        if i == end - 1:
            for k in (3, 4):
                for d in w_steps:
                    w_move(k, d).wait_recv()
                    w_move(k + 2, d).start()

    w_local.wait()
    for d in w_steps:
        wz_copy(d).wait_send()
        for k in range(7):
            w_move(k, d).wait_send()
            if k in (1, 2, 5, 6):
                w_move(k, d).wait_recv()

    for k in range(per_row):
        n_store(batch - 1, k).wait()
    for u in range(max(0, units - OWN_RING), units):
        for which in range(2):
            dkv_store(u, which).wait()

    def drain(b, carry):
        @pl.when(first_chip)
        def _():
            kv_to_chip(b).wait_send()

        @pl.when(first_core)
        def _():
            kv_to_partner(b).wait_send()

        @pl.when(second_chip)
        def _():
            kv_forward(b).wait_send()

        o_local_copy(b).wait()
        for k, step_, ok in hops:
            @pl.when(jnp.logical_and(ok, jnp.logical_or(b < units - LATE, far_from_end(step_))))
            def _(k=k, step_=step_):
                o_copy(b, k, step_).wait_send()

        for age in range(1, tp - 1):
            for step_ in (1, -1):
                @pl.when(relays(age, step_))
                def _(age=age, step_=step_):
                    relay_copy(b, age, step_).wait_send()

        for src in range(tp):
            way = jnp.where(z > src, 1, -1)
            gone = jnp.abs(z - src)
            far = jnp.where(way > 0, z, tp - 1 - z)
            taken = jnp.logical_and(gone <= tp - 2, far < tp - 1)
            late = jnp.logical_and(b >= units - LATE, jnp.logical_and(gone == 1, far == tp - 1))

            @pl.when(jnp.logical_and(z != src, jnp.logical_not(jnp.logical_or(taken, late))))
            def _(src=src):
                o_arrived(src, b)

        return carry

    lax.fori_loop(0, units, drain, 0)

    for b in range(max(0, units - 2), units):
        dq_store(b, b % 2).wait()

        @pl.when(second_core)
        def _(b=b):
            part_copy(b, b % 2).wait_send()

        @pl.when(second_chip)
        def _(b=b):
            far_copy(b, b % 2).wait_send()

    for b in range(max(0, units - CHIP_BUFS), units):
        @pl.when(second_chip)
        def _(b=b):
            chip_copy(b).wait_send()


def front(x, dy, wq, wk, wv, wo, pos, table, gain, seq, tp, cp):
    tokens, d_model = x.shape
    hidden = wq.shape[1]
    batch = tokens // seq
    units = batch * HALVES
    half = hidden // HALVES
    tile = seq // 2
    hbm = pl.BlockSpec(memory_space=pl.ANY)
    vmem = pl.BlockSpec(memory_space=pltpu.VMEM)
    dma = pltpu.SemaphoreType.DMA
    bf = lambda *shape: pltpu.VMEM(shape, BF16)
    f32 = lambda *shape: pltpu.VMEM(shape, F32)
    return pl.pallas_call(
        functools.partial(front_kernel, batch, seq, tp, cp),
        in_specs=[hbm] * 6 + [vmem] * 3,
        out_specs=[hbm] * 5,
        out_shape=[
            jax.ShapeDtypeStruct((tokens, d_model), BF16),
            jax.ShapeDtypeStruct((tp, tokens, hidden), BF16),
            jax.ShapeDtypeStruct((tokens, hidden), BF16),
            jax.ShapeDtypeStruct((2, tokens, hidden), BF16),
            jax.ShapeDtypeStruct((tp, hidden, d_model), BF16),
        ],
        scratch_shapes=[
            bf(3, d_model, hidden), bf(hidden, d_model), f32(tokens, HEAD_DIM), f32(tokens, HEAD_DIM),
            bf(Q_RING, seq, hidden), bf(Q_RING, seq, hidden), bf(2, tile, d_model), bf(2, tile, d_model), bf(2, tile, d_model),
            bf(units, 2, seq, half), bf(3, units, 2, seq, half),
            f32(4, seq, seq), f32(4, seq, seq), f32(1, seq), f32(1, seq), f32(1, seq), f32(HEAD_DIM, seq), f32(HEAD_DIM, seq),
            bf(units, seq, half), bf(2, seq, half),
            bf(OWN_RING, 2, seq, half), bf(2, 2, seq, half), bf(CHIP_BUFS, 2, seq, half), bf(2, 2, seq, half),
            bf(units, 2, seq, half), bf(units, 2, seq, half),
            dma((4,)), dma((1,)), dma((tp,)), dma((tp,)), dma((7, tp)), dma((7, tp)),
            dma((2,)), dma((2,)), dma((2,)), dma((units,)), dma((units,)), dma((units,)), dma((3, units)),
            dma((units,)), dma((2, units)), dma((tp, units)), dma((2, 2, units)), dma((2,)),
            dma((2,)), dma((2,)), dma((CHIP_BUFS,)), dma((units,)), dma((units,)), dma((units, 2)),
        ],
        compiler_params=pltpu.CompilerParams(collective_id=1, has_side_effects=True, vmem_limit_bytes=63 << 20),
        cost_estimate=pl.CostEstimate(flops=60 * tokens * seq * hidden, bytes_accessed=16 * tokens * d_model, transcendentals=4 * tokens * seq * (hidden // HEAD_DIM)),
        name="front",
    )(x, dy, wq, wk, wv, wo, pos, table, gain)


PART_RING = 4
RS_RING = 5
FORWARD_LAG = 11
JOB_LAG = 5
OUT_LAG = 4
EARLY = 4


def back_kernel(groups, rows, tp, cp, seq, dq_hbm, dkv_hbm, x_hbm, dy_hbm, o_old, n_hbm, wq_hbm, wk_hbm, wv_hbm, wo_hbm, gain_ref,
                gx_hbm, y_hbm, ga_hbm, gb_hbm, gg_ref, o_out,
                wq_ref, wk_ref, wv_ref, wo_ref, dq_all, dkv_all, o_t, part, rs_r, rs_l, send_r, send_l, tot, gx_buf,
                o_in, x_in, xo_in, dyo_in, y_buf, n_in, dy_in, away, part_in, mine, gain_all,
                w_sem, in_sem, fin_sem, job_sem, y_sem, own_sem, rss_r, rss_l, rsr_r, rsr_l, ag0_r, ag0_l, agf_r, agf_l, agr_r, agr_l,
                away_send, away_recv, mine_own, mine_part, mine_chip, ga_recv, chip_recv, gb_send, gb_recv, gs_sem, gr_sem, late_send, late_recv):
    o_hbm = o_out
    z = lax.axis_index("tp")
    r = lax.axis_index("cp")
    core = lax.rem(r, 2)
    chip = lax.div(r, 2)
    last = tp - 1
    slots = tp - 1
    span = tp * rows
    tokens, d_model = x_hbm.shape
    hidden = dq_hbm.shape[1]
    chunk = min(512, d_model)
    blocks = ga_hbm.shape[0]
    width = ga_hbm.shape[1]
    pairs = blocks // 2
    partner = {"cp": r + 1 - 2 * core}
    peer = {"cp": r + 2 - 4 * chip}

    head = min(EARLY, groups) * span
    weight_loads = [pltpu.make_async_copy(src, dst, w_sem.at[k]) for k, (src, dst) in enumerate((
        (dq_hbm.at[:head, :], dq_all.at[:head, :]), (dkv_hbm.at[:, :head, :], dkv_all.at[:, :head, :]), (wq_hbm, wq_ref), (wk_hbm, wk_ref), (wv_hbm, wv_ref)))]
    rest_loads = [] if head == tokens else [
        pltpu.make_async_copy(dq_hbm.at[head:, :], dq_all.at[head:, :], w_sem.at[6]),
        pltpu.make_async_copy(dkv_hbm.at[:, head:, :], dkv_all.at[:, head:, :], w_sem.at[7]),
    ]
    out_loads = [pltpu.make_async_copy(wo_hbm, wo_ref, w_sem.at[5])]
    for copy in weight_loads:
        copy.start()

    barrier = pltpu.get_barrier_semaphore()
    peers = [(dt, dc) for dt in range(tp) for dc in range(cp) if dt or dc]
    for dt, dc in peers:
        pl.semaphore_signal(barrier, inc=1, device_id={"tp": lax.rem(z + dt, tp), "cp": lax.rem(r + dc, cp)}, device_id_type=MESH)

    def remote(src, dst, ssem, rsem, dev):
        return pltpu.make_async_remote_copy(src_ref=src, dst_ref=dst, send_sem=ssem, recv_sem=rsem, device_id=dev, device_id_type=MESH)

    right = {"tp": jnp.where(z < last, z + 1, z)}
    left = {"tp": jnp.where(z > 0, z - 1, z)}

    def group_rows(i):
        return pl.ds(pl.multiple_of(i * span, span), span)

    def tile_rows(i, owner):
        return pl.ds(pl.multiple_of(i * span + owner * rows, rows), rows)

    def inputs(i, slot):
        g = group_rows(i)
        return [
            pltpu.make_async_copy(o_hbm.at[:, g, :], o_in.at[slot], in_sem.at[slot, 0]),
            pltpu.make_async_copy(x_hbm.at[g, :], x_in.at[slot], in_sem.at[slot, 1]),
        ]

    def final_inputs(i, slot):
        g = tile_rows(i, z)
        return [
            pltpu.make_async_copy(x_hbm.at[g, :], xo_in.at[slot], fin_sem.at[slot, 0]),
            pltpu.make_async_copy(dy_hbm.at[g, :], dyo_in.at[slot], fin_sem.at[slot, 1]),
        ]

    def y_copy(i, slot):
        return pltpu.make_async_copy(y_buf.at[slot], y_hbm.at[group_rows(i), :], y_sem.at[slot])

    def rs_copy(i, s, to_right):
        ring = lax.rem(i, RS_RING)
        if to_right:
            return remote(send_r.at[s], rs_r.at[ring, s], rss_r.at[s], rsr_r.at[ring, s], right)
        return remote(send_l.at[s], rs_l.at[ring, s], rss_l.at[s], rsr_l.at[ring, s], left)

    def rs_send(i, s):
        for to_right in (True, False):
            far = z if to_right else last - z
            owner = (z + slots - s) if to_right else (z - slots + s)
            buf, held = (send_r, rs_r) if to_right else (send_l, rs_l)

            @pl.when(jnp.logical_and(jnp.logical_and(i >= 0, i < groups), jnp.logical_and(far <= s, far < last)))
            def _(to_right=to_right, far=far, owner=owner, buf=buf, held=held):
                @pl.when(i > 0)
                def _():
                    rs_copy(i - 1, s, to_right).wait_send()

                cur = lax.rem(i, PART_RING)
                own = pl.ds(pl.multiple_of(owner * rows, rows), rows)
                if s == 0:
                    buf[s] = part[cur, own, :].astype(BF16)
                else:
                    @pl.when(far == 0)
                    def _():
                        buf[s] = part[cur, own, :].astype(BF16)

                    @pl.when(far > 0)
                    def _():
                        rs_copy(i, s - 1, to_right).wait_recv()
                        buf[s] = (part[cur, own, :] + held[lax.rem(i, RS_RING), s - 1].astype(F32)).astype(BF16)

                rs_copy(i, s, to_right).start()

    def ag_own(i, slot, to_right):
        src = gx_buf.at[slot]
        dst = gx_hbm.at[tile_rows(i, z), :]
        if to_right:
            return remote(src, dst, ag0_r.at[slot], agr_r.at[i, 0], right)
        return remote(src, dst, ag0_l.at[slot], agr_l.at[i, 0], left)

    def own_copy(i, slot):
        return pltpu.make_async_copy(gx_buf.at[slot], gx_hbm.at[tile_rows(i, z), :], own_sem.at[slot])

    def ag_forward(i, a, to_right):
        owner = z - a if to_right else z + a
        tile = gx_hbm.at[tile_rows(i, owner), :]
        if to_right:
            return remote(tile, tile, agf_r.at[a], agr_r.at[i, a], right)
        return remote(tile, tile, agf_l.at[a], agr_l.at[i, a], left)

    def ag_wait(i, a, to_right):
        tile = gx_hbm.at[tile_rows(i, 0), :]
        sem = agr_r.at[i, a] if to_right else agr_l.at[i, a]
        remote(tile, tile, agf_r.at[a], sem, right).wait_recv()

    def ag_step(i, a):
        for to_right in (True, False):
            far = z if to_right else last - z

            @pl.when(jnp.logical_and(jnp.logical_and(i >= 0, i < groups), far >= a))
            def _(to_right=to_right, far=far):
                ag_wait(i, a - 1, to_right)
                if a < slots:
                    @pl.when(far < last)
                    def _():
                        @pl.when(i > 0)
                        def _():
                            ag_forward(i - 1, a, to_right).wait_send()

                        ag_forward(i, a, to_right).start()

    def ag_first(i, slot):
        own_copy(i, slot).start()
        for to_right in (True, False):
            far = z if to_right else last - z

            @pl.when(far < last)
            def _(to_right=to_right):
                ag_own(i, slot, to_right).start()

    def ag_first_done(i, slot):
        own_copy(i, slot).wait()
        for to_right in (True, False):
            far = z if to_right else last - z

            @pl.when(far < last)
            def _(to_right=to_right):
                ag_own(i, slot, to_right).wait_send()

    def partial_norm(i):
        cur = lax.rem(i, PART_RING)
        g = group_rows(i)
        for c in range(0, d_model, chunk):
            cols = slice(c, c + chunk)
            part[cur, :, cols] = (
                dot_nt(dq_all[g, :], wq_ref[cols, :]) + dot_nt(dkv_all[0, g, :], wk_ref[cols, :]) + dot_nt(dkv_all[1, g, :], wv_ref[cols, :])
            )

    def project_out(cur):
        for c in range(0, d_model, chunk):
            cols = slice(c, c + chunk)
            acc = x_in[cur, :, cols].astype(F32)
            for t in range(tp):
                acc += dot_nn(o_in[cur, t], wo_ref[t, :, cols])
            y_buf[cur, :, cols] = acc.astype(BF16)

    def finalize(i):
        slot = lax.rem(i, 2)
        own = pl.ds(pl.multiple_of(z * rows, rows), rows)
        tot[...] = part[lax.rem(i, PART_RING), own, :]

        @pl.when(z > 0)
        def _():
            rs_copy(i, slots - 1, True).wait_recv()
            tot[...] += rs_r[lax.rem(i, RS_RING), slots - 1].astype(F32)

        @pl.when(z < last)
        def _():
            rs_copy(i, slots - 1, False).wait_recv()
            tot[...] += rs_l[lax.rem(i, RS_RING), slots - 1].astype(F32)

        @pl.when(i > 1)
        def _():
            ag_first_done(i - 2, slot)

        for copy in final_inputs(i, slot):
            copy.wait()
        x = xo_in[slot].astype(F32)
        centred = x - jnp.mean(x, axis=-1, keepdims=True)
        inv_std = lax.rsqrt(jnp.mean(centred * centred, axis=-1, keepdims=True) + LN_EPS)
        x_hat = centred * inv_std
        dn = tot[...]
        gg_ref[...] += jnp.sum(dn * x_hat, axis=0, keepdims=True)
        d_hat = dn * gain_ref[...]
        dx = inv_std * (d_hat - jnp.mean(d_hat, axis=-1, keepdims=True) - x_hat * jnp.mean(d_hat * x_hat, axis=-1, keepdims=True))
        gx_buf[slot] = (dyo_in[slot].astype(F32) + dx).astype(BF16)
        ag_first(i, slot)

    def block_of(t):
        return 2 * lax.div(t, 2) + jnp.where(lax.rem(t, 2) == 0, 1 - core, core)

    def job_loads(t, slot):
        cols = pl.ds(pl.multiple_of(block_of(t) * width, width), width)
        return [
            pltpu.make_async_copy(n_hbm.at[:, cols], n_in.at[slot], job_sem.at[slot, 0]),
            pltpu.make_async_copy(dy_hbm.at[:, cols], dy_in.at[slot], job_sem.at[slot, 1]),
        ]

    def away_copy(p):
        ring = lax.rem(p, 2)
        return remote(away, part_in.at[ring], away_send.at[0], away_recv.at[ring], partner)

    def job_block(t, put):
        slot = lax.rem(t, 2)
        n_t = n_in[slot].T
        put(0, hidden, dot_nn(n_t, dq_all[...]))
        put(hidden, hidden, dot_nn(n_t, dkv_all[0]))
        put(2 * hidden, hidden, dot_nn(n_t, dkv_all[1]))
        for k in range(hidden // width):
            put(3 * hidden + k * width, width, dot_nn(o_t[k * width:(k + 1) * width, :], dy_in[slot]))

    def mine_to_own(p, slot):
        return pltpu.make_async_copy(mine.at[slot], ga_hbm.at[2 * p + core], mine_own.at[slot])

    def mine_to_part(p, slot):
        return remote(mine.at[slot], ga_hbm.at[2 * p + core], mine_part.at[slot], ga_recv.at[p], partner)

    def mine_to_chip(p, slot):
        return remote(mine.at[slot], gb_hbm.at[2 * p + core], mine_chip.at[slot], chip_recv.at[p], peer)

    def mine_done(p, slot):
        mine_to_own(p, slot).wait()
        mine_to_part(p, slot).wait_send()
        mine_to_chip(p, slot).wait_send()

    def chip_forward(p):
        b = 2 * p + core
        return remote(gb_hbm.at[b], gb_hbm.at[b], gb_send.at[p], gb_recv.at[p], partner)

    def job(t):
        p = lax.div(t, 2)
        for copy in job_loads(t, lax.rem(t, 2)):
            copy.wait()

        @pl.when(t + 1 < blocks)
        def _():
            for copy in job_loads(t + 1, 1 - lax.rem(t, 2)):
                copy.start()

        @pl.when(lax.rem(t, 2) == 0)
        def _():
            @pl.when(p > 0)
            def _():
                away_copy(p - 1).wait_send()

            def put(at, size, value):
                away[:, at:at + size] = value

            job_block(t, put)
            away_copy(p).start()

        @pl.when(lax.rem(t, 2) == 1)
        def _():
            slot = lax.rem(p, 2)
            away_copy(p).wait_recv()

            @pl.when(p > 1)
            def _():
                mine_done(p - 2, slot)

            def put(at, size, value):
                mine[slot, :, at:at + size] = (value + part_in[slot, :, at:at + size]).astype(BF16)

            job_block(t, put)
            mine_to_chip(p, slot).start()
            mine_to_part(p, slot).start()
            mine_to_own(p, slot).start()

    gg_ref[...] = jnp.zeros_like(gg_ref)
    o_loads = [pltpu.make_async_copy(o_hbm.at[z, :, k * width:(k + 1) * width], n_in.at[k], job_sem.at[k, 0]) for k in range(hidden // width)]
    me = z * cp + r

    def gain_copy(dt, dc):
        to = {"tp": lax.rem(z + dt, tp), "cp": lax.rem(r + dc, cp)}
        return remote(gain_all.at[me], gain_all.at[me], gs_sem.at[dt * cp + dc], gr_sem.at[me], to)

    def gain_wait(dt, dc):
        sender = lax.rem(z + dt, tp) * cp + lax.rem(r + dc, cp)
        remote(gain_all.at[sender], gain_all.at[sender], gs_sem.at[0], gr_sem.at[sender], right).wait_recv()

    units = tokens // seq * HALVES
    half = hidden // HALVES
    late_units = range(max(0, units - LATE), units)
    late_wait = max(0, late_units[0] // HALVES * seq // span + OUT_LAG - 2)
    sends_late = jnp.logical_or(z == 1, z == last - 1)
    gets_late = jnp.logical_or(z == 0, z == last)

    def late_copy(n, src, dst):
        u = late_units[n]
        place = o_out.at[src, u // HALVES * seq:(u // HALVES + 1) * seq, u % HALVES * half:(u % HALVES + 1) * half]
        return remote(place, place, late_send.at[n], late_recv.at[n], {"tp": dst})

    def late_move(n):
        return late_copy(n, z, jnp.where(z == 1, 0, last))

    for copy in weight_loads:
        copy.wait()
    for copy in inputs(0, 0) + o_loads + rest_loads + out_loads:
        copy.start()
    partial_norm(0)
    pl.semaphore_wait(barrier, len(peers))
    for n in range(len(late_units)):
        @pl.when(sends_late)
        def _(n=n):
            late_move(n).start()

    def step(i, carry):
        @pl.when(jnp.logical_and(gets_late, i == late_wait))
        def _():
            for n in range(len(late_units)):
                late_copy(n, jnp.where(z == 0, 1, last - 1), z).wait_recv()

        for a in reversed(range(1, slots + 1)):
            ag_step(i - slots - a, a)

        @pl.when(i == OUT_LAG)
        def _():
            for copy in out_loads:
                copy.wait()

        @pl.when(jnp.logical_and(i >= OUT_LAG, i < groups + OUT_LAG))
        def _():
            j = i - OUT_LAG
            at = lax.rem(j, 2)
            for copy in inputs(j, at):
                copy.wait()

            @pl.when(j + 1 < groups)
            def _():
                for copy in inputs(j + 1, 1 - at):
                    copy.start()

            @pl.when(j >= 2)
            def _():
                y_copy(j - 2, at).wait()

            project_out(at)
            y_copy(j, at).start()

        @pl.when(jnp.logical_and(i >= slots, i < groups + slots))
        def _():
            finalize(i - slots)

        @pl.when(i == groups + slots - 1)
        def _():
            gain_all[me] = gg_ref[...]
            for dt, dc in peers:
                gain_copy(dt, dc).start()

        @pl.when(jnp.logical_and(i >= slots - 1, i < groups + slots - 1))
        def _():
            for copy in final_inputs(i - slots + 1, lax.rem(i - slots + 1, 2)):
                copy.start()

        @pl.when(i == EARLY)
        def _():
            for copy in rest_loads:
                copy.wait()

        @pl.when(jnp.logical_and(i >= 1, i < groups))
        def _():
            partial_norm(i)

        @pl.when(i == JOB_LAG - 1)
        def _():
            for k, copy in enumerate(o_loads):
                copy.wait()
                o_t[k * width:(k + 1) * width, :] = n_in[k].T
            for copy in job_loads(0, 0):
                copy.start()

        @pl.when(jnp.logical_and(i >= JOB_LAG, i < JOB_LAG + blocks))
        def _():
            job(i - JOB_LAG)

        for k in reversed(range(slots)):
            rs_send(i - k, k)

        @pl.when(jnp.logical_and(lax.rem(i, 2) == 1, jnp.logical_and(i >= FORWARD_LAG, i < FORWARD_LAG + 2 * pairs)))
        def _():
            p = lax.div(i - FORWARD_LAG, 2)
            mine_to_chip(p, 0).wait_recv()
            chip_forward(p).start()

        return carry

    lax.fori_loop(0, max(groups + 2 * slots, groups + OUT_LAG, blocks + JOB_LAG, 2 * pairs + FORWARD_LAG - 1), step, 0)

    for i in (groups - 2, groups - 1):
        y_copy(i, i % 2).wait()
        ag_first_done(i, i % 2)
    for to_right in (True, False):
        far = z if to_right else last - z
        for s in range(slots):
            @pl.when(jnp.logical_and(far <= s, far < last))
            def _(s=s, to_right=to_right):
                rs_copy(groups - 1, s, to_right).wait_send()
        for a in range(1, slots):
            @pl.when(jnp.logical_and(far >= a, far < last))
            def _(a=a, to_right=to_right):
                ag_forward(groups - 1, a, to_right).wait_send()
    for n in range(len(late_units)):
        @pl.when(sends_late)
        def _(n=n):
            late_move(n).wait_send()

    away_copy(pairs - 1).wait_send()
    for p in range(max(0, pairs - 2), pairs):
        mine_done(p, p % 2)
    for p in range(pairs):
        chip_forward(p).wait_send()
        chip_forward(p).wait_recv()
        mine_to_part(p, 0).wait_recv()
    for dt, dc in peers:
        gain_wait(dt, dc)
        gain_copy(dt, dc).wait_send()
    total = gain_all[0]
    for j in range(1, tp * cp):
        total += gain_all[j]
    gg_ref[...] = total


def backward_norm(dq, dkv, x, dy, o_all, normed, wq, wk, wv, wo_all, gain, rows, seq, tp, cp):
    tokens, hidden = dq.shape
    d_model = x.shape[1]
    span = tp * rows
    groups = tokens // span
    slots = tp - 1
    width = WIDTH
    blocks = d_model // width
    pairs = blocks // 2
    hbm = pl.BlockSpec(memory_space=pl.ANY)
    vmem = pl.BlockSpec(memory_space=pltpu.VMEM)
    dma = pltpu.SemaphoreType.DMA
    bf = lambda *shape: pltpu.VMEM(shape, BF16)
    f32 = lambda *shape: pltpu.VMEM(shape, F32)
    return pl.pallas_call(
        functools.partial(back_kernel, groups, rows, tp, cp, seq),
        in_specs=[hbm] * 10 + [vmem],
        out_specs=[hbm, hbm, hbm, hbm, vmem, hbm],
        input_output_aliases={4: 5},
        out_shape=[
            jax.ShapeDtypeStruct((tokens, d_model), BF16),
            jax.ShapeDtypeStruct((tokens, d_model), BF16),
            jax.ShapeDtypeStruct((blocks, width, 4 * hidden), BF16),
            jax.ShapeDtypeStruct((blocks, width, 4 * hidden), BF16),
            jax.ShapeDtypeStruct((1, d_model), F32),
            jax.ShapeDtypeStruct(o_all.shape, BF16),
        ],
        scratch_shapes=[
            bf(d_model, hidden), bf(d_model, hidden), bf(d_model, hidden), bf(tp, hidden, d_model),
            bf(tokens, hidden), bf(2, tokens, hidden), bf(hidden, tokens),
            f32(PART_RING, span, d_model), bf(RS_RING, slots, rows, d_model), bf(RS_RING, slots, rows, d_model),
            bf(slots, rows, d_model), bf(slots, rows, d_model), f32(rows, d_model), bf(2, rows, d_model),
            bf(2, tp, span, hidden), bf(2, span, d_model), bf(2, rows, d_model), bf(2, rows, d_model), bf(2, span, d_model),
            bf(2, tokens, width), bf(2, tokens, width),
            f32(width, 4 * hidden), f32(2, width, 4 * hidden), bf(2, width, 4 * hidden), f32(tp * cp, 1, d_model),
            dma((8,)), dma((2, 2)), dma((2, 2)), dma((2, 2)), dma((2,)), dma((2,)),
            dma((slots,)), dma((slots,)), dma((RS_RING, slots)), dma((RS_RING, slots)),
            dma((2,)), dma((2,)), dma((slots,)), dma((slots,)), dma((groups, slots)), dma((groups, slots)),
            dma((1,)), dma((2,)), dma((2,)), dma((2,)), dma((2,)), dma((pairs,)), dma((pairs,)), dma((pairs,)), dma((pairs,)),
            dma((tp * cp,)), dma((tp * cp,)), dma((max(LATE, 1),)), dma((max(LATE, 1),)),
        ],
        compiler_params=pltpu.CompilerParams(collective_id=0, has_side_effects=True, vmem_limit_bytes=63 << 20),
        cost_estimate=pl.CostEstimate(flops=22 * tokens * hidden * d_model, bytes_accessed=16 * tokens * d_model, transcendentals=0),
        name="backward_norm",
    )(dq, dkv, x, dy, o_all, normed, wq, wk, wv, wo_all, gain)


def finish_kernel(y_ref, gx_ref, ga_ref, gb_ref, gg_ref, yo_ref, gxo_ref, wq_ref, wk_ref, wv_ref, wo_ref, ggo_ref):
    ggo_ref[...] = gg_ref[...]
    yo_ref[...] = y_ref[...]
    gxo_ref[...] = gx_ref[...]
    rows = ga_ref.shape[1]
    width = rows * PARTS
    hidden = wq_ref.shape[1]
    for k, ref in enumerate((wq_ref, wk_ref, wv_ref)):
        cols = slice(k * hidden, (k + 1) * hidden)
        ref[...] = ga_ref[0, :, cols].astype(F32) + gb_ref[0, :, cols].astype(F32)
    for k in range(hidden // width):
        cols = slice(3 * hidden + k * width, 3 * hidden + (k + 1) * width)
        at = k * width + lax.rem(pl.program_id(0), PARTS) * rows
        wo_ref[pl.ds(pl.multiple_of(at, rows), rows), :] = ga_ref[0, :, cols].astype(F32) + gb_ref[0, :, cols].astype(F32)


def finish(y, gx, ga, gb, gg):
    tokens, d_model = y.shape
    blocks, width, packed = ga.shape
    hidden = packed // 4
    steps = blocks * PARTS
    tile = pl.BlockSpec((tokens // steps, d_model), lambda j: (j, 0))
    block = pl.BlockSpec((1, width // PARTS, packed), lambda j: (j // PARTS, j % PARTS, 0))
    wide = pl.BlockSpec((width // PARTS, hidden), lambda j: (j, 0))
    line = pl.BlockSpec((1, d_model), lambda j: (0, 0))
    return pl.pallas_call(
        finish_kernel,
        grid=(steps,),
        in_specs=[tile, tile, block, block, line],
        out_specs=[tile, tile, wide, wide, wide, pl.BlockSpec((hidden, width), lambda j: (0, j // PARTS)), line],
        out_shape=[jax.ShapeDtypeStruct((tokens, d_model), BF16)] * 2 + [jax.ShapeDtypeStruct((d_model, hidden), F32)] * 3 + [jax.ShapeDtypeStruct((hidden, d_model), F32), jax.ShapeDtypeStruct((1, d_model), F32)],
        compiler_params=pltpu.CompilerParams(dimension_semantics=("arbitrary",), vmem_limit_bytes=48 << 20),
        cost_estimate=pl.CostEstimate(flops=8 * d_model * hidden, bytes_accessed=8 * tokens * d_model + 32 * d_model * hidden, transcendentals=0),
        name="finish",
    )(y, gx, ga, gb, gg)


def solution(mesh):
    cp_size = mesh.shape["cp"]
    tp_size = mesh.shape["tp"]

    def device_step(x_in, segment_ids, positions, w_query, w_key, w_value, w_out, norm_gain, grad_out):
        batch, seq, d_model = x_in.shape
        tokens = batch * seq
        x = x_in.reshape(tokens, d_model)
        dy = grad_out.reshape(tokens, d_model)

        gain = norm_gain.reshape(1, d_model)
        normed, o_all, dq, dkv, w_all = front(x, dy, w_query, w_key, w_value, w_out, positions, jnp.asarray(angle_table(), BF16), gain, seq, tp_size, cp_size)
        grad_x, y_out, sum_a, sum_b, grad_gain, _ = backward_norm(dq, dkv, x, dy, o_all, normed, w_query, w_key, w_value, w_all, gain, ROWS, seq, tp_size, cp_size)
        y_out, grad_x, grad_wq, grad_wk, grad_wv, grad_wo, grad_gain = finish(y_out, grad_x, sum_a, sum_b, grad_gain)
        grad_gain = grad_gain.reshape(d_model)
        return y_out.reshape(x_in.shape), grad_x.reshape(x_in.shape), grad_gain, grad_wq, grad_wk, grad_wv, grad_wo

    in_specs = (P("dp", "cp", None), P("dp", "cp"), P("dp", "cp"), P(None, "tp"), P(None, "tp"), P(None, "tp"), P("tp", None), P(None), P("dp", "cp", None))
    out_specs = (P("dp", "cp", None), P("dp", "cp", None), P("dp"), P("dp", "tp"), P("dp", "tp"), P("dp", "tp"), P(("dp", "tp"), None))
    return jax.shard_map(device_step, mesh=mesh, in_specs=in_specs, out_specs=out_specs, check_vma=False)
```

```python
import functools
import math

import jax
import jax.numpy as jnp
import numpy as np
from jax import lax
from jax.experimental import pallas as pl
from jax.experimental.pallas import tpu as pltpu
from jax.sharding import PartitionSpec as P

HEAD_DIM = 128
ROPE_THETA = 8000000.0
LN_EPS = 1e-5
NEG_BIG = -1e30
SCALE = HEAD_DIM ** -0.5
EXP2_SCALE = SCALE * math.log2(math.e)
F32 = jnp.float32
BF16 = jnp.bfloat16
NT = (((1,), (1,)), ((), ()))


def dot_nn(a, b):
    return jnp.dot(a, b, preferred_element_type=F32)


def dot_nt(a, b):
    return lax.dot_general(a, b, NT, preferred_element_type=F32)


def dot_tn(a, b):
    return lax.dot_general(a, b, (((0,), (0,)), ((), ())), preferred_element_type=F32)


def swap_pairs(t, sign):
    lane = lax.broadcasted_iota(jnp.int32, t.shape, 1)
    even = (lane % 2) == 0
    up = pltpu.roll(t, HEAD_DIM - 1, 1)
    down = pltpu.roll(t, 1, 1)
    return jnp.where(even, -up, down) if sign > 0 else jnp.where(even, up, -down)


def rope(t, cos_t, sin_t, sign):
    return t * cos_t + swap_pairs(t, sign) * sin_t


def angle_table():
    inv_freq = ROPE_THETA ** (-np.arange(0, HEAD_DIM, 2, dtype=np.float32) / np.float32(HEAD_DIM))
    freq = np.repeat(inv_freq.astype(np.float64), 2)[None, :]
    low = np.arange(POS_LOW)[:, None] * freq
    high = POS_LOW * np.arange(HEAD_DIM - POS_LOW)[:, None] * freq
    table = np.zeros((HEAD_DIM, 12 * HEAD_DIM), np.float32)
    for k, (first, value) in enumerate(((0, np.cos(low)), (0, np.sin(low)), (POS_LOW, np.cos(high)), (POS_LOW, np.sin(high)))):
        rest = value.astype(np.float32)
        for p in range(3):
            piece = rest.astype(BF16).astype(np.float32)
            at = (3 * k + p) * HEAD_DIM
            table[first:first + value.shape[0], at:at + HEAD_DIM] = piece
            rest = rest - piece
    return table


def put_rope(dst, raw, cos_t, sin_t):
    for h in range(raw.shape[1] // HEAD_DIM):
        cols = slice(h * HEAD_DIM, (h + 1) * HEAD_DIM)
        dst[:, cols] = rope(raw[:, cols], cos_t, sin_t, 1.0).astype(BF16)


MESH = pl.DeviceIdType.MESH
SUB = 384
ROWS = 32
WIDTH = 256
PARTS = 1
HALVES = 2
RELAY_LAG = 1
LATE = 3
SUM_LAG = 4
CHIP_BUFS = 4
OWN_RING = 6
Q_RING = 3
AHEAD = 2
POS_LOW = 64
W_TWIN = 1
W_PARTNER = 3
W_CHIP = 7


def front_kernel(batch, seq, tp, cp, x_hbm, dy_hbm, wq_hbm, wk_hbm, wv_hbm, wo_hbm, pos_ref, table_ref, gain_ref,
                 n_hbm, o_all, dq_hbm, dkv_hbm, w_all,
                 big, wo_ref, cos_ref, sin_ref, q_ring, do_ring, x_in, dy_in, n_buf, kv_own, kvr, s_scr, dp_scr, m_scr, l_scr, d_scr, ot_scr, dqt_scr,
                 o_buf, dq_buf, g_own, g_part, g_chip, g_far, xin, part_in,
                 w_sem, wl_sem, wz_send, wz_recv, wx_send, wx_recv,
                 x_sem, dy_sem, n_sem, kvs_part, kvs_chip, kvs_far, kv_recv, o_local, o_send, o_recv, relay_send, dq_sem,
                 far_send, part_send, chip_send, x_recv, part_recv, dkv_sem):
    z = lax.axis_index("tp")
    r = lax.axis_index("cp")
    dp = lax.axis_index("dp")
    core = lax.rem(r, 2)
    chip = lax.div(r, 2)
    d_model = x_hbm.shape[1]
    hidden = wq_hbm.shape[1]
    heads = hidden // HEAD_DIM
    first_chip, second_chip = chip == 0, chip == 1
    first_core, second_core = core == 0, core == 1
    partner = {"cp": r + 1 - 2 * core}
    peer = {"cp": r + 2 - 4 * chip}
    twin = {"dp": 1 - dp}

    tile = x_in.shape[1]
    per_row = seq // tile

    def row(b):
        return pl.ds(pl.multiple_of(b * seq, seq), seq)

    def tile_rows(b, k):
        return pl.ds(pl.multiple_of(b * seq + k * tile, tile), tile)

    def x_load(b, k):
        return pltpu.make_async_copy(x_hbm.at[tile_rows(b, k), :], x_in.at[k], x_sem.at[k])

    def dy_load(b, k):
        return pltpu.make_async_copy(dy_hbm.at[tile_rows(b, k), :], dy_in.at[k], dy_sem.at[k])

    def n_store(b, k):
        return pltpu.make_async_copy(n_buf.at[k], n_hbm.at[tile_rows(b, k), :], n_sem.at[k])

    weight_loads = [pltpu.make_async_copy(src, dst, w_sem.at[k]) for k, (src, dst) in enumerate(((wk_hbm, big.at[0]), (wv_hbm, big.at[1]), (wq_hbm, big.at[2]), (wo_hbm, wo_ref)))]
    x_load(0, 0).start()
    for copy in weight_loads[:2]:
        copy.start()
    for k in range(1, per_row):
        x_load(0, k).start()
    for copy in weight_loads[2:]:
        copy.start()
    for k in range(per_row):
        dy_load(0, k).start()

    units = batch * HALVES
    half = hidden // HALVES

    def where(u):
        return lax.div(u, HALVES), lax.rem(u, HALVES)

    def half_cols(g):
        return pl.ds(pl.multiple_of(g * half, half), half)

    barrier = pltpu.get_barrier_semaphore()
    for dev in [partner, peer, twin] + [{"tp": lax.rem(z + dt, tp)} for dt in range(1, tp)]:
        pl.semaphore_signal(barrier, inc=1, device_id=dev, device_id_type=MESH)

    def remote(src, dst, ssem, rsem, dev):
        return pltpu.make_async_remote_copy(src_ref=src, dst_ref=dst, send_sem=ssem, recv_sem=rsem, device_id=dev, device_id_type=MESH)

    share = hidden // 8

    def share_rows(y, c, g):
        return pl.ds(pl.multiple_of((4 * y + 2 * c + g) * share, share), share)

    mine, twins = share_rows(chip, core, dp), share_rows(chip, core, 1 - dp)
    peers, peer_twins = share_rows(1 - chip, core, dp), share_rows(1 - chip, core, 1 - dp)

    def wz_copy(d):
        return remote(wo_hbm.at[mine, :], w_all.at[z, mine, :], wz_send.at[d], wz_recv.at[z], {"tp": lax.rem(z + d, tp)})

    def wz_wait(d):
        src = lax.rem(z + d, tp)
        remote(wo_hbm.at[mine, :], w_all.at[src, mine, :], wz_send.at[d], wz_recv.at[src], partner).wait_recv()

    def w_copy(k, d, rows, dev):
        place = w_all.at[lax.rem(z + d, tp), rows, :]
        return remote(place, place, wx_send.at[k, d], wx_recv.at[k, d], dev)

    def w_move(k, d):
        rows, dev = ((mine, twin), (mine, partner), (twins, partner), (mine, peer), (twins, peer), (peers, partner), (peer_twins, partner))[k]
        return w_copy(k, d, rows, dev)

    w_steps = range(1, tp)

    def kv_to_partner(u):
        return remote(kv_own.at[u], kvr.at[0, u], kvs_part.at[u], kv_recv.at[0, u], partner)

    def kv_to_chip(u):
        return remote(kv_own.at[u], kvr.at[1, u], kvs_chip.at[u], kv_recv.at[1, u], peer)

    def kv_forward(u):
        return remote(kvr.at[1, u], kvr.at[2, u], kvs_far.at[u], kv_recv.at[2, u], partner)

    w_local = pltpu.make_async_copy(wo_ref, w_all.at[z], wl_sem.at[0])

    def angles(b, k):
        rows = tile_rows(b, k)
        pos = jnp.broadcast_to(pos_ref[pl.ds(b, 1), k * tile:(k + 1) * tile], (HEAD_DIM, tile)).T
        lane = lax.broadcasted_iota(jnp.int32, (tile, HEAD_DIM), 1)
        low = lane < POS_LOW
        pick = jnp.where(low, lax.rem(pos, POS_LOW), POS_LOW + lax.div(pos, POS_LOW)) == lane
        found = dot_nn(jnp.where(pick, 1.0, 0.0).astype(BF16), table_ref[...])

        def part(k):
            at = 3 * k * HEAD_DIM
            return found[:, at:at + HEAD_DIM] + found[:, at + HEAD_DIM:at + 2 * HEAD_DIM] + found[:, at + 2 * HEAD_DIM:at + 3 * HEAD_DIM]

        cos_b, sin_b, cos_a, sin_a = part(0), part(1), part(2), part(3)
        cos_ref[rows, :] = cos_a * cos_b - sin_a * sin_b
        sin_ref[rows, :] = sin_a * cos_b + cos_a * sin_b

    def project_row(b, first=False):
        ring = lax.rem(b, Q_RING)
        for k in range(per_row):
            rows = tile_rows(b, k)
            inside = slice(k * tile, (k + 1) * tile)
            x_load(b, k).wait()

            @pl.when(b > 0)
            def _(k=k):
                n_store(b - 1, k).wait()

            angles(b, k)
            x = x_in[k].astype(F32)
            centred = x - jnp.mean(x, axis=-1, keepdims=True)
            inv_std = lax.rsqrt(jnp.mean(centred * centred, axis=-1, keepdims=True) + LN_EPS)
            n_buf[k] = ((centred * inv_std) * gain_ref[...]).astype(BF16)
            n_store(b, k).start()

            @pl.when(b + 1 < batch)
            def _(k=k):
                x_load(b + 1, k).start()

            if first and k == 0:
                for copy in weight_loads[:2]:
                    copy.wait()
            for g in range(HALVES):
                u = b * HALVES + g
                cols = slice(g * half, (g + 1) * half)
                put_rope(kv_own.at[u, 0, inside, :], dot_nn(n_buf[k], big[0, :, cols]), cos_ref[rows, :], sin_ref[rows, :])
                kv_own[u, 1, inside, :] = dot_nn(n_buf[k], big[1, :, cols]).astype(BF16)

        if first:
            pl.semaphore_wait(barrier, tp + 2)
        for g in range(HALVES):
            u = b * HALVES + g

            @pl.when(first_chip)
            def _(u=u):
                kv_to_chip(u).start()

            @pl.when(first_core)
            def _(u=u):
                kv_to_partner(u).start()

        if first:
            for d in range(1, tp):
                wz_copy(d).start()
            for copy in weight_loads[2:]:
                copy.wait()
            w_local.start()

        for k in range(per_row):
            rows = tile_rows(b, k)
            inside = slice(k * tile, (k + 1) * tile)
            dy_load(b, k).wait()
            put_rope(q_ring.at[ring, inside, :], dot_nn(n_buf[k], big[2]), cos_ref[rows, :], sin_ref[rows, :])
            do_ring[ring, inside, :] = dot_nt(dy_in[k], wo_ref[...]).astype(BF16)

            @pl.when(b + 1 < batch)
            def _(k=k):
                dy_load(b + 1, k).start()

    def o_place(src, u):
        b, g = where(u)
        return o_all.at[src, b, g]

    def o_local_copy(b):
        return pltpu.make_async_copy(o_buf.at[b], o_place(z, b), o_local.at[b])

    def o_copy(b, k, step):
        return remote(o_buf.at[b], o_place(z, b), o_send.at[k, b], o_recv.at[z, b], {"tp": jnp.clip(z + step, 0, tp - 1)})

    hops = [(k, step, jnp.logical_and(z + step >= 0, z + step < tp)) for k, step in enumerate((1, -1))]

    def far_from_end(step):
        return jnp.logical_and(z + step != 0, z + step != tp - 1)

    def o_start(b):
        o_local_copy(b).start()
        for k, step, ok in hops:
            @pl.when(jnp.logical_and(ok, jnp.logical_or(b < units - LATE, far_from_end(step))))
            def _(k=k, step=step):
                o_copy(b, k, step).start()

    def o_arrived(src, b):
        remote(o_place(src, b), o_place(src, b), relay_send.at[0, 0, b], o_recv.at[src, b], partner).wait_recv()

    def relay_copy(b, age, step):
        src = jnp.clip(z - age * step, 0, tp - 1)
        return remote(o_place(src, b), o_place(src, b), relay_send.at[age - 1, (1 - step) // 2, b], o_recv.at[src, b], {"tp": jnp.clip(z + step, 0, tp - 1)})

    def relays(age, step):
        far = z if step > 0 else tp - 1 - z
        return jnp.logical_and(far >= age, far < tp - 1)

    def relay(b, age):
        for step in (1, -1):
            @pl.when(relays(age, step))
            def _(step=step):
                o_arrived(jnp.clip(z - age * step, 0, tp - 1), b)
                relay_copy(b, age, step).start()

    def far_copy(b, par):
        return remote(g_far.at[par], xin.at[b], far_send.at[par], x_recv.at[b], partner)

    def part_copy(b, par):
        return remote(g_part.at[par], part_in.at[b], part_send.at[par], part_recv.at[b], partner)

    def chip_copy(b):
        par = lax.rem(b, CHIP_BUFS)
        return remote(g_chip.at[par], xin.at[b], chip_send.at[par], x_recv.at[b], peer)

    def chip_sum(b):
        @pl.when(second_chip)
        def _():
            par = lax.rem(b, CHIP_BUFS)
            far_copy(b, 0).wait_recv()
            g_chip[par] = (g_chip[par].astype(F32) + xin[b].astype(F32)).astype(BF16)
            chip_copy(b).start()

    def dkv_store(u, which):
        b, g = where(u)
        return pltpu.make_async_copy(g_own.at[lax.rem(u, OWN_RING), which], dkv_hbm.at[which, row(b), half_cols(g)], dkv_sem.at[u, which])

    def key_grads(u):
        @pl.when(first_core)
        def _():
            part_copy(u, 0).wait_recv()

        @pl.when(first_chip)
        def _():
            chip_copy(u).wait_recv()

        b, g = where(u)
        rows = row(b)
        for which in range(2):
            for h in range(half // HEAD_DIM):
                cols = slice(h * HEAD_DIM, (h + 1) * HEAD_DIM)
                own = g_own.at[lax.rem(u, OWN_RING), which, :, cols]
                acc = own[...].astype(F32)
                acc = acc + jnp.where(first_core, part_in[u, which, :, cols].astype(F32), 0.0)
                acc = (acc + jnp.where(first_chip, xin[u, which, :, cols].astype(F32), 0.0)).astype(BF16)
                if which == 0:
                    acc = rope(acc.astype(F32), cos_ref[rows, :], sin_ref[rows, :], -1.0).astype(BF16)
                own[...] = acc
            dkv_store(u, which).start()

    def dq_store(b, par):
        return pltpu.make_async_copy(dq_buf.at[par], dq_hbm.at[row(where(b)[0]), half_cols(where(b)[1])], dq_sem.at[par])

    subs = range(0, seq, SUB)

    def attend_unit(i, par):
        b, g = where(i)
        rows = row(b)
        ring = lax.rem(b, Q_RING)
        start = r * seq + lax.broadcasted_iota(jnp.int32, (1, seq), 1) - pos_ref[pl.ds(b, 1), :]
        chip_par = lax.rem(i, CHIP_BUFS)
        keys_of = [kv_own.at[i]] + [kvr.at[s, i] for s in range(3)]
        places = [g_part.at[par], g_chip.at[chip_par], g_far.at[par]]

        def grad(slot, which, cols):
            return places[slot - 1].at[which, :, cols] if slot else g_own.at[lax.rem(i, OWN_RING), which, :, cols]

        live = [None, second_core, second_chip, second_chip]
        piece = [r, r + 1 - 2 * core, r + 2 - 4 * chip, r + 3 - 2 * core - 4 * chip]

        def each(body):
            body(0)
            for slot in (1, 2, 3):
                pl.when(live[slot])(functools.partial(body, slot))

        def one_head(h, carry):
            cols = pl.ds(pl.multiple_of(h * HEAD_DIM, HEAD_DIM), HEAD_DIM)
            full = pl.ds(pl.multiple_of(g * half + h * HEAD_DIM, HEAD_DIM), HEAD_DIM)
            q = q_ring[ring, :, full]
            do = do_ring[ring, :, full]
            m_scr[...] = jnp.full(m_scr.shape, NEG_BIG, F32)
            l_scr[...] = jnp.zeros_like(l_scr)
            d_scr[...] = jnp.zeros_like(d_scr)
            ot_scr[...] = jnp.zeros_like(ot_scr)
            dqt_scr[...] = jnp.zeros_like(dqt_scr)

            def scores(slot):
                base = piece[slot] * seq
                top = None
                for s in subs:
                    raw = dot_nt(keys_of[slot][0, s:s + SUB, cols], q)
                    local = lax.broadcasted_iota(jnp.int32, raw.shape, 0) + s
                    allowed = (local + base) >= start
                    if slot == 0:
                        allowed = jnp.logical_and(allowed, local <= lax.broadcasted_iota(jnp.int32, raw.shape, 1))
                    raw = jnp.where(allowed, raw, NEG_BIG)
                    s_scr[slot, s:s + SUB, :] = raw
                    high = jnp.max(raw, axis=0, keepdims=True)
                    top = high if top is None else jnp.maximum(top, high)
                m_scr[...] = jnp.maximum(m_scr[...], top)

            def exps(slot):
                top = m_scr[...]
                total = None
                for s in subs:
                    e = jnp.exp2((s_scr[slot, s:s + SUB, :] - top) * EXP2_SCALE)
                    s_scr[slot, s:s + SUB, :] = e
                    part = jnp.sum(e, axis=0, keepdims=True)
                    total = part if total is None else total + part
                l_scr[...] += total

            def values(slot):
                inv = l_scr[...]
                total, out = None, None
                for s in subs:
                    v = keys_of[slot][1, s:s + SUB, cols]
                    prob = s_scr[slot, s:s + SUB, :] * inv
                    low = prob.astype(BF16)
                    dp = dot_nt(v, do)
                    dp_scr[slot, s:s + SUB, :] = dp
                    part = jnp.sum(prob * dp, axis=0, keepdims=True)
                    total = part if total is None else total + part
                    grad(slot, 1, cols)[s:s + SUB, :] = dot_nn(low, do).astype(BF16)
                    piece_out = dot_nn(v.T, low)
                    out = piece_out if out is None else out + piece_out
                d_scr[...] += total
                ot_scr[...] += out

            def keys(slot):
                inv, mean = l_scr[...], d_scr[...]
                out = None
                for s in subs:
                    k = keys_of[slot][0, s:s + SUB, cols]
                    ds = ((s_scr[slot, s:s + SUB, :] * inv) * (dp_scr[slot, s:s + SUB, :] - mean)).astype(BF16)
                    grad(slot, 0, cols)[s:s + SUB, :] = (dot_nn(ds, q) * SCALE).astype(BF16)
                    piece_out = dot_nn(k.T, ds)
                    out = piece_out if out is None else out + piece_out
                dqt_scr[...] += out

            each(scores)
            each(exps)
            l_scr[...] = 1.0 / l_scr[...]
            each(values)
            each(keys)
            o_buf[i, :, cols] = ot_scr[...].T.astype(BF16)
            dq_buf[par, :, cols] = rope(dqt_scr[...].T * SCALE, cos_ref[rows, :], sin_ref[rows, :], -1.0).astype(BF16)
            return carry

        lax.fori_loop(0, heads // HALVES, one_head, 0)

    def step(i, carry):
        par = lax.rem(i, 2)
        @pl.when(jnp.logical_and(lax.rem(i, HALVES) == 0, lax.div(i, HALVES) + AHEAD < batch))
        def _():
            project_row(lax.div(i, HALVES) + AHEAD)

        @pl.when(i >= OWN_RING)
        def _():
            for which in range(2):
                dkv_store(i - OWN_RING, which).wait()

        @pl.when(second_chip)
        def _():
            kv_to_chip(i).wait_recv()
            kv_forward(i).start()

        @pl.when(second_core)
        def _():
            kv_to_partner(i).wait_recv()

        @pl.when(second_chip)
        def _():
            kv_forward(i).wait_recv()

        @pl.when(i >= 2)
        def _():
            dq_store(i - 2, par).wait()

            @pl.when(second_core)
            def _():
                part_copy(i - 2, par).wait_send()

            @pl.when(second_chip)
            def _():
                far_copy(i - 2, par).wait_send()

        @pl.when(jnp.logical_and(second_chip, i >= CHIP_BUFS))
        def _():
            chip_copy(i - CHIP_BUFS).wait_send()

        attend_unit(i, par)
        o_start(i)
        dq_store(i, par).start()

        @pl.when(second_chip)
        def _():
            far_copy(i, par).start()

        @pl.when(second_core)
        def _():
            part_copy(i, par).start()

        @pl.when(i >= 1)
        def _():
            chip_sum(i - 1)

        for age in range(1, tp - 1):
            @pl.when(i >= age * RELAY_LAG)
            def _(age=age):
                relay(i - age * RELAY_LAG, age)

        @pl.when(i >= SUM_LAG)
        def _():
            key_grads(i - SUM_LAG)

        @pl.when(i == min(W_TWIN, units - 1))
        def _():
            for d in w_steps:
                wz_wait(d)
                w_move(0, d).start()
                w_move(1, d).start()

                @pl.when(second_chip)
                def _(d=d):
                    w_move(3, d).start()

        @pl.when(i == min(W_PARTNER, units - 1))
        def _():
            for d in w_steps:
                w_move(0, d).wait_recv()
                w_move(2, d).start()

                @pl.when(second_chip)
                def _(d=d):
                    w_move(4, d).start()

        @pl.when(jnp.logical_and(first_chip, i == min(W_CHIP, units - 1)))
        def _():
            for k in (3, 4):
                for d in w_steps:
                    w_move(k, d).start()

        return carry

    for b in range(min(AHEAD, batch)):
        project_row(b, b == 0)
    lax.fori_loop(0, units, step, 0)
    chip_sum(units - 1)

    end = units + max(SUM_LAG, (tp - 2) * RELAY_LAG)
    for i in range(units, end):
        for age in range(1, tp - 1):
            if 0 <= i - age * RELAY_LAG < units:
                relay(i - age * RELAY_LAG, age)
        if 0 <= i - SUM_LAG < units:
            key_grads(i - SUM_LAG)
        if i == end - 1:
            for k in (3, 4):
                for d in w_steps:
                    w_move(k, d).wait_recv()
                    w_move(k + 2, d).start()

    w_local.wait()
    for d in w_steps:
        wz_copy(d).wait_send()
        for k in range(7):
            w_move(k, d).wait_send()
            if k in (1, 2, 5, 6):
                w_move(k, d).wait_recv()

    for k in range(per_row):
        n_store(batch - 1, k).wait()
    for u in range(max(0, units - OWN_RING), units):
        for which in range(2):
            dkv_store(u, which).wait()

    def drain(b, carry):
        @pl.when(first_chip)
        def _():
            kv_to_chip(b).wait_send()

        @pl.when(first_core)
        def _():
            kv_to_partner(b).wait_send()

        @pl.when(second_chip)
        def _():
            kv_forward(b).wait_send()

        o_local_copy(b).wait()
        for k, step_, ok in hops:
            @pl.when(jnp.logical_and(ok, jnp.logical_or(b < units - LATE, far_from_end(step_))))
            def _(k=k, step_=step_):
                o_copy(b, k, step_).wait_send()

        for age in range(1, tp - 1):
            for step_ in (1, -1):
                @pl.when(relays(age, step_))
                def _(age=age, step_=step_):
                    relay_copy(b, age, step_).wait_send()

        for src in range(tp):
            way = jnp.where(z > src, 1, -1)
            gone = jnp.abs(z - src)
            far = jnp.where(way > 0, z, tp - 1 - z)
            taken = jnp.logical_and(gone <= tp - 2, far < tp - 1)
            late = jnp.logical_and(b >= units - LATE, jnp.logical_and(gone == 1, far == tp - 1))

            @pl.when(jnp.logical_and(z != src, jnp.logical_not(jnp.logical_or(taken, late))))
            def _(src=src):
                o_arrived(src, b)

        return carry

    lax.fori_loop(0, units, drain, 0)

    for b in range(max(0, units - 2), units):
        dq_store(b, b % 2).wait()

        @pl.when(second_core)
        def _(b=b):
            part_copy(b, b % 2).wait_send()

        @pl.when(second_chip)
        def _(b=b):
            far_copy(b, b % 2).wait_send()

    for b in range(max(0, units - CHIP_BUFS), units):
        @pl.when(second_chip)
        def _(b=b):
            chip_copy(b).wait_send()


def front(x, dy, wq, wk, wv, wo, pos, table, gain, seq, tp, cp):
    tokens, d_model = x.shape
    hidden = wq.shape[1]
    batch = tokens // seq
    units = batch * HALVES
    half = hidden // HALVES
    tile = seq // 2
    hbm = pl.BlockSpec(memory_space=pl.ANY)
    vmem = pl.BlockSpec(memory_space=pltpu.VMEM)
    dma = pltpu.SemaphoreType.DMA
    bf = lambda *shape: pltpu.VMEM(shape, BF16)
    f32 = lambda *shape: pltpu.VMEM(shape, F32)
    return pl.pallas_call(
        functools.partial(front_kernel, batch, seq, tp, cp),
        in_specs=[hbm] * 6 + [vmem] * 3,
        out_specs=[hbm] * 5,
        out_shape=[
            jax.ShapeDtypeStruct((tokens, d_model), BF16),
            jax.ShapeDtypeStruct((tp, batch, HALVES, seq, half), BF16),
            jax.ShapeDtypeStruct((tokens, hidden), BF16),
            jax.ShapeDtypeStruct((2, tokens, hidden), BF16),
            jax.ShapeDtypeStruct((tp, hidden, d_model), BF16),
        ],
        scratch_shapes=[
            bf(3, d_model, hidden), bf(hidden, d_model), f32(tokens, HEAD_DIM), f32(tokens, HEAD_DIM),
            bf(Q_RING, seq, hidden), bf(Q_RING, seq, hidden), bf(2, tile, d_model), bf(2, tile, d_model), bf(2, tile, d_model),
            bf(units, 2, seq, half), bf(3, units, 2, seq, half),
            f32(4, seq, seq), f32(4, seq, seq), f32(1, seq), f32(1, seq), f32(1, seq), f32(HEAD_DIM, seq), f32(HEAD_DIM, seq),
            bf(units, seq, half), bf(2, seq, half),
            bf(OWN_RING, 2, seq, half), bf(2, 2, seq, half), bf(CHIP_BUFS, 2, seq, half), bf(2, 2, seq, half),
            bf(units, 2, seq, half), bf(units, 2, seq, half),
            dma((4,)), dma((1,)), dma((tp,)), dma((tp,)), dma((7, tp)), dma((7, tp)),
            dma((2,)), dma((2,)), dma((2,)), dma((units,)), dma((units,)), dma((units,)), dma((3, units)),
            dma((units,)), dma((2, units)), dma((tp, units)), dma((2, 2, units)), dma((2,)),
            dma((2,)), dma((2,)), dma((CHIP_BUFS,)), dma((units,)), dma((units,)), dma((units, 2)),
        ],
        compiler_params=pltpu.CompilerParams(collective_id=1, has_side_effects=True, vmem_limit_bytes=63 << 20),
        cost_estimate=pl.CostEstimate(flops=60 * tokens * seq * hidden, bytes_accessed=16 * tokens * d_model, transcendentals=4 * tokens * seq * (hidden // HEAD_DIM)),
        name="front",
    )(x, dy, wq, wk, wv, wo, pos, table, gain)


PART_RING = 4
RS_RING = 5
FORWARD_LAG = 11
JOB_LAG = 5
OUT_LAG = 4
EARLY = 4


def back_kernel(groups, rows, tp, cp, seq, dq_hbm, dkv_hbm, x_hbm, dy_hbm, o_old, n_hbm, wq_hbm, wk_hbm, wv_hbm, wo_hbm, gain_ref,
                gx_hbm, y_hbm, ga_hbm, gb_hbm, gg_ref, o_out,
                wq_ref, wk_ref, wv_ref, wo_ref, dq_all, dkv_all, o_t, part, rs_r, rs_l, send_r, send_l, tot, gx_buf,
                o_in, x_in, xo_in, dyo_in, y_buf, n_in, dy_in, away, part_in, mine, gain_all,
                w_sem, in_sem, fin_sem, job_sem, y_sem, own_sem, rss_r, rss_l, rsr_r, rsr_l, ag0_r, ag0_l, agf_r, agf_l, agr_r, agr_l,
                away_send, away_recv, mine_own, mine_part, mine_chip, ga_recv, chip_recv, gb_send, gb_recv, gs_sem, gr_sem, late_send, late_recv, o_sem):
    o_hbm = o_out
    z = lax.axis_index("tp")
    r = lax.axis_index("cp")
    core = lax.rem(r, 2)
    chip = lax.div(r, 2)
    last = tp - 1
    slots = tp - 1
    span = tp * rows
    tokens, d_model = x_hbm.shape
    hidden = dq_hbm.shape[1]
    chunk = min(512, d_model)
    blocks = ga_hbm.shape[0]
    width = ga_hbm.shape[1]
    half = hidden // HALVES
    pairs = blocks // 2
    partner = {"cp": r + 1 - 2 * core}
    peer = {"cp": r + 2 - 4 * chip}

    head = min(EARLY, groups) * span
    weight_loads = [pltpu.make_async_copy(src, dst, w_sem.at[k]) for k, (src, dst) in enumerate((
        (dq_hbm.at[:head, :], dq_all.at[:head, :]), (dkv_hbm.at[:, :head, :], dkv_all.at[:, :head, :]), (wq_hbm, wq_ref), (wk_hbm, wk_ref), (wv_hbm, wv_ref)))]
    rest_loads = [] if head == tokens else [
        pltpu.make_async_copy(dq_hbm.at[head:, :], dq_all.at[head:, :], w_sem.at[6]),
        pltpu.make_async_copy(dkv_hbm.at[:, head:, :], dkv_all.at[:, head:, :], w_sem.at[7]),
    ]
    out_loads = [pltpu.make_async_copy(wo_hbm, wo_ref, w_sem.at[5])]
    for copy in weight_loads:
        copy.start()

    barrier = pltpu.get_barrier_semaphore()
    peers = [(dt, dc) for dt in range(tp) for dc in range(cp) if dt or dc]
    for dt, dc in peers:
        pl.semaphore_signal(barrier, inc=1, device_id={"tp": lax.rem(z + dt, tp), "cp": lax.rem(r + dc, cp)}, device_id_type=MESH)

    def remote(src, dst, ssem, rsem, dev):
        return pltpu.make_async_remote_copy(src_ref=src, dst_ref=dst, send_sem=ssem, recv_sem=rsem, device_id=dev, device_id_type=MESH)

    right = {"tp": jnp.where(z < last, z + 1, z)}
    left = {"tp": jnp.where(z > 0, z - 1, z)}

    def group_rows(i):
        return pl.ds(pl.multiple_of(i * span, span), span)

    def tile_rows(i, owner):
        return pl.ds(pl.multiple_of(i * span + owner * rows, rows), rows)

    def inputs(i, slot):
        g = group_rows(i)
        return [
            pltpu.make_async_copy(o_hbm.at[:, lax.div(i, seq // span), :, pl.ds(pl.multiple_of(lax.rem(i, seq // span) * span, span), span), :], o_in.at[slot], in_sem.at[slot, 0]),
            pltpu.make_async_copy(x_hbm.at[g, :], x_in.at[slot], in_sem.at[slot, 1]),
        ]

    def final_inputs(i, slot):
        g = tile_rows(i, z)
        return [
            pltpu.make_async_copy(x_hbm.at[g, :], xo_in.at[slot], fin_sem.at[slot, 0]),
            pltpu.make_async_copy(dy_hbm.at[g, :], dyo_in.at[slot], fin_sem.at[slot, 1]),
        ]

    def y_copy(i, slot):
        return pltpu.make_async_copy(y_buf.at[slot], y_hbm.at[group_rows(i), :], y_sem.at[slot])

    def rs_copy(i, s, to_right):
        ring = lax.rem(i, RS_RING)
        if to_right:
            return remote(send_r.at[s], rs_r.at[ring, s], rss_r.at[s], rsr_r.at[ring, s], right)
        return remote(send_l.at[s], rs_l.at[ring, s], rss_l.at[s], rsr_l.at[ring, s], left)

    def rs_send(i, s):
        for to_right in (True, False):
            far = z if to_right else last - z
            owner = (z + slots - s) if to_right else (z - slots + s)
            buf, held = (send_r, rs_r) if to_right else (send_l, rs_l)

            @pl.when(jnp.logical_and(jnp.logical_and(i >= 0, i < groups), jnp.logical_and(far <= s, far < last)))
            def _(to_right=to_right, far=far, owner=owner, buf=buf, held=held):
                @pl.when(i > 0)
                def _():
                    rs_copy(i - 1, s, to_right).wait_send()

                cur = lax.rem(i, PART_RING)
                own = pl.ds(pl.multiple_of(owner * rows, rows), rows)
                if s == 0:
                    buf[s] = part[cur, own, :].astype(BF16)
                else:
                    @pl.when(far == 0)
                    def _():
                        buf[s] = part[cur, own, :].astype(BF16)

                    @pl.when(far > 0)
                    def _():
                        rs_copy(i, s - 1, to_right).wait_recv()
                        buf[s] = (part[cur, own, :] + held[lax.rem(i, RS_RING), s - 1].astype(F32)).astype(BF16)

                rs_copy(i, s, to_right).start()

    def ag_own(i, slot, to_right):
        src = gx_buf.at[slot]
        dst = gx_hbm.at[tile_rows(i, z), :]
        if to_right:
            return remote(src, dst, ag0_r.at[slot], agr_r.at[i, 0], right)
        return remote(src, dst, ag0_l.at[slot], agr_l.at[i, 0], left)

    def own_copy(i, slot):
        return pltpu.make_async_copy(gx_buf.at[slot], gx_hbm.at[tile_rows(i, z), :], own_sem.at[slot])

    def ag_forward(i, a, to_right):
        owner = z - a if to_right else z + a
        tile = gx_hbm.at[tile_rows(i, owner), :]
        if to_right:
            return remote(tile, tile, agf_r.at[a], agr_r.at[i, a], right)
        return remote(tile, tile, agf_l.at[a], agr_l.at[i, a], left)

    def ag_wait(i, a, to_right):
        tile = gx_hbm.at[tile_rows(i, 0), :]
        sem = agr_r.at[i, a] if to_right else agr_l.at[i, a]
        remote(tile, tile, agf_r.at[a], sem, right).wait_recv()

    def ag_step(i, a):
        for to_right in (True, False):
            far = z if to_right else last - z

            @pl.when(jnp.logical_and(jnp.logical_and(i >= 0, i < groups), far >= a))
            def _(to_right=to_right, far=far):
                ag_wait(i, a - 1, to_right)
                if a < slots:
                    @pl.when(far < last)
                    def _():
                        @pl.when(i > 0)
                        def _():
                            ag_forward(i - 1, a, to_right).wait_send()

                        ag_forward(i, a, to_right).start()

    def ag_first(i, slot):
        own_copy(i, slot).start()
        for to_right in (True, False):
            far = z if to_right else last - z

            @pl.when(far < last)
            def _(to_right=to_right):
                ag_own(i, slot, to_right).start()

    def ag_first_done(i, slot):
        own_copy(i, slot).wait()
        for to_right in (True, False):
            far = z if to_right else last - z

            @pl.when(far < last)
            def _(to_right=to_right):
                ag_own(i, slot, to_right).wait_send()

    def partial_norm(i):
        cur = lax.rem(i, PART_RING)
        g = group_rows(i)
        for c in range(0, d_model, chunk):
            cols = slice(c, c + chunk)
            part[cur, :, cols] = (
                dot_nt(dq_all[g, :], wq_ref[cols, :]) + dot_nt(dkv_all[0, g, :], wk_ref[cols, :]) + dot_nt(dkv_all[1, g, :], wv_ref[cols, :])
            )

    def project_out(cur):
        for c in range(0, d_model, chunk):
            cols = slice(c, c + chunk)
            acc = x_in[cur, :, cols].astype(F32)
            for t in range(tp):
                for h in range(HALVES):
                    acc += dot_nn(o_in[cur, t, h], wo_ref[t, h * half:(h + 1) * half, cols])
            y_buf[cur, :, cols] = acc.astype(BF16)

    def finalize(i):
        slot = lax.rem(i, 2)
        own = pl.ds(pl.multiple_of(z * rows, rows), rows)
        tot[...] = part[lax.rem(i, PART_RING), own, :]

        @pl.when(z > 0)
        def _():
            rs_copy(i, slots - 1, True).wait_recv()
            tot[...] += rs_r[lax.rem(i, RS_RING), slots - 1].astype(F32)

        @pl.when(z < last)
        def _():
            rs_copy(i, slots - 1, False).wait_recv()
            tot[...] += rs_l[lax.rem(i, RS_RING), slots - 1].astype(F32)

        @pl.when(i > 1)
        def _():
            ag_first_done(i - 2, slot)

        for copy in final_inputs(i, slot):
            copy.wait()
        x = xo_in[slot].astype(F32)
        centred = x - jnp.mean(x, axis=-1, keepdims=True)
        inv_std = lax.rsqrt(jnp.mean(centred * centred, axis=-1, keepdims=True) + LN_EPS)
        x_hat = centred * inv_std
        dn = tot[...]
        gg_ref[...] += jnp.sum(dn * x_hat, axis=0, keepdims=True)
        d_hat = dn * gain_ref[...]
        dx = inv_std * (d_hat - jnp.mean(d_hat, axis=-1, keepdims=True) - x_hat * jnp.mean(d_hat * x_hat, axis=-1, keepdims=True))
        gx_buf[slot] = (dyo_in[slot].astype(F32) + dx).astype(BF16)
        ag_first(i, slot)

    def block_of(t):
        return 2 * lax.div(t, 2) + jnp.where(lax.rem(t, 2) == 0, 1 - core, core)

    def job_loads(t, slot):
        cols = pl.ds(pl.multiple_of(block_of(t) * width, width), width)
        return [
            pltpu.make_async_copy(n_hbm.at[:, cols], n_in.at[slot], job_sem.at[slot, 0]),
            pltpu.make_async_copy(dy_hbm.at[:, cols], dy_in.at[slot], job_sem.at[slot, 1]),
        ]

    def away_copy(p):
        ring = lax.rem(p, 2)
        return remote(away, part_in.at[ring], away_send.at[0], away_recv.at[ring], partner)

    def job_block(t, put):
        slot = lax.rem(t, 2)
        n_t = n_in[slot].T
        put(0, hidden, dot_nn(n_t, dq_all[...]))
        put(hidden, hidden, dot_nn(n_t, dkv_all[0]))
        put(2 * hidden, hidden, dot_nn(n_t, dkv_all[1]))
        for k in range(hidden // width):
            put(3 * hidden + k * width, width, dot_nn(o_t[k * width:(k + 1) * width, :], dy_in[slot]))

    def mine_to_own(p, slot):
        return pltpu.make_async_copy(mine.at[slot], ga_hbm.at[2 * p + core], mine_own.at[slot])

    def mine_to_part(p, slot):
        return remote(mine.at[slot], ga_hbm.at[2 * p + core], mine_part.at[slot], ga_recv.at[p], partner)

    def mine_to_chip(p, slot):
        return remote(mine.at[slot], gb_hbm.at[2 * p + core], mine_chip.at[slot], chip_recv.at[p], peer)

    def mine_done(p, slot):
        mine_to_own(p, slot).wait()
        mine_to_part(p, slot).wait_send()
        mine_to_chip(p, slot).wait_send()

    def chip_forward(p):
        b = 2 * p + core
        return remote(gb_hbm.at[b], gb_hbm.at[b], gb_send.at[p], gb_recv.at[p], partner)

    def job(t):
        p = lax.div(t, 2)
        for copy in job_loads(t, lax.rem(t, 2)):
            copy.wait()

        @pl.when(t + 1 < blocks)
        def _():
            for copy in job_loads(t + 1, 1 - lax.rem(t, 2)):
                copy.start()

        @pl.when(lax.rem(t, 2) == 0)
        def _():
            @pl.when(p > 0)
            def _():
                away_copy(p - 1).wait_send()

            def put(at, size, value):
                away[:, at:at + size] = value

            job_block(t, put)
            away_copy(p).start()

        @pl.when(lax.rem(t, 2) == 1)
        def _():
            slot = lax.rem(p, 2)
            away_copy(p).wait_recv()

            @pl.when(p > 1)
            def _():
                mine_done(p - 2, slot)

            def put(at, size, value):
                mine[slot, :, at:at + size] = (value + part_in[slot, :, at:at + size]).astype(BF16)

            job_block(t, put)
            mine_to_chip(p, slot).start()
            mine_to_part(p, slot).start()
            mine_to_own(p, slot).start()

    gg_ref[...] = jnp.zeros_like(gg_ref)
    o_loads = [pltpu.make_async_copy(o_hbm.at[z, b, k], n_in.at[k, b * seq:(b + 1) * seq, :], o_sem.at[k, b]) for k in range(HALVES) for b in range(tokens // seq)]
    me = z * cp + r

    def gain_copy(dt, dc):
        to = {"tp": lax.rem(z + dt, tp), "cp": lax.rem(r + dc, cp)}
        return remote(gain_all.at[me], gain_all.at[me], gs_sem.at[dt * cp + dc], gr_sem.at[me], to)

    def gain_wait(dt, dc):
        sender = lax.rem(z + dt, tp) * cp + lax.rem(r + dc, cp)
        remote(gain_all.at[sender], gain_all.at[sender], gs_sem.at[0], gr_sem.at[sender], right).wait_recv()

    units = tokens // seq * HALVES
    late_units = range(max(0, units - LATE), units)
    late_wait = max(0, late_units[0] // HALVES * seq // span + OUT_LAG - 2)
    sends_late = jnp.logical_or(z == 1, z == last - 1)
    gets_late = jnp.logical_or(z == 0, z == last)

    def late_copy(n, src, dst):
        u = late_units[n]
        place = o_out.at[src, u // HALVES, u % HALVES]
        return remote(place, place, late_send.at[n], late_recv.at[n], {"tp": dst})

    def late_move(n):
        return late_copy(n, z, jnp.where(z == 1, 0, last))

    for copy in weight_loads:
        copy.wait()
    for copy in inputs(0, 0) + o_loads + rest_loads + out_loads:
        copy.start()
    partial_norm(0)
    pl.semaphore_wait(barrier, len(peers))
    for n in range(len(late_units)):
        @pl.when(sends_late)
        def _(n=n):
            late_move(n).start()

    def step(i, carry):
        @pl.when(jnp.logical_and(gets_late, i == late_wait))
        def _():
            for n in range(len(late_units)):
                late_copy(n, jnp.where(z == 0, 1, last - 1), z).wait_recv()

        for a in reversed(range(1, slots + 1)):
            ag_step(i - slots - a, a)

        @pl.when(i == OUT_LAG)
        def _():
            for copy in out_loads:
                copy.wait()

        @pl.when(jnp.logical_and(i >= OUT_LAG, i < groups + OUT_LAG))
        def _():
            j = i - OUT_LAG
            at = lax.rem(j, 2)
            for copy in inputs(j, at):
                copy.wait()

            @pl.when(j + 1 < groups)
            def _():
                for copy in inputs(j + 1, 1 - at):
                    copy.start()

            @pl.when(j >= 2)
            def _():
                y_copy(j - 2, at).wait()

            project_out(at)
            y_copy(j, at).start()

        @pl.when(jnp.logical_and(i >= slots, i < groups + slots))
        def _():
            finalize(i - slots)

        @pl.when(i == groups + slots - 1)
        def _():
            gain_all[me] = gg_ref[...]
            for dt, dc in peers:
                gain_copy(dt, dc).start()

        @pl.when(jnp.logical_and(i >= slots - 1, i < groups + slots - 1))
        def _():
            for copy in final_inputs(i - slots + 1, lax.rem(i - slots + 1, 2)):
                copy.start()

        @pl.when(i == EARLY)
        def _():
            for copy in rest_loads:
                copy.wait()

        @pl.when(jnp.logical_and(i >= 1, i < groups))
        def _():
            partial_norm(i)

        @pl.when(i == JOB_LAG - 1)
        def _():
            for copy in o_loads:
                copy.wait()
            for k in range(HALVES):
                o_t[k * half:(k + 1) * half, :] = n_in[k].T
            for copy in job_loads(0, 0):
                copy.start()

        @pl.when(jnp.logical_and(i >= JOB_LAG, i < JOB_LAG + blocks))
        def _():
            job(i - JOB_LAG)

        for k in reversed(range(slots)):
            rs_send(i - k, k)

        @pl.when(jnp.logical_and(lax.rem(i, 2) == 1, jnp.logical_and(i >= FORWARD_LAG, i < FORWARD_LAG + 2 * pairs)))
        def _():
            p = lax.div(i - FORWARD_LAG, 2)
            mine_to_chip(p, 0).wait_recv()
            chip_forward(p).start()

        return carry

    lax.fori_loop(0, max(groups + 2 * slots, groups + OUT_LAG, blocks + JOB_LAG, 2 * pairs + FORWARD_LAG - 1), step, 0)

    for i in (groups - 2, groups - 1):
        y_copy(i, i % 2).wait()
        ag_first_done(i, i % 2)
    for to_right in (True, False):
        far = z if to_right else last - z
        for s in range(slots):
            @pl.when(jnp.logical_and(far <= s, far < last))
            def _(s=s, to_right=to_right):
                rs_copy(groups - 1, s, to_right).wait_send()
        for a in range(1, slots):
            @pl.when(jnp.logical_and(far >= a, far < last))
            def _(a=a, to_right=to_right):
                ag_forward(groups - 1, a, to_right).wait_send()
    for n in range(len(late_units)):
        @pl.when(sends_late)
        def _(n=n):
            late_move(n).wait_send()

    away_copy(pairs - 1).wait_send()
    for p in range(max(0, pairs - 2), pairs):
        mine_done(p, p % 2)
    for p in range(pairs):
        chip_forward(p).wait_send()
        chip_forward(p).wait_recv()
        mine_to_part(p, 0).wait_recv()
    for dt, dc in peers:
        gain_wait(dt, dc)
        gain_copy(dt, dc).wait_send()
    total = gain_all[0]
    for j in range(1, tp * cp):
        total += gain_all[j]
    gg_ref[...] = total


def backward_norm(dq, dkv, x, dy, o_all, normed, wq, wk, wv, wo_all, gain, rows, seq, tp, cp):
    tokens, hidden = dq.shape
    d_model = x.shape[1]
    span = tp * rows
    groups = tokens // span
    slots = tp - 1
    width = WIDTH
    blocks = d_model // width
    pairs = blocks // 2
    hbm = pl.BlockSpec(memory_space=pl.ANY)
    vmem = pl.BlockSpec(memory_space=pltpu.VMEM)
    dma = pltpu.SemaphoreType.DMA
    bf = lambda *shape: pltpu.VMEM(shape, BF16)
    f32 = lambda *shape: pltpu.VMEM(shape, F32)
    return pl.pallas_call(
        functools.partial(back_kernel, groups, rows, tp, cp, seq),
        in_specs=[hbm] * 10 + [vmem],
        out_specs=[hbm, hbm, hbm, hbm, vmem, hbm],
        input_output_aliases={4: 5},
        out_shape=[
            jax.ShapeDtypeStruct((tokens, d_model), BF16),
            jax.ShapeDtypeStruct((tokens, d_model), BF16),
            jax.ShapeDtypeStruct((blocks, width, 4 * hidden), BF16),
            jax.ShapeDtypeStruct((blocks, width, 4 * hidden), BF16),
            jax.ShapeDtypeStruct((1, d_model), F32),
            jax.ShapeDtypeStruct(o_all.shape, BF16),
        ],
        scratch_shapes=[
            bf(d_model, hidden), bf(d_model, hidden), bf(d_model, hidden), bf(tp, hidden, d_model),
            bf(tokens, hidden), bf(2, tokens, hidden), bf(hidden, tokens),
            f32(PART_RING, span, d_model), bf(RS_RING, slots, rows, d_model), bf(RS_RING, slots, rows, d_model),
            bf(slots, rows, d_model), bf(slots, rows, d_model), f32(rows, d_model), bf(2, rows, d_model),
            bf(2, tp, HALVES, span, hidden // HALVES), bf(2, span, d_model), bf(2, rows, d_model), bf(2, rows, d_model), bf(2, span, d_model),
            bf(2, tokens, width), bf(2, tokens, width),
            f32(width, 4 * hidden), f32(2, width, 4 * hidden), bf(2, width, 4 * hidden), f32(tp * cp, 1, d_model),
            dma((8,)), dma((2, 2)), dma((2, 2)), dma((2, 2)), dma((2,)), dma((2,)),
            dma((slots,)), dma((slots,)), dma((RS_RING, slots)), dma((RS_RING, slots)),
            dma((2,)), dma((2,)), dma((slots,)), dma((slots,)), dma((groups, slots)), dma((groups, slots)),
            dma((1,)), dma((2,)), dma((2,)), dma((2,)), dma((2,)), dma((pairs,)), dma((pairs,)), dma((pairs,)), dma((pairs,)),
            dma((tp * cp,)), dma((tp * cp,)), dma((max(LATE, 1),)), dma((max(LATE, 1),)), dma((HALVES, tokens // seq)),
        ],
        compiler_params=pltpu.CompilerParams(collective_id=0, has_side_effects=True, vmem_limit_bytes=63 << 20),
        cost_estimate=pl.CostEstimate(flops=22 * tokens * hidden * d_model, bytes_accessed=16 * tokens * d_model, transcendentals=0),
        name="backward_norm",
    )(dq, dkv, x, dy, o_all, normed, wq, wk, wv, wo_all, gain)


def finish_kernel(y_ref, gx_ref, ga_ref, gb_ref, gg_ref, yo_ref, gxo_ref, wq_ref, wk_ref, wv_ref, wo_ref, ggo_ref):
    ggo_ref[...] = gg_ref[...]
    yo_ref[...] = y_ref[...]
    gxo_ref[...] = gx_ref[...]
    rows = ga_ref.shape[1]
    width = rows * PARTS
    hidden = wq_ref.shape[1]
    for k, ref in enumerate((wq_ref, wk_ref, wv_ref)):
        cols = slice(k * hidden, (k + 1) * hidden)
        ref[...] = ga_ref[0, :, cols].astype(F32) + gb_ref[0, :, cols].astype(F32)
    for k in range(hidden // width):
        cols = slice(3 * hidden + k * width, 3 * hidden + (k + 1) * width)
        at = k * width + lax.rem(pl.program_id(0), PARTS) * rows
        wo_ref[pl.ds(pl.multiple_of(at, rows), rows), :] = ga_ref[0, :, cols].astype(F32) + gb_ref[0, :, cols].astype(F32)


def finish(y, gx, ga, gb, gg):
    tokens, d_model = y.shape
    blocks, width, packed = ga.shape
    hidden = packed // 4
    steps = blocks * PARTS
    tile = pl.BlockSpec((tokens // steps, d_model), lambda j: (j, 0))
    block = pl.BlockSpec((1, width // PARTS, packed), lambda j: (j // PARTS, j % PARTS, 0))
    wide = pl.BlockSpec((width // PARTS, hidden), lambda j: (j, 0))
    line = pl.BlockSpec((1, d_model), lambda j: (0, 0))
    return pl.pallas_call(
        finish_kernel,
        grid=(steps,),
        in_specs=[tile, tile, block, block, line],
        out_specs=[tile, tile, wide, wide, wide, pl.BlockSpec((hidden, width), lambda j: (0, j // PARTS)), line],
        out_shape=[jax.ShapeDtypeStruct((tokens, d_model), BF16)] * 2 + [jax.ShapeDtypeStruct((d_model, hidden), F32)] * 3 + [jax.ShapeDtypeStruct((hidden, d_model), F32), jax.ShapeDtypeStruct((1, d_model), F32)],
        compiler_params=pltpu.CompilerParams(dimension_semantics=("arbitrary",), vmem_limit_bytes=48 << 20),
        cost_estimate=pl.CostEstimate(flops=8 * d_model * hidden, bytes_accessed=8 * tokens * d_model + 32 * d_model * hidden, transcendentals=0),
        name="finish",
    )(y, gx, ga, gb, gg)


def solution(mesh):
    cp_size = mesh.shape["cp"]
    tp_size = mesh.shape["tp"]

    def device_step(x_in, segment_ids, positions, w_query, w_key, w_value, w_out, norm_gain, grad_out):
        batch, seq, d_model = x_in.shape
        tokens = batch * seq
        x = x_in.reshape(tokens, d_model)
        dy = grad_out.reshape(tokens, d_model)

        gain = norm_gain.reshape(1, d_model)
        normed, o_all, dq, dkv, w_all = front(x, dy, w_query, w_key, w_value, w_out, positions, jnp.asarray(angle_table(), BF16), gain, seq, tp_size, cp_size)
        grad_x, y_out, sum_a, sum_b, grad_gain, _ = backward_norm(dq, dkv, x, dy, o_all, normed, w_query, w_key, w_value, w_all, gain, ROWS, seq, tp_size, cp_size)
        y_out, grad_x, grad_wq, grad_wk, grad_wv, grad_wo, grad_gain = finish(y_out, grad_x, sum_a, sum_b, grad_gain)
        grad_gain = grad_gain.reshape(d_model)
        return y_out.reshape(x_in.shape), grad_x.reshape(x_in.shape), grad_gain, grad_wq, grad_wk, grad_wv, grad_wo

    in_specs = (P("dp", "cp", None), P("dp", "cp"), P("dp", "cp"), P(None, "tp"), P(None, "tp"), P(None, "tp"), P("tp", None), P(None), P("dp", "cp", None))
    out_specs = (P("dp", "cp", None), P("dp", "cp", None), P("dp"), P("dp", "tp"), P("dp", "tp"), P("dp", "tp"), P(("dp", "tp"), None))
    return jax.shard_map(device_step, mesh=mesh, in_specs=in_specs, out_specs=out_specs, check_vma=False)
```

```python
import functools
import math

import jax
import jax.numpy as jnp
import numpy as np
from jax import lax
from jax.experimental import pallas as pl
from jax.experimental.pallas import tpu as pltpu
from jax.sharding import PartitionSpec as P

HEAD_DIM = 128
ROPE_THETA = 8000000.0
LN_EPS = 1e-5
NEG_BIG = -1e30
SCALE = HEAD_DIM ** -0.5
EXP2_SCALE = SCALE * math.log2(math.e)
F32 = jnp.float32
BF16 = jnp.bfloat16
NT = (((1,), (1,)), ((), ()))


def dot_nn(a, b):
    return jnp.dot(a, b, preferred_element_type=F32)


def dot_nt(a, b):
    return lax.dot_general(a, b, NT, preferred_element_type=F32)


def dot_tn(a, b):
    return lax.dot_general(a, b, (((0,), (0,)), ((), ())), preferred_element_type=F32)


def swap_pairs(t, sign):
    lane = lax.broadcasted_iota(jnp.int32, t.shape, 1)
    even = (lane % 2) == 0
    up = pltpu.roll(t, HEAD_DIM - 1, 1)
    down = pltpu.roll(t, 1, 1)
    return jnp.where(even, -up, down) if sign > 0 else jnp.where(even, up, -down)


def rope(t, cos_t, sin_t, sign):
    return t * cos_t + swap_pairs(t, sign) * sin_t


def angle_table():
    inv_freq = ROPE_THETA ** (-np.arange(0, HEAD_DIM, 2, dtype=np.float32) / np.float32(HEAD_DIM))
    freq = np.repeat(inv_freq.astype(np.float64), 2)[None, :]
    low = np.arange(POS_LOW)[:, None] * freq
    high = POS_LOW * np.arange(HEAD_DIM - POS_LOW)[:, None] * freq
    table = np.zeros((HEAD_DIM, 12 * HEAD_DIM), np.float32)
    for k, (first, value) in enumerate(((0, np.cos(low)), (0, np.sin(low)), (POS_LOW, np.cos(high)), (POS_LOW, np.sin(high)))):
        rest = value.astype(np.float32)
        for p in range(3):
            piece = rest.astype(BF16).astype(np.float32)
            at = (3 * k + p) * HEAD_DIM
            table[first:first + value.shape[0], at:at + HEAD_DIM] = piece
            rest = rest - piece
    return table


def put_rope(dst, raw, cos_t, sin_t):
    for h in range(raw.shape[1] // HEAD_DIM):
        cols = slice(h * HEAD_DIM, (h + 1) * HEAD_DIM)
        dst[:, cols] = rope(raw[:, cols], cos_t, sin_t, 1.0).astype(BF16)


MESH = pl.DeviceIdType.MESH
SUB = 384
ROWS = 32
WIDTH = 256
PARTS = 1
HALVES = 2
RELAY_LAG = 1
LATE = 3
SUM_LAG = 4
CHIP_BUFS = 4
OWN_RING = 6
Q_RING = 3
AHEAD = 2
POS_LOW = 64
W_TWIN = 1
W_PARTNER = 3
W_CHIP = 7


def front_kernel(batch, seq, tp, cp, x_hbm, dy_hbm, wq_hbm, wk_hbm, wv_hbm, wo_hbm, pos_ref, table_ref, gain_ref,
                 n_hbm, o_all, dq_hbm, dkv_hbm, w_all,
                 big, wo_ref, cos_ref, sin_ref, q_ring, do_ring, x_in, dy_in, n_buf, kv_own, kvr, s_scr, dp_scr, m_scr, l_scr, d_scr, ot_scr, dqt_scr,
                 o_buf, dq_buf, g_own, g_part, g_chip, g_far, xin, part_in,
                 w_sem, wl_sem, wz_send, wz_recv, wx_send, wx_recv,
                 x_sem, dy_sem, n_sem, kvs_part, kvs_chip, kvs_far, kv_recv, o_local, o_send, o_recv, relay_send, dq_sem,
                 far_send, part_send, chip_send, x_recv, part_recv, dkv_sem):
    z = lax.axis_index("tp")
    r = lax.axis_index("cp")
    dp = lax.axis_index("dp")
    core = lax.rem(r, 2)
    chip = lax.div(r, 2)
    d_model = x_hbm.shape[1]
    hidden = wq_hbm.shape[1]
    heads = hidden // HEAD_DIM
    first_chip, second_chip = chip == 0, chip == 1
    first_core, second_core = core == 0, core == 1
    partner = {"cp": r + 1 - 2 * core}
    peer = {"cp": r + 2 - 4 * chip}
    twin = {"dp": 1 - dp}

    tile = x_in.shape[1]
    per_row = seq // tile

    def row(b):
        return pl.ds(pl.multiple_of(b * seq, seq), seq)

    def tile_rows(b, k):
        return pl.ds(pl.multiple_of(b * seq + k * tile, tile), tile)

    def x_load(b, k):
        return pltpu.make_async_copy(x_hbm.at[tile_rows(b, k), :], x_in.at[k], x_sem.at[k])

    def dy_load(b, k):
        return pltpu.make_async_copy(dy_hbm.at[tile_rows(b, k), :], dy_in.at[k], dy_sem.at[k])

    def n_store(b, k):
        return pltpu.make_async_copy(n_buf.at[k], n_hbm.at[tile_rows(b, k), :], n_sem.at[k])

    weight_loads = [pltpu.make_async_copy(src, dst, w_sem.at[k]) for k, (src, dst) in enumerate(((wk_hbm, big.at[0]), (wv_hbm, big.at[1]), (wq_hbm, big.at[2]), (wo_hbm, wo_ref)))]
    x_load(0, 0).start()
    for copy in weight_loads[:2]:
        copy.start()
    for k in range(1, per_row):
        x_load(0, k).start()
    for copy in weight_loads[2:]:
        copy.start()
    for k in range(per_row):
        dy_load(0, k).start()

    units = batch * HALVES
    half = hidden // HALVES

    def where(u):
        return lax.div(u, HALVES), lax.rem(u, HALVES)

    def half_cols(g):
        return pl.ds(pl.multiple_of(g * half, half), half)

    barrier = pltpu.get_barrier_semaphore()
    for dev in [partner, peer, twin] + [{"tp": lax.rem(z + dt, tp)} for dt in range(1, tp)]:
        pl.semaphore_signal(barrier, inc=1, device_id=dev, device_id_type=MESH)

    def remote(src, dst, ssem, rsem, dev):
        return pltpu.make_async_remote_copy(src_ref=src, dst_ref=dst, send_sem=ssem, recv_sem=rsem, device_id=dev, device_id_type=MESH)

    share = hidden // 8

    def share_rows(y, c, g):
        return pl.ds(pl.multiple_of((4 * y + 2 * c + g) * share, share), share)

    mine, twins = share_rows(chip, core, dp), share_rows(chip, core, 1 - dp)
    peers, peer_twins = share_rows(1 - chip, core, dp), share_rows(1 - chip, core, 1 - dp)

    def wz_copy(d):
        return remote(wo_hbm.at[mine, :], w_all.at[z, mine, :], wz_send.at[d], wz_recv.at[z], {"tp": lax.rem(z + d, tp)})

    def wz_wait(d):
        src = lax.rem(z + d, tp)
        remote(wo_hbm.at[mine, :], w_all.at[src, mine, :], wz_send.at[d], wz_recv.at[src], partner).wait_recv()

    def w_copy(k, d, rows, dev):
        place = w_all.at[lax.rem(z + d, tp), rows, :]
        return remote(place, place, wx_send.at[k, d], wx_recv.at[k, d], dev)

    def w_move(k, d):
        rows, dev = ((mine, twin), (mine, partner), (twins, partner), (mine, peer), (twins, peer), (peers, partner), (peer_twins, partner))[k]
        return w_copy(k, d, rows, dev)

    w_steps = range(1, tp)

    def kv_to_partner(u):
        return remote(kv_own.at[u], kvr.at[0, u], kvs_part.at[u], kv_recv.at[0, u], partner)

    def kv_to_chip(u):
        return remote(kv_own.at[u], kvr.at[1, u], kvs_chip.at[u], kv_recv.at[1, u], peer)

    def kv_forward(u):
        return remote(kvr.at[1, u], kvr.at[2, u], kvs_far.at[u], kv_recv.at[2, u], partner)

    w_local = pltpu.make_async_copy(wo_ref, w_all.at[z], wl_sem.at[0])

    def angles(b, k):
        rows = tile_rows(b, k)
        pos = jnp.broadcast_to(pos_ref[pl.ds(b, 1), k * tile:(k + 1) * tile], (HEAD_DIM, tile)).T
        lane = lax.broadcasted_iota(jnp.int32, (tile, HEAD_DIM), 1)
        low = lane < POS_LOW
        pick = jnp.where(low, lax.rem(pos, POS_LOW), POS_LOW + lax.div(pos, POS_LOW)) == lane
        found = dot_nn(jnp.where(pick, 1.0, 0.0).astype(BF16), table_ref[...])

        def part(k):
            at = 3 * k * HEAD_DIM
            return found[:, at:at + HEAD_DIM] + found[:, at + HEAD_DIM:at + 2 * HEAD_DIM] + found[:, at + 2 * HEAD_DIM:at + 3 * HEAD_DIM]

        cos_b, sin_b, cos_a, sin_a = part(0), part(1), part(2), part(3)
        cos_ref[rows, :] = cos_a * cos_b - sin_a * sin_b
        sin_ref[rows, :] = sin_a * cos_b + cos_a * sin_b

    def project_row(b, first=False):
        ring = lax.rem(b, Q_RING)
        for k in range(per_row):
            rows = tile_rows(b, k)
            inside = slice(k * tile, (k + 1) * tile)
            x_load(b, k).wait()

            @pl.when(b > 0)
            def _(k=k):
                n_store(b - 1, k).wait()

            angles(b, k)
            x = x_in[k].astype(F32)
            centred = x - jnp.mean(x, axis=-1, keepdims=True)
            inv_std = lax.rsqrt(jnp.mean(centred * centred, axis=-1, keepdims=True) + LN_EPS)
            n_buf[k] = ((centred * inv_std) * gain_ref[...]).astype(BF16)
            n_store(b, k).start()

            @pl.when(b + 1 < batch)
            def _(k=k):
                x_load(b + 1, k).start()

            if first and k == 0:
                for copy in weight_loads[:2]:
                    copy.wait()
            for g in range(HALVES):
                u = b * HALVES + g
                cols = slice(g * half, (g + 1) * half)
                put_rope(kv_own.at[u, 0, inside, :], dot_nn(n_buf[k], big[0, :, cols]), cos_ref[rows, :], sin_ref[rows, :])
                kv_own[u, 1, inside, :] = dot_nn(n_buf[k], big[1, :, cols]).astype(BF16)

        if first:
            pl.semaphore_wait(barrier, tp + 2)
        for g in range(HALVES):
            u = b * HALVES + g

            @pl.when(first_chip)
            def _(u=u):
                kv_to_chip(u).start()

            @pl.when(first_core)
            def _(u=u):
                kv_to_partner(u).start()

        if first:
            for d in range(1, tp):
                wz_copy(d).start()
            for copy in weight_loads[2:]:
                copy.wait()
            w_local.start()

        for k in range(per_row):
            rows = tile_rows(b, k)
            inside = slice(k * tile, (k + 1) * tile)
            dy_load(b, k).wait()
            put_rope(q_ring.at[ring, inside, :], dot_nn(n_buf[k], big[2]), cos_ref[rows, :], sin_ref[rows, :])
            do_ring[ring, inside, :] = dot_nt(dy_in[k], wo_ref[...]).astype(BF16)

            @pl.when(b + 1 < batch)
            def _(k=k):
                dy_load(b + 1, k).start()

    def o_place(src, u):
        b, g = where(u)
        return o_all.at[src, row(b), half_cols(g)]

    def o_local_copy(b):
        return pltpu.make_async_copy(o_buf.at[b], o_place(z, b), o_local.at[b])

    def o_copy(b, k, step):
        return remote(o_buf.at[b], o_place(z, b), o_send.at[k, b], o_recv.at[z, b], {"tp": jnp.clip(z + step, 0, tp - 1)})

    hops = [(k, step, jnp.logical_and(z + step >= 0, z + step < tp)) for k, step in enumerate((1, -1))]

    def far_from_end(step):
        return jnp.logical_and(z + step != 0, z + step != tp - 1)

    def o_start(b):
        o_local_copy(b).start()
        for k, step, ok in hops:
            @pl.when(jnp.logical_and(ok, jnp.logical_or(b < units - LATE, far_from_end(step))))
            def _(k=k, step=step):
                o_copy(b, k, step).start()

    def o_arrived(src, b):
        remote(o_place(src, b), o_place(src, b), relay_send.at[0, 0, b], o_recv.at[src, b], partner).wait_recv()

    def relay_copy(b, age, step):
        src = jnp.clip(z - age * step, 0, tp - 1)
        return remote(o_place(src, b), o_place(src, b), relay_send.at[age - 1, (1 - step) // 2, b], o_recv.at[src, b], {"tp": jnp.clip(z + step, 0, tp - 1)})

    def relays(age, step):
        far = z if step > 0 else tp - 1 - z
        return jnp.logical_and(far >= age, far < tp - 1)

    def relay(b, age):
        for step in (1, -1):
            @pl.when(relays(age, step))
            def _(step=step):
                o_arrived(jnp.clip(z - age * step, 0, tp - 1), b)
                relay_copy(b, age, step).start()

    def far_copy(b, par):
        return remote(g_far.at[par], xin.at[b], far_send.at[par], x_recv.at[b], partner)

    def part_copy(b, par):
        return remote(g_part.at[par], part_in.at[b], part_send.at[par], part_recv.at[b], partner)

    def chip_copy(b):
        par = lax.rem(b, CHIP_BUFS)
        return remote(g_chip.at[par], xin.at[b], chip_send.at[par], x_recv.at[b], peer)

    def chip_sum(b):
        @pl.when(second_chip)
        def _():
            par = lax.rem(b, CHIP_BUFS)
            far_copy(b, 0).wait_recv()
            g_chip[par] = (g_chip[par].astype(F32) + xin[b].astype(F32)).astype(BF16)
            chip_copy(b).start()

    def dkv_store(u, which):
        b, g = where(u)
        return pltpu.make_async_copy(g_own.at[lax.rem(u, OWN_RING), which], dkv_hbm.at[which, row(b), half_cols(g)], dkv_sem.at[u, which])

    def key_grads(u):
        @pl.when(first_core)
        def _():
            part_copy(u, 0).wait_recv()

        @pl.when(first_chip)
        def _():
            chip_copy(u).wait_recv()

        b, g = where(u)
        rows = row(b)
        for which in range(2):
            for h in range(half // HEAD_DIM):
                cols = slice(h * HEAD_DIM, (h + 1) * HEAD_DIM)
                own = g_own.at[lax.rem(u, OWN_RING), which, :, cols]
                acc = own[...].astype(F32)
                acc = acc + jnp.where(first_core, part_in[u, which, :, cols].astype(F32), 0.0)
                acc = (acc + jnp.where(first_chip, xin[u, which, :, cols].astype(F32), 0.0)).astype(BF16)
                if which == 0:
                    acc = rope(acc.astype(F32), cos_ref[rows, :], sin_ref[rows, :], -1.0).astype(BF16)
                own[...] = acc
            dkv_store(u, which).start()

    def dq_store(b, par):
        return pltpu.make_async_copy(dq_buf.at[par], dq_hbm.at[row(where(b)[0]), half_cols(where(b)[1])], dq_sem.at[par])

    subs = range(0, seq, SUB)

    def attend_unit(i, par):
        b, g = where(i)
        rows = row(b)
        ring = lax.rem(b, Q_RING)
        start = r * seq + lax.broadcasted_iota(jnp.int32, (1, seq), 1) - pos_ref[pl.ds(b, 1), :]
        chip_par = lax.rem(i, CHIP_BUFS)
        keys_of = [kv_own.at[i]] + [kvr.at[s, i] for s in range(3)]
        places = [g_part.at[par], g_chip.at[chip_par], g_far.at[par]]

        def grad(slot, which, cols):
            return places[slot - 1].at[which, :, cols] if slot else g_own.at[lax.rem(i, OWN_RING), which, :, cols]

        live = [None, second_core, second_chip, second_chip]
        piece = [r, r + 1 - 2 * core, r + 2 - 4 * chip, r + 3 - 2 * core - 4 * chip]

        def each(body):
            body(0)
            for slot in (1, 2, 3):
                pl.when(live[slot])(functools.partial(body, slot))

        def one_head(h, carry):
            cols = pl.ds(pl.multiple_of(h * HEAD_DIM, HEAD_DIM), HEAD_DIM)
            full = pl.ds(pl.multiple_of(g * half + h * HEAD_DIM, HEAD_DIM), HEAD_DIM)
            q = q_ring[ring, :, full]
            do = do_ring[ring, :, full]
            m_scr[...] = jnp.full(m_scr.shape, NEG_BIG, F32)
            l_scr[...] = jnp.zeros_like(l_scr)
            d_scr[...] = jnp.zeros_like(d_scr)
            ot_scr[...] = jnp.zeros_like(ot_scr)
            dqt_scr[...] = jnp.zeros_like(dqt_scr)

            def scores(slot):
                base = piece[slot] * seq
                top = None
                for s in subs:
                    raw = dot_nt(keys_of[slot][0, s:s + SUB, cols], q)
                    local = lax.broadcasted_iota(jnp.int32, raw.shape, 0) + s
                    allowed = (local + base) >= start
                    if slot == 0:
                        allowed = jnp.logical_and(allowed, local <= lax.broadcasted_iota(jnp.int32, raw.shape, 1))
                    raw = jnp.where(allowed, raw, NEG_BIG)
                    s_scr[slot, s:s + SUB, :] = raw
                    high = jnp.max(raw, axis=0, keepdims=True)
                    top = high if top is None else jnp.maximum(top, high)
                m_scr[...] = jnp.maximum(m_scr[...], top)

            def exps(slot):
                top = m_scr[...]
                total = None
                for s in subs:
                    e = jnp.exp2((s_scr[slot, s:s + SUB, :] - top) * EXP2_SCALE)
                    s_scr[slot, s:s + SUB, :] = e
                    part = jnp.sum(e, axis=0, keepdims=True)
                    total = part if total is None else total + part
                l_scr[...] += total

            def values(slot):
                inv = l_scr[...]
                total, out = None, None
                for s in subs:
                    v = keys_of[slot][1, s:s + SUB, cols]
                    prob = s_scr[slot, s:s + SUB, :] * inv
                    low = prob.astype(BF16)
                    dp = dot_nt(v, do)
                    dp_scr[slot, s:s + SUB, :] = dp
                    part = jnp.sum(prob * dp, axis=0, keepdims=True)
                    total = part if total is None else total + part
                    grad(slot, 1, cols)[s:s + SUB, :] = dot_nn(low, do).astype(BF16)
                    piece_out = dot_nn(v.T, low)
                    out = piece_out if out is None else out + piece_out
                d_scr[...] += total
                ot_scr[...] += out

            def keys(slot):
                inv, mean = l_scr[...], d_scr[...]
                out = None
                for s in subs:
                    k = keys_of[slot][0, s:s + SUB, cols]
                    ds = ((s_scr[slot, s:s + SUB, :] * inv) * (dp_scr[slot, s:s + SUB, :] - mean)).astype(BF16)
                    grad(slot, 0, cols)[s:s + SUB, :] = (dot_nn(ds, q) * SCALE).astype(BF16)
                    piece_out = dot_nn(k.T, ds)
                    out = piece_out if out is None else out + piece_out
                dqt_scr[...] += out

            each(scores)
            each(exps)
            l_scr[...] = 1.0 / l_scr[...]
            each(values)
            each(keys)
            o_buf[i, :, cols] = ot_scr[...].T.astype(BF16)
            dq_buf[par, :, cols] = rope(dqt_scr[...].T * SCALE, cos_ref[rows, :], sin_ref[rows, :], -1.0).astype(BF16)
            return carry

        lax.fori_loop(0, heads // HALVES, one_head, 0)

    def step(i, carry):
        par = lax.rem(i, 2)
        @pl.when(jnp.logical_and(lax.rem(i, HALVES) == 0, lax.div(i, HALVES) + AHEAD < batch))
        def _():
            project_row(lax.div(i, HALVES) + AHEAD)

        @pl.when(i >= OWN_RING)
        def _():
            for which in range(2):
                dkv_store(i - OWN_RING, which).wait()

        @pl.when(second_chip)
        def _():
            kv_to_chip(i).wait_recv()
            kv_forward(i).start()

        @pl.when(second_core)
        def _():
            kv_to_partner(i).wait_recv()

        @pl.when(second_chip)
        def _():
            kv_forward(i).wait_recv()

        @pl.when(i >= 2)
        def _():
            dq_store(i - 2, par).wait()

            @pl.when(second_core)
            def _():
                part_copy(i - 2, par).wait_send()

            @pl.when(second_chip)
            def _():
                far_copy(i - 2, par).wait_send()

        @pl.when(jnp.logical_and(second_chip, i >= CHIP_BUFS))
        def _():
            chip_copy(i - CHIP_BUFS).wait_send()

        attend_unit(i, par)
        o_start(i)
        dq_store(i, par).start()

        @pl.when(second_chip)
        def _():
            far_copy(i, par).start()

        @pl.when(second_core)
        def _():
            part_copy(i, par).start()

        @pl.when(i >= 1)
        def _():
            chip_sum(i - 1)

        for age in range(1, tp - 1):
            @pl.when(i >= age * RELAY_LAG)
            def _(age=age):
                relay(i - age * RELAY_LAG, age)

        @pl.when(i >= SUM_LAG)
        def _():
            key_grads(i - SUM_LAG)

        @pl.when(i == min(W_TWIN, units - 1))
        def _():
            for d in w_steps:
                wz_wait(d)
                w_move(0, d).start()
                w_move(1, d).start()

                @pl.when(second_chip)
                def _(d=d):
                    w_move(3, d).start()

        @pl.when(i == min(W_PARTNER, units - 1))
        def _():
            for d in w_steps:
                w_move(0, d).wait_recv()
                w_move(2, d).start()

        @pl.when(jnp.logical_and(first_chip, i == min(W_CHIP, units - 1)))
        def _():
            for k in (3, 4):
                for d in w_steps:
                    w_move(k, d).start()

        return carry

    for b in range(min(AHEAD, batch)):
        project_row(b, b == 0)
    lax.fori_loop(0, units, step, 0)
    chip_sum(units - 1)

    @pl.when(second_chip)
    def _():
        for d in w_steps:
            w_move(4, d).start()

    end = units + max(SUM_LAG, (tp - 2) * RELAY_LAG)
    for i in range(units, end):
        for age in range(1, tp - 1):
            if 0 <= i - age * RELAY_LAG < units:
                relay(i - age * RELAY_LAG, age)
        if 0 <= i - SUM_LAG < units:
            key_grads(i - SUM_LAG)
        if i == end - 1:
            for k in (3, 4):
                for d in w_steps:
                    w_move(k, d).wait_recv()
                    w_move(k + 2, d).start()

    w_local.wait()
    for d in w_steps:
        wz_copy(d).wait_send()
        for k in range(7):
            w_move(k, d).wait_send()
            if k in (1, 2, 5, 6):
                w_move(k, d).wait_recv()

    for k in range(per_row):
        n_store(batch - 1, k).wait()
    for u in range(max(0, units - OWN_RING), units):
        for which in range(2):
            dkv_store(u, which).wait()

    def drain(b, carry):
        @pl.when(first_chip)
        def _():
            kv_to_chip(b).wait_send()

        @pl.when(first_core)
        def _():
            kv_to_partner(b).wait_send()

        @pl.when(second_chip)
        def _():
            kv_forward(b).wait_send()

        o_local_copy(b).wait()
        for k, step_, ok in hops:
            @pl.when(jnp.logical_and(ok, jnp.logical_or(b < units - LATE, far_from_end(step_))))
            def _(k=k, step_=step_):
                o_copy(b, k, step_).wait_send()

        for age in range(1, tp - 1):
            for step_ in (1, -1):
                @pl.when(relays(age, step_))
                def _(age=age, step_=step_):
                    relay_copy(b, age, step_).wait_send()

        for src in range(tp):
            way = jnp.where(z > src, 1, -1)
            gone = jnp.abs(z - src)
            far = jnp.where(way > 0, z, tp - 1 - z)
            taken = jnp.logical_and(gone <= tp - 2, far < tp - 1)
            late = jnp.logical_and(b >= units - LATE, jnp.logical_and(gone == 1, far == tp - 1))

            @pl.when(jnp.logical_and(z != src, jnp.logical_not(jnp.logical_or(taken, late))))
            def _(src=src):
                o_arrived(src, b)

        return carry

    lax.fori_loop(0, units, drain, 0)

    for b in range(max(0, units - 2), units):
        dq_store(b, b % 2).wait()

        @pl.when(second_core)
        def _(b=b):
            part_copy(b, b % 2).wait_send()

        @pl.when(second_chip)
        def _(b=b):
            far_copy(b, b % 2).wait_send()

    for b in range(max(0, units - CHIP_BUFS), units):
        @pl.when(second_chip)
        def _(b=b):
            chip_copy(b).wait_send()


def front(x, dy, wq, wk, wv, wo, pos, table, gain, seq, tp, cp):
    tokens, d_model = x.shape
    hidden = wq.shape[1]
    batch = tokens // seq
    units = batch * HALVES
    half = hidden // HALVES
    tile = seq // 2
    hbm = pl.BlockSpec(memory_space=pl.ANY)
    vmem = pl.BlockSpec(memory_space=pltpu.VMEM)
    dma = pltpu.SemaphoreType.DMA
    bf = lambda *shape: pltpu.VMEM(shape, BF16)
    f32 = lambda *shape: pltpu.VMEM(shape, F32)
    return pl.pallas_call(
        functools.partial(front_kernel, batch, seq, tp, cp),
        in_specs=[hbm] * 6 + [vmem] * 3,
        out_specs=[hbm] * 5,
        out_shape=[
            jax.ShapeDtypeStruct((tokens, d_model), BF16),
            jax.ShapeDtypeStruct((tp, tokens, hidden), BF16),
            jax.ShapeDtypeStruct((tokens, hidden), BF16),
            jax.ShapeDtypeStruct((2, tokens, hidden), BF16),
            jax.ShapeDtypeStruct((tp, hidden, d_model), BF16),
        ],
        scratch_shapes=[
            bf(3, d_model, hidden), bf(hidden, d_model), f32(tokens, HEAD_DIM), f32(tokens, HEAD_DIM),
            bf(Q_RING, seq, hidden), bf(Q_RING, seq, hidden), bf(2, tile, d_model), bf(2, tile, d_model), bf(2, tile, d_model),
            bf(units, 2, seq, half), bf(3, units, 2, seq, half),
            f32(4, seq, seq), f32(4, seq, seq), f32(1, seq), f32(1, seq), f32(1, seq), f32(HEAD_DIM, seq), f32(HEAD_DIM, seq),
            bf(units, seq, half), bf(2, seq, half),
            bf(OWN_RING, 2, seq, half), bf(2, 2, seq, half), bf(CHIP_BUFS, 2, seq, half), bf(2, 2, seq, half),
            bf(units, 2, seq, half), bf(units, 2, seq, half),
            dma((4,)), dma((1,)), dma((tp,)), dma((tp,)), dma((7, tp)), dma((7, tp)),
            dma((2,)), dma((2,)), dma((2,)), dma((units,)), dma((units,)), dma((units,)), dma((3, units)),
            dma((units,)), dma((2, units)), dma((tp, units)), dma((2, 2, units)), dma((2,)),
            dma((2,)), dma((2,)), dma((CHIP_BUFS,)), dma((units,)), dma((units,)), dma((units, 2)),
        ],
        compiler_params=pltpu.CompilerParams(collective_id=1, has_side_effects=True, vmem_limit_bytes=63 << 20),
        cost_estimate=pl.CostEstimate(flops=60 * tokens * seq * hidden, bytes_accessed=16 * tokens * d_model, transcendentals=4 * tokens * seq * (hidden // HEAD_DIM)),
        name="front",
    )(x, dy, wq, wk, wv, wo, pos, table, gain)


PART_RING = 4
RS_RING = 5
FORWARD_LAG = 11
JOB_LAG = 5
OUT_LAG = 4
EARLY = 4


def back_kernel(groups, rows, tp, cp, seq, dq_hbm, dkv_hbm, x_hbm, dy_hbm, o_old, n_hbm, wq_hbm, wk_hbm, wv_hbm, wo_hbm, gain_ref,
                gx_hbm, y_hbm, ga_hbm, gb_hbm, gg_ref, o_out,
                wq_ref, wk_ref, wv_ref, wo_ref, dq_all, dkv_all, o_t, part, rs_r, rs_l, send_r, send_l, tot, gx_buf,
                o_in, x_in, xo_in, dyo_in, y_buf, n_in, dy_in, away, part_in, mine, gain_all,
                w_sem, in_sem, fin_sem, job_sem, y_sem, own_sem, rss_r, rss_l, rsr_r, rsr_l, ag0_r, ag0_l, agf_r, agf_l, agr_r, agr_l,
                away_send, away_recv, mine_own, mine_part, mine_chip, ga_recv, chip_recv, gb_send, gb_recv, gs_sem, gr_sem, late_send, late_recv):
    o_hbm = o_out
    z = lax.axis_index("tp")
    r = lax.axis_index("cp")
    core = lax.rem(r, 2)
    chip = lax.div(r, 2)
    last = tp - 1
    slots = tp - 1
    span = tp * rows
    tokens, d_model = x_hbm.shape
    hidden = dq_hbm.shape[1]
    chunk = min(512, d_model)
    blocks = ga_hbm.shape[0]
    width = ga_hbm.shape[1]
    pairs = blocks // 2
    partner = {"cp": r + 1 - 2 * core}
    peer = {"cp": r + 2 - 4 * chip}

    head = min(EARLY, groups) * span
    weight_loads = [pltpu.make_async_copy(src, dst, w_sem.at[k]) for k, (src, dst) in enumerate((
        (dq_hbm.at[:head, :], dq_all.at[:head, :]), (dkv_hbm.at[:, :head, :], dkv_all.at[:, :head, :]), (wq_hbm, wq_ref), (wk_hbm, wk_ref), (wv_hbm, wv_ref)))]
    rest_loads = [] if head == tokens else [
        pltpu.make_async_copy(dq_hbm.at[head:, :], dq_all.at[head:, :], w_sem.at[6]),
        pltpu.make_async_copy(dkv_hbm.at[:, head:, :], dkv_all.at[:, head:, :], w_sem.at[7]),
    ]
    out_loads = [pltpu.make_async_copy(wo_hbm, wo_ref, w_sem.at[5])]
    for copy in weight_loads:
        copy.start()

    barrier = pltpu.get_barrier_semaphore()
    peers = [(dt, dc) for dt in range(tp) for dc in range(cp) if dt or dc]
    for dt, dc in peers:
        pl.semaphore_signal(barrier, inc=1, device_id={"tp": lax.rem(z + dt, tp), "cp": lax.rem(r + dc, cp)}, device_id_type=MESH)

    def remote(src, dst, ssem, rsem, dev):
        return pltpu.make_async_remote_copy(src_ref=src, dst_ref=dst, send_sem=ssem, recv_sem=rsem, device_id=dev, device_id_type=MESH)

    right = {"tp": jnp.where(z < last, z + 1, z)}
    left = {"tp": jnp.where(z > 0, z - 1, z)}

    def group_rows(i):
        return pl.ds(pl.multiple_of(i * span, span), span)

    def tile_rows(i, owner):
        return pl.ds(pl.multiple_of(i * span + owner * rows, rows), rows)

    def inputs(i, slot):
        g = group_rows(i)
        return [
            pltpu.make_async_copy(o_hbm.at[:, g, :], o_in.at[slot], in_sem.at[slot, 0]),
            pltpu.make_async_copy(x_hbm.at[g, :], x_in.at[slot], in_sem.at[slot, 1]),
        ]

    def final_inputs(i, slot):
        g = tile_rows(i, z)
        return [
            pltpu.make_async_copy(x_hbm.at[g, :], xo_in.at[slot], fin_sem.at[slot, 0]),
            pltpu.make_async_copy(dy_hbm.at[g, :], dyo_in.at[slot], fin_sem.at[slot, 1]),
        ]

    def y_copy(i, slot):
        return pltpu.make_async_copy(y_buf.at[slot], y_hbm.at[group_rows(i), :], y_sem.at[slot])

    def rs_copy(i, s, to_right):
        ring = lax.rem(i, RS_RING)
        if to_right:
            return remote(send_r.at[s], rs_r.at[ring, s], rss_r.at[s], rsr_r.at[ring, s], right)
        return remote(send_l.at[s], rs_l.at[ring, s], rss_l.at[s], rsr_l.at[ring, s], left)

    def rs_send(i, s):
        for to_right in (True, False):
            far = z if to_right else last - z
            owner = (z + slots - s) if to_right else (z - slots + s)
            buf, held = (send_r, rs_r) if to_right else (send_l, rs_l)

            @pl.when(jnp.logical_and(jnp.logical_and(i >= 0, i < groups), jnp.logical_and(far <= s, far < last)))
            def _(to_right=to_right, far=far, owner=owner, buf=buf, held=held):
                @pl.when(i > 0)
                def _():
                    rs_copy(i - 1, s, to_right).wait_send()

                cur = lax.rem(i, PART_RING)
                own = pl.ds(pl.multiple_of(owner * rows, rows), rows)
                if s == 0:
                    buf[s] = part[cur, own, :].astype(BF16)
                else:
                    @pl.when(far == 0)
                    def _():
                        buf[s] = part[cur, own, :].astype(BF16)

                    @pl.when(far > 0)
                    def _():
                        rs_copy(i, s - 1, to_right).wait_recv()
                        buf[s] = (part[cur, own, :] + held[lax.rem(i, RS_RING), s - 1].astype(F32)).astype(BF16)

                rs_copy(i, s, to_right).start()

    def ag_own(i, slot, to_right):
        src = gx_buf.at[slot]
        dst = gx_hbm.at[tile_rows(i, z), :]
        if to_right:
            return remote(src, dst, ag0_r.at[slot], agr_r.at[i, 0], right)
        return remote(src, dst, ag0_l.at[slot], agr_l.at[i, 0], left)

    def own_copy(i, slot):
        return pltpu.make_async_copy(gx_buf.at[slot], gx_hbm.at[tile_rows(i, z), :], own_sem.at[slot])

    def ag_forward(i, a, to_right):
        owner = z - a if to_right else z + a
        tile = gx_hbm.at[tile_rows(i, owner), :]
        if to_right:
            return remote(tile, tile, agf_r.at[a], agr_r.at[i, a], right)
        return remote(tile, tile, agf_l.at[a], agr_l.at[i, a], left)

    def ag_wait(i, a, to_right):
        tile = gx_hbm.at[tile_rows(i, 0), :]
        sem = agr_r.at[i, a] if to_right else agr_l.at[i, a]
        remote(tile, tile, agf_r.at[a], sem, right).wait_recv()

    def ag_step(i, a):
        for to_right in (True, False):
            far = z if to_right else last - z

            @pl.when(jnp.logical_and(jnp.logical_and(i >= 0, i < groups), far >= a))
            def _(to_right=to_right, far=far):
                ag_wait(i, a - 1, to_right)
                if a < slots:
                    @pl.when(far < last)
                    def _():
                        @pl.when(i > 0)
                        def _():
                            ag_forward(i - 1, a, to_right).wait_send()

                        ag_forward(i, a, to_right).start()

    def ag_first(i, slot):
        own_copy(i, slot).start()
        for to_right in (True, False):
            far = z if to_right else last - z

            @pl.when(far < last)
            def _(to_right=to_right):
                ag_own(i, slot, to_right).start()

    def ag_first_done(i, slot):
        own_copy(i, slot).wait()
        for to_right in (True, False):
            far = z if to_right else last - z

            @pl.when(far < last)
            def _(to_right=to_right):
                ag_own(i, slot, to_right).wait_send()

    def partial_norm(i):
        cur = lax.rem(i, PART_RING)
        g = group_rows(i)
        for c in range(0, d_model, chunk):
            cols = slice(c, c + chunk)
            part[cur, :, cols] = (
                dot_nt(dq_all[g, :], wq_ref[cols, :]) + dot_nt(dkv_all[0, g, :], wk_ref[cols, :]) + dot_nt(dkv_all[1, g, :], wv_ref[cols, :])
            )

    def project_out(cur):
        for c in range(0, d_model, chunk):
            cols = slice(c, c + chunk)
            acc = x_in[cur, :, cols].astype(F32)
            for t in range(tp):
                acc += dot_nn(o_in[cur, t], wo_ref[t, :, cols])
            y_buf[cur, :, cols] = acc.astype(BF16)

    def finalize(i):
        slot = lax.rem(i, 2)
        own = pl.ds(pl.multiple_of(z * rows, rows), rows)
        tot[...] = part[lax.rem(i, PART_RING), own, :]

        @pl.when(z > 0)
        def _():
            rs_copy(i, slots - 1, True).wait_recv()
            tot[...] += rs_r[lax.rem(i, RS_RING), slots - 1].astype(F32)

        @pl.when(z < last)
        def _():
            rs_copy(i, slots - 1, False).wait_recv()
            tot[...] += rs_l[lax.rem(i, RS_RING), slots - 1].astype(F32)

        @pl.when(i > 1)
        def _():
            ag_first_done(i - 2, slot)

        for copy in final_inputs(i, slot):
            copy.wait()
        x = xo_in[slot].astype(F32)
        centred = x - jnp.mean(x, axis=-1, keepdims=True)
        inv_std = lax.rsqrt(jnp.mean(centred * centred, axis=-1, keepdims=True) + LN_EPS)
        x_hat = centred * inv_std
        dn = tot[...]
        gg_ref[...] += jnp.sum(dn * x_hat, axis=0, keepdims=True)
        d_hat = dn * gain_ref[...]
        dx = inv_std * (d_hat - jnp.mean(d_hat, axis=-1, keepdims=True) - x_hat * jnp.mean(d_hat * x_hat, axis=-1, keepdims=True))
        gx_buf[slot] = (dyo_in[slot].astype(F32) + dx).astype(BF16)
        ag_first(i, slot)

    def block_of(t):
        return 2 * lax.div(t, 2) + jnp.where(lax.rem(t, 2) == 0, 1 - core, core)

    def job_loads(t, slot):
        cols = pl.ds(pl.multiple_of(block_of(t) * width, width), width)
        return [
            pltpu.make_async_copy(n_hbm.at[:, cols], n_in.at[slot], job_sem.at[slot, 0]),
            pltpu.make_async_copy(dy_hbm.at[:, cols], dy_in.at[slot], job_sem.at[slot, 1]),
        ]

    def away_copy(p):
        ring = lax.rem(p, 2)
        return remote(away, part_in.at[ring], away_send.at[0], away_recv.at[ring], partner)

    def job_block(t, put):
        slot = lax.rem(t, 2)
        n_t = n_in[slot].T
        put(0, hidden, dot_nn(n_t, dq_all[...]))
        put(hidden, hidden, dot_nn(n_t, dkv_all[0]))
        put(2 * hidden, hidden, dot_nn(n_t, dkv_all[1]))
        for k in range(hidden // width):
            put(3 * hidden + k * width, width, dot_nn(o_t[k * width:(k + 1) * width, :], dy_in[slot]))

    def mine_to_own(p, slot):
        return pltpu.make_async_copy(mine.at[slot], ga_hbm.at[2 * p + core], mine_own.at[slot])

    def mine_to_part(p, slot):
        return remote(mine.at[slot], ga_hbm.at[2 * p + core], mine_part.at[slot], ga_recv.at[p], partner)

    def mine_to_chip(p, slot):
        return remote(mine.at[slot], gb_hbm.at[2 * p + core], mine_chip.at[slot], chip_recv.at[p], peer)

    def mine_done(p, slot):
        mine_to_own(p, slot).wait()
        mine_to_part(p, slot).wait_send()
        mine_to_chip(p, slot).wait_send()

    def chip_forward(p):
        b = 2 * p + core
        return remote(gb_hbm.at[b], gb_hbm.at[b], gb_send.at[p], gb_recv.at[p], partner)

    def job(t):
        p = lax.div(t, 2)
        for copy in job_loads(t, lax.rem(t, 2)):
            copy.wait()

        @pl.when(t + 1 < blocks)
        def _():
            for copy in job_loads(t + 1, 1 - lax.rem(t, 2)):
                copy.start()

        @pl.when(lax.rem(t, 2) == 0)
        def _():
            @pl.when(p > 0)
            def _():
                away_copy(p - 1).wait_send()

            def put(at, size, value):
                away[:, at:at + size] = value

            job_block(t, put)
            away_copy(p).start()

        @pl.when(lax.rem(t, 2) == 1)
        def _():
            slot = lax.rem(p, 2)
            away_copy(p).wait_recv()

            @pl.when(p > 1)
            def _():
                mine_done(p - 2, slot)

            def put(at, size, value):
                mine[slot, :, at:at + size] = (value + part_in[slot, :, at:at + size]).astype(BF16)

            job_block(t, put)
            mine_to_chip(p, slot).start()
            mine_to_part(p, slot).start()
            mine_to_own(p, slot).start()

    gg_ref[...] = jnp.zeros_like(gg_ref)
    o_loads = [pltpu.make_async_copy(o_hbm.at[z, :, k * width:(k + 1) * width], n_in.at[k], job_sem.at[k, 0]) for k in range(hidden // width)]
    me = z * cp + r

    def gain_copy(dt, dc):
        to = {"tp": lax.rem(z + dt, tp), "cp": lax.rem(r + dc, cp)}
        return remote(gain_all.at[me], gain_all.at[me], gs_sem.at[dt * cp + dc], gr_sem.at[me], to)

    def gain_wait(dt, dc):
        sender = lax.rem(z + dt, tp) * cp + lax.rem(r + dc, cp)
        remote(gain_all.at[sender], gain_all.at[sender], gs_sem.at[0], gr_sem.at[sender], right).wait_recv()

    units = tokens // seq * HALVES
    half = hidden // HALVES
    late_units = range(max(0, units - LATE), units)
    late_wait = max(0, late_units[0] // HALVES * seq // span + OUT_LAG - 2)
    sends_late = jnp.logical_or(z == 1, z == last - 1)
    gets_late = jnp.logical_or(z == 0, z == last)

    def late_copy(n, src, dst):
        u = late_units[n]
        place = o_out.at[src, u // HALVES * seq:(u // HALVES + 1) * seq, u % HALVES * half:(u % HALVES + 1) * half]
        return remote(place, place, late_send.at[n], late_recv.at[n], {"tp": dst})

    def late_move(n):
        return late_copy(n, z, jnp.where(z == 1, 0, last))

    for copy in weight_loads:
        copy.wait()
    for copy in inputs(0, 0) + o_loads + rest_loads + out_loads:
        copy.start()
    partial_norm(0)
    pl.semaphore_wait(barrier, len(peers))
    for n in range(len(late_units)):
        @pl.when(sends_late)
        def _(n=n):
            late_move(n).start()

    def step(i, carry):
        @pl.when(jnp.logical_and(gets_late, i == late_wait))
        def _():
            for n in range(len(late_units)):
                late_copy(n, jnp.where(z == 0, 1, last - 1), z).wait_recv()

        for a in reversed(range(1, slots + 1)):
            ag_step(i - slots - a, a)

        @pl.when(i == OUT_LAG)
        def _():
            for copy in out_loads:
                copy.wait()

        @pl.when(jnp.logical_and(i >= OUT_LAG, i < groups + OUT_LAG))
        def _():
            j = i - OUT_LAG
            at = lax.rem(j, 2)
            for copy in inputs(j, at):
                copy.wait()

            @pl.when(j + 1 < groups)
            def _():
                for copy in inputs(j + 1, 1 - at):
                    copy.start()

            @pl.when(j >= 2)
            def _():
                y_copy(j - 2, at).wait()

            project_out(at)
            y_copy(j, at).start()

        @pl.when(jnp.logical_and(i >= slots, i < groups + slots))
        def _():
            finalize(i - slots)

        @pl.when(i == groups + slots - 1)
        def _():
            gain_all[me] = gg_ref[...]
            for dt, dc in peers:
                gain_copy(dt, dc).start()

        @pl.when(jnp.logical_and(i >= slots - 1, i < groups + slots - 1))
        def _():
            for copy in final_inputs(i - slots + 1, lax.rem(i - slots + 1, 2)):
                copy.start()

        @pl.when(i == EARLY)
        def _():
            for copy in rest_loads:
                copy.wait()

        @pl.when(jnp.logical_and(i >= 1, i < groups))
        def _():
            partial_norm(i)

        @pl.when(i == JOB_LAG - 1)
        def _():
            for k, copy in enumerate(o_loads):
                copy.wait()
                o_t[k * width:(k + 1) * width, :] = n_in[k].T
            for copy in job_loads(0, 0):
                copy.start()

        @pl.when(jnp.logical_and(i >= JOB_LAG, i < JOB_LAG + blocks))
        def _():
            job(i - JOB_LAG)

        for k in reversed(range(slots)):
            rs_send(i - k, k)

        @pl.when(jnp.logical_and(lax.rem(i, 2) == 1, jnp.logical_and(i >= FORWARD_LAG, i < FORWARD_LAG + 2 * pairs)))
        def _():
            p = lax.div(i - FORWARD_LAG, 2)
            mine_to_chip(p, 0).wait_recv()
            chip_forward(p).start()

        return carry

    lax.fori_loop(0, max(groups + 2 * slots, groups + OUT_LAG, blocks + JOB_LAG, 2 * pairs + FORWARD_LAG - 1), step, 0)

    for i in (groups - 2, groups - 1):
        y_copy(i, i % 2).wait()
        ag_first_done(i, i % 2)
    for to_right in (True, False):
        far = z if to_right else last - z
        for s in range(slots):
            @pl.when(jnp.logical_and(far <= s, far < last))
            def _(s=s, to_right=to_right):
                rs_copy(groups - 1, s, to_right).wait_send()
        for a in range(1, slots):
            @pl.when(jnp.logical_and(far >= a, far < last))
            def _(a=a, to_right=to_right):
                ag_forward(groups - 1, a, to_right).wait_send()
    for n in range(len(late_units)):
        @pl.when(sends_late)
        def _(n=n):
            late_move(n).wait_send()

    away_copy(pairs - 1).wait_send()
    for p in range(max(0, pairs - 2), pairs):
        mine_done(p, p % 2)
    for p in range(pairs):
        chip_forward(p).wait_send()
        chip_forward(p).wait_recv()
        mine_to_part(p, 0).wait_recv()
    for dt, dc in peers:
        gain_wait(dt, dc)
        gain_copy(dt, dc).wait_send()
    total = gain_all[0]
    for j in range(1, tp * cp):
        total += gain_all[j]
    gg_ref[...] = total


def backward_norm(dq, dkv, x, dy, o_all, normed, wq, wk, wv, wo_all, gain, rows, seq, tp, cp):
    tokens, hidden = dq.shape
    d_model = x.shape[1]
    span = tp * rows
    groups = tokens // span
    slots = tp - 1
    width = WIDTH
    blocks = d_model // width
    pairs = blocks // 2
    hbm = pl.BlockSpec(memory_space=pl.ANY)
    vmem = pl.BlockSpec(memory_space=pltpu.VMEM)
    dma = pltpu.SemaphoreType.DMA
    bf = lambda *shape: pltpu.VMEM(shape, BF16)
    f32 = lambda *shape: pltpu.VMEM(shape, F32)
    return pl.pallas_call(
        functools.partial(back_kernel, groups, rows, tp, cp, seq),
        in_specs=[hbm] * 10 + [vmem],
        out_specs=[hbm, hbm, hbm, hbm, vmem, hbm],
        input_output_aliases={4: 5},
        out_shape=[
            jax.ShapeDtypeStruct((tokens, d_model), BF16),
            jax.ShapeDtypeStruct((tokens, d_model), BF16),
            jax.ShapeDtypeStruct((blocks, width, 4 * hidden), BF16),
            jax.ShapeDtypeStruct((blocks, width, 4 * hidden), BF16),
            jax.ShapeDtypeStruct((1, d_model), F32),
            jax.ShapeDtypeStruct(o_all.shape, BF16),
        ],
        scratch_shapes=[
            bf(d_model, hidden), bf(d_model, hidden), bf(d_model, hidden), bf(tp, hidden, d_model),
            bf(tokens, hidden), bf(2, tokens, hidden), bf(hidden, tokens),
            f32(PART_RING, span, d_model), bf(RS_RING, slots, rows, d_model), bf(RS_RING, slots, rows, d_model),
            bf(slots, rows, d_model), bf(slots, rows, d_model), f32(rows, d_model), bf(2, rows, d_model),
            bf(2, tp, span, hidden), bf(2, span, d_model), bf(2, rows, d_model), bf(2, rows, d_model), bf(2, span, d_model),
            bf(2, tokens, width), bf(2, tokens, width),
            f32(width, 4 * hidden), f32(2, width, 4 * hidden), bf(2, width, 4 * hidden), f32(tp * cp, 1, d_model),
            dma((8,)), dma((2, 2)), dma((2, 2)), dma((2, 2)), dma((2,)), dma((2,)),
            dma((slots,)), dma((slots,)), dma((RS_RING, slots)), dma((RS_RING, slots)),
            dma((2,)), dma((2,)), dma((slots,)), dma((slots,)), dma((groups, slots)), dma((groups, slots)),
            dma((1,)), dma((2,)), dma((2,)), dma((2,)), dma((2,)), dma((pairs,)), dma((pairs,)), dma((pairs,)), dma((pairs,)),
            dma((tp * cp,)), dma((tp * cp,)), dma((max(LATE, 1),)), dma((max(LATE, 1),)),
        ],
        compiler_params=pltpu.CompilerParams(collective_id=0, has_side_effects=True, vmem_limit_bytes=63 << 20),
        cost_estimate=pl.CostEstimate(flops=22 * tokens * hidden * d_model, bytes_accessed=16 * tokens * d_model, transcendentals=0),
        name="backward_norm",
    )(dq, dkv, x, dy, o_all, normed, wq, wk, wv, wo_all, gain)


def finish_kernel(y_ref, gx_ref, ga_ref, gb_ref, gg_ref, yo_ref, gxo_ref, wq_ref, wk_ref, wv_ref, wo_ref, ggo_ref):
    ggo_ref[...] = gg_ref[...]
    yo_ref[...] = y_ref[...]
    gxo_ref[...] = gx_ref[...]
    rows = ga_ref.shape[1]
    width = rows * PARTS
    hidden = wq_ref.shape[1]
    for k, ref in enumerate((wq_ref, wk_ref, wv_ref)):
        cols = slice(k * hidden, (k + 1) * hidden)
        ref[...] = ga_ref[0, :, cols].astype(F32) + gb_ref[0, :, cols].astype(F32)
    for k in range(hidden // width):
        cols = slice(3 * hidden + k * width, 3 * hidden + (k + 1) * width)
        at = k * width + lax.rem(pl.program_id(0), PARTS) * rows
        wo_ref[pl.ds(pl.multiple_of(at, rows), rows), :] = ga_ref[0, :, cols].astype(F32) + gb_ref[0, :, cols].astype(F32)


def finish(y, gx, ga, gb, gg):
    tokens, d_model = y.shape
    blocks, width, packed = ga.shape
    hidden = packed // 4
    steps = blocks * PARTS
    tile = pl.BlockSpec((tokens // steps, d_model), lambda j: (j, 0))
    block = pl.BlockSpec((1, width // PARTS, packed), lambda j: (j // PARTS, j % PARTS, 0))
    wide = pl.BlockSpec((width // PARTS, hidden), lambda j: (j, 0))
    line = pl.BlockSpec((1, d_model), lambda j: (0, 0))
    return pl.pallas_call(
        finish_kernel,
        grid=(steps,),
        in_specs=[tile, tile, block, block, line],
        out_specs=[tile, tile, wide, wide, wide, pl.BlockSpec((hidden, width), lambda j: (0, j // PARTS)), line],
        out_shape=[jax.ShapeDtypeStruct((tokens, d_model), BF16)] * 2 + [jax.ShapeDtypeStruct((d_model, hidden), F32)] * 3 + [jax.ShapeDtypeStruct((hidden, d_model), F32), jax.ShapeDtypeStruct((1, d_model), F32)],
        compiler_params=pltpu.CompilerParams(dimension_semantics=("arbitrary",), vmem_limit_bytes=48 << 20),
        cost_estimate=pl.CostEstimate(flops=8 * d_model * hidden, bytes_accessed=8 * tokens * d_model + 32 * d_model * hidden, transcendentals=0),
        name="finish",
    )(y, gx, ga, gb, gg)


def solution(mesh):
    cp_size = mesh.shape["cp"]
    tp_size = mesh.shape["tp"]

    def device_step(x_in, segment_ids, positions, w_query, w_key, w_value, w_out, norm_gain, grad_out):
        batch, seq, d_model = x_in.shape
        tokens = batch * seq
        x = x_in.reshape(tokens, d_model)
        dy = grad_out.reshape(tokens, d_model)

        gain = norm_gain.reshape(1, d_model)
        normed, o_all, dq, dkv, w_all = front(x, dy, w_query, w_key, w_value, w_out, positions, jnp.asarray(angle_table(), BF16), gain, seq, tp_size, cp_size)
        grad_x, y_out, sum_a, sum_b, grad_gain, _ = backward_norm(dq, dkv, x, dy, o_all, normed, w_query, w_key, w_value, w_all, gain, ROWS, seq, tp_size, cp_size)
        y_out, grad_x, grad_wq, grad_wk, grad_wv, grad_wo, grad_gain = finish(y_out, grad_x, sum_a, sum_b, grad_gain)
        grad_gain = grad_gain.reshape(d_model)
        return y_out.reshape(x_in.shape), grad_x.reshape(x_in.shape), grad_gain, grad_wq, grad_wk, grad_wv, grad_wo

    in_specs = (P("dp", "cp", None), P("dp", "cp"), P("dp", "cp"), P(None, "tp"), P(None, "tp"), P(None, "tp"), P("tp", None), P(None), P("dp", "cp", None))
    out_specs = (P("dp", "cp", None), P("dp", "cp", None), P("dp"), P("dp", "tp"), P("dp", "tp"), P("dp", "tp"), P(("dp", "tp"), None))
    return jax.shard_map(device_step, mesh=mesh, in_specs=in_specs, out_specs=out_specs, check_vma=False)
```
